32 devices in a mesh: dp: 8 (over y, x, core), tensor: 4 (over z).
Axes of the slice: x: 2, y: 2, z: 4, core: 2. Of those that a mesh axis runs over, the one named last changes fastest.
Arguments:
- layer_input: bfloat16 [4096, 2048], P(('dp', 'tensor')), may hold values from -6 to 6
- segment_ids: int32 [4096], P('dp'), may hold values from 0 to 15, as said below
- norm_attn: bfloat16 [2048], P('dp'), may hold values from 0.5 to 1.5
- w_query: bfloat16 [2048, 2048], P('dp', 'tensor')
- w_key: bfloat16 [2048, 256], P('dp', 'tensor')
- w_value: bfloat16 [2048, 256], P('dp', 'tensor'), may hold values from -0.125 to 0.125
- w_output: bfloat16 [2048, 2048], P('tensor', 'dp'), may hold values from -0.5 to 0.5
- norm_ffn: bfloat16 [2048], P('dp'), may hold values from 0.5 to 1.5
- w_gate: bfloat16 [2048, 5632], P('dp', 'tensor'), may hold values from -0.125 to 0.125
- w_up: bfloat16 [2048, 5632], P('dp', 'tensor'), may hold values from -0.125 to 0.125
- w_down: bfloat16 [5632, 2048], P('tensor', 'dp'), may hold values from -0.078125 to 0.078125
- cotangent: bfloat16 [4096, 2048], P(('dp', 'tensor')), may hold values from -6 to 6
Outputs:
- layer_output: bfloat16 [4096, 2048], P(('dp', 'tensor'))
- grad_input: float32 [4096, 2048], P(('dp', 'tensor'))
- grad_norm_attn: float32 [2048], P('dp')
- grad_w_query: float32 [2048, 2048], P('dp', 'tensor')
- grad_w_key: float32 [2048, 256], P('dp', 'tensor')
- grad_w_value: float32 [2048, 256], P('dp', 'tensor')
- grad_w_output: float32 [2048, 2048], P('tensor', 'dp')
- grad_norm_ffn: float32 [2048], P('dp')
- grad_w_gate: float32 [2048, 5632], P('dp', 'tensor')
- grad_w_up: float32 [2048, 5632], P('dp', 'tensor')
- grad_w_down: float32 [5632, 2048], P('tensor', 'dp')
The draws below stay inside these ranges and needn't reach their ends.
Inputs may be any that keep to these rules, and one draw needn't show every extreme that they name: `segment_ids`: within each aligned block of 512 rows the ids start at 0, never fall and rise by one at each new sequence, so that a block holds 1 to 16 sequences; in every draw some block is a single sequence of 512 rows and some block holds 16.
All inputs are finite; a program needn't handle non-finite values.
Results may differ from the reference program's by a relative error of at most 0.014.
Values may be sent and summed in bfloat16 or wider, within the bound.
A program may use at most 192 MiB of HBM per device.

```python
import math
import jax
import jax.numpy as jnp
from jax import lax

D = 2048
H = 32
KV = 4
HD = 64
FF = 5632
TOK_DEV = 512
TOKENS = 4096
N_DP = 8


def shared_keys(key):
    return jax.random.normal(jax.random.fold_in(key, 11), (D, KV * HD), jnp.float32) * D ** (-0.5)


def draw_w_key(key, part):
    return shared_keys(key).astype(jnp.bfloat16)


def draw_w_query(key, part):
    query_base = jax.random.normal(jax.random.fold_in(key, 23), (D, H * HD), jnp.float32) * D ** (-0.5)
    return query_base.astype(jnp.bfloat16)


def draw_segment_ids(key, part):
    cut_count = min(15, TOK_DEV - 1)
    single_block = jax.random.randint(jax.random.fold_in(key, 3), (), 0, N_DP)
    fullest_block = (single_block + 1) % N_DP

    def one_block(block_index):
        block_key = jax.random.fold_in(key, block_index + 100)
        block_cuts = jax.random.randint(jax.random.fold_in(block_key, 1), (), 0, cut_count + 1)
        block_cuts = jnp.where(block_index == fullest_block, cut_count, block_cuts)
        block_cuts = jnp.where(block_index == single_block, 0, block_cuts)
        cut_rows = jax.random.permutation(jax.random.fold_in(block_key, 2), TOK_DEV - 1)[:cut_count] + 1
        row_index = jnp.arange(TOK_DEV, dtype=jnp.int32)
        cut_marks = (row_index[:, None] == cut_rows[None, :]) & (jnp.arange(cut_count)[None, :] < block_cuts)
        return jnp.cumsum(jnp.any(cut_marks, axis=1).astype(jnp.int32))
    return jax.vmap(one_block)(jnp.arange(N_DP)).reshape(TOKENS).astype(jnp.int32)


def raised(entries, rng, source, target, parts, factor):
    def block_of(dim):
        return (jnp.arange(entries.shape[dim]) // (entries.shape[dim] // parts)).reshape((-1,) + (1,) * (entries.ndim - 1 - dim))

    one_side = jax.random.permutation(rng, parts)[block_of(target)]
    second = (block_of(target) + parts // 2) % parts
    return jnp.where((block_of(source) == one_side) | (block_of(source) == second), factor * entries, entries)


def steps_of(key, shape, cuts, least, largest):
    level, own = 1.0, jax.random.fold_in(key, 6)
    for dim, parts in cuts:
        draws = jnp.exp(jax.random.uniform(jax.random.fold_in(own, dim), (parts,), jnp.float32, least / len(cuts), largest / len(cuts)))
        level = level * jnp.repeat(draws, shape[dim] // parts).reshape([-1 if axis == dim else 1 for axis in range(len(shape))])
    return level


def bell_draw(key, dims, spread, most, cuts=(), held_as=jnp.bfloat16):
    result = spread * jax.random.normal(key, dims, jnp.float32)
    if cuts:
        result = result * steps_of(key, dims, cuts, -0.22, 0.18)
    return jnp.clip(result, -most, most).astype(held_as)


def bell_draw_with(key, dims, scale, limit, cuts, heavy, kind=jnp.bfloat16):
    drawn = scale * jax.random.normal(key, dims, jnp.float32)
    if cuts:
        drawn = drawn * steps_of(key, dims, cuts, -0.22, 0.18)
    return jnp.clip(raised(drawn, jax.random.fold_in(key, 3), *heavy), -limit, limit).astype(kind)


def setup_inputs(seed: int = 0) -> dict:
    streams_of = jax.random.split(jax.random.key(seed), 13)
    layer_input = bell_draw(streams_of[0], (TOKENS, D), 1.0, 6.0, ((0, 32),))
    segment_ids = draw_segment_ids(jax.random.fold_in(streams_of[12], 71), 0)
    norm_attn = jnp.clip(1.0 + 0.1 * jax.random.normal(streams_of[2], (D,), jnp.float32), 0.5, 1.5).astype(jnp.bfloat16)
    w_query = draw_w_query(jax.random.fold_in(streams_of[12], 71), 0)
    w_key = draw_w_key(jax.random.fold_in(streams_of[12], 71), 0)
    w_value = bell_draw(streams_of[5], (D, KV * HD), D ** -0.5, 0.125, ((0, 8), (1, 4)))
    w_output = bell_draw(streams_of[6], (H * HD, D), (H * HD // 16) ** -0.5, 0.5, ((0, 4), (1, 8)))
    norm_ffn = jnp.clip(1.0 + 0.1 * jax.random.normal(streams_of[7], (D,), jnp.float32), 0.5, 1.5).astype(jnp.bfloat16)
    w_gate = bell_draw(streams_of[8], (D, FF), D ** -0.5, 0.125, ((0, 8), (1, 4)))
    w_up = bell_draw(streams_of[9], (D, FF), D ** -0.5, 0.125, ((0, 8), (1, 4)))
    w_down = bell_draw(streams_of[10], (FF, D), FF ** -0.5, 0.078125, ((0, 4), (1, 8)))
    cotangent = bell_draw_with(streams_of[11], (TOKENS, D), 1.0, 6.0, ((0, 32),), (0, 1, 32, 2.75))
    return dict(layer_input=layer_input, segment_ids=segment_ids, norm_attn=norm_attn, w_query=w_query, w_key=w_key, w_value=w_value, w_output=w_output, norm_ffn=norm_ffn, w_gate=w_gate, w_up=w_up, w_down=w_down, cotangent=cotangent)


EPSILON = 1e-05
NEGATIVE = -1e+30

def rope_tables(segments, head_dim):
    row_count = segments.shape[0]
    row_index = jnp.arange(row_count, dtype=jnp.int32)
    change = jnp.concatenate([jnp.ones((1,), jnp.int32), (segments[1:] != segments[:-1]).astype(jnp.int32)])
    starts = lax.cummax(jnp.where(change > 0, row_index, jnp.zeros_like(row_index)), axis=0)
    position = (row_index - starts).astype(jnp.float32)
    half_dim = head_dim // 2
    frequency = jnp.exp(jnp.arange(half_dim, dtype=jnp.float32) * (-math.log(10000.0) / half_dim))
    angles = position[:, None] * frequency[None, :]
    return (jnp.cos(angles)[:, None, :], jnp.sin(angles)[:, None, :])

def rotate(tensor, cosine, sine):
    half_dim = tensor.shape[-1] // 2
    first_half = tensor[..., :half_dim]
    second_half = tensor[..., half_dim:]
    return jnp.concatenate([first_half * cosine - second_half * sine, second_half * cosine + first_half * sine], axis=-1)

def unrotate(tensor, cosine, sine):
    half_dim = tensor.shape[-1] // 2
    first_half = tensor[..., :half_dim]
    second_half = tensor[..., half_dim:]
    return jnp.concatenate([first_half * cosine + second_half * sine, second_half * cosine - first_half * sine], axis=-1)

def visible(segments):
    row_index = jnp.arange(segments.shape[0], dtype=jnp.int32)
    same_seq = segments[:, None] == segments[None, :]
    return same_seq & (row_index[:, None] >= row_index[None, :])

def normalize(values, gain):
    inverse = lax.rsqrt(lax.optimization_barrier(jnp.mean(values * values, axis=-1, keepdims=True)) + EPSILON)
    unit_rows = values * inverse
    return (unit_rows, inverse, (unit_rows * gain.astype(jnp.float32)).astype(jnp.bfloat16))

def normalize_back(grad_normed, unit_rows, inverse, gain):
    scaled = grad_normed * gain.astype(jnp.float32)
    grad_values = inverse * (scaled - unit_rows * lax.optimization_barrier(jnp.mean(scaled * unit_rows, axis=-1, keepdims=True)))
    return (grad_values, lax.optimization_barrier(jnp.sum(grad_normed * unit_rows, axis=0)))

def block_pass(weights, layer_rows, segments, cotangent_rows):
    norm_attn, w_query, w_key, w_value, w_output, norm_ffn, w_gate, w_up, w_down = weights
    row_count = layer_rows.shape[0]
    kv_heads = w_key.shape[1] // HD
    query_count = w_query.shape[1] // HD
    group = query_count // kv_heads
    score_scale = HD ** (-0.5)
    cosine, sine = rope_tables(segments, HD)
    allowed = visible(segments)
    residual_in = layer_rows.astype(jnp.float32)
    unit_attn, inverse_attn, normed_attn = normalize(residual_in, norm_attn)
    query_heads = rotate(jnp.dot(normed_attn, w_query, preferred_element_type=jnp.float32).reshape(row_count, query_count, HD), cosine, sine).astype(jnp.bfloat16)
    key_heads = rotate(jnp.dot(normed_attn, w_key, preferred_element_type=jnp.float32).reshape(row_count, kv_heads, HD), cosine, sine).astype(jnp.bfloat16)
    value_heads = jnp.dot(normed_attn, w_value, preferred_element_type=jnp.float32).astype(jnp.bfloat16).reshape(row_count, kv_heads, HD)
    query_groups = query_heads.reshape(row_count, kv_heads, group, HD).astype(jnp.float32)
    scores = jnp.einsum('rkgd,skd->kgrs', query_groups, key_heads.astype(jnp.float32)) * score_scale
    scores = jnp.where(allowed[None, None], scores, NEGATIVE)
    row_max = lax.optimization_barrier(jnp.max(scores, axis=-1, keepdims=True))
    log_total = row_max + jnp.log(lax.optimization_barrier(jnp.sum(jnp.exp(scores - row_max), axis=-1, keepdims=True)))
    attn_probs = jnp.exp(scores - log_total)
    probs_low = attn_probs.astype(jnp.bfloat16)
    mixed_heads = jnp.einsum('kgrs,skd->rkgd', probs_low.astype(jnp.float32), value_heads.astype(jnp.float32)).astype(jnp.bfloat16)
    mixed_flat = mixed_heads.reshape(row_count, query_count * HD)
    hidden_res = residual_in + jnp.dot(mixed_flat, w_output, preferred_element_type=jnp.float32)
    unit_ffn, inverse_ffn, normed_ffn = normalize(hidden_res, norm_ffn)
    gate_rows = jnp.dot(normed_ffn, w_gate, preferred_element_type=jnp.float32)
    up_rows = jnp.dot(normed_ffn, w_up, preferred_element_type=jnp.float32)
    sigmoid_gate = jax.nn.sigmoid(gate_rows)
    active = (gate_rows * sigmoid_gate * up_rows).astype(jnp.bfloat16)
    layer_output = (hidden_res + jnp.dot(active, w_down, preferred_element_type=jnp.float32)).astype(jnp.bfloat16)
    grad_active = jnp.dot(cotangent_rows, w_down.T, preferred_element_type=jnp.float32)
    grad_w_down = jnp.dot(active.T, cotangent_rows, preferred_element_type=jnp.float32)
    grad_up_rows = (grad_active * gate_rows * sigmoid_gate).astype(jnp.bfloat16)
    grad_gate_rows = (grad_active * up_rows * sigmoid_gate * (1.0 + gate_rows * (1.0 - sigmoid_gate))).astype(jnp.bfloat16)
    grad_w_gate = jnp.dot(normed_ffn.T, grad_gate_rows, preferred_element_type=jnp.float32)
    grad_w_up = jnp.dot(normed_ffn.T, grad_up_rows, preferred_element_type=jnp.float32)
    grad_normed_ffn = jnp.dot(grad_gate_rows, w_gate.T, preferred_element_type=jnp.float32) + jnp.dot(grad_up_rows, w_up.T, preferred_element_type=jnp.float32)
    grad_hidden, grad_norm_ffn = normalize_back(grad_normed_ffn, unit_ffn, inverse_ffn, norm_ffn)
    grad_hidden = cotangent_rows.astype(jnp.float32) + grad_hidden
    branch_grad = grad_hidden.astype(jnp.bfloat16)
    grad_mixed = jnp.dot(branch_grad, w_output.T, preferred_element_type=jnp.float32).astype(jnp.bfloat16)
    grad_w_output = jnp.dot(mixed_flat.T, branch_grad, preferred_element_type=jnp.float32)
    grad_groups = grad_mixed.reshape(row_count, kv_heads, group, HD).astype(jnp.float32)
    grad_probs = jnp.einsum('rkgd,skd->kgrs', grad_groups, value_heads.astype(jnp.float32))
    row_delta = lax.optimization_barrier(jnp.sum(grad_groups * mixed_heads.astype(jnp.float32), axis=-1))
    row_delta = jnp.transpose(row_delta, (1, 2, 0))[..., None]
    grad_scores = (attn_probs * (grad_probs - row_delta)).astype(jnp.bfloat16).astype(jnp.float32)
    grad_query_rot = jnp.einsum('kgrs,skd->rkgd', grad_scores, key_heads.astype(jnp.float32)) * score_scale
    grad_key_rot = jnp.einsum('kgrs,rkgd->skd', grad_scores, query_groups) * score_scale
    grad_value_heads = jnp.einsum('kgrs,rkgd->skd', probs_low.astype(jnp.float32), grad_groups)
    grad_queries = unrotate(grad_query_rot.reshape(row_count, query_count, HD), cosine, sine).reshape(row_count, query_count * HD).astype(jnp.bfloat16)
    grad_keys = unrotate(grad_key_rot, cosine, sine).reshape(row_count, kv_heads * HD).astype(jnp.bfloat16)
    grad_values = grad_value_heads.reshape(row_count, kv_heads * HD).astype(jnp.bfloat16)
    grad_w_query = jnp.dot(normed_attn.T, grad_queries, preferred_element_type=jnp.float32)
    grad_w_key = jnp.dot(normed_attn.T, grad_keys, preferred_element_type=jnp.float32)
    grad_w_value = jnp.dot(normed_attn.T, grad_values, preferred_element_type=jnp.float32)
    grad_normed_attn = jnp.dot(grad_queries, w_query.T, preferred_element_type=jnp.float32)
    grad_normed_attn = grad_normed_attn + jnp.dot(grad_keys, w_key.T, preferred_element_type=jnp.float32)
    grad_normed_attn = grad_normed_attn + jnp.dot(grad_values, w_value.T, preferred_element_type=jnp.float32)
    grad_residual, grad_norm_attn = normalize_back(grad_normed_attn, unit_attn, inverse_attn, norm_attn)
    grad_input = grad_hidden + grad_residual
    grads = (grad_norm_attn, grad_w_query, grad_w_key, grad_w_value, grad_w_output, grad_norm_ffn, grad_w_gate, grad_w_up, grad_w_down)
    return (layer_output, grad_input, grads)

def reference(layer_input, segment_ids, norm_attn, w_query, w_key, w_value, w_output, norm_ffn, w_gate, w_up, w_down, cotangent):
    weights = (norm_attn, w_query, w_key, w_value, w_output, norm_ffn, w_gate, w_up, w_down)
    block_count = layer_input.shape[0] // TOK_DEV

    def step(carry, pieces):
        rows_in, segments, cotangent_rows = pieces
        layer_output, grad_input, grads = block_pass(weights, rows_in, segments, cotangent_rows)
        return (tuple((total + piece for total, piece in zip(carry, grads))), (layer_output, grad_input))
    zeros = tuple((jnp.zeros(weight.shape, jnp.float32) for weight in weights))
    pieces = (layer_input.reshape(block_count, TOK_DEV, D), segment_ids.reshape(block_count, TOK_DEV), cotangent.reshape(block_count, TOK_DEV, D))
    totals, (outputs, grad_inputs) = lax.scan(step, zeros, pieces)
    return (outputs.reshape(TOKENS, D), grad_inputs.reshape(TOKENS, D), totals[0], totals[1], totals[2], totals[3], totals[4], totals[5], totals[6], totals[7], totals[8])
```

```python
import functools
import math

import jax
import jax.numpy as jnp
from jax import lax
from jax.experimental import pallas as pl
from jax.experimental.pallas import tpu as pltpu
from jax.sharding import PartitionSpec as P

HD = 64
EPSILON = 1e-05
NEGATIVE = -1e30
LANES = 128
BF = jnp.bfloat16
F32 = jnp.float32
VMEM_BYTES = 66_000_000


def spans(bits):
    masks = [0]
    for bit in bits:
        masks = masks + [mask | (1 << bit) for mask in masks]
    return masks


def flip(index, mask, width):
    total = 0
    for bit in range(width):
        own = lax.rem(lax.div(index, 1 << bit), 2)
        if isinstance(mask, int):
            other = (mask >> bit) & 1
        else:
            other = lax.rem(lax.div(mask, 1 << bit), 2)
        total = total + lax.rem(own + other, 2) * (1 << bit)
    return total


def aligned(value, step):
    return value if isinstance(value, int) else pl.multiple_of(value, step)


def remote(src, dst, send_sem, recv_sem, device):
    return pltpu.make_async_remote_copy(
        src_ref=src,
        dst_ref=dst,
        send_sem=send_sem,
        recv_sem=recv_sem,
        device_id=device,
        device_id_type=pl.DeviceIdType.MESH,
    )


def dot(left, right, left_dim=1, right_dim=0):
    return lax.dot_general(
        left, right, (((left_dim,), (right_dim,)), ((), ())), preferred_element_type=F32
    )


def tiles_of(size, most):
    units = size // LANES
    parts = -(-units // most)
    cuts, start = [], 0
    for part in range(parts):
        width = (units // parts + (1 if part < units % parts else 0)) * LANES
        cuts.append((start, width))
        start += width
    return cuts


def enter(t, nt, me, width, barrier, everyone_along_tensor=False):
    signal = functools.partial(
        pl.semaphore_signal, barrier, inc=1, device_id_type=pl.DeviceIdType.MESH
    )
    for mask in range(1, 1 << width):
        signal(device_id={"dp": flip(me, mask, width)})
    if everyone_along_tensor:
        for step in range(1, nt):
            signal(device_id={"tensor": lax.rem(t + step, nt)})
        pl.semaphore_wait(barrier, (1 << width) - 1 + nt - 1)
        return

    @pl.when(t > 0)
    def _():
        signal(device_id={"tensor": t - 1})

    @pl.when(t < nt - 1)
    def _():
        signal(device_id={"tensor": t + 1})

    neighbours = lax.min(t, 1) + lax.min(nt - 1 - t, 1)
    pl.semaphore_wait(barrier, (1 << width) - 1 + neighbours)


class LineGather:
    def __init__(self, full, t, nt, sems):
        self.full, self.t, self.nt, self.sems = full, t, nt, sems
        self.rows = full.shape[0] // nt

    def window(self, j):
        return self.full.at[pl.ds(pl.multiple_of(j * self.rows, self.rows), self.rows), :]

    def right(self, j):
        return remote(
            self.window(j), self.window(j), self.sems.at[0, j], self.sems.at[2, j],
            {"tensor": lax.rem(self.t + 1, self.nt)},
        )

    def left(self, j):
        return remote(
            self.window(j), self.window(j), self.sems.at[1, j], self.sems.at[3, j],
            {"tensor": lax.rem(self.t + self.nt - 1, self.nt)},
        )

    def start(self):
        @pl.when(self.t < self.nt - 1)
        def _():
            self.right(self.t).start()

        @pl.when(self.t > 0)
        def _():
            self.left(self.t).start()

    def step(self, s):
        t, nt = self.t, self.nt

        @pl.when(t >= s)
        def _():
            self.right(t - s).wait_recv()

            @pl.when(t < nt - 1)
            def _():
                self.right(t - s).start()

        @pl.when(t + s < nt)
        def _():
            self.left(t + s).wait_recv()

            @pl.when(t > 0)
            def _():
                self.left(t + s).start()

    def finish(self):
        t, nt = self.t, self.nt
        for s in range(nt):
            @pl.when((t >= s) & (t < nt - 1))
            def _():
                self.right(t - s).wait_send()

            @pl.when((t + s < nt) & (t > 0))
            def _():
                self.left(t + s).wait_send()


class LineScatter:
    def __init__(self, part, sent, from_left, from_right, t, nt, cuts, sems):
        self.part, self.sent = part, sent
        self.from_left, self.from_right = from_left, from_right
        self.t, self.nt, self.cuts, self.sems = t, nt, cuts, sems
        self.rows = sent.shape[1]
        self.width = sent.shape[2] // cuts

    def cols(self, c):
        if isinstance(c, int):
            return slice(c * self.width, (c + 1) * self.width)
        return pl.ds(pl.multiple_of(c * self.width, self.width), self.width)

    def right(self, j, c):
        cols = self.cols(c)
        return remote(
            self.sent.at[j, :, cols], self.from_left.at[j, :, cols],
            self.sems.at[0, j, c], self.sems.at[2, j, c],
            {"tensor": lax.rem(self.t + 1, self.nt)},
        )

    def left(self, j, c):
        cols = self.cols(c)
        return remote(
            self.sent.at[j, :, cols], self.from_right.at[j, :, cols],
            self.sems.at[1, j, c], self.sems.at[3, j, c],
            {"tensor": lax.rem(self.t + self.nt - 1, self.nt)},
        )

    def mine(self, j, c):
        rows = pl.ds(pl.multiple_of(j * self.rows, self.rows), self.rows)
        return self.part[rows, self.cols(c)]

    def edge(self, c):
        t, nt = self.t, self.nt

        @pl.when(t == 0)
        def _():
            @pl.loop(0, nt - 1)
            def _(k):
                j = nt - 1 - k
                self.sent[j, :, self.cols(c)] = self.mine(j, c).astype(BF)
                self.right(j, c).start()

        @pl.when(t == nt - 1)
        def _():
            @pl.loop(0, nt - 1)
            def _(j):
                self.sent[j, :, self.cols(c)] = self.mine(j, c).astype(BF)
                self.left(j, c).start()

    def round(self, k):
        t, nt = self.t, self.nt
        j_right, j_left = nt - 1 - k, k

        @pl.loop(0, self.cuts)
        def _(c):
            @pl.when((t > 0) & (j_right > t))
            def _():
                self.right(j_right, c).wait_recv()
                total = self.mine(j_right, c) + self.from_left[j_right, :, self.cols(c)].astype(F32)
                self.sent[j_right, :, self.cols(c)] = total.astype(BF)
                self.right(j_right, c).start()

            @pl.when((t < nt - 1) & (j_left < t))
            def _():
                self.left(j_left, c).wait_recv()
                total = self.mine(j_left, c) + self.from_right[j_left, :, self.cols(c)].astype(F32)
                self.sent[j_left, :, self.cols(c)] = total.astype(BF)
                self.left(j_left, c).start()

    def own(self, store):
        t, nt = self.t, self.nt
        rows = pl.ds(pl.multiple_of(t * self.rows, self.rows), self.rows)
        for c in range(self.cuts):
            cols = self.cols(c)

            @pl.when(t > 0)
            def _():
                self.right(t, c).wait_recv()
                self.part[rows, cols] += self.from_left[t, :, cols].astype(F32)

            @pl.when(t < nt - 1)
            def _():
                self.left(t, c).wait_recv()
                self.part[rows, cols] += self.from_right[t, :, cols].astype(F32)

            store(cols, self.part[rows, cols])

    def finish(self):
        t, nt = self.t, self.nt
        for j in range(nt):
            for c in range(self.cuts):
                @pl.when(j > t)
                def _():
                    self.right(j, c).wait_send()

                @pl.when(j < t)
                def _():
                    self.left(j, c).wait_send()


class Cube:
    def setup(self, me, width, half_send, half_recv, pair_send, pair_recv):
        self.me, self.width = me, width
        self.hs, self.hr, self.ps, self.pr = half_send, half_recv, pair_send, pair_recv
        self.bits = list(range(1, width))
        self.orders = (self.bits, self.bits[::-1])
        self.masks = spans(self.bits)
        self.stages = len(self.bits)

    def at(self, mask):
        return flip(self.me, mask, self.width)


class BlockGather(Cube):
    def __init__(self, own, full, by_rows, me, width, *sems):
        self.setup(me, width, *sems)
        self.own_ref, self.full, self.by_rows = own, full, by_rows

    def half(self, h):
        rows = self.own_ref.shape[0] // 2
        return self.own_ref.at[pl.ds(h * rows, rows), :]

    def window(self, who, h=None):
        rows, cols = self.own_ref.shape
        take, start = (rows, 0) if h is None else (rows // 2, h * (rows // 2))
        if self.by_rows:
            return self.full.at[pl.ds(aligned(who * rows + start, take), take), :]
        return self.full.at[pl.ds(start, take), pl.ds(aligned(who * cols, cols), cols)]

    def hop(self, stage, h, m):
        order = self.orders[h]
        bit = 1 << order[stage]
        slot = (m | bit) >> 1
        src = self.half(h) if m == 0 else self.window(self.at(m), h)
        return remote(
            src, self.window(self.at(m), h), self.hs.at[h, slot], self.hr.at[h, slot],
            {"dp": self.at(bit)},
        )

    def send(self, stage):
        for h in range(2):
            for m in spans(self.orders[h][:stage]):
                self.hop(stage, h, m).start()

    def wait(self, stage):
        for h in range(2):
            bit = 1 << self.orders[h][stage]
            for m in spans(self.orders[h][:stage]):
                slot = (m | bit) >> 1
                landed = self.window(self.at(m | bit), h)
                remote(
                    landed, landed, self.hs.at[h, slot], self.hr.at[h, slot], {"dp": self.at(bit)}
                ).wait_recv()

    def pair(self, m):
        src = self.own_ref if m == 0 else self.window(self.at(m))
        return remote(
            src, self.window(self.at(m)), self.ps.at[m >> 1], self.pr.at[m >> 1],
            {"dp": self.at(1)},
        )

    def pair_send(self):
        for m in self.masks:
            self.pair(m).start()

    def pair_wait(self):
        for m in self.masks:
            landed = self.window(self.at(m | 1))
            remote(
                landed, landed, self.ps.at[m >> 1], self.pr.at[m >> 1], {"dp": self.at(1)}
            ).wait_recv()

    def place(self, sem):
        return pltpu.make_async_copy(self.own_ref, self.window(self.me), sem)

    def drain(self):
        for stage in range(self.stages):
            for h in range(2):
                for m in spans(self.orders[h][:stage]):
                    self.hop(stage, h, m).wait_send()
        for m in self.masks:
            self.pair(m).wait_send()


class BlockScatter(Cube):
    def __init__(self, chunk, out_sent, total, landed, store, me, width, *sems):
        self.setup(me, width, *sems)
        self.chunk, self.sent, self.total, self.landed = chunk, out_sent, total, landed
        self.store = store
        self.slots = 1 << (width - 1)

    def pair(self, slot):
        return remote(
            self.sent.at[slot], self.total.at[slot], self.ps.at[slot], self.pr.at[slot],
            {"dp": self.at(1)},
        )

    def give(self):
        @pl.loop(0, self.slots)
        def _(k):
            slot = self.slots - 1 - k
            self.sent[slot] = self.chunk(self.at(2 * slot + 1)).astype(BF)
            self.pair(slot).start()

    def given(self):
        @pl.loop(0, self.slots)
        def _(slot):
            self.pair(slot).wait_send()

    def take(self):
        @pl.loop(0, self.slots)
        def _(k):
            slot = self.slots - 1 - k
            term = self.chunk(self.at(2 * slot))
            self.pair(slot).wait_recv()
            self.total[slot] = (term + self.total[slot].astype(F32)).astype(BF)

    def moves(self, stage):
        for h in range(2):
            order = self.orders[h]
            last = self.stages - 1 - stage
            bit = 1 << order[last]
            for m in spans(order[:last]):
                yield h, bit, m | bit

    def hop(self, h, bit, m):
        rows = self.total.shape[1] // 2
        return remote(
            self.total.at[m >> 1, pl.ds(h * rows, rows), :], self.landed.at[h, (m >> 1) - 1],
            self.hs.at[h, m >> 1], self.hr.at[h, m >> 1], {"dp": self.at(bit)},
        )

    def send(self, stage):
        for h, bit, m in self.moves(stage):
            self.hop(h, bit, m).start()

    def add(self, stage):
        rows = self.total.shape[1] // 2
        for h, bit, m in self.moves(stage):
            self.hop(h, bit, m).wait_recv()
            keep = (m ^ bit) >> 1
            at = slice(h * rows, (h + 1) * rows)
            total = self.total[keep, at, :].astype(F32) + self.landed[h, (m >> 1) - 1].astype(F32)
            if stage == self.stages - 1:
                self.store(at, total)
            else:
                self.total[keep, at, :] = total.astype(BF)

    def drain(self):
        for stage in range(self.stages):
            for h, bit, m in self.moves(stage):
                self.hop(h, bit, m).wait_send()


def inverse_of(rows):
    return lax.rsqrt(jnp.mean(rows * rows, axis=-1, keepdims=True) + EPSILON)


def times_gain(unit, gains, which, store):
    parts, _, width = gains.shape
    for d in range(parts):
        cols = slice(d * width, (d + 1) * width)
        store(cols, unit[:, cols] * gains[d, which : which + 1, :])


def lane_index(shape):
    return lax.broadcasted_iota(jnp.int32, shape, len(shape) - 1)


def rope_into(cos_ref, sin_ref, segc, segr):
    rows = segc.shape[0]
    before = (segr[...] < segc[...]).astype(F32)
    start = jnp.sum(before, axis=1, keepdims=True)
    position = lax.broadcasted_iota(jnp.int32, (rows, 1), 0).astype(F32) - start
    lane = lane_index((rows, LANES))
    half = HD // 2
    frequency = jnp.exp(lax.rem(lane, half).astype(F32) * (-math.log(10000.0) / half))
    angle = position * frequency
    cos_ref[...] = jnp.cos(angle)
    sine = jnp.sin(angle)
    sin_ref[...] = jnp.where(lax.rem(lane, HD) < half, -sine, sine)


def swapped(x):
    lane = lane_index(x.shape)
    half = HD // 2
    return jnp.where(
        lax.rem(lane, HD) < half,
        pltpu.roll(x, LANES - half, 1),
        pltpu.roll(x, half, 1),
    )


def bias_into(bias, segc, segr):
    rows = segc.shape[0]
    query = lax.broadcasted_iota(jnp.int32, (rows, rows), 0)
    key = lax.broadcasted_iota(jnp.int32, (rows, rows), 1)
    seen = (segr[...] == segc[...]) & (query >= key)
    bias[...] = jnp.where(seen, 0.0, NEGATIVE)


def pad_pair(keys_values, keys, values):
    low = lane_index(keys_values.shape) < HD
    key = jnp.where(low, keys_values, 0.0)
    value = jnp.where(low, 0.0, keys_values)
    keys[0] = key.astype(BF)
    keys[1] = pltpu.roll(key, HD, 1).astype(BF)
    values[0] = pltpu.roll(value, HD, 1).astype(BF)
    values[1] = value.astype(BF)


def query_cuts(rows):
    block = 256 if rows % 256 == 0 else rows
    return [(start, block, start + block) for start in range(0, rows, block)]


def attend_pairs(first, last, qo, kpad, vpad, bias, mo, lo):
    rows = qo.shape[0]
    lane = lane_index((1, LANES))

    @pl.loop(first, last)
    def _(pair):
        lanes = pl.ds(pl.multiple_of(pair * LANES, LANES), LANES)
        for start, block, seen in query_cuts(rows):
            at = slice(start, start + block)
            query = qo[at, lanes]
            mixed = jnp.zeros((block, LANES), F32)
            logs = lo[at, :]
            for side in range(2):
                scores = dot(query, kpad[side, :seen, :], 1, 1) + bias[at, :seen]
                top = jnp.max(scores, axis=-1, keepdims=True)
                probs = jnp.exp(scores - top)
                total = jnp.sum(probs, axis=-1, keepdims=True)
                mixed = mixed + dot(probs.astype(BF), vpad[side, :seen, :]) / total
                logs = jnp.where(lane == 2 * pair + side, top + jnp.log(total), logs)
            lo[at, :] = logs
            mo[at, lanes] = mixed.astype(BF)


def front_kernel(
    nt, width,
    x, cot, gain, segc, segr, wqkv, wo, gate, up, down,
    wqkv_f, wo_f, gate_f, up_f, down_f, na, cf, nf, qo, kvo, mo, lo, hid, gall, cos, sin,
    part, sent, from_left, from_right, wqkv_v, wo_v, bias, kpad, vpad,
    gain_sem, place_sem, line_na, line_cf, line_nf, scatter_sem, hs, hr, ps, pr,
):
    me, t = lax.axis_index("dp"), lax.axis_index("tensor")
    nd = 1 << width
    rows, model = x.shape
    queries = qo.shape[1]
    enter(t, nt, me, width, pltpu.get_barrier_semaphore())

    gathers = []
    for w, (own, full, by_rows) in enumerate(
        ((wqkv, wqkv_f, True), (wo, wo_f, False), (gate, gate_f, True), (up, up_f, True), (down, down_f, False))
    ):
        gathers.append(
            BlockGather(own, full, by_rows, me, width, hs.at[w], hr.at[w], ps.at[w], pr.at[w])
        )
    g_qkv, g_out, g_gate, g_up, g_down = gathers

    def gain_copy(mask):
        return remote(
            gain, gall.at[me], gain_sem.at[0, mask], gain_sem.at[1, mask],
            {"dp": flip(me, mask, width)},
        )

    for mask in range(1, nd):
        gain_copy(mask).start()
    gall[me] = gain[...]
    stages = g_qkv.stages
    for g in (g_qkv, g_out, g_gate):
        g.send(0)
    for w, g in enumerate(gathers):
        g.place(place_sem.at[w]).start()
    for mask in range(1, nd):
        slot = gall.at[flip(me, mask, width)]
        remote(
            slot, slot, gain_sem.at[0, mask], gain_sem.at[1, mask], {"dp": flip(me, mask, width)}
        ).wait_recv()

    def forward(g, stage):
        g.wait(stage)
        if stage + 1 < stages:
            g.send(stage + 1)
        else:
            g.pair_send()

    local = pl.ds(pl.multiple_of(t * rows, rows), rows)
    residual = x[...].astype(F32)

    def store_na(cols, value):
        na[local, cols] = value.astype(BF)

    times_gain(residual * inverse_of(residual), gall, 0, store_na)
    cf[local, :] = cot[...]
    tokens = LineGather(na, t, nt, line_na)
    tokens.start()
    for s in range(stages - 1):
        forward(g_qkv, s)
        forward(g_out, s)
    rope_into(cos, sin, segc, segr)
    bias_into(bias, segc, segr)
    lo[...] = jnp.zeros_like(lo)
    fills = [
        lambda: (forward(g_gate, 0), g_up.send(0)),
        lambda: (forward(g_qkv, stages - 1), forward(g_out, stages - 1), g_down.send(0)),
    ]
    for s in range(1, nt):
        tokens.step(s)
        if fills:
            fills.pop(0)()
    for fill in fills:
        fill()

    cots = LineGather(cf, t, nt, line_cf)
    cots.start()

    g_qkv.place(place_sem.at[0]).wait()
    g_qkv.pair_wait()
    load = pltpu.make_async_copy(wqkv_f, wqkv_v, place_sem.at[5])
    load.start()
    g_out.place(place_sem.at[1]).wait()
    g_out.pair_wait()
    load_out = pltpu.make_async_copy(wo_f, wo_v, place_sem.at[6])
    load_out.start()
    load.wait()

    wide = wqkv_v.shape[1]
    part[:, :wide] = dot(na[...], wqkv_v[...])
    c, s_ = cos[...], sin[...]
    for start in range(0, queries, LANES):
        lanes = slice(start, start + LANES)
        value = part[:, lanes]
        qo[:, lanes] = ((value * c + swapped(value) * s_) * HD ** (-0.5)).astype(BF)
    value = part[:, queries : queries + LANES]
    keyed = jnp.where(lane_index(value.shape) < HD, value * c + swapped(value) * s_, value)
    kvo[...] = keyed.astype(BF)
    pad_pair(keyed, kpad, vpad)

    pairs = queries // LANES
    later = [
        lambda: forward(g_up, 0),
        lambda: forward(g_down, 0),
    ]
    for s in range(1, stages):
        later.append(functools.partial(forward, g_gate, s))
        later.append(functools.partial(forward, g_up, s))
        later.append(functools.partial(forward, g_down, s))
    attend_pairs(0, pairs // 2, qo, kpad, vpad, bias, mo, lo)
    later.pop(0)()
    cots.step(1)
    attend_pairs(pairs // 2, pairs, qo, kpad, vpad, bias, mo, lo)
    later.pop(0)()
    load_out.wait()

    summed = LineScatter(part, sent, from_left, from_right, t, nt, scatter_sem.shape[2], scatter_sem)
    for cut in range(summed.cuts):
        cols = summed.cols(cut)
        part[:, cols] = dot(mo[...], wo_v[:, cols])
        summed.edge(cut)
    for k in range(nt - 1):
        summed.round(k)
        if k + 2 < nt:
            cots.step(k + 2)
        if later:
            later.pop(0)()

    def store_hidden(cols, value):
        hid[:, cols] = x[:, cols].astype(F32) + value

    summed.own(store_hidden)
    hidden = hid[...]

    def store_nf(cols, value):
        nf[local, cols] = value.astype(BF)

    times_gain(hidden * inverse_of(hidden), gall, 1, store_nf)
    tokens_ffn = LineGather(nf, t, nt, line_nf)
    tokens_ffn.start()
    for s in range(1, nt):
        if later:
            later.pop(0)()
        tokens_ffn.step(s)
    for fill in later:
        fill()
    for w, g in enumerate(gathers):
        if w >= 2:
            g.place(place_sem.at[w]).wait()
            g.pair_wait()
    for g in gathers:
        g.drain()
    for mask in range(1, nd):
        gain_copy(mask).wait_send()
    tokens.finish()
    cots.finish()
    tokens_ffn.finish()
    summed.finish()


def vmem():
    return pl.BlockSpec(memory_space=pltpu.VMEM)


def hbm():
    return pl.BlockSpec(memory_space=pl.ANY)


def scatter_scratch(tokens, nt, model):
    rows = tokens // nt
    return [
        pltpu.VMEM((tokens, model), F32),
        pltpu.VMEM((nt, rows, model), BF),
        pltpu.VMEM((nt, rows, model), BF),
        pltpu.VMEM((nt, rows, model), BF),
    ]


def dma(*shape):
    return pltpu.SemaphoreType.DMA(shape)


CUTS = 4


def front(nt, nd, x, cot, gain, segc, segr, wqkv, wo, gate, up, down):
    width = nd.bit_length() - 1
    rows, model = x.shape
    tokens = segc.shape[0]
    queries = wo.shape[0]
    hidden = gate.shape[1]
    half = nd // 2
    shape = jax.ShapeDtypeStruct
    outs = [
        (shape((model, wqkv.shape[1]), BF), hbm()),
        (shape((queries, model), BF), hbm()),
        (shape((model, hidden), BF), hbm()),
        (shape((model, hidden), BF), hbm()),
        (shape((hidden, model), BF), hbm()),
        (shape((tokens, model), BF), vmem()),
        (shape((tokens, model), BF), vmem()),
        (shape((tokens, model), BF), vmem()),
        (shape((tokens, queries), BF), vmem()),
        (shape((tokens, LANES), BF), vmem()),
        (shape((tokens, queries), BF), vmem()),
        (shape((tokens, LANES), F32), vmem()),
        (shape((rows, model), F32), vmem()),
        (shape((nd,) + gain.shape, F32), vmem()),
        (shape((tokens, LANES), F32), vmem()),
        (shape((tokens, LANES), F32), vmem()),
    ]
    return pl.pallas_call(
        functools.partial(front_kernel, nt, width),
        out_shape=[o for o, _ in outs],
        in_specs=[vmem()] * 10,
        out_specs=[s for _, s in outs],
        scratch_shapes=scatter_scratch(tokens, nt, model)
        + [
            pltpu.VMEM((model, wqkv.shape[1]), BF),
            pltpu.VMEM((queries, model), BF),
            pltpu.VMEM((tokens, tokens), F32),
            pltpu.VMEM((2, tokens, LANES), BF),
            pltpu.VMEM((2, tokens, LANES), BF),
            dma(2, nd),
            dma(7),
            dma(4, nt),
            dma(4, nt),
            dma(4, nt),
            dma(4, nt, CUTS),
            dma(5, 2, half),
            dma(5, 2, half),
            dma(5, half),
            dma(5, half),
        ],
        compiler_params=pltpu.CompilerParams(
            collective_id=0, has_side_effects=True, vmem_limit_bytes=VMEM_BYTES
        ),
        name="front",
    )(x, cot, gain, segc, segr, wqkv, wo, gate, up, down)


def back_through_norm(raw, grads, gains, which, store, store_gain):
    parts, _, width = gains.shape
    cuts = [slice(d * width, (d + 1) * width) for d in range(parts)]
    model = parts * width
    square = sum(jnp.sum(raw(c) * raw(c), axis=-1, keepdims=True) for c in cuts)
    inverse = lax.rsqrt(square / model + EPSILON)
    mean = 0.0
    for d, c in enumerate(cuts):
        unit = raw(c) * inverse
        grad = grads(c)
        store_gain(c, jnp.sum(grad * unit, axis=0, keepdims=True))
        mean = mean + jnp.sum(grad * gains[d, which : which + 1, :] * unit, axis=-1, keepdims=True)
    mean = mean / model
    for d, c in enumerate(cuts):
        unit = raw(c) * inverse
        store(c, inverse * (grads(c) * gains[d, which : which + 1, :] - unit * mean))


def ffn_kernel(
    nt, width,
    nf, cf, hid, cot, gall, gate_f, up_f, down_f,
    act, branch, gh, gains, d_gate, d_up, d_down,
    gate_v, up_v, down_v, wide, dg, du, sent, from_left, from_right, given, totals, landed,
    load_sem, out_sem, scatter_sem, line_sem, hs, hr, ps, pr,
):
    me, t = lax.axis_index("dp"), lax.axis_index("tensor")
    rows, model = hid.shape
    tokens, hidden = act.shape
    shard = model >> width
    cuts = tiles_of(hidden, 6)
    span = max(size for _, size in cuts)
    loads = []
    for i, (start, size) in enumerate(cuts):
        at = pl.ds(start, size)
        loads.append(
            [
                pltpu.make_async_copy(gate_f.at[:, at], gate_v.at[:, at], load_sem.at[i, 0]),
                pltpu.make_async_copy(up_f.at[:, at], up_v.at[:, at], load_sem.at[i, 1]),
                pltpu.make_async_copy(down_f.at[at, :], down_v.at[at, :], load_sem.at[i, 2]),
            ]
        )
        for load in loads[-1]:
            load.start()
    enter(t, nt, me, width, pltpu.get_barrier_semaphore())

    block = 64
    for i, (start, size) in enumerate(cuts):
        at = slice(start, start + size)
        for load in loads[i]:
            load.wait()
        wide[:, 0:size] = dot(nf[...], gate_v[:, at])
        wide[:, span : span + size] = dot(nf[...], up_v[:, at])
        wide[:, 2 * span : 2 * span + size] = dot(cf[...], down_v[at, :], 1, 1)

        @pl.loop(0, tokens // block)
        def _(k):
            these = pl.ds(pl.multiple_of(k * block, block), block)
            g = wide[these, 0:size]
            u = wide[these, span : span + size]
            ga = wide[these, 2 * span : 2 * span + size]
            sig = 1.0 / (1.0 + jnp.exp(-g))
            gs = g * sig
            act[these, at] = (gs * u).astype(BF)
            du[these, at] = (ga * gs).astype(BF)
            dg[these, at] = (ga * u * sig * (1.0 + g * (1.0 - sig))).astype(BF)

    summed = LineScatter(
        wide, sent, from_left, from_right, t, nt, scatter_sem.shape[2], scatter_sem
    )
    for cut in range(summed.cuts):
        cols = summed.cols(cut)
        wide[:, cols] = dot(dg[...], gate_v[cols, :], 1, 1) + dot(du[...], up_v[cols, :], 1, 1)
        summed.edge(cut)

    def keep(place):
        def store(at, value):
            wide[place + at.start : place + at.stop, :hidden] = value

        return store

    def turned(at, value):
        d_down[:, at] = value.T

    scatters = []
    for w, (left, right, store) in enumerate(
        ((nf, dg, keep(0)), (nf, du, keep(shard)), (cf, act, turned))
    ):
        def chunk(d, left=left, right=right):
            return dot(left[:, pl.ds(pl.multiple_of(d * shard, shard), shard)], right[...], 0, 0)

        scatters.append(
            BlockScatter(
                chunk, given, totals.at[w], landed.at[w], store, me, width,
                hs.at[w], hr.at[w], ps.at[w], pr.at[w],
            )
        )
    s_gate, s_up, s_down = scatters
    stages = s_gate.stages

    def take(s):
        s.take()
        s.send(0)

    fills = [
        lambda: take(s_gate),
        lambda: (s_gate.given(), s_up.give()),
        lambda: take(s_up),
    ]
    s_gate.give()
    for k in range(nt - 1):
        summed.round(k)
        if fills:
            fills.pop(0)()
    for fill in fills:
        fill()

    def store_raw(cols, value):
        gh[:, cols] = value

    summed.own(store_raw)
    local = pl.ds(pl.multiple_of(t * rows, rows), rows)
    gains[...] = jnp.zeros_like(gains)

    def store(cols, value):
        total = cot[:, cols].astype(F32) + value
        gh[:, cols] = total
        branch[local, cols] = total.astype(BF)

    def store_gain(cols, value):
        gains[1:2, cols] = value

    back_through_norm(lambda c: hid[:, c], lambda c: gh[:, c], gall, 1, store, store_gain)
    line = LineGather(branch, t, nt, line_sem)
    line.start()
    s_up.given()
    s_down.give()
    take(s_down)

    def on(s, stage):
        s.add(stage)
        if stage + 1 < stages:
            s.send(stage + 1)

    fills = [functools.partial(on, s, stage) for stage in range(stages) for s in scatters]
    for s in range(1, nt):
        line.step(s)
        if fills:
            fills.pop(0)()
    for fill in fills:
        fill()
    out = [
        pltpu.make_async_copy(wide.at[pl.ds(0, shard), pl.ds(0, hidden)], d_gate, out_sem.at[0]),
        pltpu.make_async_copy(wide.at[pl.ds(shard, shard), pl.ds(0, hidden)], d_up, out_sem.at[1]),
    ]
    for copy in out:
        copy.start()
    s_down.given()
    for s in scatters:
        s.drain()
    line.finish()
    summed.finish()
    for copy in out:
        copy.wait()


def ffn(nt, nd, nf, cf, hid, cot, gall, gate_f, up_f, down_f):
    width = nd.bit_length() - 1
    rows, model = hid.shape
    tokens = nf.shape[0]
    hidden = gate_f.shape[1]
    shard = model // nd
    half = nd // 2
    shape = jax.ShapeDtypeStruct
    span = max(size for _, size in tiles_of(hidden, 6))
    outs = [
        (shape((tokens, hidden), BF), vmem()),
        (shape((tokens, model), BF), vmem()),
        (shape((rows, model), F32), vmem()),
        (shape((8, model), F32), vmem()),
        (shape((shard, hidden), F32), hbm()),
        (shape((shard, hidden), F32), hbm()),
        (shape((hidden, shard), F32), vmem()),
    ]
    scratch = scatter_scratch(tokens, nt, model)
    scratch[0] = pltpu.VMEM((max(tokens, 2 * shard), max(model, 3 * span)), F32)
    return pl.pallas_call(
        functools.partial(ffn_kernel, nt, width),
        out_shape=[o for o, _ in outs],
        in_specs=[vmem()] * 5 + [hbm()] * 3,
        out_specs=[s for _, s in outs],
        scratch_shapes=[
            pltpu.VMEM((model, hidden), BF),
            pltpu.VMEM((model, hidden), BF),
            pltpu.VMEM((hidden, model), BF),
            scratch[0],
            pltpu.VMEM((tokens, hidden), BF),
            pltpu.VMEM((tokens, hidden), BF),
        ]
        + scratch[1:]
        + [
            pltpu.VMEM((half, shard, hidden), BF),
            pltpu.VMEM((3, half, shard, hidden), BF),
            pltpu.VMEM((3, 2, half - 1, shard // 2, hidden), BF),
            dma(len(tiles_of(hidden, 6)), 3),
            dma(2),
            dma(4, nt, CUTS),
            dma(4, nt),
            dma(3, 2, half),
            dma(3, 2, half),
            dma(3, half),
            dma(3, half),
        ],
        compiler_params=pltpu.CompilerParams(
            collective_id=1, has_side_effects=True, vmem_limit_bytes=VMEM_BYTES
        ),
        name="ffn",
    )(nf, cf, hid, cot, gall, gate_f, up_f, down_f)


def attend_back_pairs(first, last, qo, gm, mo, lo, kpad, vpad, bias, cos, sin, dqkv, dkey, dval):
    rows = qo.shape[0]

    @pl.loop(first, last)
    def _(pair):
        lanes = pl.ds(pl.multiple_of(pair * LANES, LANES), LANES)
        for start, block, seen in query_cuts(rows):
            at = slice(start, start + block)
            lane = lane_index((block, LANES))
            query, grad = qo[at, lanes], gm[at, lanes]
            both = grad.astype(F32) * mo[at, lanes].astype(F32)
            logs = lo[at, :]
            dq = jnp.zeros((block, LANES), F32)
            for side in range(2):
                inside = (lane >= HD) if side else (lane < HD)
                delta = jnp.sum(jnp.where(inside, both, 0.0), axis=-1, keepdims=True)
                log = jnp.sum(
                    jnp.where(lane == 2 * pair + side, logs, 0.0), axis=-1, keepdims=True
                )
                key, value = kpad[side, :seen, :], vpad[side, :seen, :]
                probs = jnp.exp(dot(query, key, 1, 1) + bias[at, :seen] - log)
                grad_scores = (probs * (dot(grad, value, 1, 1) - delta)).astype(BF)
                dq = dq + dot(grad_scores, key)
                dkey[side, :seen, :] += dot(grad_scores, query, 0, 0)
                dval[side, :seen, :] += dot(probs.astype(BF), grad, 0, 0)
            dq = dq * HD ** (-0.5)
            dqkv[at, lanes] = (dq * cos[at, :] - swapped(dq) * sin[at, :]).astype(BF)


def back_kernel(
    nt, width,
    branch, na, mo, qo, kvo, lo, cos, sin, segc, segr, x, hid, gh, gparts, gall, act,
    wqkv_f, wo_f, down_f,
    y, gi, gain_out, d_qkv, d_wo,
    wqkv_v, wo_v, down_v, part, sent, from_left, from_right, sent2, from_left2, from_right2,
    bias, kpad, vpad, gm, dqkv, dkey, dval,
    given_q, totals_q, landed_q, given_o, totals_o, landed_o,
    gsum, zslots, dslots,
    load_sem, scatter_sem, scatter_sem2, zsem, dsem, hs, hr, ps, pr,
):
    me, t = lax.axis_index("dp"), lax.axis_index("tensor")
    nd = 1 << width
    rows, model = hid.shape
    tokens, queries = qo.shape
    shard = model >> width
    loads = [
        pltpu.make_async_copy(wo_f, wo_v, load_sem.at[0]),
        pltpu.make_async_copy(down_f, down_v, load_sem.at[1]),
        pltpu.make_async_copy(wqkv_f, wqkv_v, load_sem.at[2]),
    ]
    for load in loads:
        load.start()
    enter(t, nt, me, width, pltpu.get_barrier_semaphore(), everyone_along_tensor=True)

    bias_into(bias, segc, segr)
    pad_pair(kvo[...].astype(F32), kpad, vpad)
    dkey[...] = jnp.zeros_like(dkey)
    dval[...] = jnp.zeros_like(dval)
    loads[0].wait()
    gm[...] = dot(branch[...], wo_v[...], 1, 1).astype(BF)
    loads[1].wait()
    cuts = scatter_sem.shape[2]
    outward = LineScatter(part, sent, from_left, from_right, t, nt, cuts, scatter_sem)
    for cut in range(cuts):
        cols = outward.cols(cut)
        part[:, cols] = dot(act[...], down_v[:, cols])
        outward.edge(cut)

    pairs = queries // LANES
    steps = min(nt, pairs)
    for k in range(steps):
        attend_back_pairs(
            k * pairs // steps, (k + 1) * pairs // steps,
            qo, gm, mo, lo, kpad, vpad, bias, cos, sin, dqkv, dkey, dval,
        )
        if k < nt - 1:
            outward.round(k)
    for k in range(steps, nt - 1):
        outward.round(k)

    def store_y(cols, value):
        y[:, cols] = (hid[:, cols] + value).astype(BF)

    outward.own(store_y)
    key = dkey[0] + pltpu.roll(dkey[1], HD, 1)
    value = pltpu.roll(dval[0], HD, 1) + dval[1]
    key = key * cos[...] - swapped(key) * sin[...]
    dqkv[:, queries : queries + LANES] = jnp.where(
        lane_index(key.shape) < HD, key, value
    ).astype(BF)

    loads[2].wait()
    inward = LineScatter(part, sent2, from_left2, from_right2, t, nt, cuts, scatter_sem2)
    for cut in range(cuts):
        cols = inward.cols(cut)
        part[:, cols] = dot(dqkv[...], wqkv_v[cols, :], 1, 1)
        inward.edge(cut)

    def chunk_of(left, right):
        def chunk(d):
            return dot(left[:, pl.ds(pl.multiple_of(d * shard, shard), shard)], right[...], 0, 0)

        return chunk

    def store_qkv(at, value):
        d_qkv[at, :] = value

    def store_wo(at, value):
        d_wo[:, at] = value.T

    s_qkv = BlockScatter(
        chunk_of(na, dqkv), given_q, totals_q, landed_q, store_qkv, me, width,
        hs.at[0], hr.at[0], ps.at[0], pr.at[0],
    )
    s_out = BlockScatter(
        chunk_of(branch, mo), given_o, totals_o, landed_o, store_wo, me, width,
        hs.at[1], hr.at[1], ps.at[1], pr.at[1],
    )
    stages = s_qkv.stages

    def take(s):
        s.take()
        s.send(0)

    def on(s, stage):
        s.add(stage)
        if stage + 1 < stages:
            s.send(stage + 1)

    fills = [
        lambda: (take(s_qkv), s_out.give()),
        lambda: take(s_out),
        lambda: None,
    ]
    fills += [functools.partial(on, s, stage) for stage in range(stages) for s in (s_qkv, s_out)]
    s_qkv.give()
    for k in range(nt - 1):
        inward.round(k)
        if fills:
            fills.pop(0)()
    for fill in fills:
        fill()

    def store_raw(cols, value):
        gi[:, cols] = value

    inward.own(store_raw)
    gsum[...] = gparts[...]

    def store(cols, value):
        gi[:, cols] = gh[:, cols] + value

    def store_gain(cols, value):
        gsum[0:1, cols] = value

    back_through_norm(
        lambda c: x[:, c].astype(F32), lambda c: gi[:, c], gall, 0, store, store_gain
    )

    zslots[t] = gsum[...]

    def along(step):
        return remote(
            zslots.at[t], zslots.at[t], zsem.at[0, step], zsem.at[1, step],
            {"tensor": lax.rem(t + step, nt)},
        )

    for step in range(1, nt):
        along(step).start()
    for step in range(1, nt):
        slot = zslots.at[lax.rem(t + nt - step, nt)]
        remote(
            slot, slot, zsem.at[0, step], zsem.at[1, step], {"tensor": lax.rem(t + step, nt)}
        ).wait_recv()
    gsum[...] = sum(zslots[i] for i in range(nt))

    def across(mask):
        peer = flip(me, mask, width)
        return remote(
            gsum.at[:, pl.ds(pl.multiple_of(peer * shard, shard), shard)], dslots.at[me],
            dsem.at[0, mask], dsem.at[1, mask], {"dp": peer},
        )

    for mask in range(1, nd):
        across(mask).start()
    dslots[me] = gsum[:, pl.ds(pl.multiple_of(me * shard, shard), shard)]
    for mask in range(1, nd):
        peer = flip(me, mask, width)
        slot = dslots.at[peer]
        remote(slot, slot, dsem.at[0, mask], dsem.at[1, mask], {"dp": peer}).wait_recv()
    gain_out[...] = sum(dslots[i] for i in range(nd))

    for step in range(1, nt):
        along(step).wait_send()
    for mask in range(1, nd):
        across(mask).wait_send()
    for s in (s_qkv, s_out):
        s.given()
        s.drain()
    outward.finish()
    inward.finish()


def back(nt, nd, branch, na, mo, qo, kvo, lo, cos, sin, segc, segr, x, hid, gh, gparts, gall, act, wqkv_f, wo_f, down_f):
    width = nd.bit_length() - 1
    rows, model = hid.shape
    tokens, queries = qo.shape
    hidden = down_f.shape[0]
    wide = wqkv_f.shape[1]
    shard = model // nd
    half = nd // 2
    shape = jax.ShapeDtypeStruct
    outs = [
        shape((rows, model), BF),
        shape((rows, model), F32),
        shape((8, shard), F32),
        shape((shard, wide), F32),
        shape((queries, shard), F32),
    ]
    scratch = scatter_scratch(tokens, nt, model)
    cube = lambda size: [
        pltpu.VMEM((half, shard, size), BF),
        pltpu.VMEM((half, shard, size), BF),
        pltpu.VMEM((2, half - 1, shard // 2, size), BF),
    ]
    return pl.pallas_call(
        functools.partial(back_kernel, nt, width),
        out_shape=outs,
        in_specs=[vmem()] * 16 + [hbm()] * 3,
        out_specs=[vmem()] * len(outs),
        scratch_shapes=[
            pltpu.VMEM((model, wide), BF),
            pltpu.VMEM((queries, model), BF),
            pltpu.VMEM((hidden, model), BF),
        ]
        + scratch
        + scratch[1:]
        + [
            pltpu.VMEM((tokens, tokens), F32),
            pltpu.VMEM((2, tokens, LANES), BF),
            pltpu.VMEM((2, tokens, LANES), BF),
            pltpu.VMEM((tokens, queries), BF),
            pltpu.VMEM((tokens, wide), BF),
            pltpu.VMEM((2, tokens, LANES), F32),
            pltpu.VMEM((2, tokens, LANES), F32),
        ]
        + cube(wide)
        + cube(queries)
        + [
            pltpu.VMEM((8, model), F32),
            pltpu.VMEM((nt, 8, model), F32),
            pltpu.VMEM((nd, 8, shard), F32),
            dma(3),
            dma(4, nt, CUTS),
            dma(4, nt, CUTS),
            dma(2, nt),
            dma(2, nd),
            dma(2, 2, half),
            dma(2, 2, half),
            dma(2, half),
            dma(2, half),
        ],
        compiler_params=pltpu.CompilerParams(
            collective_id=2, has_side_effects=True, vmem_limit_bytes=VMEM_BYTES
        ),
        name="back",
    )(branch, na, mo, qo, kvo, lo, cos, sin, segc, segr, x, hid, gh, gparts, gall, act, wqkv_f, wo_f, down_f)


def narrow_scatter(value, axis, scatter_dimension, tiled):
    low = value.astype(BF) if value.ndim == 2 else value
    return lax.psum_scatter(low, axis, scatter_dimension=scatter_dimension, tiled=tiled).astype(F32)


def rope_tables(segments, head_dim):
    row_count = segments.shape[0]
    row_index = jnp.arange(row_count, dtype=jnp.int32)
    change = jnp.concatenate(
        [jnp.ones((1,), jnp.int32), (segments[1:] != segments[:-1]).astype(jnp.int32)]
    )
    starts = lax.cummax(jnp.where(change > 0, row_index, jnp.zeros_like(row_index)), axis=0)
    position = (row_index - starts).astype(F32)
    half_dim = head_dim // 2
    frequency = jnp.exp(jnp.arange(half_dim, dtype=F32) * (-math.log(10000.0) / half_dim))
    angles = position[:, None] * frequency[None, :]
    return (jnp.cos(angles)[:, None, :], jnp.sin(angles)[:, None, :])


def rotate(tensor, cosine, sine):
    half_dim = tensor.shape[-1] // 2
    first_half = tensor[..., :half_dim]
    second_half = tensor[..., half_dim:]
    return jnp.concatenate(
        [first_half * cosine - second_half * sine, second_half * cosine + first_half * sine],
        axis=-1,
    )


def unrotate(tensor, cosine, sine):
    half_dim = tensor.shape[-1] // 2
    first_half = tensor[..., :half_dim]
    second_half = tensor[..., half_dim:]
    return jnp.concatenate(
        [first_half * cosine + second_half * sine, second_half * cosine - first_half * sine],
        axis=-1,
    )


def visible(segments):
    row_index = jnp.arange(segments.shape[0], dtype=jnp.int32)
    same_seq = segments[:, None] == segments[None, :]
    return same_seq & (row_index[:, None] >= row_index[None, :])


def normalize(values, gain):
    inverse = lax.rsqrt(jnp.mean(values * values, axis=-1, keepdims=True) + EPSILON)
    unit_rows = values * inverse
    return (unit_rows, inverse, (unit_rows * gain.astype(F32)).astype(BF))


def normalize_back(grad_normed, unit_rows, inverse, gain):
    scaled = grad_normed * gain.astype(F32)
    grad_values = inverse * (
        scaled - unit_rows * jnp.mean(scaled * unit_rows, axis=-1, keepdims=True)
    )
    return (grad_values, jnp.sum(grad_normed * unit_rows, axis=0))


def contract(left, right, left_dim, right_dim):
    return lax.dot_general(
        left, right, (((left_dim,), (right_dim,)), ((), ())), preferred_element_type=F32
    )


def block_scores(query_block, key_heads, allowed_block, score_scale):
    scores = (
        jnp.einsum("rkgd,skd->kgrs", query_block, key_heads, preferred_element_type=F32)
        * score_scale
    )
    return jnp.where(allowed_block[None, None], scores, NEGATIVE)


def attend_forward(query_groups, key_heads, value_heads, allowed, score_scale):
    scores = block_scores(query_groups, key_heads, allowed, score_scale)
    row_max = jnp.max(scores, axis=-1, keepdims=True)
    log_total = row_max + jnp.log(jnp.sum(jnp.exp(scores - row_max), axis=-1, keepdims=True))
    probs_low = jnp.exp(scores - log_total).astype(BF)
    mixed_parts = jnp.einsum(
        "kgrs,skd->rkgd", probs_low, value_heads, preferred_element_type=F32
    ).astype(BF)
    return (mixed_parts, log_total)


def attend_backward(
    query_groups, key_heads, value_heads, mixed_heads, grad_mixed, log_totals, allowed, score_scale
):
    scores = block_scores(query_groups, key_heads, allowed, score_scale)
    attn_probs = jnp.exp(scores - log_totals)
    probs_low = attn_probs.astype(BF)
    grad_probs = jnp.einsum(
        "rkgd,skd->kgrs", grad_mixed, value_heads, preferred_element_type=F32
    )
    row_delta = jnp.sum(grad_mixed.astype(F32) * mixed_heads.astype(F32), axis=-1)
    row_delta = jnp.transpose(row_delta, (1, 2, 0))[..., None]
    grad_scores = (attn_probs * (grad_probs - row_delta)).astype(BF)
    query_parts = (
        jnp.einsum("kgrs,skd->rkgd", grad_scores, key_heads, preferred_element_type=F32)
        * score_scale
    )
    grad_key_rot = (
        jnp.einsum("kgrs,rkgd->skd", grad_scores, query_groups, preferred_element_type=F32)
        * score_scale
    )
    grad_value_heads = jnp.einsum(
        "kgrs,rkgd->skd", probs_low, grad_mixed, preferred_element_type=F32
    )
    return (query_parts, grad_key_rot, grad_value_heads)


def plain_device(
    layer_input,
    segment_ids,
    norm_attn,
    w_query,
    w_key,
    w_value,
    w_output,
    norm_ffn,
    w_gate,
    w_up,
    w_down,
    cotangent,
):
    score_scale = HD ** (-0.5)
    query_full, key_full, value_full, output_full, gain_attn = (
        lax.all_gather(w_query, "dp", axis=0, tiled=True),
        lax.all_gather(w_key, "dp", axis=0, tiled=True),
        lax.all_gather(w_value, "dp", axis=0, tiled=True),
        lax.all_gather(w_output, "dp", axis=1, tiled=True),
        lax.all_gather(norm_attn, "dp", axis=0, tiled=True),
    )
    gate_full, up_full, down_full, gain_ffn = (
        lax.all_gather(w_gate, "dp", axis=0, tiled=True),
        lax.all_gather(w_up, "dp", axis=0, tiled=True),
        lax.all_gather(w_down, "dp", axis=1, tiled=True),
        lax.all_gather(norm_ffn, "dp", axis=0, tiled=True),
    )
    heads_local = query_full.shape[1] // HD
    kv_local = key_full.shape[1] // HD
    group = heads_local // kv_local
    residual_in = layer_input.astype(F32)
    unit_attn, inverse_attn, normed_local = normalize(residual_in, gain_attn)
    normed_attn = lax.all_gather(normed_local, "tensor", axis=0, tiled=True)
    row_count = normed_attn.shape[0]
    cosine, sine = rope_tables(segment_ids, HD)
    allowed = visible(segment_ids)
    query_heads = rotate(
        jnp.dot(normed_attn, query_full, preferred_element_type=F32).reshape(
            row_count, heads_local, HD
        ),
        cosine,
        sine,
    ).astype(BF)
    query_groups = query_heads.reshape(row_count, kv_local, group, HD)
    key_heads = rotate(
        jnp.dot(normed_attn, key_full, preferred_element_type=F32).reshape(
            row_count, kv_local, HD
        ),
        cosine,
        sine,
    ).astype(BF)
    value_heads = (
        jnp.dot(normed_attn, value_full, preferred_element_type=F32)
        .astype(BF)
        .reshape(row_count, kv_local, HD)
    )
    mixed_heads, log_totals = attend_forward(
        query_groups, key_heads, value_heads, allowed, score_scale
    )
    mixed_flat = mixed_heads.reshape(row_count, heads_local * HD)
    hidden_res = residual_in + narrow_scatter(
        jnp.dot(mixed_flat, output_full, preferred_element_type=F32),
        "tensor",
        scatter_dimension=0,
        tiled=True,
    )
    unit_ffn, inverse_ffn, normed_ffn_local = normalize(hidden_res, gain_ffn)
    normed_ffn = lax.all_gather(normed_ffn_local, "tensor", axis=0, tiled=True)
    gate_rows = jnp.dot(normed_ffn, gate_full, preferred_element_type=F32)
    up_rows = jnp.dot(normed_ffn, up_full, preferred_element_type=F32)
    sigmoid_gate = jax.nn.sigmoid(gate_rows)
    active = (gate_rows * sigmoid_gate * up_rows).astype(BF)
    layer_output = (
        hidden_res
        + narrow_scatter(
            jnp.dot(active, down_full, preferred_element_type=F32).astype(BF),
            "tensor",
            scatter_dimension=0,
            tiled=True,
        ).astype(F32)
    ).astype(BF)
    query_full, key_full, value_full, output_full, gate_full, up_full, down_full = (
        lax.all_gather(w_query, "dp", axis=0, tiled=True),
        lax.all_gather(w_key, "dp", axis=0, tiled=True),
        lax.all_gather(w_value, "dp", axis=0, tiled=True),
        lax.all_gather(w_output, "dp", axis=1, tiled=True),
        lax.all_gather(w_gate, "dp", axis=0, tiled=True),
        lax.all_gather(w_up, "dp", axis=0, tiled=True),
        lax.all_gather(w_down, "dp", axis=1, tiled=True),
    )
    cotangent_full = lax.all_gather(cotangent, "tensor", axis=0, tiled=True)
    grad_active = contract(cotangent_full, down_full, 1, 1)
    grad_w_down = contract(active, cotangent_full, 0, 0)
    grad_up_rows = (grad_active * gate_rows * sigmoid_gate).astype(BF)
    grad_gate_rows = (
        grad_active * up_rows * sigmoid_gate * (1.0 + gate_rows * (1.0 - sigmoid_gate))
    ).astype(BF)
    grad_w_gate = contract(normed_ffn, grad_gate_rows, 0, 0)
    grad_w_up = contract(normed_ffn, grad_up_rows, 0, 0)
    grad_normed_ffn = narrow_scatter(
        contract(grad_gate_rows, gate_full, 1, 1) + contract(grad_up_rows, up_full, 1, 1),
        "tensor",
        scatter_dimension=0,
        tiled=True,
    )
    grad_hidden, gain_ffn_part = normalize_back(grad_normed_ffn, unit_ffn, inverse_ffn, gain_ffn)
    grad_hidden = cotangent.astype(F32) + grad_hidden
    branch_full = lax.all_gather(grad_hidden.astype(BF), "tensor", axis=0, tiled=True)
    grad_mixed = contract(branch_full, output_full, 1, 1).astype(BF)
    grad_w_output = contract(mixed_flat, branch_full, 0, 0)
    grad_query_rot, grad_key_rot, grad_value_heads = attend_backward(
        query_groups,
        key_heads,
        value_heads,
        mixed_heads,
        grad_mixed.reshape(row_count, kv_local, group, HD),
        log_totals,
        allowed,
        score_scale,
    )
    grad_queries = (
        unrotate(grad_query_rot.reshape(row_count, heads_local, HD), cosine, sine)
        .reshape(row_count, heads_local * HD)
        .astype(BF)
    )
    grad_keys = (
        unrotate(grad_key_rot, cosine, sine).reshape(row_count, kv_local * HD).astype(BF)
    )
    grad_values = grad_value_heads.reshape(row_count, kv_local * HD).astype(BF)
    grad_w_query = contract(normed_attn, grad_queries, 0, 0)
    grad_w_key = contract(normed_attn, grad_keys, 0, 0)
    grad_w_value = contract(normed_attn, grad_values, 0, 0)
    grad_normed_attn = narrow_scatter(
        contract(grad_queries, query_full, 1, 1)
        + contract(grad_keys, key_full, 1, 1)
        + contract(grad_values, value_full, 1, 1),
        "tensor",
        scatter_dimension=0,
        tiled=True,
    )
    grad_residual, gain_attn_part = normalize_back(
        grad_normed_attn, unit_attn, inverse_attn, gain_attn
    )
    grad_input = grad_hidden + grad_residual
    gain_attn_total, gain_ffn_total = lax.psum((gain_attn_part, gain_ffn_part), "tensor")
    owned = (
        narrow_scatter(grad_w_query, "dp", scatter_dimension=0, tiled=True),
        narrow_scatter(grad_w_key, "dp", scatter_dimension=0, tiled=True),
        narrow_scatter(grad_w_value, "dp", scatter_dimension=0, tiled=True),
        narrow_scatter(grad_w_output, "dp", scatter_dimension=1, tiled=True),
        narrow_scatter(gain_attn_total, "dp", scatter_dimension=0, tiled=True),
        narrow_scatter(gain_ffn_total, "dp", scatter_dimension=0, tiled=True),
        narrow_scatter(grad_w_gate, "dp", scatter_dimension=0, tiled=True),
        narrow_scatter(grad_w_up, "dp", scatter_dimension=0, tiled=True),
        narrow_scatter(grad_w_down, "dp", scatter_dimension=1, tiled=True),
    )
    return (
        layer_output,
        grad_input,
        owned[4],
        owned[0],
        owned[1],
        owned[2],
        owned[3],
        owned[5],
        owned[6],
        owned[7],
        owned[8],
    )


def with_kernels(nt, nd, layer_input, segment_ids, norm_attn, w_query, w_key, w_value, w_output, norm_ffn, w_gate, w_up, w_down, cotangent):
    gain = jnp.pad(jnp.stack([norm_attn, norm_ffn]).astype(F32), ((0, 6), (0, 0)))
    wqkv = jnp.concatenate([w_query, w_key, w_value], axis=1)
    segc, segr = segment_ids[:, None], segment_ids[None, :]
    (wqkv_f, wo_f, gate_f, up_f, down_f, na, cf, nf, qo, kvo, mo, lo, hid, gall, cos, sin) = front(
        nt, nd, layer_input, cotangent, gain, segc, segr, wqkv, w_output, w_gate, w_up, w_down
    )
    act, branch, gh, gparts, d_gate, d_up, d_down = ffn(
        nt, nd, nf, cf, hid, cotangent, gall, gate_f, up_f, down_f
    )
    y, gi, gains, d_qkv, d_wo = back(
        nt, nd, branch, na, mo, qo, kvo, lo, cos, sin, segc, segr, layer_input, hid, gh, gparts,
        gall, act, wqkv_f, wo_f, down_f,
    )
    q, k = w_query.shape[1], w_query.shape[1] + w_key.shape[1]
    return (
        y, gi, gains[0], d_qkv[:, :q], d_qkv[:, q:k], d_qkv[:, k:], d_wo, gains[1], d_gate, d_up, d_down
    )


def fits(nt, nd, shards):
    layer_input, segment_ids, norm_attn, w_query, w_key, w_value, w_output, norm_ffn, w_gate, w_up, w_down, _ = shards
    return (
        nd >= 4
        and nd & (nd - 1) == 0
        and nt >= 2
        and norm_attn.shape[0] % LANES == 0
        and w_output.shape[1] % LANES == 0
        and w_gate.shape[1] % LANES == 0
        and w_query.shape[1] % LANES == 0
        and w_key.shape[1] == HD
        and segment_ids.shape[0] == nt * layer_input.shape[0]
        and segment_ids.shape[0] % LANES == 0
    )


def on_device(nt, nd, *shards):
    if fits(nt, nd, shards):
        return with_kernels(nt, nd, *shards)
    return plain_device(*shards)


def solution(mesh):
    placed = (
        P(("dp", "tensor"), None),
        P("dp"),
        P("dp"),
        P("dp", "tensor"),
        P("dp", "tensor"),
        P("dp", "tensor"),
        P("tensor", "dp"),
        P("dp"),
        P("dp", "tensor"),
        P("dp", "tensor"),
        P("tensor", "dp"),
        P(("dp", "tensor"), None),
    )
    return jax.shard_map(
        functools.partial(on_device, mesh.shape["tensor"], mesh.shape["dp"]),
        mesh=mesh,
        in_specs=placed,
        out_specs=(
            P(("dp", "tensor"), None),
            P(("dp", "tensor"), None),
            P("dp"),
            P("dp", "tensor"),
            P("dp", "tensor"),
            P("dp", "tensor"),
            P("tensor", "dp"),
            P("dp"),
            P("dp", "tensor"),
            P("dp", "tensor"),
            P("tensor", "dp"),
        ),
        check_vma=False,
    )
```

```python
import functools
import math

import jax
import jax.numpy as jnp
from jax import lax
from jax.experimental import pallas as pl
from jax.experimental.pallas import tpu as pltpu
from jax.sharding import PartitionSpec as P

HD = 64
EPSILON = 1e-05
NEGATIVE = -1e30
LANES = 128
BF = jnp.bfloat16
F32 = jnp.float32
VMEM_BYTES = 66_000_000


def spans(bits):
    masks = [0]
    for bit in bits:
        masks = masks + [mask | (1 << bit) for mask in masks]
    return masks


def flip(index, mask, width):
    total = 0
    for bit in range(width):
        own = lax.rem(lax.div(index, 1 << bit), 2)
        if isinstance(mask, int):
            other = (mask >> bit) & 1
        else:
            other = lax.rem(lax.div(mask, 1 << bit), 2)
        total = total + lax.rem(own + other, 2) * (1 << bit)
    return total


def aligned(value, step):
    return value if isinstance(value, int) else pl.multiple_of(value, step)


def remote(src, dst, send_sem, recv_sem, device):
    return pltpu.make_async_remote_copy(
        src_ref=src,
        dst_ref=dst,
        send_sem=send_sem,
        recv_sem=recv_sem,
        device_id=device,
        device_id_type=pl.DeviceIdType.MESH,
    )


def dot(left, right, left_dim=1, right_dim=0):
    return lax.dot_general(
        left, right, (((left_dim,), (right_dim,)), ((), ())), preferred_element_type=F32
    )


def tiles_of(size, most):
    units = size // LANES
    parts = -(-units // most)
    cuts, start = [], 0
    for part in range(parts):
        width = (units // parts + (1 if part < units % parts else 0)) * LANES
        cuts.append((start, width))
        start += width
    return cuts


def enter(t, nt, me, width, barrier, everyone_along_tensor=False):
    signal = functools.partial(
        pl.semaphore_signal, barrier, inc=1, device_id_type=pl.DeviceIdType.MESH
    )
    for mask in range(1, 1 << width):
        signal(device_id={"dp": flip(me, mask, width)})
    if everyone_along_tensor:
        for step in range(1, nt):
            signal(device_id={"tensor": lax.rem(t + step, nt)})
        pl.semaphore_wait(barrier, (1 << width) - 1 + nt - 1)
        return

    @pl.when(t > 0)
    def _():
        signal(device_id={"tensor": t - 1})

    @pl.when(t < nt - 1)
    def _():
        signal(device_id={"tensor": t + 1})

    neighbours = lax.min(t, 1) + lax.min(nt - 1 - t, 1)
    pl.semaphore_wait(barrier, (1 << width) - 1 + neighbours)


class LineGather:
    def __init__(self, full, row, size, t, nt, sems):
        self.full, self.row, self.size = full, row, size
        self.t, self.nt, self.sems = t, nt, sems
        self.pieces = sems.shape[2]

    def window(self, j, s):
        return self.full.at[pl.ds(aligned(self.row(j, s), self.size), self.size), :]

    def right(self, j, s):
        at = self.window(j, s)
        return remote(
            at, at, self.sems.at[0, j, s], self.sems.at[2, j, s],
            {"tensor": lax.rem(self.t + 1, self.nt)},
        )

    def left(self, j, s):
        at = self.window(j, s)
        return remote(
            at, at, self.sems.at[1, j, s], self.sems.at[3, j, s],
            {"tensor": lax.rem(self.t + self.nt - 1, self.nt)},
        )

    def start(self, s):
        @pl.when(self.t < self.nt - 1)
        def _():
            self.right(self.t, s).start()

        @pl.when(self.t > 0)
        def _():
            self.left(self.t, s).start()

    def step(self, k, s):
        t, nt = self.t, self.nt

        @pl.when(t >= k)
        def _():
            self.right(t - k, s).wait_recv()

            @pl.when(t < nt - 1)
            def _():
                self.right(t - k, s).start()

        @pl.when(t + k < nt)
        def _():
            self.left(t + k, s).wait_recv()

            @pl.when(t > 0)
            def _():
                self.left(t + k, s).start()

    def finish(self):
        t, nt = self.t, self.nt

        @pl.loop(0, nt)
        def _(k):
            for s in range(self.pieces):
                @pl.when((t >= k) & (t < nt - 1))
                def _():
                    self.right(t - k, s).wait_send()

                @pl.when((t + k < nt) & (t > 0))
                def _():
                    self.left(t + k, s).wait_send()


class LineScatter:
    def __init__(self, part, row, sent, arrived, t, nt, sems):
        self.part, self.row, self.sent, self.arrived = part, row, sent, arrived
        self.t, self.nt, self.sems = t, nt, sems
        self.pieces = sems.shape[3]
        self.size = sent.shape[1] // self.pieces
        self.model = sent.shape[2]
        self.near = lax.div(2 * t, nt)
        self.far = 1 - self.near

    def sub(self, s):
        return pl.ds(s * self.size, self.size)

    def depth(self, way):
        return (1 - way) * self.t + way * (self.nt - 1 - self.t)

    def goal(self, way, i):
        return (1 - way) * (self.nt - 1 - i) + way * i

    def move(self, way, j, s):
        return remote(
            self.sent.at[j, self.sub(s), :], self.arrived.at[way, j, self.sub(s), :],
            self.sems.at[0, way, j, s], self.sems.at[1, way, j, s],
            {"tensor": lax.rem(self.t + self.nt + 1 - 2 * way, self.nt)},
        )

    def rows(self, j, s):
        return pl.ds(aligned(self.row(j, s), self.size), self.size)

    def mine(self, j, s):
        return self.part[self.rows(j, s), : self.model]

    def edge(self, s):
        t, nt = self.t, self.nt

        @pl.when((t == 0) | (t == nt - 1))
        def _():
            way = lax.div(t, nt - 1)

            @pl.loop(0, nt - 1)
            def _(i):
                j = self.goal(way, i)
                self.sent[j, self.sub(s), :] = self.mine(j, s).astype(BF)
                self.move(way, j, s).start()

    def relay(self, way, s):
        depth = self.depth(way)

        @pl.when(depth > 0)
        def _():
            @pl.loop(0, self.nt - 1 - depth)
            def _(i):
                j = self.goal(way, i)
                self.move(way, j, s).wait_recv()
                total = self.mine(j, s) + self.arrived[way, j, self.sub(s), :].astype(F32)
                self.sent[j, self.sub(s), :] = total.astype(BF)
                self.move(way, j, s).start()

    def own(self, s):
        t = self.t
        rows = self.rows(t, s)
        for way in (self.near, self.far):
            @pl.when(self.depth(way) > 0)
            def _():
                self.move(way, t, s).wait_recv()
                self.part[rows, : self.model] += self.arrived[way, t, self.sub(s), :].astype(F32)

        return rows

    def finish(self):
        for way in range(2):
            @pl.loop(0, self.nt - 1 - self.depth(way))
            def _(i):
                for s in range(self.pieces):
                    self.move(way, self.goal(way, i), s).wait_send()


class Cube:
    def setup(self, me, width, half_send, half_recv, pair_send, pair_recv):
        self.me, self.width = me, width
        self.hs, self.hr, self.ps, self.pr = half_send, half_recv, pair_send, pair_recv
        self.bits = list(range(1, width))
        self.orders = (self.bits, self.bits[::-1])
        self.masks = spans(self.bits)
        self.stages = len(self.bits)

    def at(self, mask):
        return flip(self.me, mask, self.width)


class BlockGather(Cube):
    def __init__(self, own, full, by_rows, me, width, *sems):
        self.setup(me, width, *sems)
        self.own_ref, self.full, self.by_rows = own, full, by_rows

    def half(self, h):
        rows = self.own_ref.shape[0] // 2
        return self.own_ref.at[pl.ds(h * rows, rows), :]

    def window(self, who, h=None):
        rows, cols = self.own_ref.shape
        take, start = (rows, 0) if h is None else (rows // 2, h * (rows // 2))
        if self.by_rows:
            return self.full.at[pl.ds(aligned(who * rows + start, take), take), :]
        return self.full.at[pl.ds(start, take), pl.ds(aligned(who * cols, cols), cols)]

    def hop(self, stage, h, m):
        order = self.orders[h]
        bit = 1 << order[stage]
        slot = (m | bit) >> 1
        src = self.half(h) if m == 0 else self.window(self.at(m), h)
        return remote(
            src, self.window(self.at(m), h), self.hs.at[h, slot], self.hr.at[h, slot],
            {"dp": self.at(bit)},
        )

    def send(self, stage):
        for h in range(2):
            for m in spans(self.orders[h][:stage]):
                self.hop(stage, h, m).start()

    def wait(self, stage):
        for h in range(2):
            bit = 1 << self.orders[h][stage]
            for m in spans(self.orders[h][:stage]):
                slot = (m | bit) >> 1
                landed = self.window(self.at(m | bit), h)
                remote(
                    landed, landed, self.hs.at[h, slot], self.hr.at[h, slot], {"dp": self.at(bit)}
                ).wait_recv()

    def pair(self, m):
        src = self.own_ref if m == 0 else self.window(self.at(m))
        return remote(
            src, self.window(self.at(m)), self.ps.at[m >> 1], self.pr.at[m >> 1],
            {"dp": self.at(1)},
        )

    def pair_send(self):
        for m in self.masks:
            self.pair(m).start()

    def pair_wait(self):
        for m in self.masks:
            landed = self.window(self.at(m | 1))
            remote(
                landed, landed, self.ps.at[m >> 1], self.pr.at[m >> 1], {"dp": self.at(1)}
            ).wait_recv()

    def place(self, sem):
        return pltpu.make_async_copy(self.own_ref, self.window(self.me), sem)

    def drain(self):
        for stage in range(self.stages):
            for h in range(2):
                for m in spans(self.orders[h][:stage]):
                    self.hop(stage, h, m).wait_send()
        for m in self.masks:
            self.pair(m).wait_send()


class BlockScatter(Cube):
    def __init__(self, chunk, out_sent, total, landed, store, me, width, *sems):
        self.setup(me, width, *sems)
        self.chunk, self.sent, self.total, self.landed = chunk, out_sent, total, landed
        self.store = store
        self.slots = 1 << (width - 1)

    def pair(self, slot):
        return remote(
            self.sent.at[slot], self.total.at[slot], self.ps.at[slot], self.pr.at[slot],
            {"dp": self.at(1)},
        )

    def give(self):
        @pl.loop(0, self.slots)
        def _(k):
            slot = self.slots - 1 - k
            self.sent[slot] = self.chunk(self.at(2 * slot + 1)).astype(BF)
            self.pair(slot).start()

    def given(self):
        @pl.loop(0, self.slots)
        def _(slot):
            self.pair(slot).wait_send()

    def take(self):
        @pl.loop(0, self.slots)
        def _(k):
            slot = self.slots - 1 - k
            term = self.chunk(self.at(2 * slot))
            self.pair(slot).wait_recv()
            self.total[slot] = (term + self.total[slot].astype(F32)).astype(BF)

    def moves(self, stage):
        for h in range(2):
            order = self.orders[h]
            last = self.stages - 1 - stage
            bit = 1 << order[last]
            for m in spans(order[:last]):
                yield h, bit, m | bit

    def hop(self, h, bit, m):
        rows = self.total.shape[1] // 2
        return remote(
            self.total.at[m >> 1, pl.ds(h * rows, rows), :], self.landed.at[h, (m >> 1) - 1],
            self.hs.at[h, m >> 1], self.hr.at[h, m >> 1], {"dp": self.at(bit)},
        )

    def send(self, stage):
        for h, bit, m in self.moves(stage):
            self.hop(h, bit, m).start()

    def add(self, stage):
        rows = self.total.shape[1] // 2
        for h, bit, m in self.moves(stage):
            self.hop(h, bit, m).wait_recv()
            keep = (m ^ bit) >> 1
            at = slice(h * rows, (h + 1) * rows)
            total = self.total[keep, at, :].astype(F32) + self.landed[h, (m >> 1) - 1].astype(F32)
            if stage == self.stages - 1:
                self.store(at, total)
            else:
                self.total[keep, at, :] = total.astype(BF)

    def drain(self):
        for stage in range(self.stages):
            for h, bit, m in self.moves(stage):
                self.hop(h, bit, m).wait_send()


def inverse_of(rows):
    return lax.rsqrt(jnp.mean(rows * rows, axis=-1, keepdims=True) + EPSILON)


def times_gain(unit, gains, which, store):
    parts, _, width = gains.shape
    for d in range(parts):
        cols = slice(d * width, (d + 1) * width)
        store(cols, unit[:, cols] * gains[d, which : which + 1, :])


def lane_index(shape):
    return lax.broadcasted_iota(jnp.int32, shape, len(shape) - 1)


def column_of(segr):
    rows = segr.shape[1]
    wide = jnp.broadcast_to(segr[...].astype(F32), (8, rows))
    return jnp.transpose(wide)[:, 0:1]


def rope_into(cos_ref, sin_ref, segr):
    rows = segr.shape[1]
    before = (segr[...].astype(F32) < column_of(segr)).astype(F32)
    start = jnp.sum(before, axis=1, keepdims=True)
    position = lax.broadcasted_iota(jnp.int32, (rows, 1), 0).astype(F32) - start
    lane = lane_index((rows, LANES))
    half = HD // 2
    frequency = jnp.exp(lax.rem(lane, half).astype(F32) * (-math.log(10000.0) / half))
    angle = position * frequency
    cos_ref[...] = jnp.cos(angle)
    sine = jnp.sin(angle)
    sin_ref[...] = jnp.where(lax.rem(lane, HD) < half, -sine, sine)


def swapped(x):
    lane = lane_index(x.shape)
    half = HD // 2
    return jnp.where(
        lax.rem(lane, HD) < half,
        pltpu.roll(x, LANES - half, 1),
        pltpu.roll(x, half, 1),
    )


def bias_into(bias, segr):
    rows = segr.shape[1]
    query = lax.broadcasted_iota(jnp.int32, (rows, rows), 0)
    key = lax.broadcasted_iota(jnp.int32, (rows, rows), 1)
    seen = (segr[...].astype(F32) == column_of(segr)) & (query >= key)
    bias[...] = jnp.where(seen, 0.0, NEGATIVE)


def pad_pair(keys_values, keys, values):
    low = lane_index(keys_values.shape) < HD
    key = jnp.where(low, keys_values, 0.0)
    value = jnp.where(low, 0.0, keys_values)
    keys[0] = key.astype(BF)
    keys[1] = pltpu.roll(key, HD, 1).astype(BF)
    values[0] = pltpu.roll(value, HD, 1).astype(BF)
    values[1] = value.astype(BF)


def query_cuts(rows):
    block = 256 if rows % 256 == 0 else rows
    return [(start, block, start + block) for start in range(0, rows, block)]


def attend_pairs(first, last, qo, kpad, vpad, bias, mo, lo):
    rows = qo.shape[0]
    lane = lane_index((1, LANES))

    @pl.loop(first, last)
    def _(pair):
        lanes = pl.ds(pl.multiple_of(pair * LANES, LANES), LANES)
        for start, block, seen in query_cuts(rows):
            at = slice(start, start + block)
            query = qo[at, lanes]
            mixed = jnp.zeros((block, LANES), F32)
            logs = lo[at, :]
            for side in range(2):
                scores = dot(query, kpad[side, :seen, :], 1, 1) + bias[at, :seen]
                top = jnp.max(scores, axis=-1, keepdims=True)
                probs = jnp.exp(scores - top)
                total = jnp.sum(probs, axis=-1, keepdims=True)
                mixed = mixed + dot(probs.astype(BF), vpad[side, :seen, :]) / total
                logs = jnp.where(lane == 2 * pair + side, top + jnp.log(total), logs)
            lo[at, :] = logs
            mo[at, lanes] = mixed.astype(BF)


def back_through_norm(raw, grads, gains, which, store, store_gain):
    parts, _, width = gains.shape
    cuts = [slice(d * width, (d + 1) * width) for d in range(parts)]
    model = parts * width
    square = sum(jnp.sum(raw(c) * raw(c), axis=-1, keepdims=True) for c in cuts)
    inverse = lax.rsqrt(square / model + EPSILON)
    mean = 0.0
    for d, c in enumerate(cuts):
        unit = raw(c) * inverse
        grad = grads(c)
        store_gain(c, jnp.sum(grad * unit, axis=0, keepdims=True))
        mean = mean + jnp.sum(grad * gains[d, which : which + 1, :] * unit, axis=-1, keepdims=True)
    mean = mean / model
    for d, c in enumerate(cuts):
        unit = raw(c) * inverse
        store(c, inverse * (grads(c) * gains[d, which : which + 1, :] - unit * mean))


PIECES = 4


def vmem():
    return pl.BlockSpec(memory_space=pltpu.VMEM)


def hbm():
    return pl.BlockSpec(memory_space=pl.ANY)


def dma(*shape):
    return pltpu.SemaphoreType.DMA(shape)


def line_scratch(nt, rows, model):
    return [pltpu.VMEM((nt, rows, model), BF), pltpu.VMEM((2, nt, rows, model), BF)]


def ticks(pieces, nt):
    return [
        [(k, tick - k) for k in range(1, nt) if 0 <= tick - k < pieces]
        for tick in range(pieces + nt - 1)
    ]


def fore_kernel(
    nt, width,
    x, cot, gain_a, gain_f, segr, wq, wkt, wvt, wo, gate, up, down,
    wqkv_f, wo_f, na_o, cf, qo, kvo, mo, lo, gall, cos, sin, act, branch, gh, gains, y, d_gate, d_up,
    rowsbuf, hid, gate_v, up_v, down_v, part, sent, arrived, totals, landed, own_qkv, gain,
    gain_sem, place_sem, out_sem, x_sem, cot_sem, nf_sem, br_sem, o_sem, gn_sem, y_sem, hs, hr, ps, pr,
):
    me, t = lax.axis_index("dp"), lax.axis_index("tensor")
    nd = 1 << width
    rows, model = x.shape
    tokens = nt * rows
    queries = wq.shape[1]
    hidden = gate.shape[1]
    shard = model >> width
    wide = own_qkv.shape[1]
    pieces = PIECES
    size = rows // pieces

    def natural(j, s):
        return j * rows + s * size

    def shuffled(j, s):
        return (s * nt + j) * size

    local = pl.ds(pl.multiple_of(t * rows, rows), rows)
    rowsbuf[local, :] = x[...]
    gain[...] = jnp.zeros_like(gain)
    gain[0:1, :] = gain_a[...].astype(F32)
    gain[1:2, :] = gain_f[...].astype(F32)
    own_qkv[:, :queries] = wq[...]
    turned = jnp.concatenate([wkt[...].astype(F32), wvt[...].astype(F32)], axis=0)
    own_qkv[:, queries:] = jnp.transpose(turned).astype(BF)
    with jax.named_scope("enter"):
        enter(t, nt, me, width, pltpu.get_barrier_semaphore())

    tokens_x = LineGather(rowsbuf, natural, size, t, nt, x_sem)
    for s in range(pieces):
        tokens_x.start(s)
    gathers = []
    for w, (own, full, by_rows) in enumerate(
        ((own_qkv, wqkv_f, True), (wo, wo_f, False), (gate, gate_v, True), (up, up_v, True), (down, down_v, False))
    ):
        gathers.append(
            BlockGather(own, full, by_rows, me, width, hs.at[w], hr.at[w], ps.at[w], pr.at[w])
        )
    g_qkv, g_out, g_gate, g_up, g_down = gathers
    stages = g_qkv.stages

    def gain_copy(mask):
        return remote(
            gain, gall.at[me], gain_sem.at[0, mask], gain_sem.at[1, mask],
            {"dp": flip(me, mask, width)},
        )

    for mask in range(1, nd):
        gain_copy(mask).start()
    for g in (g_qkv, g_out, g_gate):
        g.send(0)
    for w, g in enumerate(gathers):
        g.place(place_sem.at[w]).start()
    gall[me] = gain[...]

    def forward(g, stage):
        g.wait(stage)
        if stage + 1 < stages:
            g.send(stage + 1)
        else:
            g.pair_send()

    for s in range(pieces):
        cf[pl.ds(pl.multiple_of(shuffled(t, s), size), size), :] = cot[s * size : (s + 1) * size, :]
    cots = LineGather(cf, shuffled, size, t, nt, cot_sem)
    scatter_o = LineScatter(part, natural, sent, arrived, t, nt, o_sem)

    def attention(na, wqkv_v, wo_v, bias, kpad, vpad):
        bias_into(bias, segr)
        rope_into(cos, sin, segr)
        lo[...] = jnp.zeros_like(lo)
        for mask in range(1, nd):
            slot = gall.at[flip(me, mask, width)]
            remote(
                slot, slot, gain_sem.at[0, mask], gain_sem.at[1, mask],
                {"dp": flip(me, mask, width)},
            ).wait_recv()

        def norm(j):
            @pl.loop(0, pieces)
            def _(s):
                these = pl.ds(pl.multiple_of(j * rows + s * size, size), size)
                value = rowsbuf[these, :].astype(F32)

                def store(cols, normed):
                    na[these, cols] = normed.astype(BF)

                times_gain(value * inverse_of(value), gall, 0, store)

        norm(t)
        for stage in range(stages - 1):
            forward(g_qkv, stage)
            forward(g_out, stage)
        fills = [
            lambda: (forward(g_gate, 0), g_up.send(0)),
            lambda: (forward(g_qkv, stages - 1), forward(g_out, stages - 1), g_down.send(0)),
        ]
        load = pltpu.make_async_copy(wqkv_f, wqkv_v, place_sem.at[5])
        load_out = pltpu.make_async_copy(wo_f, wo_v, place_sem.at[6])

        def fetch():
            g_qkv.place(place_sem.at[0]).wait()
            g_qkv.pair_wait()
            load.start()
            g_out.place(place_sem.at[1]).wait()
            g_out.pair_wait()
            load_out.start()

        for k in range(1, nt):
            if k == nt - 1:
                for fill in fills:
                    fill()
                fills = []
                with jax.named_scope("fetch"):
                    fetch()
            with jax.named_scope("x_step"):
                for s in range(pieces):
                    tokens_x.step(k, s)
            if k == nt - 1:
                for s in range(pieces):
                    cots.start(s)

            @pl.when(t >= k)
            def _():
                norm(t - k)

            @pl.when(t + k < nt)
            def _():
                norm(t + k)

            if fills:
                with jax.named_scope("x_fill"):
                    fills.pop(0)()
        keep = pltpu.make_async_copy(na, na_o, out_sem.at[0])
        keep.start()
        with jax.named_scope("wait_qkv"):
            load.wait()
        with jax.named_scope("qkv"):
            part[:, :wide] = dot(na[...], wqkv_v[...])
            c, s_ = cos[...], sin[...]
            for start in range(0, queries, LANES):
                lanes = slice(start, start + LANES)
                value = part[:, lanes]
                qo[:, lanes] = ((value * c + swapped(value) * s_) * HD ** (-0.5)).astype(BF)
            value = part[:, queries : queries + LANES]
            keyed = jnp.where(lane_index(value.shape) < HD, value * c + swapped(value) * s_, value)
            kvo[...] = keyed.astype(BF)
            pad_pair(keyed, kpad, vpad)
        pairs = queries // LANES
        with jax.named_scope("g1"):
            for stage in range(1, stages):
                forward(g_gate, stage)
        with jax.named_scope("att"):
            attend_pairs(0, pairs, qo, kpad, vpad, bias, mo, lo)
        load_out.wait()
        with jax.named_scope("outproj"):
            for start, width_ in tiles_of(model, 4):
                cols = slice(start, start + width_)
                part[:, cols] = dot(mo[...], wo_v[:, cols])
        keep.wait()
        tokens_x.finish()

    pl.run_scoped(
        attention,
        pltpu.VMEM((tokens, model), BF),
        pltpu.VMEM((model, wide), BF),
        pltpu.VMEM((queries, model), BF),
        pltpu.VMEM((tokens, tokens), F32),
        pltpu.VMEM((2, tokens, LANES), BF),
        pltpu.VMEM((2, tokens, LANES), BF),
    )

    gather_nf = LineGather(rowsbuf, shuffled, size, t, nt, nf_sem)

    def take_hidden(s):
        at = scatter_o.own(s)
        block = slice(s * size, (s + 1) * size)
        hidden_rows = x[block, :].astype(F32) + part[at, :model]
        hid[block, :] = hidden_rows
        there = pl.ds(pl.multiple_of(shuffled(t, s), size), size)

        def store(cols, normed):
            rowsbuf[there, cols] = normed.astype(BF)

        times_gain(hidden_rows * inverse_of(hidden_rows), gall, 1, store)
        gather_nf.start(s)

    scatter_o.edge(0)
    scatter_o.edge(1)
    with jax.named_scope("cot1"):
        for s in range(pieces):
            cots.step(1, s)
    with jax.named_scope("u0"):
        forward(g_up, 0)
    later = [
        lambda: ([cots.step(2, s) for s in range(pieces)], forward(g_down, 0)),
        lambda: [cots.step(k, s) for k in range(3, nt) for s in range(pieces)],
        lambda: [forward(g_up, stage) for stage in range(1, stages)],
        lambda: [forward(g_down, stage) for stage in range(1, stages)],
    ]
    steps = ticks(pieces, nt)

    def flow(tick, scatter, gather, take):
        todo = list(steps[tick])
        if 0 < tick < pieces - 1:
            scatter.edge(tick + 1)
        scatter.relay(scatter.near, tick)
        if todo:
            gather.step(*todo.pop(0))
        scatter.relay(scatter.far, tick)
        if todo:
            gather.step(*todo.pop(0))
        take(tick)
        for late in todo:
            gather.step(*late)

    for tick in range(pieces):
        with jax.named_scope("o_tick"):
            flow(tick, scatter_o, gather_nf, take_hidden)
        if later:
            with jax.named_scope("o_later"):
                later.pop(0)()
    for fill in later:
        fill()

    def feed(dg, du, given):
        cuts = tiles_of(hidden, 6)
        span = max(width_ for _, width_ in cuts)
        half = tokens // 2
        block = 64
        draft = half

        def tile(h, i):
            start, width_ = cuts[i]
            at = slice(start, start + width_)
            mine = slice(h * half, (h + 1) * half)
            held = slice(draft, draft + half)
            part[held, 0:width_] = dot(rowsbuf[mine, :], gate_v[:, at])
            part[held, span : span + width_] = dot(rowsbuf[mine, :], up_v[:, at])
            part[held, 2 * span : 2 * span + width_] = dot(cf[mine, :], down_v[at, :], 1, 1)

            @pl.loop(0, half // block)
            def _(k):
                from_ = pl.ds(pl.multiple_of(draft + k * block, block), block)
                to = pl.ds(pl.multiple_of(h * half + k * block, block), block)
                g = part[from_, 0:width_]
                u = part[from_, span : span + width_]
                ga = part[from_, 2 * span : 2 * span + width_]
                sig = 1.0 / (1.0 + jnp.exp(-g))
                gs = g * sig
                act[to, at] = (gs * u).astype(BF)
                du[to, at] = (ga * gs).astype(BF)
                dg[to, at] = (ga * u * sig * (1.0 + g * (1.0 - sig))).astype(BF)

        def back_dots(h):
            mine = slice(h * half, (h + 1) * half)
            for start, width_ in tiles_of(model, 4):
                cols = slice(start, start + width_)
                part[mine, cols] = dot(dg[mine, :], gate_v[cols, :], 1, 1) + dot(
                    du[mine, :], up_v[cols, :], 1, 1
                )

        scatter_gn = LineScatter(part, shuffled, sent, arrived, t, nt, gn_sem)
        gather_br = LineGather(branch, natural, size, t, nt, br_sem)
        gains[...] = jnp.zeros_like(gains)

        def take_grad(s):
            at = scatter_gn.own(s)
            block_ = slice(s * size, (s + 1) * size)
            there = pl.ds(pl.multiple_of(natural(t, s), size), size)

            def store(cols, value):
                total = cot[block_, cols].astype(F32) + value
                gh[block_, cols] = total
                branch[there, cols] = total.astype(BF)

            def store_gain(cols, value):
                gains[1:2, cols] += value

            back_through_norm(
                lambda c: hid[block_, c], lambda c: part[at, c], gall, 1, store, store_gain
            )
            gather_br.start(s)

        def chunk_of(left, right):
            def chunk(d):
                return dot(left[:, pl.ds(pl.multiple_of(d * shard, shard), shard)], right[...], 0, 0)

            return chunk

        def keep(place):
            def store(at, value):
                part[place + at.start : place + at.stop, :hidden] = value

            return store

        s_gate, s_up = [
            BlockScatter(
                chunk_of(rowsbuf, grad), given, totals.at[w], landed.at[w], keep(w * shard), me, width,
                hs.at[5 + w], hr.at[5 + w], ps.at[5 + w], pr.at[5 + w],
            )
            for w, grad in enumerate((dg, du))
        ]

        def take(s):
            s.take()
            s.send(0)

        with jax.named_scope("wait_ffn"):
            for w in (2, 3, 4):
                gathers[w].place(place_sem.at[w]).wait()
                gathers[w].pair_wait()
        work = [lambda i=i: tile(0, i) for i in range(len(cuts))]
        for late in steps[pieces:]:
            with jax.named_scope("nf_step"):
                for k, s in late:
                    gather_nf.step(k, s)
            if work:
                with jax.named_scope("tile"):
                    work.pop(0)()
        for job in work:
            job()
        scatter_o.finish()
        with jax.named_scope("back_dots"):
            back_dots(0)
        scatter_gn.edge(0)
        scatter_gn.edge(1)
        with jax.named_scope("tile"):
            tile(1, 0)
        with jax.named_scope("gn_round"):
            scatter_gn.relay(scatter_gn.near, 0)
        with jax.named_scope("tile"):
            for i in range(1, len(cuts)):
                tile(1, i)
        with jax.named_scope("gn_round"):
            scatter_gn.relay(scatter_gn.far, 0)
        with jax.named_scope("back_dots"):
            back_dots(1)
        with jax.named_scope("gn_take"):
            take_grad(0)
        with jax.named_scope("gn_fill"):
            s_gate.give()
        fills = [
            lambda: take(s_gate),
            lambda: (s_gate.given(), s_up.give()),
            lambda: take(s_up),
        ]
        for tick in range(1, pieces):
            with jax.named_scope("gn_tick"):
                flow(tick, scatter_gn, gather_br, take_grad)
            if fills:
                with jax.named_scope("gn_fill"):
                    fills.pop(0)()
        for k, s in steps[pieces]:
            gather_br.step(k, s)

        with jax.named_scope("down"):
            scatter_gn.finish()
            scatter_y = LineScatter(part, shuffled, sent, arrived, t, nt, y_sem)
            for start, width_ in tiles_of(model, 4):
                cols = slice(start, start + width_)
                part[:, cols] = dot(act[...], down_v[:, cols])
            for s in range(pieces):
                scatter_y.edge(s)

        def on(s, stage):
            s.add(stage)
            if stage + 1 < stages:
                s.send(stage + 1)

        rest = list(steps[pieces + 1 :])
        fills = [functools.partial(on, s, stage) for stage in range(stages - 1) for s in (s_gate, s_up)]
        for s in range(pieces):
            with jax.named_scope("y_round"):
                scatter_y.relay(scatter_y.near, s)
                scatter_y.relay(scatter_y.far, s)
            if rest:
                with jax.named_scope("br_step"):
                    for k, s_ in rest.pop(0):
                        gather_br.step(k, s_)
            if fills:
                with jax.named_scope("y_fill"):
                    fills.pop(0)()
        with jax.named_scope("y_own"):
            for late in rest:
                for k, s_ in late:
                    gather_br.step(k, s_)
            for fill in fills:
                fill()
            for s in range(pieces):
                at = scatter_y.own(s)
                block_ = slice(s * size, (s + 1) * size)
                y[block_, :] = (hid[block_, :] + part[at, :model]).astype(BF)
        with jax.named_scope("end"):
            copies = []
            for w, (s, out) in enumerate(((s_gate, d_gate), (s_up, d_up))):
                s.add(stages - 1)
                copies.append(
                    pltpu.make_async_copy(
                        part.at[pl.ds(w * shard, shard), pl.ds(0, hidden)], out, out_sem.at[1 + w]
                    )
                )
                copies[-1].start()
            s_up.given()
            for s in (s_gate, s_up):
                s.drain()
            gather_br.finish()
            scatter_y.finish()
            for copy in copies:
                copy.wait()

    pl.run_scoped(
        feed,
        pltpu.VMEM((tokens, hidden), BF),
        pltpu.VMEM((tokens, hidden), BF),
        pltpu.VMEM((nd // 2, shard, hidden), BF),
    )
    for g in gathers:
        g.drain()
    for mask in range(1, nd):
        gain_copy(mask).wait_send()
    cots.finish()
    gather_nf.finish()


def fore(nt, nd, x, cot, gain_a, gain_f, segr, wq, wkt, wvt, wo, gate, up, down):
    width = nd.bit_length() - 1
    rows, model = x.shape
    tokens = nt * rows
    queries = wq.shape[1]
    hidden = gate.shape[1]
    shard = model // nd
    half = nd // 2
    wide = queries + LANES
    span = max(width_ for _, width_ in tiles_of(hidden, 6))
    shape = jax.ShapeDtypeStruct
    outs = [
        (shape((model, wide), BF), hbm()),
        (shape((queries, model), BF), hbm()),
        (shape((tokens, model), BF), hbm()),
        (shape((tokens, model), BF), vmem()),
        (shape((tokens, queries), BF), vmem()),
        (shape((tokens, LANES), BF), vmem()),
        (shape((tokens, queries), BF), vmem()),
        (shape((tokens, LANES), F32), vmem()),
        (shape((nd, 8, shard), F32), vmem()),
        (shape((tokens, LANES), F32), vmem()),
        (shape((tokens, LANES), F32), vmem()),
        (shape((tokens, hidden), BF), vmem()),
        (shape((tokens, model), BF), vmem()),
        (shape((rows, model), F32), vmem()),
        (shape((8, model), F32), vmem()),
        (shape((rows, model), BF), vmem()),
        (shape((shard, hidden), F32), hbm()),
        (shape((shard, hidden), F32), hbm()),
    ]
    return pl.pallas_call(
        functools.partial(fore_kernel, nt, width),
        out_shape=[o for o, _ in outs],
        in_specs=[vmem()] * 8 + [hbm()] * 4,
        out_specs=[s for _, s in outs],
        scratch_shapes=[
            pltpu.VMEM((tokens, model), BF),
            pltpu.VMEM((rows, model), F32),
            pltpu.VMEM((model, hidden), BF),
            pltpu.VMEM((model, hidden), BF),
            pltpu.VMEM((hidden, model), BF),
            pltpu.VMEM((max(tokens, 2 * shard), max(model, 3 * span)), F32),
        ]
        + line_scratch(nt, rows, model)
        + [
            pltpu.VMEM((2, half, shard, hidden), BF),
            pltpu.VMEM((2, 2, half - 1, shard // 2, hidden), BF),
            pltpu.VMEM((shard, wide), BF),
            pltpu.VMEM((8, shard), F32),
            dma(2, nd),
            dma(7),
            dma(3),
            dma(4, nt, PIECES),
            dma(4, nt, PIECES),
            dma(4, nt, PIECES),
            dma(4, nt, PIECES),
            dma(2, 2, nt, PIECES),
            dma(2, 2, nt, PIECES),
            dma(2, 2, nt, PIECES),
            dma(7, 2, half),
            dma(7, 2, half),
            dma(7, half),
            dma(7, half),
        ],
        compiler_params=pltpu.CompilerParams(
            collective_id=0, has_side_effects=True, vmem_limit_bytes=VMEM_BYTES
        ),
        name="fore",
    )(x, cot, gain_a, gain_f, segr, wq, wkt, wvt, wo, gate, up, down)


def attend_back_pairs(first, last, qo, gm, mo, lo, kpad, vpad, bias, cos, sin, dqkv, dkey, dval):
    rows = qo.shape[0]

    @pl.loop(first, last)
    def _(pair):
        lanes = pl.ds(pl.multiple_of(pair * LANES, LANES), LANES)
        for start, block, seen in query_cuts(rows):
            at = slice(start, start + block)
            lane = lane_index((block, LANES))
            query, grad = qo[at, lanes], gm[at, lanes]
            both = grad.astype(F32) * mo[at, lanes].astype(F32)
            logs = lo[at, :]
            dq = jnp.zeros((block, LANES), F32)
            for side in range(2):
                inside = (lane >= HD) if side else (lane < HD)
                delta = jnp.sum(jnp.where(inside, both, 0.0), axis=-1, keepdims=True)
                log = jnp.sum(
                    jnp.where(lane == 2 * pair + side, logs, 0.0), axis=-1, keepdims=True
                )
                key, value = kpad[side, :seen, :], vpad[side, :seen, :]
                probs = jnp.exp(dot(query, key, 1, 1) + bias[at, :seen] - log)
                grad_scores = (probs * (dot(grad, value, 1, 1) - delta)).astype(BF)
                dq = dq + dot(grad_scores, key)
                dkey[side, :seen, :] += dot(grad_scores, query, 0, 0)
                dval[side, :seen, :] += dot(probs.astype(BF), grad, 0, 0)
            dq = dq * HD ** (-0.5)
            dqkv[at, lanes] = (dq * cos[at, :] - swapped(dq) * sin[at, :]).astype(BF)


def back_kernel(
    nt, width,
    branch, cf, act, mo, qo, kvo, lo, cos, sin, segr, x, gh, gparts, gall, na_f, wqkv_f, wo_f,
    gi, gain_out, d_wq, d_kv, d_wo, d_down,
    na, wqkv_v, wo_v, part, sent, arrived,
    bias, kpad, vpad, gm, dqkv, dkey, dval,
    given_d, totals_d, landed_d, given_q, totals_q, landed_q, given_o, totals_o, landed_o,
    gsum, zslots, dslots,
    load_sem, scatter_sem, zsem, dsem, hs, hr, ps, pr,
):
    me, t = lax.axis_index("dp"), lax.axis_index("tensor")
    nd = 1 << width
    rows, model = x.shape
    tokens, queries = qo.shape
    shard = model >> width
    pieces = PIECES
    size = rows // pieces
    loads = [
        pltpu.make_async_copy(wo_f, wo_v, load_sem.at[0]),
        pltpu.make_async_copy(wqkv_f, wqkv_v, load_sem.at[1]),
        pltpu.make_async_copy(na_f, na, load_sem.at[2]),
    ]
    for load in loads:
        load.start()
    bias_into(bias, segr)
    pad_pair(kvo[...].astype(F32), kpad, vpad)
    dkey[...] = jnp.zeros_like(dkey)
    dval[...] = jnp.zeros_like(dval)
    gsum[...] = gparts[...]
    with jax.named_scope("b_enter"):
        enter(t, nt, me, width, pltpu.get_barrier_semaphore(), everyone_along_tensor=True)

    def chunk_of(left, right):
        def chunk(d):
            return dot(left[:, pl.ds(pl.multiple_of(d * shard, shard), shard)], right[...], 0, 0)

        return chunk

    def store_down(at, value):
        d_down[:, at] = value.T

    def store_qkv(at, value):
        d_wq[at, :] = value[:, :queries]
        d_kv[:, at] = value[:, queries:].T

    def store_wo(at, value):
        d_wo[:, at] = value.T

    s_down, s_qkv, s_out = [
        BlockScatter(
            chunk_of(left, right), given, totals, landed, store, me, width,
            hs.at[w], hr.at[w], ps.at[w], pr.at[w],
        )
        for w, (left, right, given, totals, landed, store) in enumerate(
            (
                (cf, act, given_d, totals_d, landed_d, store_down),
                (na, dqkv, given_q, totals_q, landed_q, store_qkv),
                (branch, mo, given_o, totals_o, landed_o, store_wo),
            )
        )
    ]
    stages = s_down.stages

    with jax.named_scope("b_gm"):
        loads[0].wait()
        gm[...] = dot(branch[...], wo_v[...], 1, 1).astype(BF)
    with jax.named_scope("b_give"):
        s_down.give()
    with jax.named_scope("b_att"):
        attend_back_pairs(
            0, queries // LANES, qo, gm, mo, lo, kpad, vpad, bias, cos, sin, dqkv, dkey, dval
        )
        key = dkey[0] + pltpu.roll(dkey[1], HD, 1)
        value = pltpu.roll(dval[0], HD, 1) + dval[1]
        key = key * cos[...] - swapped(key) * sin[...]
        dqkv[:, queries : queries + LANES] = jnp.where(
            lane_index(key.shape) < HD, key, value
        ).astype(BF)

    inward = LineScatter(
        part, lambda j, s: j * rows + s * size, sent, arrived, t, nt, scatter_sem
    )
    with jax.named_scope("b_part"):
        loads[1].wait()
        for start, width_ in tiles_of(model, 4):
            part[:, start : start + width_] = dot(dqkv[...], wqkv_v[start : start + width_, :], 1, 1)
        for s in range(pieces):
            inward.edge(s)
        loads[2].wait()

    def take(s):
        s.take()
        s.send(0)

    def on(s, stage):
        s.add(stage)
        if stage + 1 < stages:
            s.send(stage + 1)

    def take_grad(s):
        at = inward.own(s)
        block = slice(s * size, (s + 1) * size)

        def store(cols, value):
            gi[block, cols] = gh[block, cols] + value

        def store_gain(cols, value):
            gsum[0:1, cols] += value

        back_through_norm(
            lambda c: x[block, c].astype(F32), lambda c: part[at, c], gall, 0, store, store_gain
        )

    fills = [
        lambda: s_qkv.give(),
        lambda: (take(s_qkv), s_out.give()),
        lambda: take(s_out),
    ]
    fills += [functools.partial(on, s, stage) for stage in range(stages) for s in (s_down, s_qkv, s_out)]
    with jax.named_scope("b_take"):
        take(s_down)
    for s in range(pieces):
        with jax.named_scope("b_round"):
            inward.relay(inward.near, s)
            inward.relay(inward.far, s)
        with jax.named_scope("b_fill"):
            if fills:
                fills.pop(0)()
    with jax.named_scope("b_own"):
        for s in range(pieces):
            take_grad(s)
            if fills and s < pieces - 1:
                fills.pop(0)()

    with jax.named_scope("b_gains"):
        zslots[t] = gsum[...]

        def along(step):
            return remote(
                zslots.at[t], zslots.at[t], zsem.at[0, step], zsem.at[1, step],
                {"tensor": lax.rem(t + step, nt)},
            )

        for step in range(1, nt):
            along(step).start()
    with jax.named_scope("b_rest"):
        for fill in fills:
            fill()
    with jax.named_scope("b_gains"):
        for step in range(1, nt):
            slot = zslots.at[lax.rem(t + nt - step, nt)]
            remote(
                slot, slot, zsem.at[0, step], zsem.at[1, step], {"tensor": lax.rem(t + step, nt)}
            ).wait_recv()
        gsum[...] = sum(zslots[i] for i in range(nt))

        def across(mask):
            peer = flip(me, mask, width)
            return remote(
                gsum.at[:, pl.ds(pl.multiple_of(peer * shard, shard), shard)], dslots.at[me],
                dsem.at[0, mask], dsem.at[1, mask], {"dp": peer},
            )

        for mask in range(1, nd):
            across(mask).start()
        dslots[me] = gsum[:, pl.ds(pl.multiple_of(me * shard, shard), shard)]
        for mask in range(1, nd):
            peer = flip(me, mask, width)
            slot = dslots.at[peer]
            remote(slot, slot, dsem.at[0, mask], dsem.at[1, mask], {"dp": peer}).wait_recv()
        gain_out[...] = sum(dslots[i] for i in range(nd))

    for step in range(1, nt):
        along(step).wait_send()
    for mask in range(1, nd):
        across(mask).wait_send()
    for s in (s_down, s_qkv, s_out):
        s.given()
        s.drain()
    inward.finish()


def back(nt, nd, branch, cf, act, mo, qo, kvo, lo, cos, sin, segr, x, gh, gparts, gall, na, wqkv_f, wo_f):
    width = nd.bit_length() - 1
    rows, model = x.shape
    tokens, queries = qo.shape
    hidden = act.shape[1]
    wide = wqkv_f.shape[1]
    shard = model // nd
    half = nd // 2
    shape = jax.ShapeDtypeStruct
    outs = [
        shape((rows, model), F32),
        shape((8, shard), F32),
        shape((shard, queries), F32),
        shape((LANES, shard), F32),
        shape((queries, shard), F32),
        shape((hidden, shard), F32),
    ]

    def cube(size):
        return [
            pltpu.VMEM((half, shard, size), BF),
            pltpu.VMEM((half, shard, size), BF),
            pltpu.VMEM((2, half - 1, shard // 2, size), BF),
        ]

    return pl.pallas_call(
        functools.partial(back_kernel, nt, width),
        out_shape=outs,
        in_specs=[vmem()] * 14 + [hbm()] * 3,
        out_specs=[vmem()] * len(outs),
        scratch_shapes=[
            pltpu.VMEM((tokens, model), BF),
            pltpu.VMEM((model, wide), BF),
            pltpu.VMEM((queries, model), BF),
            pltpu.VMEM((tokens, model), F32),
        ]
        + line_scratch(nt, rows, model)
        + [
            pltpu.VMEM((tokens, tokens), F32),
            pltpu.VMEM((2, tokens, LANES), BF),
            pltpu.VMEM((2, tokens, LANES), BF),
            pltpu.VMEM((tokens, queries), BF),
            pltpu.VMEM((tokens, wide), BF),
            pltpu.VMEM((2, tokens, LANES), F32),
            pltpu.VMEM((2, tokens, LANES), F32),
        ]
        + cube(hidden)
        + cube(wide)
        + cube(queries)
        + [
            pltpu.VMEM((8, model), F32),
            pltpu.VMEM((nt, 8, model), F32),
            pltpu.VMEM((nd, 8, shard), F32),
            dma(3),
            dma(2, 2, nt, PIECES),
            dma(2, nt),
            dma(2, nd),
            dma(3, 2, half),
            dma(3, 2, half),
            dma(3, half),
            dma(3, half),
        ],
        compiler_params=pltpu.CompilerParams(
            collective_id=1, has_side_effects=True, vmem_limit_bytes=VMEM_BYTES
        ),
        name="back",
    )(branch, cf, act, mo, qo, kvo, lo, cos, sin, segr, x, gh, gparts, gall, na, wqkv_f, wo_f)


def narrow_scatter(value, axis, scatter_dimension, tiled):
    low = value.astype(BF) if value.ndim == 2 else value
    return lax.psum_scatter(low, axis, scatter_dimension=scatter_dimension, tiled=tiled).astype(F32)


def rope_tables(segments, head_dim):
    row_count = segments.shape[0]
    row_index = jnp.arange(row_count, dtype=jnp.int32)
    change = jnp.concatenate(
        [jnp.ones((1,), jnp.int32), (segments[1:] != segments[:-1]).astype(jnp.int32)]
    )
    starts = lax.cummax(jnp.where(change > 0, row_index, jnp.zeros_like(row_index)), axis=0)
    position = (row_index - starts).astype(F32)
    half_dim = head_dim // 2
    frequency = jnp.exp(jnp.arange(half_dim, dtype=F32) * (-math.log(10000.0) / half_dim))
    angles = position[:, None] * frequency[None, :]
    return (jnp.cos(angles)[:, None, :], jnp.sin(angles)[:, None, :])


def rotate(tensor, cosine, sine):
    half_dim = tensor.shape[-1] // 2
    first_half = tensor[..., :half_dim]
    second_half = tensor[..., half_dim:]
    return jnp.concatenate(
        [first_half * cosine - second_half * sine, second_half * cosine + first_half * sine],
        axis=-1,
    )


def unrotate(tensor, cosine, sine):
    half_dim = tensor.shape[-1] // 2
    first_half = tensor[..., :half_dim]
    second_half = tensor[..., half_dim:]
    return jnp.concatenate(
        [first_half * cosine + second_half * sine, second_half * cosine - first_half * sine],
        axis=-1,
    )


def visible(segments):
    row_index = jnp.arange(segments.shape[0], dtype=jnp.int32)
    same_seq = segments[:, None] == segments[None, :]
    return same_seq & (row_index[:, None] >= row_index[None, :])


def normalize(values, gain):
    inverse = lax.rsqrt(jnp.mean(values * values, axis=-1, keepdims=True) + EPSILON)
    unit_rows = values * inverse
    return (unit_rows, inverse, (unit_rows * gain.astype(F32)).astype(BF))


def normalize_back(grad_normed, unit_rows, inverse, gain):
    scaled = grad_normed * gain.astype(F32)
    grad_values = inverse * (
        scaled - unit_rows * jnp.mean(scaled * unit_rows, axis=-1, keepdims=True)
    )
    return (grad_values, jnp.sum(grad_normed * unit_rows, axis=0))


def contract(left, right, left_dim, right_dim):
    return lax.dot_general(
        left, right, (((left_dim,), (right_dim,)), ((), ())), preferred_element_type=F32
    )


def block_scores(query_block, key_heads, allowed_block, score_scale):
    scores = (
        jnp.einsum("rkgd,skd->kgrs", query_block, key_heads, preferred_element_type=F32)
        * score_scale
    )
    return jnp.where(allowed_block[None, None], scores, NEGATIVE)


def attend_forward(query_groups, key_heads, value_heads, allowed, score_scale):
    scores = block_scores(query_groups, key_heads, allowed, score_scale)
    row_max = jnp.max(scores, axis=-1, keepdims=True)
    log_total = row_max + jnp.log(jnp.sum(jnp.exp(scores - row_max), axis=-1, keepdims=True))
    probs_low = jnp.exp(scores - log_total).astype(BF)
    mixed_parts = jnp.einsum(
        "kgrs,skd->rkgd", probs_low, value_heads, preferred_element_type=F32
    ).astype(BF)
    return (mixed_parts, log_total)


def attend_backward(
    query_groups, key_heads, value_heads, mixed_heads, grad_mixed, log_totals, allowed, score_scale
):
    scores = block_scores(query_groups, key_heads, allowed, score_scale)
    attn_probs = jnp.exp(scores - log_totals)
    probs_low = attn_probs.astype(BF)
    grad_probs = jnp.einsum(
        "rkgd,skd->kgrs", grad_mixed, value_heads, preferred_element_type=F32
    )
    row_delta = jnp.sum(grad_mixed.astype(F32) * mixed_heads.astype(F32), axis=-1)
    row_delta = jnp.transpose(row_delta, (1, 2, 0))[..., None]
    grad_scores = (attn_probs * (grad_probs - row_delta)).astype(BF)
    query_parts = (
        jnp.einsum("kgrs,skd->rkgd", grad_scores, key_heads, preferred_element_type=F32)
        * score_scale
    )
    grad_key_rot = (
        jnp.einsum("kgrs,rkgd->skd", grad_scores, query_groups, preferred_element_type=F32)
        * score_scale
    )
    grad_value_heads = jnp.einsum(
        "kgrs,rkgd->skd", probs_low, grad_mixed, preferred_element_type=F32
    )
    return (query_parts, grad_key_rot, grad_value_heads)


def plain_device(
    layer_input,
    segment_ids,
    norm_attn,
    w_query,
    w_key,
    w_value,
    w_output,
    norm_ffn,
    w_gate,
    w_up,
    w_down,
    cotangent,
):
    score_scale = HD ** (-0.5)
    query_full, key_full, value_full, output_full, gain_attn = (
        lax.all_gather(w_query, "dp", axis=0, tiled=True),
        lax.all_gather(w_key, "dp", axis=0, tiled=True),
        lax.all_gather(w_value, "dp", axis=0, tiled=True),
        lax.all_gather(w_output, "dp", axis=1, tiled=True),
        lax.all_gather(norm_attn, "dp", axis=0, tiled=True),
    )
    gate_full, up_full, down_full, gain_ffn = (
        lax.all_gather(w_gate, "dp", axis=0, tiled=True),
        lax.all_gather(w_up, "dp", axis=0, tiled=True),
        lax.all_gather(w_down, "dp", axis=1, tiled=True),
        lax.all_gather(norm_ffn, "dp", axis=0, tiled=True),
    )
    heads_local = query_full.shape[1] // HD
    kv_local = key_full.shape[1] // HD
    group = heads_local // kv_local
    residual_in = layer_input.astype(F32)
    unit_attn, inverse_attn, normed_local = normalize(residual_in, gain_attn)
    normed_attn = lax.all_gather(normed_local, "tensor", axis=0, tiled=True)
    row_count = normed_attn.shape[0]
    cosine, sine = rope_tables(segment_ids, HD)
    allowed = visible(segment_ids)
    query_heads = rotate(
        jnp.dot(normed_attn, query_full, preferred_element_type=F32).reshape(
            row_count, heads_local, HD
        ),
        cosine,
        sine,
    ).astype(BF)
    query_groups = query_heads.reshape(row_count, kv_local, group, HD)
    key_heads = rotate(
        jnp.dot(normed_attn, key_full, preferred_element_type=F32).reshape(
            row_count, kv_local, HD
        ),
        cosine,
        sine,
    ).astype(BF)
    value_heads = (
        jnp.dot(normed_attn, value_full, preferred_element_type=F32)
        .astype(BF)
        .reshape(row_count, kv_local, HD)
    )
    mixed_heads, log_totals = attend_forward(
        query_groups, key_heads, value_heads, allowed, score_scale
    )
    mixed_flat = mixed_heads.reshape(row_count, heads_local * HD)
    hidden_res = residual_in + narrow_scatter(
        jnp.dot(mixed_flat, output_full, preferred_element_type=F32),
        "tensor",
        scatter_dimension=0,
        tiled=True,
    )
    unit_ffn, inverse_ffn, normed_ffn_local = normalize(hidden_res, gain_ffn)
    normed_ffn = lax.all_gather(normed_ffn_local, "tensor", axis=0, tiled=True)
    gate_rows = jnp.dot(normed_ffn, gate_full, preferred_element_type=F32)
    up_rows = jnp.dot(normed_ffn, up_full, preferred_element_type=F32)
    sigmoid_gate = jax.nn.sigmoid(gate_rows)
    active = (gate_rows * sigmoid_gate * up_rows).astype(BF)
    layer_output = (
        hidden_res
        + narrow_scatter(
            jnp.dot(active, down_full, preferred_element_type=F32).astype(BF),
            "tensor",
            scatter_dimension=0,
            tiled=True,
        ).astype(F32)
    ).astype(BF)
    query_full, key_full, value_full, output_full, gate_full, up_full, down_full = (
        lax.all_gather(w_query, "dp", axis=0, tiled=True),
        lax.all_gather(w_key, "dp", axis=0, tiled=True),
        lax.all_gather(w_value, "dp", axis=0, tiled=True),
        lax.all_gather(w_output, "dp", axis=1, tiled=True),
        lax.all_gather(w_gate, "dp", axis=0, tiled=True),
        lax.all_gather(w_up, "dp", axis=0, tiled=True),
        lax.all_gather(w_down, "dp", axis=1, tiled=True),
    )
    cotangent_full = lax.all_gather(cotangent, "tensor", axis=0, tiled=True)
    grad_active = contract(cotangent_full, down_full, 1, 1)
    grad_w_down = contract(active, cotangent_full, 0, 0)
    grad_up_rows = (grad_active * gate_rows * sigmoid_gate).astype(BF)
    grad_gate_rows = (
        grad_active * up_rows * sigmoid_gate * (1.0 + gate_rows * (1.0 - sigmoid_gate))
    ).astype(BF)
    grad_w_gate = contract(normed_ffn, grad_gate_rows, 0, 0)
    grad_w_up = contract(normed_ffn, grad_up_rows, 0, 0)
    grad_normed_ffn = narrow_scatter(
        contract(grad_gate_rows, gate_full, 1, 1) + contract(grad_up_rows, up_full, 1, 1),
        "tensor",
        scatter_dimension=0,
        tiled=True,
    )
    grad_hidden, gain_ffn_part = normalize_back(grad_normed_ffn, unit_ffn, inverse_ffn, gain_ffn)
    grad_hidden = cotangent.astype(F32) + grad_hidden
    branch_full = lax.all_gather(grad_hidden.astype(BF), "tensor", axis=0, tiled=True)
    grad_mixed = contract(branch_full, output_full, 1, 1).astype(BF)
    grad_w_output = contract(mixed_flat, branch_full, 0, 0)
    grad_query_rot, grad_key_rot, grad_value_heads = attend_backward(
        query_groups,
        key_heads,
        value_heads,
        mixed_heads,
        grad_mixed.reshape(row_count, kv_local, group, HD),
        log_totals,
        allowed,
        score_scale,
    )
    grad_queries = (
        unrotate(grad_query_rot.reshape(row_count, heads_local, HD), cosine, sine)
        .reshape(row_count, heads_local * HD)
        .astype(BF)
    )
    grad_keys = (
        unrotate(grad_key_rot, cosine, sine).reshape(row_count, kv_local * HD).astype(BF)
    )
    grad_values = grad_value_heads.reshape(row_count, kv_local * HD).astype(BF)
    grad_w_query = contract(normed_attn, grad_queries, 0, 0)
    grad_w_key = contract(normed_attn, grad_keys, 0, 0)
    grad_w_value = contract(normed_attn, grad_values, 0, 0)
    grad_normed_attn = narrow_scatter(
        contract(grad_queries, query_full, 1, 1)
        + contract(grad_keys, key_full, 1, 1)
        + contract(grad_values, value_full, 1, 1),
        "tensor",
        scatter_dimension=0,
        tiled=True,
    )
    grad_residual, gain_attn_part = normalize_back(
        grad_normed_attn, unit_attn, inverse_attn, gain_attn
    )
    grad_input = grad_hidden + grad_residual
    gain_attn_total, gain_ffn_total = lax.psum((gain_attn_part, gain_ffn_part), "tensor")
    owned = (
        narrow_scatter(grad_w_query, "dp", scatter_dimension=0, tiled=True),
        narrow_scatter(grad_w_key, "dp", scatter_dimension=0, tiled=True),
        narrow_scatter(grad_w_value, "dp", scatter_dimension=0, tiled=True),
        narrow_scatter(grad_w_output, "dp", scatter_dimension=1, tiled=True),
        narrow_scatter(gain_attn_total, "dp", scatter_dimension=0, tiled=True),
        narrow_scatter(gain_ffn_total, "dp", scatter_dimension=0, tiled=True),
        narrow_scatter(grad_w_gate, "dp", scatter_dimension=0, tiled=True),
        narrow_scatter(grad_w_up, "dp", scatter_dimension=0, tiled=True),
        narrow_scatter(grad_w_down, "dp", scatter_dimension=1, tiled=True),
    )
    return (
        layer_output,
        grad_input,
        owned[4],
        owned[0],
        owned[1],
        owned[2],
        owned[3],
        owned[5],
        owned[6],
        owned[7],
        owned[8],
    )


def with_kernels(nt, nd, layer_input, segment_ids, norm_attn, w_query, w_key, w_value, w_output, norm_ffn, w_gate, w_up, w_down, cotangent):
    segr = segment_ids[None, :]
    (wqkv_f, wo_f, na, cf, qo, kvo, mo, lo, gall, cos, sin, act, branch, gh, gparts, y, d_gate, d_up) = fore(
        nt, nd, layer_input, cotangent, norm_attn[None, :], norm_ffn[None, :], segr,
        w_query, w_key.T, w_value.T, w_output, w_gate, w_up, w_down,
    )
    gi, gains, d_wq, d_kv, d_wo, d_down = back(
        nt, nd, branch, cf, act, mo, qo, kvo, lo, cos, sin, segr, layer_input, gh, gparts, gall,
        na, wqkv_f, wo_f,
    )
    k = w_key.shape[1]
    return (
        y, gi, gains[0], d_wq, d_kv[:k].T, d_kv[k:].T, d_wo, gains[1], d_gate, d_up, d_down
    )


def fits(nt, nd, shards):
    layer_input, segment_ids, norm_attn, w_query, w_key, w_value, w_output, norm_ffn, w_gate, w_up, w_down, _ = shards
    return (
        nd >= 4
        and nd & (nd - 1) == 0
        and nt >= 2
        and norm_attn.shape[0] % LANES == 0
        and w_output.shape[1] % LANES == 0
        and w_gate.shape[1] % LANES == 0
        and w_query.shape[1] % LANES == 0
        and w_key.shape[1] == HD
        and segment_ids.shape[0] == nt * layer_input.shape[0]
        and segment_ids.shape[0] % LANES == 0
    )


def on_device(nt, nd, *shards):
    if fits(nt, nd, shards):
        return with_kernels(nt, nd, *shards)
    return plain_device(*shards)


def solution(mesh):
    placed = (
        P(("dp", "tensor"), None),
        P("dp"),
        P("dp"),
        P("dp", "tensor"),
        P("dp", "tensor"),
        P("dp", "tensor"),
        P("tensor", "dp"),
        P("dp"),
        P("dp", "tensor"),
        P("dp", "tensor"),
        P("tensor", "dp"),
        P(("dp", "tensor"), None),
    )
    return jax.shard_map(
        functools.partial(on_device, mesh.shape["tensor"], mesh.shape["dp"]),
        mesh=mesh,
        in_specs=placed,
        out_specs=(
            P(("dp", "tensor"), None),
            P(("dp", "tensor"), None),
            P("dp"),
            P("dp", "tensor"),
            P("dp", "tensor"),
            P("dp", "tensor"),
            P("tensor", "dp"),
            P("dp"),
            P("dp", "tensor"),
            P("dp", "tensor"),
            P("tensor", "dp"),
        ),
        check_vma=False,
    )
```

```python
import functools
import math

import jax
import jax.numpy as jnp
from jax import lax
from jax.experimental import pallas as pl
from jax.experimental.pallas import tpu as pltpu
from jax.sharding import PartitionSpec as P

HD = 64
EPSILON = 1e-05
NEGATIVE = -1e30
LANES = 128
BF = jnp.bfloat16
F32 = jnp.float32
VMEM_BYTES = 67_000_000


def spans(bits):
    masks = [0]
    for bit in bits:
        masks = masks + [mask | (1 << bit) for mask in masks]
    return masks


def flip(index, mask, width):
    total = 0
    for bit in range(width):
        own = lax.rem(lax.div(index, 1 << bit), 2)
        if isinstance(mask, int):
            other = (mask >> bit) & 1
        else:
            other = lax.rem(lax.div(mask, 1 << bit), 2)
        total = total + lax.rem(own + other, 2) * (1 << bit)
    return total


def aligned(value, step):
    return value if isinstance(value, int) else pl.multiple_of(value, step)


def remote(src, dst, send_sem, recv_sem, device):
    return pltpu.make_async_remote_copy(
        src_ref=src,
        dst_ref=dst,
        send_sem=send_sem,
        recv_sem=recv_sem,
        device_id=device,
        device_id_type=pl.DeviceIdType.MESH,
    )


def dot(left, right, left_dim=1, right_dim=0):
    return lax.dot_general(
        left, right, (((left_dim,), (right_dim,)), ((), ())), preferred_element_type=F32
    )


def tiles_of(size, most):
    units = size // LANES
    parts = -(-units // most)
    cuts, start = [], 0
    for part in range(parts):
        width = (units // parts + (1 if part < units % parts else 0)) * LANES
        cuts.append((start, width))
        start += width
    return cuts


def enter(t, nt, me, width, barrier, everyone_along_tensor=False):
    signal = functools.partial(
        pl.semaphore_signal, barrier, inc=1, device_id_type=pl.DeviceIdType.MESH
    )
    for mask in range(1, 1 << width):
        signal(device_id={"dp": flip(me, mask, width)})
    if everyone_along_tensor:
        for step in range(1, nt):
            signal(device_id={"tensor": lax.rem(t + step, nt)})
        pl.semaphore_wait(barrier, (1 << width) - 1 + nt - 1)
        return

    @pl.when(t > 0)
    def _():
        signal(device_id={"tensor": t - 1})

    @pl.when(t < nt - 1)
    def _():
        signal(device_id={"tensor": t + 1})

    neighbours = lax.min(t, 1) + lax.min(nt - 1 - t, 1)
    pl.semaphore_wait(barrier, (1 << width) - 1 + neighbours)


class LineGather:
    def __init__(self, full, row, size, t, nt, sems):
        self.full, self.row, self.size = full, row, size
        self.t, self.nt, self.sems = t, nt, sems
        self.pieces = sems.shape[2]

    def window(self, j, s):
        return self.full.at[pl.ds(aligned(self.row(j, s), self.size), self.size), :]

    def right(self, j, s):
        at = self.window(j, s)
        return remote(
            at, at, self.sems.at[0, j, s], self.sems.at[2, j, s],
            {"tensor": lax.rem(self.t + 1, self.nt)},
        )

    def left(self, j, s):
        at = self.window(j, s)
        return remote(
            at, at, self.sems.at[1, j, s], self.sems.at[3, j, s],
            {"tensor": lax.rem(self.t + self.nt - 1, self.nt)},
        )

    def start(self, s):
        @pl.when(self.t < self.nt - 1)
        def _():
            self.right(self.t, s).start()

        @pl.when(self.t > 0)
        def _():
            self.left(self.t, s).start()

    def step(self, k, s):
        t, nt = self.t, self.nt

        @pl.when(t >= k)
        def _():
            self.right(t - k, s).wait_recv()

            @pl.when(t < nt - 1)
            def _():
                self.right(t - k, s).start()

        @pl.when(t + k < nt)
        def _():
            self.left(t + k, s).wait_recv()

            @pl.when(t > 0)
            def _():
                self.left(t + k, s).start()

    def finish(self):
        t, nt = self.t, self.nt

        @pl.loop(0, nt)
        def _(k):
            for s in range(self.pieces):
                @pl.when((t >= k) & (t < nt - 1))
                def _():
                    self.right(t - k, s).wait_send()

                @pl.when((t + k < nt) & (t > 0))
                def _():
                    self.left(t + k, s).wait_send()


class LineScatter:
    def __init__(self, part, row, sent, arrived, t, nt, sems):
        self.part, self.row, self.sent, self.arrived = part, row, sent, arrived
        self.t, self.nt, self.sems = t, nt, sems
        self.pieces = sems.shape[3]
        self.size = sent.shape[1] // self.pieces
        self.model = sent.shape[2]
        self.near = lax.div(2 * t, nt)
        self.far = 1 - self.near

    def sub(self, s):
        return pl.ds(s * self.size, self.size)

    def depth(self, way):
        return (1 - way) * self.t + way * (self.nt - 1 - self.t)

    def goal(self, way, i):
        return (1 - way) * (self.nt - 1 - i) + way * i

    def slot(self, way, j):
        return j + 1 - way

    def move(self, way, j, s):
        return remote(
            self.sent.at[j, self.sub(s), :], self.arrived.at[self.slot(way, j), self.sub(s), :],
            self.sems.at[0, way, j, s], self.sems.at[1, way, j, s],
            {"tensor": lax.rem(self.t + self.nt + 1 - 2 * way, self.nt)},
        )

    def rows(self, j, s):
        return pl.ds(aligned(self.row(j, s), self.size), self.size)

    def mine(self, j, s):
        return self.part[self.rows(j, s), : self.model]

    def edge(self, s):
        t, nt = self.t, self.nt

        @pl.when((t == 0) | (t == nt - 1))
        def _():
            way = lax.div(t, nt - 1)

            @pl.loop(0, nt - 1)
            def _(i):
                j = self.goal(way, i)
                self.sent[j, self.sub(s), :] = self.mine(j, s).astype(BF)
                self.move(way, j, s).start()

    def relay(self, way, s):
        depth = self.depth(way)

        @pl.when(depth > 0)
        def _():
            @pl.loop(0, self.nt - 1 - depth)
            def _(i):
                j = self.goal(way, i)
                self.move(way, j, s).wait_recv()
                total = self.mine(j, s) + self.arrived[self.slot(way, j), self.sub(s), :].astype(F32)
                self.sent[j, self.sub(s), :] = total.astype(BF)
                self.move(way, j, s).start()

    def own(self, s):
        t = self.t
        rows = self.rows(t, s)
        for way in (self.near, self.far):
            @pl.when(self.depth(way) > 0)
            def _():
                self.move(way, t, s).wait_recv()
                self.part[rows, : self.model] += self.arrived[self.slot(way, t), self.sub(s), :].astype(F32)

        return rows

    def finish(self):
        for way in range(2):
            @pl.loop(0, self.nt - 1 - self.depth(way))
            def _(i):
                for s in range(self.pieces):
                    self.move(way, self.goal(way, i), s).wait_send()


class Cube:
    def setup(self, me, width, half_send, half_recv, pair_send, pair_recv):
        self.me, self.width = me, width
        self.hs, self.hr, self.ps, self.pr = half_send, half_recv, pair_send, pair_recv
        self.bits = list(range(1, width))
        self.orders = (self.bits, self.bits[::-1])
        self.masks = spans(self.bits)
        self.stages = len(self.bits)

    def at(self, mask):
        return flip(self.me, mask, self.width)


class BlockGather(Cube):
    def __init__(self, own, full, by_rows, me, width, *sems):
        self.setup(me, width, *sems)
        self.own_ref, self.full, self.by_rows = own, full, by_rows

    def half(self, h):
        rows = self.own_ref.shape[0] // 2
        return self.own_ref.at[pl.ds(h * rows, rows), :]

    def window(self, who, h=None):
        rows, cols = self.own_ref.shape
        take, start = (rows, 0) if h is None else (rows // 2, h * (rows // 2))
        if self.by_rows:
            return self.full.at[pl.ds(aligned(who * rows + start, take), take), :]
        return self.full.at[pl.ds(start, take), pl.ds(aligned(who * cols, cols), cols)]

    def hop(self, stage, h, m):
        order = self.orders[h]
        bit = 1 << order[stage]
        slot = (m | bit) >> 1
        src = self.half(h) if m == 0 else self.window(self.at(m), h)
        return remote(
            src, self.window(self.at(m), h), self.hs.at[h, slot], self.hr.at[h, slot],
            {"dp": self.at(bit)},
        )

    def send(self, stage):
        for h in range(2):
            for m in spans(self.orders[h][:stage]):
                self.hop(stage, h, m).start()

    def wait(self, stage):
        for h in range(2):
            bit = 1 << self.orders[h][stage]
            for m in spans(self.orders[h][:stage]):
                slot = (m | bit) >> 1
                landed = self.window(self.at(m | bit), h)
                remote(
                    landed, landed, self.hs.at[h, slot], self.hr.at[h, slot], {"dp": self.at(bit)}
                ).wait_recv()

    def pair(self, m):
        src = self.own_ref if m == 0 else self.window(self.at(m))
        return remote(
            src, self.window(self.at(m)), self.ps.at[m >> 1], self.pr.at[m >> 1],
            {"dp": self.at(1)},
        )

    def pair_send(self):
        for m in self.masks:
            self.pair(m).start()

    def pair_wait(self):
        for m in self.masks:
            landed = self.window(self.at(m | 1))
            remote(
                landed, landed, self.ps.at[m >> 1], self.pr.at[m >> 1], {"dp": self.at(1)}
            ).wait_recv()

    def place(self, sem):
        return pltpu.make_async_copy(self.own_ref, self.window(self.me), sem)

    def drain(self):
        for stage in range(self.stages):
            for h in range(2):
                for m in spans(self.orders[h][:stage]):
                    self.hop(stage, h, m).wait_send()
        for m in self.masks:
            self.pair(m).wait_send()


class BlockScatter(Cube):
    def __init__(self, chunk, out_sent, total, landed, store, me, width, *sems):
        self.setup(me, width, *sems)
        self.chunk, self.sent, self.total, self.landed = chunk, out_sent, total, landed
        self.store = store
        self.slots = 1 << (width - 1)

    def pair(self, slot):
        return remote(
            self.sent.at[slot], self.total.at[slot], self.ps.at[slot], self.pr.at[slot],
            {"dp": self.at(1)},
        )

    def give(self):
        @pl.loop(0, self.slots)
        def _(k):
            slot = self.slots - 1 - k
            self.sent[slot] = self.chunk(self.at(2 * slot + 1)).astype(BF)
            self.pair(slot).start()

    def given(self):
        @pl.loop(0, self.slots)
        def _(slot):
            self.pair(slot).wait_send()

    def take(self):
        @pl.loop(0, self.slots)
        def _(k):
            slot = self.slots - 1 - k
            term = self.chunk(self.at(2 * slot))
            self.pair(slot).wait_recv()
            self.total[slot] = (term + self.total[slot].astype(F32)).astype(BF)

    def moves(self, stage):
        for h in range(2):
            order = self.orders[h]
            last = self.stages - 1 - stage
            bit = 1 << order[last]
            for m in spans(order[:last]):
                yield h, bit, m | bit

    def hop(self, h, bit, m):
        rows = self.total.shape[1] // 2
        return remote(
            self.total.at[m >> 1, pl.ds(h * rows, rows), :], self.landed.at[h, (m >> 1) - 1],
            self.hs.at[h, m >> 1], self.hr.at[h, m >> 1], {"dp": self.at(bit)},
        )

    def send(self, stage):
        for h, bit, m in self.moves(stage):
            self.hop(h, bit, m).start()

    def add(self, stage):
        rows = self.total.shape[1] // 2
        for h, bit, m in self.moves(stage):
            self.hop(h, bit, m).wait_recv()
            keep = (m ^ bit) >> 1
            at = slice(h * rows, (h + 1) * rows)
            total = self.total[keep, at, :].astype(F32) + self.landed[h, (m >> 1) - 1].astype(F32)
            if stage == self.stages - 1:
                self.store(at, total)
            else:
                self.total[keep, at, :] = total.astype(BF)

    def drain(self):
        for stage in range(self.stages):
            for h, bit, m in self.moves(stage):
                self.hop(h, bit, m).wait_send()


def inverse_of(rows):
    return lax.rsqrt(jnp.mean(rows * rows, axis=-1, keepdims=True) + EPSILON)


def times_gain(unit, gains, which, store):
    parts, _, width = gains.shape
    for d in range(parts):
        cols = slice(d * width, (d + 1) * width)
        store(cols, unit[:, cols] * gains[d, which : which + 1, :])


def lane_index(shape):
    return lax.broadcasted_iota(jnp.int32, shape, len(shape) - 1)


def column_of(segr):
    rows = segr.shape[1]
    wide = jnp.broadcast_to(segr[...].astype(F32), (8, rows))
    return jnp.transpose(wide)[:, 0:1]


def rope_into(cos_ref, sin_ref, segr):
    rows = segr.shape[1]
    before = (segr[...].astype(F32) < column_of(segr)).astype(F32)
    start = jnp.sum(before, axis=1, keepdims=True)
    position = lax.broadcasted_iota(jnp.int32, (rows, 1), 0).astype(F32) - start
    lane = lane_index((rows, LANES))
    half = HD // 2
    frequency = jnp.exp(lax.rem(lane, half).astype(F32) * (-math.log(10000.0) / half))
    angle = position * frequency
    cos_ref[...] = jnp.cos(angle)
    sine = jnp.sin(angle)
    sin_ref[...] = jnp.where(lax.rem(lane, HD) < half, -sine, sine)


def swapped(x):
    lane = lane_index(x.shape)
    half = HD // 2
    return jnp.where(
        lax.rem(lane, HD) < half,
        pltpu.roll(x, LANES - half, 1),
        pltpu.roll(x, half, 1),
    )


def bias_into(bias, segr):
    rows = segr.shape[1]
    query = lax.broadcasted_iota(jnp.int32, (rows, rows), 0)
    key = lax.broadcasted_iota(jnp.int32, (rows, rows), 1)
    seen = (segr[...].astype(F32) == column_of(segr)) & (query >= key)
    bias[...] = jnp.where(seen, 0.0, NEGATIVE)


def pad_pair(keys_values, keys, values):
    low = lane_index(keys_values.shape) < HD
    key = jnp.where(low, keys_values, 0.0)
    value = jnp.where(low, 0.0, keys_values)
    keys[0] = key.astype(BF)
    keys[1] = pltpu.roll(key, HD, 1).astype(BF)
    values[0] = pltpu.roll(value, HD, 1).astype(BF)
    values[1] = value.astype(BF)


def query_cuts(rows):
    block = 256 if rows % 256 == 0 else rows
    return [(start, block, start + block) for start in range(0, rows, block)]


def attend_pairs(first, last, qo, kpad, vpad, bias, mo, lo):
    rows = qo.shape[0]
    lane = lane_index((1, LANES))

    @pl.loop(first, last)
    def _(pair):
        lanes = pl.ds(pl.multiple_of(pair * LANES, LANES), LANES)
        for start, block, seen in query_cuts(rows):
            at = slice(start, start + block)
            query = qo[at, lanes]
            mixed = jnp.zeros((block, LANES), F32)
            logs = lo[at, :]
            for side in range(2):
                scores = dot(query, kpad[side, :seen, :], 1, 1) + bias[at, :seen]
                top = jnp.max(scores, axis=-1, keepdims=True)
                probs = jnp.exp(scores - top)
                total = jnp.sum(probs, axis=-1, keepdims=True)
                mixed = mixed + dot(probs.astype(BF), vpad[side, :seen, :]) / total
                logs = jnp.where(lane == 2 * pair + side, top + jnp.log(total), logs)
            lo[at, :] = logs
            mo[at, lanes] = mixed.astype(BF)


def back_through_norm(raw, grads, gains, which, store, store_gain):
    parts, _, width = gains.shape
    cuts = [slice(d * width, (d + 1) * width) for d in range(parts)]
    model = parts * width
    square = sum(jnp.sum(raw(c) * raw(c), axis=-1, keepdims=True) for c in cuts)
    inverse = lax.rsqrt(square / model + EPSILON)
    mean = 0.0
    for d, c in enumerate(cuts):
        unit = raw(c) * inverse
        grad = grads(c)
        store_gain(c, jnp.sum(grad * unit, axis=0, keepdims=True))
        mean = mean + jnp.sum(grad * gains[d, which : which + 1, :] * unit, axis=-1, keepdims=True)
    mean = mean / model
    for d, c in enumerate(cuts):
        unit = raw(c) * inverse
        store(c, inverse * (grads(c) * gains[d, which : which + 1, :] - unit * mean))


def attend_back_pairs(first, last, qo, gm, mo, lo, kpad, vpad, bias, cos, sin, dqkv, dkey, dval):
    rows = qo.shape[0]

    @pl.loop(first, last)
    def _(pair):
        lanes = pl.ds(pl.multiple_of(pair * LANES, LANES), LANES)
        for start, block, seen in query_cuts(rows):
            at = slice(start, start + block)
            lane = lane_index((block, LANES))
            query, grad = qo[at, lanes], gm[at, lanes]
            both = grad.astype(F32) * mo[at, lanes].astype(F32)
            logs = lo[at, :]
            dq = jnp.zeros((block, LANES), F32)
            for side in range(2):
                inside = (lane >= HD) if side else (lane < HD)
                delta = jnp.sum(jnp.where(inside, both, 0.0), axis=-1, keepdims=True)
                log = jnp.sum(
                    jnp.where(lane == 2 * pair + side, logs, 0.0), axis=-1, keepdims=True
                )
                key, value = kpad[side, :seen, :], vpad[side, :seen, :]
                probs = jnp.exp(dot(query, key, 1, 1) + bias[at, :seen] - log)
                grad_scores = (probs * (dot(grad, value, 1, 1) - delta)).astype(BF)
                dq = dq + dot(grad_scores, key)
                dkey[side, :seen, :] += dot(grad_scores, query, 0, 0)
                dval[side, :seen, :] += dot(probs.astype(BF), grad, 0, 0)
            dq = dq * HD ** (-0.5)
            dqkv[at, lanes] = (dq * cos[at, :] - swapped(dq) * sin[at, :]).astype(BF)


PIECES = 4


def vmem():
    return pl.BlockSpec(memory_space=pltpu.VMEM)


def hbm():
    return pl.BlockSpec(memory_space=pl.ANY)


def dma(*shape):
    return pltpu.SemaphoreType.DMA(shape)


def line_scratch(nt, rows, model):
    return [pltpu.VMEM((nt, rows, model), BF), pltpu.VMEM((nt + 1, rows, model), BF)]


def ticks(pieces, nt):
    return [
        [(k, tick - k) for k in range(1, nt) if 0 <= tick - k < pieces]
        for tick in range(pieces + nt - 1)
    ]


def layer_kernel(
    nt, width,
    x, cot, gain_a, gain_f, segr, wq, wkt, wvt, wo, gate, up, down,
    y, gi, gain_out, d_wq, d_kv, d_wo, d_down, d_gate, d_up, wqkv_f, wo_f, na_f,
    rowsbuf, cf, branch, act, hid, gate_v, up_v, down_v, part, sent, arrived, totals, landed, stage_v,
    own_qkv, gain, gall, qo, kvo, mo, lo, cos, sin, gsum, zslots, dslots,
    gain_sem, place_sem, out_sem, x_sem, cot_sem, nf_sem, br_sem, o_sem, gn_sem, y_sem, gi_sem,
    hs, hr, ps, pr, zsem, dsem, ready, calm,
):
    me, t = lax.axis_index("dp"), lax.axis_index("tensor")
    nd = 1 << width
    rows, model = x.shape
    tokens = nt * rows
    queries = wq.shape[1]
    hidden = gate.shape[1]
    shard = model >> width
    wide = own_qkv.shape[1]
    pieces = PIECES
    size = rows // pieces

    def natural(j, s):
        return j * rows + s * size

    def shuffled(j, s):
        return (s * nt + j) * size

    local = pl.ds(pl.multiple_of(t * rows, rows), rows)
    rowsbuf[local, :] = x[...]
    gain[...] = jnp.zeros_like(gain)
    gain[0:1, :] = gain_a[...].astype(F32)
    gain[1:2, :] = gain_f[...].astype(F32)
    own_qkv[:, :queries] = wq[...]
    turned = jnp.concatenate([wkt[...].astype(F32), wvt[...].astype(F32)], axis=0)
    own_qkv[:, queries:] = jnp.transpose(turned).astype(BF)
    with jax.named_scope("enter"):
        enter(t, nt, me, width, pltpu.get_barrier_semaphore())

    tokens_x = LineGather(rowsbuf, natural, size, t, nt, x_sem)
    for s in range(pieces):
        tokens_x.start(s)
    gathers = []
    for w, (own, full, by_rows) in enumerate(
        ((own_qkv, wqkv_f, True), (wo, wo_f, False), (gate, gate_v, True), (up, up_v, True), (down, down_v, False))
    ):
        gathers.append(
            BlockGather(own, full, by_rows, me, width, hs.at[w], hr.at[w], ps.at[w], pr.at[w])
        )
    g_qkv, g_out, g_gate, g_up, g_down = gathers
    stages = g_qkv.stages

    def gain_copy(mask):
        return remote(
            gain, gall.at[me], gain_sem.at[0, mask], gain_sem.at[1, mask],
            {"dp": flip(me, mask, width)},
        )

    for mask in range(1, nd):
        gain_copy(mask).start()
    for g in (g_qkv, g_out, g_gate):
        g.send(0)
    for w, g in enumerate(gathers):
        g.place(place_sem.at[w]).start()
    gall[me] = gain[...]

    def forward(g, stage):
        g.wait(stage)
        if stage + 1 < stages:
            g.send(stage + 1)
        else:
            g.pair_send()

    for s in range(pieces):
        cf[pl.ds(pl.multiple_of(shuffled(t, s), size), size), :] = cot[s * size : (s + 1) * size, :]
    cots = LineGather(cf, shuffled, size, t, nt, cot_sem)
    scatter_o = LineScatter(part, natural, sent, arrived, t, nt, o_sem)

    def attention(na, wqkv_v, wo_v, bias, kpad, vpad):
        bias_into(bias, segr)
        rope_into(cos, sin, segr)
        lo[...] = jnp.zeros_like(lo)
        for mask in range(1, nd):
            slot = gall.at[flip(me, mask, width)]
            remote(
                slot, slot, gain_sem.at[0, mask], gain_sem.at[1, mask],
                {"dp": flip(me, mask, width)},
            ).wait_recv()

        def norm(j):
            @pl.loop(0, pieces)
            def _(s):
                these = pl.ds(pl.multiple_of(j * rows + s * size, size), size)
                value = rowsbuf[these, :].astype(F32)

                def store(cols, normed):
                    na[these, cols] = normed.astype(BF)

                times_gain(value * inverse_of(value), gall, 0, store)

        norm(t)
        for stage in range(stages - 1):
            forward(g_qkv, stage)
            forward(g_out, stage)
        fills = [
            lambda: (forward(g_gate, 0), g_up.send(0)),
            lambda: (forward(g_qkv, stages - 1), forward(g_out, stages - 1), g_down.send(0)),
        ]
        load = pltpu.make_async_copy(wqkv_f, wqkv_v, place_sem.at[5])
        load_out = pltpu.make_async_copy(wo_f, wo_v, place_sem.at[6])

        def fetch():
            g_qkv.place(place_sem.at[0]).wait()
            g_qkv.pair_wait()
            load.start()
            g_out.place(place_sem.at[1]).wait()
            g_out.pair_wait()
            load_out.start()

        for k in range(1, nt):
            if k == nt - 1:
                for fill in fills:
                    fill()
                fills = []
                with jax.named_scope("fetch"):
                    fetch()
            with jax.named_scope("x_step"):
                for s in range(pieces):
                    tokens_x.step(k, s)
            if k == nt - 1:
                for s in range(pieces):
                    cots.start(s)

            @pl.when(t >= k)
            def _():
                norm(t - k)

            @pl.when(t + k < nt)
            def _():
                norm(t + k)

            if fills:
                with jax.named_scope("x_fill"):
                    fills.pop(0)()
        keep = pltpu.make_async_copy(na, na_f, out_sem.at[0])
        keep.start()
        with jax.named_scope("wait_qkv"):
            load.wait()
        with jax.named_scope("qkv"):
            part[:, :wide] = dot(na[...], wqkv_v[...])
            c, s_ = cos[...], sin[...]
            for start in range(0, queries, LANES):
                lanes = slice(start, start + LANES)
                value = part[:, lanes]
                qo[:, lanes] = ((value * c + swapped(value) * s_) * HD ** (-0.5)).astype(BF)
            value = part[:, queries : queries + LANES]
            keyed = jnp.where(lane_index(value.shape) < HD, value * c + swapped(value) * s_, value)
            kvo[...] = keyed.astype(BF)
            pad_pair(keyed, kpad, vpad)
        pairs = queries // LANES
        with jax.named_scope("att"):
            attend_pairs(0, pairs, qo, kpad, vpad, bias, mo, lo)
        load_out.wait()
        with jax.named_scope("outproj"):
            for start, width_ in tiles_of(model, 4):
                cols = slice(start, start + width_)
                part[:, cols] = dot(mo[...], wo_v[:, cols])
        keep.wait()
        tokens_x.finish()

    pl.run_scoped(
        attention,
        pltpu.VMEM((tokens, model), BF),
        pltpu.VMEM((model, wide), BF),
        pltpu.VMEM((queries, model), BF),
        pltpu.VMEM((tokens, tokens), F32),
        pltpu.VMEM((2, tokens, LANES), BF),
        pltpu.VMEM((2, tokens, LANES), BF),
    )

    gather_nf = LineGather(rowsbuf, shuffled, size, t, nt, nf_sem)

    def take_hidden(s):
        at = scatter_o.own(s)
        block = slice(s * size, (s + 1) * size)
        hidden_rows = x[block, :].astype(F32) + part[at, :model]
        hid[block, :] = hidden_rows
        there = pl.ds(pl.multiple_of(shuffled(t, s), size), size)

        def store(cols, normed):
            rowsbuf[there, cols] = normed.astype(BF)

        times_gain(hidden_rows * inverse_of(hidden_rows), gall, 1, store)
        gather_nf.start(s)

    scatter_o.edge(0)
    scatter_o.edge(1)
    with jax.named_scope("cot1"):
        for s in range(pieces):
            cots.step(1, s)
    with jax.named_scope("u0"):
        for stage in range(1, stages):
            forward(g_gate, stage)
        forward(g_up, 0)
    later = [
        lambda: ([cots.step(2, s) for s in range(pieces)], forward(g_down, 0)),
        lambda: [cots.step(k, s) for k in range(3, nt) for s in range(pieces)],
        lambda: [forward(g_up, stage) for stage in range(1, stages)],
        lambda: [forward(g_down, stage) for stage in range(1, stages)],
    ]
    steps = ticks(pieces, nt)

    def flow(tick, scatter, gather, take):
        todo = list(steps[tick])
        if 0 < tick < pieces - 1:
            scatter.edge(tick + 1)
        scatter.relay(scatter.near, tick)
        if todo:
            gather.step(*todo.pop(0))
        scatter.relay(scatter.far, tick)
        if todo:
            gather.step(*todo.pop(0))
        take(tick)
        for late in todo:
            gather.step(*late)

    for tick in range(pieces):
        with jax.named_scope("o_tick"):
            flow(tick, scatter_o, gather_nf, take_hidden)
        if later:
            with jax.named_scope("o_later"):
                later.pop(0)()
    for fill in later:
        fill()

    def chunk_of(left, right):
        def chunk(d):
            return dot(left[:, pl.ds(pl.multiple_of(d * shard, shard), shard)], right[...], 0, 0)

        return chunk

    def cube(w, totals_, landed_, store):
        return BlockScatter(
            None, None, totals_, landed_, store, me, width, hs.at[w], hr.at[w], ps.at[w], pr.at[w]
        )

    def store_stage(at, value):
        stage_v[at, :] = value

    def store_down(at, value):
        d_down[:, at] = value.T

    def store_qkv(at, value):
        d_wq[at, :] = value[:, :queries]
        d_kv[:, at] = value[:, queries:].T

    def store_wo(at, value):
        d_wo[:, at] = value.T

    for_qkv, for_wo = pl.ds(0, wide), pl.ds(wide, queries)
    s_gate = cube(5, totals.at[0], landed.at[0], store_stage)
    s_up = cube(6, totals.at[1], landed.at[1], store_stage)
    s_down = cube(7, totals.at[0], landed.at[0], store_down)
    s_qkv = cube(8, totals.at[1, :, :, for_qkv], landed.at[1, :, :, :, for_qkv], store_qkv)
    s_out = cube(9, totals.at[1, :, :, for_wo], landed.at[1, :, :, :, for_wo], store_wo)

    def take(s):
        s.take()
        s.send(0)

    def on(s, stage):
        s.add(stage)
        if stage + 1 < stages:
            s.send(stage + 1)

    gsum[...] = jnp.zeros_like(gsum)
    gather_br = LineGather(branch, natural, size, t, nt, br_sem)

    def feed(dg, du, given):
        cuts = tiles_of(hidden, 6)
        span = max(width_ for _, width_ in cuts)
        half = tokens // 2
        block = 64
        draft = half

        def tile(h, i):
            start, width_ = cuts[i]
            at = slice(start, start + width_)
            mine = slice(h * half, (h + 1) * half)
            held = slice(draft, draft + half)
            part[held, 0:width_] = dot(rowsbuf[mine, :], gate_v[:, at])
            part[held, span : span + width_] = dot(rowsbuf[mine, :], up_v[:, at])
            part[held, 2 * span : 2 * span + width_] = dot(cf[mine, :], down_v[at, :], 1, 1)

            @pl.loop(0, half // block)
            def _(k):
                from_ = pl.ds(pl.multiple_of(draft + k * block, block), block)
                to = pl.ds(pl.multiple_of(h * half + k * block, block), block)
                g = part[from_, 0:width_]
                u = part[from_, span : span + width_]
                ga = part[from_, 2 * span : 2 * span + width_]
                sig = 1.0 / (1.0 + jnp.exp(-g))
                gs = g * sig
                act[to, at] = (gs * u).astype(BF)
                du[to, at] = (ga * gs).astype(BF)
                dg[to, at] = (ga * u * sig * (1.0 + g * (1.0 - sig))).astype(BF)

        def back_dots(h):
            mine = slice(h * half, (h + 1) * half)
            for start, width_ in tiles_of(model, 4):
                cols = slice(start, start + width_)
                part[mine, cols] = dot(dg[mine, :], gate_v[cols, :], 1, 1) + dot(
                    du[mine, :], up_v[cols, :], 1, 1
                )

        scatter_gn = LineScatter(part, shuffled, sent, arrived, t, nt, gn_sem)

        def take_grad(s):
            at = scatter_gn.own(s)
            block_ = slice(s * size, (s + 1) * size)
            there = pl.ds(pl.multiple_of(natural(t, s), size), size)

            def store(cols, value):
                total = cot[block_, cols].astype(F32) + value
                gi[block_, cols] = total
                branch[there, cols] = total.astype(BF)

            def store_gain(cols, value):
                gsum[1:2, cols] += value

            back_through_norm(
                lambda c: hid[block_, c], lambda c: part[at, c], gall, 1, store, store_gain
            )
            gather_br.start(s)

        s_gate.chunk, s_up.chunk = chunk_of(rowsbuf, dg), chunk_of(rowsbuf, du)
        s_gate.sent = s_up.sent = given

        with jax.named_scope("wait_ffn"):
            for w in (2, 3, 4):
                gathers[w].place(place_sem.at[w]).wait()
                gathers[w].pair_wait()
        work = [lambda i=i: tile(0, i) for i in range(len(cuts))]
        for late in steps[pieces:]:
            with jax.named_scope("nf_step"):
                for k, s in late:
                    gather_nf.step(k, s)
            if work:
                with jax.named_scope("tile"):
                    work.pop(0)()
        for job in work:
            job()
        scatter_o.finish()
        with jax.named_scope("back_dots"):
            back_dots(0)
        scatter_gn.edge(0)
        scatter_gn.edge(1)
        with jax.named_scope("tile"):
            tile(1, 0)
        with jax.named_scope("gn_round"):
            scatter_gn.relay(scatter_gn.near, 0)
        with jax.named_scope("tile"):
            for i in range(1, len(cuts)):
                tile(1, i)
        with jax.named_scope("gn_round"):
            scatter_gn.relay(scatter_gn.far, 0)
        with jax.named_scope("back_dots"):
            back_dots(1)
        with jax.named_scope("gn_take"):
            take_grad(0)
        with jax.named_scope("gn_fill"):
            s_gate.give()
        fills = [
            lambda: take(s_gate),
            lambda: (s_gate.given(), s_up.give()),
            lambda: take(s_up),
        ]
        for tick in range(1, pieces):
            with jax.named_scope("gn_tick"):
                flow(tick, scatter_gn, gather_br, take_grad)
            if fills:
                with jax.named_scope("gn_fill"):
                    fills.pop(0)()
        for k, s in steps[pieces]:
            gather_br.step(k, s)
        scatter_gn.finish()
        s_up.given()

    pl.run_scoped(
        feed,
        pltpu.VMEM((tokens, hidden), BF),
        pltpu.VMEM((tokens, hidden), BF),
        pltpu.VMEM((nd // 2, shard, hidden), BF),
    )

    wo_v = down_v.at[pl.ds(0, queries), :]
    na_v = down_v.at[pl.ds(queries, tokens), :]
    wqkv_v = gate_v.at[:, pl.ds(0, wide)]
    gm = up_v.at[pl.ds(0, tokens), pl.ds(0, queries)]
    dqkv = up_v.at[pl.ds(tokens, tokens), pl.ds(0, wide)]

    def rear(bias, kpad, vpad, dkey, dval, given):
        scatter_y = LineScatter(part, shuffled, sent, arrived, t, nt, y_sem)
        inward = LineScatter(part, natural, sent, arrived, t, nt, gi_sem)
        with jax.named_scope("down"):
            for start, width_ in tiles_of(model, 4):
                cols = slice(start, start + width_)
                part[:, cols] = dot(act[...], down_v[:, cols])
            for s in range(pieces):
                scatter_y.edge(s)
        for g in (g_gate, g_up, g_down):
            g.drain()
        loads = [
            pltpu.make_async_copy(wo_f, wo_v, place_sem.at[0]),
            pltpu.make_async_copy(wqkv_f, wqkv_v, place_sem.at[1]),
            pltpu.make_async_copy(na_f, na_v, place_sem.at[2]),
        ]
        for load in loads:
            load.start()
        bias_into(bias, segr)
        pad_pair(kvo[...].astype(F32), kpad, vpad)
        dkey[...] = jnp.zeros_like(dkey)
        dval[...] = jnp.zeros_like(dval)
        s_down.chunk, s_down.sent = chunk_of(cf, act), given
        s_qkv.chunk, s_qkv.sent = chunk_of(na_v, dqkv), given.at[:, :, for_qkv]
        s_out.chunk, s_out.sent = chunk_of(branch, mo), given.at[:, :, for_wo]

        def pass_y(s):
            with jax.named_scope("y_relay"):
                scatter_y.relay(scatter_y.near, s)
                scatter_y.relay(scatter_y.far, s)

        def att(first, last):
            with jax.named_scope("b_att"):
                attend_back_pairs(
                    first, last, qo, gm, mo, lo, kpad, vpad, bias, cos, sin, dqkv, dkey, dval
                )

        def free(s, out, slot):
            s.add(stages - 1)
            copy = pltpu.make_async_copy(stage_v, out, out_sem.at[1 + slot])
            copy.start()
            s.drain()
            for bit in range(width):
                pl.semaphore_signal(
                    ready.at[slot], inc=1, device_id={"dp": flip(me, 1 << bit, width)},
                    device_id_type=pl.DeviceIdType.MESH,
                )
            return copy

        pairs = queries // LANES
        rest = list(steps[pieces + 1 :])
        jobs = [functools.partial(on, s, stage) for stage in range(stages - 1) for s in (s_gate, s_up)]
        for s in range(pieces - 2):
            pass_y(s)
            if rest:
                with jax.named_scope("br_step"):
                    for k, s_ in rest.pop(0):
                        gather_br.step(k, s_)
            if jobs:
                with jax.named_scope("y_fill"):
                    jobs.pop(0)()
        for late in rest:
            with jax.named_scope("br_step"):
                for k, s_ in late:
                    gather_br.step(k, s_)
        for job in jobs:
            job()
        with jax.named_scope("b_gm"):
            loads[0].wait()
            gm[...] = dot(branch[...], wo_v[...], 1, 1).astype(BF)
        att(0, pairs // 2)
        pass_y(pieces - 2)
        with jax.named_scope("free0"):
            copy_gate = free(s_gate, d_gate, 0)
        att(pairs // 2, pairs)
        pass_y(pieces - 1)
        with jax.named_scope("b_give"):
            pl.semaphore_wait(ready.at[0], width)
            s_down.give()
        key = dkey[0] + pltpu.roll(dkey[1], HD, 1)
        value = pltpu.roll(dval[0], HD, 1) + dval[1]
        key = key * cos[...] - swapped(key) * sin[...]
        dqkv[:, queries : queries + LANES] = jnp.where(
            lane_index(key.shape) < HD, key, value
        ).astype(BF)
        with jax.named_scope("y_own"):
            for s in range(pieces):
                at = scatter_y.own(s)
                block_ = slice(s * size, (s + 1) * size)
                y[block_, :] = (hid[block_, :] + part[at, :model]).astype(BF)
            scatter_y.finish()

        @pl.when(t > 0)
        def _():
            pl.semaphore_signal(
                calm.at[0], inc=1, device_id={"tensor": t - 1}, device_id_type=pl.DeviceIdType.MESH
            )

        @pl.when(t < nt - 1)
        def _():
            pl.semaphore_signal(
                calm.at[0], inc=1, device_id={"tensor": t + 1}, device_id_type=pl.DeviceIdType.MESH
            )

        with jax.named_scope("b_part"):
            loads[1].wait()
            for start, width_ in tiles_of(model, 4):
                part[:, start : start + width_] = dot(
                    dqkv[...], wqkv_v[start : start + width_, :], 1, 1
                )
        with jax.named_scope("calm"):
            pl.semaphore_wait(calm.at[0], lax.min(t, 1) + lax.min(nt - 1 - t, 1))
            for s in range(pieces):
                inward.edge(s)
            loads[2].wait()

        def take_grad(s):
            at = inward.own(s)
            block = slice(s * size, (s + 1) * size)

            def store(cols, value):
                gi[block, cols] += value

            def store_gain(cols, value):
                gsum[0:1, cols] += value

            back_through_norm(
                lambda c: x[block, c].astype(F32), lambda c: part[at, c], gall, 0, store, store_gain
            )

        copies = []

        def free_up():
            s_down.given()
            copy_gate.wait()
            copies.append(free(s_up, d_up, 1))

        def give_small():
            pl.semaphore_wait(ready.at[1], width)
            s_qkv.give()

        fills = [
            give_small,
            lambda: (take(s_qkv), s_out.give()),
            lambda: take(s_out),
        ]
        fills += [
            functools.partial(on, s, stage)
            for stage in range(stages)
            for s in (s_down, s_qkv, s_out)
        ]
        with jax.named_scope("b_take"):
            take(s_down)
        with jax.named_scope("free1"):
            free_up()
        for s in range(pieces):
            with jax.named_scope("b_relay"):
                inward.relay(inward.near, s)
                inward.relay(inward.far, s)
            with jax.named_scope("b_fill"):
                fills.pop(0)()
        with jax.named_scope("b_own"):
            for s in range(pieces):
                take_grad(s)
                if s < pieces - 1 and fills:
                    fills.pop(0)()
        with jax.named_scope("b_gains"):
            zslots[t] = gsum[...]

            def along(step):
                return remote(
                    zslots.at[t], zslots.at[t], zsem.at[0, step], zsem.at[1, step],
                    {"tensor": lax.rem(t + step, nt)},
                )

            for step in range(1, nt):
                along(step).start()
        with jax.named_scope("b_rest"):
            for fill in fills:
                fill()
        with jax.named_scope("b_gains"):
            for step in range(1, nt):
                slot = zslots.at[lax.rem(t + nt - step, nt)]
                remote(
                    slot, slot, zsem.at[0, step], zsem.at[1, step], {"tensor": lax.rem(t + step, nt)}
                ).wait_recv()
            gsum[...] = sum(zslots[i] for i in range(nt))

            def across(mask):
                peer = flip(me, mask, width)
                return remote(
                    gsum.at[:, pl.ds(pl.multiple_of(peer * shard, shard), shard)], dslots.at[me],
                    dsem.at[0, mask], dsem.at[1, mask], {"dp": peer},
                )

            for mask in range(1, nd):
                across(mask).start()
            dslots[me] = gsum[:, pl.ds(pl.multiple_of(me * shard, shard), shard)]
            for mask in range(1, nd):
                peer = flip(me, mask, width)
                slot = dslots.at[peer]
                remote(slot, slot, dsem.at[0, mask], dsem.at[1, mask], {"dp": peer}).wait_recv()
            gain_out[...] = sum(dslots[i] for i in range(nd))
            for step in range(1, nt):
                along(step).wait_send()
            for mask in range(1, nd):
                across(mask).wait_send()
        with jax.named_scope("end"):
            for s in (s_qkv, s_out):
                s.given()
            for s in (s_down, s_qkv, s_out):
                s.drain()
            inward.finish()
            for copy in copies:
                copy.wait()

    pl.run_scoped(
        rear,
        pltpu.VMEM((tokens, tokens), F32),
        pltpu.VMEM((2, tokens, LANES), BF),
        pltpu.VMEM((2, tokens, LANES), BF),
        pltpu.VMEM((2, tokens, LANES), F32),
        pltpu.VMEM((2, tokens, LANES), F32),
        pltpu.VMEM((nd // 2, shard, hidden), BF),
    )
    for g in (g_qkv, g_out):
        g.drain()
    for mask in range(1, nd):
        gain_copy(mask).wait_send()
    cots.finish()
    gather_nf.finish()
    gather_br.finish()


def layer(nt, nd, x, cot, gain_a, gain_f, segr, wq, wkt, wvt, wo, gate, up, down):
    width = nd.bit_length() - 1
    rows, model = x.shape
    tokens = nt * rows
    queries = wq.shape[1]
    hidden = gate.shape[1]
    shard = model // nd
    half = nd // 2
    wide = queries + LANES
    span = max(width_ for _, width_ in tiles_of(hidden, 6))
    shape = jax.ShapeDtypeStruct
    outs = [
        (shape((rows, model), BF), vmem()),
        (shape((rows, model), F32), vmem()),
        (shape((8, shard), F32), vmem()),
        (shape((shard, queries), F32), vmem()),
        (shape((LANES, shard), F32), vmem()),
        (shape((queries, shard), F32), vmem()),
        (shape((hidden, shard), F32), vmem()),
        (shape((shard, hidden), F32), hbm()),
        (shape((shard, hidden), F32), hbm()),
        (shape((model, wide), BF), hbm()),
        (shape((queries, model), BF), hbm()),
        (shape((tokens, model), BF), hbm()),
    ]
    return pl.pallas_call(
        functools.partial(layer_kernel, nt, width),
        out_shape=[o for o, _ in outs],
        in_specs=[vmem()] * 8 + [hbm()] * 4,
        out_specs=[s for _, s in outs],
        scratch_shapes=[
            pltpu.VMEM((tokens, model), BF),
            pltpu.VMEM((tokens, model), BF),
            pltpu.VMEM((tokens, model), BF),
            pltpu.VMEM((tokens, hidden), BF),
            pltpu.VMEM((rows, model), F32),
            pltpu.VMEM((model, hidden), BF),
            pltpu.VMEM((model, hidden), BF),
            pltpu.VMEM((hidden, model), BF),
            pltpu.VMEM((max(tokens, 2 * shard), max(model, 3 * span)), F32),
        ]
        + line_scratch(nt, rows, model)
        + [
            pltpu.VMEM((2, half, shard, hidden), BF),
            pltpu.VMEM((2, 2, half - 1, shard // 2, hidden), BF),
            pltpu.VMEM((shard, hidden), F32),
            pltpu.VMEM((shard, wide), BF),
            pltpu.VMEM((8, shard), F32),
            pltpu.VMEM((nd, 8, shard), F32),
            pltpu.VMEM((tokens, queries), BF),
            pltpu.VMEM((tokens, LANES), BF),
            pltpu.VMEM((tokens, queries), BF),
            pltpu.VMEM((tokens, LANES), F32),
            pltpu.VMEM((tokens, LANES), F32),
            pltpu.VMEM((tokens, LANES), F32),
            pltpu.VMEM((8, model), F32),
            pltpu.VMEM((nt, 8, model), F32),
            pltpu.VMEM((nd, 8, shard), F32),
            dma(2, nd),
            dma(7),
            dma(3),
            dma(4, nt, PIECES),
            dma(4, nt, PIECES),
            dma(4, nt, PIECES),
            dma(4, nt, PIECES),
            dma(2, 2, nt, PIECES),
            dma(2, 2, nt, PIECES),
            dma(2, 2, nt, PIECES),
            dma(2, 2, nt, PIECES),
            dma(10, 2, half),
            dma(10, 2, half),
            dma(10, half),
            dma(10, half),
            dma(2, nt),
            dma(2, nd),
            pltpu.SemaphoreType.REGULAR((2,)),
            pltpu.SemaphoreType.REGULAR((1,)),
        ],
        compiler_params=pltpu.CompilerParams(
            collective_id=0, has_side_effects=True, vmem_limit_bytes=VMEM_BYTES
        ),
        name="layer",
    )(x, cot, gain_a, gain_f, segr, wq, wkt, wvt, wo, gate, up, down)


def narrow_scatter(value, axis, scatter_dimension, tiled):
    low = value.astype(BF) if value.ndim == 2 else value
    return lax.psum_scatter(low, axis, scatter_dimension=scatter_dimension, tiled=tiled).astype(F32)


def rope_tables(segments, head_dim):
    row_count = segments.shape[0]
    row_index = jnp.arange(row_count, dtype=jnp.int32)
    change = jnp.concatenate(
        [jnp.ones((1,), jnp.int32), (segments[1:] != segments[:-1]).astype(jnp.int32)]
    )
    starts = lax.cummax(jnp.where(change > 0, row_index, jnp.zeros_like(row_index)), axis=0)
    position = (row_index - starts).astype(F32)
    half_dim = head_dim // 2
    frequency = jnp.exp(jnp.arange(half_dim, dtype=F32) * (-math.log(10000.0) / half_dim))
    angles = position[:, None] * frequency[None, :]
    return (jnp.cos(angles)[:, None, :], jnp.sin(angles)[:, None, :])


def rotate(tensor, cosine, sine):
    half_dim = tensor.shape[-1] // 2
    first_half = tensor[..., :half_dim]
    second_half = tensor[..., half_dim:]
    return jnp.concatenate(
        [first_half * cosine - second_half * sine, second_half * cosine + first_half * sine],
        axis=-1,
    )


def unrotate(tensor, cosine, sine):
    half_dim = tensor.shape[-1] // 2
    first_half = tensor[..., :half_dim]
    second_half = tensor[..., half_dim:]
    return jnp.concatenate(
        [first_half * cosine + second_half * sine, second_half * cosine - first_half * sine],
        axis=-1,
    )


def visible(segments):
    row_index = jnp.arange(segments.shape[0], dtype=jnp.int32)
    same_seq = segments[:, None] == segments[None, :]
    return same_seq & (row_index[:, None] >= row_index[None, :])


def normalize(values, gain):
    inverse = lax.rsqrt(jnp.mean(values * values, axis=-1, keepdims=True) + EPSILON)
    unit_rows = values * inverse
    return (unit_rows, inverse, (unit_rows * gain.astype(F32)).astype(BF))


def normalize_back(grad_normed, unit_rows, inverse, gain):
    scaled = grad_normed * gain.astype(F32)
    grad_values = inverse * (
        scaled - unit_rows * jnp.mean(scaled * unit_rows, axis=-1, keepdims=True)
    )
    return (grad_values, jnp.sum(grad_normed * unit_rows, axis=0))


def contract(left, right, left_dim, right_dim):
    return lax.dot_general(
        left, right, (((left_dim,), (right_dim,)), ((), ())), preferred_element_type=F32
    )


def block_scores(query_block, key_heads, allowed_block, score_scale):
    scores = (
        jnp.einsum("rkgd,skd->kgrs", query_block, key_heads, preferred_element_type=F32)
        * score_scale
    )
    return jnp.where(allowed_block[None, None], scores, NEGATIVE)


def attend_forward(query_groups, key_heads, value_heads, allowed, score_scale):
    scores = block_scores(query_groups, key_heads, allowed, score_scale)
    row_max = jnp.max(scores, axis=-1, keepdims=True)
    log_total = row_max + jnp.log(jnp.sum(jnp.exp(scores - row_max), axis=-1, keepdims=True))
    probs_low = jnp.exp(scores - log_total).astype(BF)
    mixed_parts = jnp.einsum(
        "kgrs,skd->rkgd", probs_low, value_heads, preferred_element_type=F32
    ).astype(BF)
    return (mixed_parts, log_total)


def attend_backward(
    query_groups, key_heads, value_heads, mixed_heads, grad_mixed, log_totals, allowed, score_scale
):
    scores = block_scores(query_groups, key_heads, allowed, score_scale)
    attn_probs = jnp.exp(scores - log_totals)
    probs_low = attn_probs.astype(BF)
    grad_probs = jnp.einsum(
        "rkgd,skd->kgrs", grad_mixed, value_heads, preferred_element_type=F32
    )
    row_delta = jnp.sum(grad_mixed.astype(F32) * mixed_heads.astype(F32), axis=-1)
    row_delta = jnp.transpose(row_delta, (1, 2, 0))[..., None]
    grad_scores = (attn_probs * (grad_probs - row_delta)).astype(BF)
    query_parts = (
        jnp.einsum("kgrs,skd->rkgd", grad_scores, key_heads, preferred_element_type=F32)
        * score_scale
    )
    grad_key_rot = (
        jnp.einsum("kgrs,rkgd->skd", grad_scores, query_groups, preferred_element_type=F32)
        * score_scale
    )
    grad_value_heads = jnp.einsum(
        "kgrs,rkgd->skd", probs_low, grad_mixed, preferred_element_type=F32
    )
    return (query_parts, grad_key_rot, grad_value_heads)


def plain_device(
    layer_input,
    segment_ids,
    norm_attn,
    w_query,
    w_key,
    w_value,
    w_output,
    norm_ffn,
    w_gate,
    w_up,
    w_down,
    cotangent,
):
    score_scale = HD ** (-0.5)
    query_full, key_full, value_full, output_full, gain_attn = (
        lax.all_gather(w_query, "dp", axis=0, tiled=True),
        lax.all_gather(w_key, "dp", axis=0, tiled=True),
        lax.all_gather(w_value, "dp", axis=0, tiled=True),
        lax.all_gather(w_output, "dp", axis=1, tiled=True),
        lax.all_gather(norm_attn, "dp", axis=0, tiled=True),
    )
    gate_full, up_full, down_full, gain_ffn = (
        lax.all_gather(w_gate, "dp", axis=0, tiled=True),
        lax.all_gather(w_up, "dp", axis=0, tiled=True),
        lax.all_gather(w_down, "dp", axis=1, tiled=True),
        lax.all_gather(norm_ffn, "dp", axis=0, tiled=True),
    )
    heads_local = query_full.shape[1] // HD
    kv_local = key_full.shape[1] // HD
    group = heads_local // kv_local
    residual_in = layer_input.astype(F32)
    unit_attn, inverse_attn, normed_local = normalize(residual_in, gain_attn)
    normed_attn = lax.all_gather(normed_local, "tensor", axis=0, tiled=True)
    row_count = normed_attn.shape[0]
    cosine, sine = rope_tables(segment_ids, HD)
    allowed = visible(segment_ids)
    query_heads = rotate(
        jnp.dot(normed_attn, query_full, preferred_element_type=F32).reshape(
            row_count, heads_local, HD
        ),
        cosine,
        sine,
    ).astype(BF)
    query_groups = query_heads.reshape(row_count, kv_local, group, HD)
    key_heads = rotate(
        jnp.dot(normed_attn, key_full, preferred_element_type=F32).reshape(
            row_count, kv_local, HD
        ),
        cosine,
        sine,
    ).astype(BF)
    value_heads = (
        jnp.dot(normed_attn, value_full, preferred_element_type=F32)
        .astype(BF)
        .reshape(row_count, kv_local, HD)
    )
    mixed_heads, log_totals = attend_forward(
        query_groups, key_heads, value_heads, allowed, score_scale
    )
    mixed_flat = mixed_heads.reshape(row_count, heads_local * HD)
    hidden_res = residual_in + narrow_scatter(
        jnp.dot(mixed_flat, output_full, preferred_element_type=F32),
        "tensor",
        scatter_dimension=0,
        tiled=True,
    )
    unit_ffn, inverse_ffn, normed_ffn_local = normalize(hidden_res, gain_ffn)
    normed_ffn = lax.all_gather(normed_ffn_local, "tensor", axis=0, tiled=True)
    gate_rows = jnp.dot(normed_ffn, gate_full, preferred_element_type=F32)
    up_rows = jnp.dot(normed_ffn, up_full, preferred_element_type=F32)
    sigmoid_gate = jax.nn.sigmoid(gate_rows)
    active = (gate_rows * sigmoid_gate * up_rows).astype(BF)
    layer_output = (
        hidden_res
        + narrow_scatter(
            jnp.dot(active, down_full, preferred_element_type=F32).astype(BF),
            "tensor",
            scatter_dimension=0,
            tiled=True,
        ).astype(F32)
    ).astype(BF)
    query_full, key_full, value_full, output_full, gate_full, up_full, down_full = (
        lax.all_gather(w_query, "dp", axis=0, tiled=True),
        lax.all_gather(w_key, "dp", axis=0, tiled=True),
        lax.all_gather(w_value, "dp", axis=0, tiled=True),
        lax.all_gather(w_output, "dp", axis=1, tiled=True),
        lax.all_gather(w_gate, "dp", axis=0, tiled=True),
        lax.all_gather(w_up, "dp", axis=0, tiled=True),
        lax.all_gather(w_down, "dp", axis=1, tiled=True),
    )
    cotangent_full = lax.all_gather(cotangent, "tensor", axis=0, tiled=True)
    grad_active = contract(cotangent_full, down_full, 1, 1)
    grad_w_down = contract(active, cotangent_full, 0, 0)
    grad_up_rows = (grad_active * gate_rows * sigmoid_gate).astype(BF)
    grad_gate_rows = (
        grad_active * up_rows * sigmoid_gate * (1.0 + gate_rows * (1.0 - sigmoid_gate))
    ).astype(BF)
    grad_w_gate = contract(normed_ffn, grad_gate_rows, 0, 0)
    grad_w_up = contract(normed_ffn, grad_up_rows, 0, 0)
    grad_normed_ffn = narrow_scatter(
        contract(grad_gate_rows, gate_full, 1, 1) + contract(grad_up_rows, up_full, 1, 1),
        "tensor",
        scatter_dimension=0,
        tiled=True,
    )
    grad_hidden, gain_ffn_part = normalize_back(grad_normed_ffn, unit_ffn, inverse_ffn, gain_ffn)
    grad_hidden = cotangent.astype(F32) + grad_hidden
    branch_full = lax.all_gather(grad_hidden.astype(BF), "tensor", axis=0, tiled=True)
    grad_mixed = contract(branch_full, output_full, 1, 1).astype(BF)
    grad_w_output = contract(mixed_flat, branch_full, 0, 0)
    grad_query_rot, grad_key_rot, grad_value_heads = attend_backward(
        query_groups,
        key_heads,
        value_heads,
        mixed_heads,
        grad_mixed.reshape(row_count, kv_local, group, HD),
        log_totals,
        allowed,
        score_scale,
    )
    grad_queries = (
        unrotate(grad_query_rot.reshape(row_count, heads_local, HD), cosine, sine)
        .reshape(row_count, heads_local * HD)
        .astype(BF)
    )
    grad_keys = (
        unrotate(grad_key_rot, cosine, sine).reshape(row_count, kv_local * HD).astype(BF)
    )
    grad_values = grad_value_heads.reshape(row_count, kv_local * HD).astype(BF)
    grad_w_query = contract(normed_attn, grad_queries, 0, 0)
    grad_w_key = contract(normed_attn, grad_keys, 0, 0)
    grad_w_value = contract(normed_attn, grad_values, 0, 0)
    grad_normed_attn = narrow_scatter(
        contract(grad_queries, query_full, 1, 1)
        + contract(grad_keys, key_full, 1, 1)
        + contract(grad_values, value_full, 1, 1),
        "tensor",
        scatter_dimension=0,
        tiled=True,
    )
    grad_residual, gain_attn_part = normalize_back(
        grad_normed_attn, unit_attn, inverse_attn, gain_attn
    )
    grad_input = grad_hidden + grad_residual
    gain_attn_total, gain_ffn_total = lax.psum((gain_attn_part, gain_ffn_part), "tensor")
    owned = (
        narrow_scatter(grad_w_query, "dp", scatter_dimension=0, tiled=True),
        narrow_scatter(grad_w_key, "dp", scatter_dimension=0, tiled=True),
        narrow_scatter(grad_w_value, "dp", scatter_dimension=0, tiled=True),
        narrow_scatter(grad_w_output, "dp", scatter_dimension=1, tiled=True),
        narrow_scatter(gain_attn_total, "dp", scatter_dimension=0, tiled=True),
        narrow_scatter(gain_ffn_total, "dp", scatter_dimension=0, tiled=True),
        narrow_scatter(grad_w_gate, "dp", scatter_dimension=0, tiled=True),
        narrow_scatter(grad_w_up, "dp", scatter_dimension=0, tiled=True),
        narrow_scatter(grad_w_down, "dp", scatter_dimension=1, tiled=True),
    )
    return (
        layer_output,
        grad_input,
        owned[4],
        owned[0],
        owned[1],
        owned[2],
        owned[3],
        owned[5],
        owned[6],
        owned[7],
        owned[8],
    )


def with_kernels(nt, nd, layer_input, segment_ids, norm_attn, w_query, w_key, w_value, w_output, norm_ffn, w_gate, w_up, w_down, cotangent):
    y, gi, gains, d_wq, d_kv, d_wo, d_down, d_gate, d_up, *_ = layer(
        nt, nd, layer_input, cotangent, norm_attn[None, :], norm_ffn[None, :], segment_ids[None, :],
        w_query, w_key.T, w_value.T, w_output, w_gate, w_up, w_down,
    )
    k = w_key.shape[1]
    return (
        y, gi, gains[0], d_wq, d_kv[:k].T, d_kv[k:].T, d_wo, gains[1], d_gate, d_up, d_down
    )


def fits(nt, nd, shards):
    layer_input, segment_ids, norm_attn, w_query, w_key, w_value, w_output, norm_ffn, w_gate, w_up, w_down, _ = shards
    return (
        nd >= 4
        and nd & (nd - 1) == 0
        and nt >= 2
        and norm_attn.shape[0] % LANES == 0
        and w_output.shape[1] % LANES == 0
        and w_gate.shape[1] % LANES == 0
        and w_query.shape[1] % LANES == 0
        and w_key.shape[1] == HD
        and segment_ids.shape[0] == nt * layer_input.shape[0]
        and segment_ids.shape[0] % LANES == 0
    )


def on_device(nt, nd, *shards):
    if fits(nt, nd, shards):
        return with_kernels(nt, nd, *shards)
    return plain_device(*shards)


def solution(mesh):
    placed = (
        P(("dp", "tensor"), None),
        P("dp"),
        P("dp"),
        P("dp", "tensor"),
        P("dp", "tensor"),
        P("dp", "tensor"),
        P("tensor", "dp"),
        P("dp"),
        P("dp", "tensor"),
        P("dp", "tensor"),
        P("tensor", "dp"),
        P(("dp", "tensor"), None),
    )
    return jax.shard_map(
        functools.partial(on_device, mesh.shape["tensor"], mesh.shape["dp"]),
        mesh=mesh,
        in_specs=placed,
        out_specs=(
            P(("dp", "tensor"), None),
            P(("dp", "tensor"), None),
            P("dp"),
            P("dp", "tensor"),
            P("dp", "tensor"),
            P("dp", "tensor"),
            P("tensor", "dp"),
            P("dp"),
            P("dp", "tensor"),
            P("dp", "tensor"),
            P("tensor", "dp"),
        ),
        check_vma=False,
    )
```

```python
import functools
import math

import jax
import jax.numpy as jnp
from jax import lax
from jax.experimental import pallas as pl
from jax.experimental.pallas import tpu as pltpu
from jax.sharding import PartitionSpec as P

HD = 64
EPSILON = 1e-05
NEGATIVE = -1e30
LANES = 128
BF = jnp.bfloat16
F32 = jnp.float32
VMEM_BYTES = 67_000_000


def spans(bits):
    masks = [0]
    for bit in bits:
        masks = masks + [mask | (1 << bit) for mask in masks]
    return masks


def flip(index, mask, width):
    total = 0
    for bit in range(width):
        own = lax.rem(lax.div(index, 1 << bit), 2)
        if isinstance(mask, int):
            other = (mask >> bit) & 1
        else:
            other = lax.rem(lax.div(mask, 1 << bit), 2)
        total = total + lax.rem(own + other, 2) * (1 << bit)
    return total


def aligned(value, step):
    return value if isinstance(value, int) else pl.multiple_of(value, step)


def remote(src, dst, send_sem, recv_sem, device):
    return pltpu.make_async_remote_copy(
        src_ref=src,
        dst_ref=dst,
        send_sem=send_sem,
        recv_sem=recv_sem,
        device_id=device,
        device_id_type=pl.DeviceIdType.MESH,
    )


def dot(left, right, left_dim=1, right_dim=0):
    return lax.dot_general(
        left, right, (((left_dim,), (right_dim,)), ((), ())), preferred_element_type=F32
    )


def tiles_of(size, most):
    units = size // LANES
    parts = -(-units // most)
    cuts, start = [], 0
    for part in range(parts):
        width = (units // parts + (1 if part < units % parts else 0)) * LANES
        cuts.append((start, width))
        start += width
    return cuts


def enter(t, nt, me, width, barrier, everyone_along_tensor=False):
    signal = functools.partial(
        pl.semaphore_signal, barrier, inc=1, device_id_type=pl.DeviceIdType.MESH
    )
    for mask in range(1, 1 << width):
        signal(device_id={"dp": flip(me, mask, width)})
    if everyone_along_tensor:
        for step in range(1, nt):
            signal(device_id={"tensor": lax.rem(t + step, nt)})
        pl.semaphore_wait(barrier, (1 << width) - 1 + nt - 1)
        return

    @pl.when(t > 0)
    def _():
        signal(device_id={"tensor": t - 1})

    @pl.when(t < nt - 1)
    def _():
        signal(device_id={"tensor": t + 1})

    neighbours = lax.min(t, 1) + lax.min(nt - 1 - t, 1)
    pl.semaphore_wait(barrier, (1 << width) - 1 + neighbours)


class LineGather:
    def __init__(self, full, row, size, t, nt, sems):
        self.full, self.row, self.size = full, row, size
        self.t, self.nt, self.sems = t, nt, sems
        self.pieces = sems.shape[2]
        self.done = set()

    def window(self, j, s):
        return self.full.at[pl.ds(aligned(self.row(j, s), self.size), self.size), :]

    def right(self, j, s):
        at = self.window(j, s)
        return remote(
            at, at, self.sems.at[0, j, s], self.sems.at[2, j, s],
            {"tensor": lax.rem(self.t + 1, self.nt)},
        )

    def left(self, j, s):
        at = self.window(j, s)
        return remote(
            at, at, self.sems.at[1, j, s], self.sems.at[3, j, s],
            {"tensor": lax.rem(self.t + self.nt - 1, self.nt)},
        )

    def start(self, s):
        @pl.when(self.t < self.nt - 1)
        def _():
            self.right(self.t, s).start()

        @pl.when(self.t > 0)
        def _():
            self.left(self.t, s).start()

    def step(self, k, s):
        t, nt = self.t, self.nt
        if k >= nt or (k, s) in self.done:
            return
        self.done.add((k, s))

        @pl.when(t >= k)
        def _():
            self.right(t - k, s).wait_recv()

            @pl.when(t < nt - 1)
            def _():
                self.right(t - k, s).start()

        @pl.when(t + k < nt)
        def _():
            self.left(t + k, s).wait_recv()

            @pl.when(t > 0)
            def _():
                self.left(t + k, s).start()

    def complete(self, pieces):
        for k in range(1, self.nt):
            for s in pieces:
                self.step(k, s)

    def finish(self):
        t, nt = self.t, self.nt

        @pl.loop(0, nt)
        def _(k):
            for s in range(self.pieces):
                @pl.when((t >= k) & (t < nt - 1))
                def _():
                    self.right(t - k, s).wait_send()

                @pl.when((t + k < nt) & (t > 0))
                def _():
                    self.left(t + k, s).wait_send()


class LineScatter:
    def __init__(self, part, row, sent, arrived, t, nt, sems):
        self.part, self.row, self.sent, self.arrived = part, row, sent, arrived
        self.t, self.nt, self.sems = t, nt, sems
        self.pieces = sems.shape[3]
        self.size = sent.shape[1] // self.pieces
        self.model = sent.shape[2]
        self.near = lax.div(2 * t, nt)
        self.far = 1 - self.near

    def sub(self, s):
        return pl.ds(s * self.size, self.size)

    def depth(self, way):
        return (1 - way) * self.t + way * (self.nt - 1 - self.t)

    def goal(self, way, i):
        return (1 - way) * (self.nt - 1 - i) + way * i

    def slot(self, way, j):
        return j + 1 - way

    def move(self, way, j, s):
        return remote(
            self.sent.at[j, self.sub(s), :], self.arrived.at[self.slot(way, j), self.sub(s), :],
            self.sems.at[0, way, j, s], self.sems.at[1, way, j, s],
            {"tensor": lax.rem(self.t + self.nt + 1 - 2 * way, self.nt)},
        )

    def rows(self, j, s):
        return pl.ds(aligned(self.row(j, s), self.size), self.size)

    def mine(self, j, s):
        return self.part[self.rows(j, s), : self.model]

    def edge(self, s):
        t, nt = self.t, self.nt

        @pl.when((t == 0) | (t == nt - 1))
        def _():
            way = lax.div(t, nt - 1)

            @pl.loop(0, nt - 1)
            def _(i):
                j = self.goal(way, i)
                self.sent[j, self.sub(s), :] = self.mine(j, s).astype(BF)
                self.move(way, j, s).start()

    def relay(self, way, s):
        depth = self.depth(way)

        @pl.when(depth > 0)
        def _():
            @pl.loop(0, self.nt - 1 - depth)
            def _(i):
                j = self.goal(way, i)
                self.move(way, j, s).wait_recv()
                total = self.mine(j, s) + self.arrived[self.slot(way, j), self.sub(s), :].astype(F32)
                self.sent[j, self.sub(s), :] = total.astype(BF)
                self.move(way, j, s).start()

    def own(self, s):
        t = self.t
        rows = self.rows(t, s)
        for way in (self.near, self.far):
            @pl.when(self.depth(way) > 0)
            def _():
                self.move(way, t, s).wait_recv()
                self.part[rows, : self.model] += self.arrived[self.slot(way, t), self.sub(s), :].astype(F32)

        return rows

    def finish(self, pieces):
        for way in range(2):
            @pl.loop(0, self.nt - 1 - self.depth(way))
            def _(i):
                for s in pieces:
                    self.move(way, self.goal(way, i), s).wait_send()


class Cube:
    def setup(self, me, width, half_send, half_recv, pair_send, pair_recv):
        self.me, self.width = me, width
        self.hs, self.hr, self.ps, self.pr = half_send, half_recv, pair_send, pair_recv
        self.bits = list(range(1, width))
        self.orders = (self.bits, self.bits[::-1])
        self.masks = spans(self.bits)
        self.stages = len(self.bits)

    def at(self, mask):
        return flip(self.me, mask, self.width)


class BlockGather(Cube):
    def __init__(self, own, full, by_rows, me, width, *sems):
        self.setup(me, width, *sems)
        self.own_ref, self.full, self.by_rows = own, full, by_rows

    def half(self, h):
        rows = self.own_ref.shape[0] // 2
        return self.own_ref.at[pl.ds(h * rows, rows), :]

    def window(self, who, h=None):
        rows, cols = self.own_ref.shape
        take, start = (rows, 0) if h is None else (rows // 2, h * (rows // 2))
        if self.by_rows:
            return self.full.at[pl.ds(aligned(who * rows + start, take), take), :]
        return self.full.at[pl.ds(start, take), pl.ds(aligned(who * cols, cols), cols)]

    def hop(self, stage, h, m):
        order = self.orders[h]
        bit = 1 << order[stage]
        slot = (m | bit) >> 1
        src = self.half(h) if m == 0 else self.window(self.at(m), h)
        return remote(
            src, self.window(self.at(m), h), self.hs.at[h, slot], self.hr.at[h, slot],
            {"dp": self.at(bit)},
        )

    def send(self, stage):
        for h in range(2):
            for m in spans(self.orders[h][:stage]):
                self.hop(stage, h, m).start()

    def wait(self, stage):
        for h in range(2):
            bit = 1 << self.orders[h][stage]
            for m in spans(self.orders[h][:stage]):
                slot = (m | bit) >> 1
                landed = self.window(self.at(m | bit), h)
                remote(
                    landed, landed, self.hs.at[h, slot], self.hr.at[h, slot], {"dp": self.at(bit)}
                ).wait_recv()

    def pair(self, m):
        src = self.own_ref if m == 0 else self.window(self.at(m))
        return remote(
            src, self.window(self.at(m)), self.ps.at[m >> 1], self.pr.at[m >> 1],
            {"dp": self.at(1)},
        )

    def pair_send(self):
        for m in self.masks:
            self.pair(m).start()

    def pair_wait(self):
        for m in self.masks:
            landed = self.window(self.at(m | 1))
            remote(
                landed, landed, self.ps.at[m >> 1], self.pr.at[m >> 1], {"dp": self.at(1)}
            ).wait_recv()

    def place(self, sem):
        return pltpu.make_async_copy(self.own_ref, self.window(self.me), sem)

    def drain(self):
        for stage in range(self.stages):
            for h in range(2):
                for m in spans(self.orders[h][:stage]):
                    self.hop(stage, h, m).wait_send()
        for m in self.masks:
            self.pair(m).wait_send()


class BlockScatter(Cube):
    def __init__(self, chunk, out_sent, total, landed, store, me, width, *sems):
        self.setup(me, width, *sems)
        self.chunk, self.sent, self.total, self.landed = chunk, out_sent, total, landed
        self.store = store
        self.slots = 1 << (width - 1)

    def pair(self, slot):
        return remote(
            self.sent.at[slot], self.total.at[slot], self.ps.at[slot], self.pr.at[slot],
            {"dp": self.at(1)},
        )

    def give(self):
        @pl.loop(0, self.slots)
        def _(k):
            slot = self.slots - 1 - k
            self.sent[slot] = self.chunk(self.at(2 * slot + 1)).astype(BF)
            self.pair(slot).start()

    def given(self):
        @pl.loop(0, self.slots)
        def _(slot):
            self.pair(slot).wait_send()

    def take(self):
        @pl.loop(0, self.slots)
        def _(k):
            slot = self.slots - 1 - k
            term = self.chunk(self.at(2 * slot))
            self.pair(slot).wait_recv()
            self.total[slot] = (term + self.total[slot].astype(F32)).astype(BF)

    def moves(self, stage):
        for h in range(2):
            order = self.orders[h]
            last = self.stages - 1 - stage
            bit = 1 << order[last]
            for m in spans(order[:last]):
                yield h, bit, m | bit

    def hop(self, h, bit, m):
        rows = self.total.shape[1] // 2
        return remote(
            self.total.at[m >> 1, pl.ds(h * rows, rows), :], self.landed.at[h, (m >> 1) - 1],
            self.hs.at[h, m >> 1], self.hr.at[h, m >> 1], {"dp": self.at(bit)},
        )

    def send(self, stage):
        for h, bit, m in self.moves(stage):
            self.hop(h, bit, m).start()

    def add(self, stage):
        rows = self.total.shape[1] // 2
        for h, bit, m in self.moves(stage):
            self.hop(h, bit, m).wait_recv()
            keep = (m ^ bit) >> 1
            at = slice(h * rows, (h + 1) * rows)
            total = self.total[keep, at, :].astype(F32) + self.landed[h, (m >> 1) - 1].astype(F32)
            if stage == self.stages - 1:
                self.store(at, total)
            else:
                self.total[keep, at, :] = total.astype(BF)

    def drain(self):
        for stage in range(self.stages):
            for h, bit, m in self.moves(stage):
                self.hop(h, bit, m).wait_send()


def inverse_of(rows):
    return lax.rsqrt(jnp.mean(rows * rows, axis=-1, keepdims=True) + EPSILON)


def times_gain(unit, gains, which, store):
    parts, _, width = gains.shape
    for d in range(parts):
        cols = slice(d * width, (d + 1) * width)
        store(cols, unit[:, cols] * gains[d, which : which + 1, :])


def lane_index(shape):
    return lax.broadcasted_iota(jnp.int32, shape, len(shape) - 1)


def column_of(segr):
    rows = segr.shape[1]
    wide = jnp.broadcast_to(segr[...].astype(F32), (8, rows))
    return jnp.transpose(wide)[:, 0:1]


def rope_into(cos_ref, sin_ref, segr):
    rows = segr.shape[1]
    before = (segr[...].astype(F32) < column_of(segr)).astype(F32)
    start = jnp.sum(before, axis=1, keepdims=True)
    position = lax.broadcasted_iota(jnp.int32, (rows, 1), 0).astype(F32) - start
    lane = lane_index((rows, LANES))
    half = HD // 2
    frequency = jnp.exp(lax.rem(lane, half).astype(F32) * (-math.log(10000.0) / half))
    angle = position * frequency
    cos_ref[...] = jnp.cos(angle)
    sine = jnp.sin(angle)
    sin_ref[...] = jnp.where(lax.rem(lane, HD) < half, -sine, sine)


def swapped(x):
    lane = lane_index(x.shape)
    half = HD // 2
    return jnp.where(
        lax.rem(lane, HD) < half,
        pltpu.roll(x, LANES - half, 1),
        pltpu.roll(x, half, 1),
    )


def bias_into(bias, segr):
    rows = segr.shape[1]
    query = lax.broadcasted_iota(jnp.int32, (rows, rows), 0)
    key = lax.broadcasted_iota(jnp.int32, (rows, rows), 1)
    seen = (segr[...].astype(F32) == column_of(segr)) & (query >= key)
    bias[...] = jnp.where(seen, 0.0, NEGATIVE)


def pad_pair(keys_values, keys, values):
    low = lane_index(keys_values.shape) < HD
    key = jnp.where(low, keys_values, 0.0)
    value = jnp.where(low, 0.0, keys_values)
    keys[0] = key.astype(BF)
    keys[1] = pltpu.roll(key, HD, 1).astype(BF)
    values[0] = pltpu.roll(value, HD, 1).astype(BF)
    values[1] = value.astype(BF)


def query_cuts(rows):
    block = 256 if rows % 256 == 0 else rows
    return [(start, block, start + block) for start in range(0, rows, block)]


def attend_pairs(first, last, qo, kpad, vpad, bias, mo, lo):
    rows = qo.shape[0]
    lane = lane_index((1, LANES))

    @pl.loop(first, last)
    def _(pair):
        lanes = pl.ds(pl.multiple_of(pair * LANES, LANES), LANES)
        for start, block, seen in query_cuts(rows):
            at = slice(start, start + block)
            query = qo[at, lanes]
            mixed = jnp.zeros((block, LANES), F32)
            logs = lo[at, :]
            for side in range(2):
                scores = dot(query, kpad[side, :seen, :], 1, 1) + bias[at, :seen]
                top = jnp.max(scores, axis=-1, keepdims=True)
                probs = jnp.exp(scores - top)
                total = jnp.sum(probs, axis=-1, keepdims=True)
                mixed = mixed + dot(probs.astype(BF), vpad[side, :seen, :]) / total
                logs = jnp.where(lane == 2 * pair + side, top + jnp.log(total), logs)
            lo[at, :] = logs
            mo[at, lanes] = mixed.astype(BF)


def back_through_norm(raw, grads, gains, which, store, store_gain):
    parts, _, width = gains.shape
    cuts = [slice(d * width, (d + 1) * width) for d in range(parts)]
    model = parts * width
    square = sum(jnp.sum(raw(c) * raw(c), axis=-1, keepdims=True) for c in cuts)
    inverse = lax.rsqrt(square / model + EPSILON)
    mean = 0.0
    for d, c in enumerate(cuts):
        unit = raw(c) * inverse
        grad = grads(c)
        store_gain(c, jnp.sum(grad * unit, axis=0, keepdims=True))
        mean = mean + jnp.sum(grad * gains[d, which : which + 1, :] * unit, axis=-1, keepdims=True)
    mean = mean / model
    for d, c in enumerate(cuts):
        unit = raw(c) * inverse
        store(c, inverse * (grads(c) * gains[d, which : which + 1, :] - unit * mean))


def attend_back_pairs(first, last, qo, gm, mo, lo, kpad, vpad, bias, cos, sin, dqkv, dkey, dval):
    rows = qo.shape[0]

    @pl.loop(first, last)
    def _(pair):
        lanes = pl.ds(pl.multiple_of(pair * LANES, LANES), LANES)
        for start, block, seen in query_cuts(rows):
            at = slice(start, start + block)
            lane = lane_index((block, LANES))
            query, grad = qo[at, lanes], gm[at, lanes]
            both = grad.astype(F32) * mo[at, lanes].astype(F32)
            logs = lo[at, :]
            dq = jnp.zeros((block, LANES), F32)
            for side in range(2):
                inside = (lane >= HD) if side else (lane < HD)
                delta = jnp.sum(jnp.where(inside, both, 0.0), axis=-1, keepdims=True)
                log = jnp.sum(
                    jnp.where(lane == 2 * pair + side, logs, 0.0), axis=-1, keepdims=True
                )
                key, value = kpad[side, :seen, :], vpad[side, :seen, :]
                probs = jnp.exp(dot(query, key, 1, 1) + bias[at, :seen] - log)
                grad_scores = (probs * (dot(grad, value, 1, 1) - delta)).astype(BF)
                dq = dq + dot(grad_scores, key)
                dkey[side, :seen, :] += dot(grad_scores, query, 0, 0)
                dval[side, :seen, :] += dot(probs.astype(BF), grad, 0, 0)
            dq = dq * HD ** (-0.5)
            dqkv[at, lanes] = (dq * cos[at, :] - swapped(dq) * sin[at, :]).astype(BF)


PIECES = 4


def vmem():
    return pl.BlockSpec(memory_space=pltpu.VMEM)


def hbm():
    return pl.BlockSpec(memory_space=pl.ANY)


def dma(*shape):
    return pltpu.SemaphoreType.DMA(shape)


def line_scratch(nt, rows, model):
    return [pltpu.VMEM((nt, rows, model), BF), pltpu.VMEM((nt + 1, rows, model), BF)]


def ticks(pieces, nt):
    return [
        [(k, tick - k) for k in range(1, nt) if 0 <= tick - k < pieces]
        for tick in range(pieces + nt - 1)
    ]


def layer_kernel(
    nt, width,
    x, cot, gain_a, gain_f, segr, wq, wkt, wvt, wo, gate, up, down,
    y_o, gi_o, gain_o, d_wq_o, d_kv_o, d_wo_o, d_down_o, d_gate, d_up, wqkv_f, wo_f, na_f,
    rowsbuf, cf, branch, act, hid, gate_v, up_v, down_v, part, sent, arrived, totals, landed, stage_v,
    y, gi, gain_out, d_wq, d_kv, d_wo, d_down,
    own_qkv, gain, gall, qo, kvo, mo, lo, cos, sin, gsum, zslots, dslots,
    gain_sem, place_sem, out_sem, x_sem, cot_sem, nf_sem, br_sem, o_sem, gn_sem, y_sem, gi_sem,
    hs, hr, ps, pr, zsem, dsem, emit_sem, ready, calm,
):
    me, t = lax.axis_index("dp"), lax.axis_index("tensor")
    nd = 1 << width
    rows, model = x.shape
    tokens = nt * rows
    queries = wq.shape[1]
    hidden = gate.shape[1]
    shard = model >> width
    wide = own_qkv.shape[1]
    pieces = PIECES
    first_half = pieces // 2
    size = rows // pieces

    def natural(j, s):
        return j * rows + s * size

    def shuffled(j, s):
        return (s * nt + j) * size

    local = pl.ds(pl.multiple_of(t * rows, rows), rows)
    rowsbuf[local, :] = x[...]
    gain[...] = jnp.zeros_like(gain)
    gain[0:1, :] = gain_a[...].astype(F32).reshape(1, shard)
    gain[1:2, :] = gain_f[...].astype(F32).reshape(1, shard)
    own_qkv[:, :queries] = wq[...]
    turned = jnp.concatenate([wkt[...].astype(F32), wvt[...].astype(F32)], axis=0)
    own_qkv[:, queries:] = jnp.transpose(turned).astype(BF)
    with jax.named_scope("enter"):
        enter(t, nt, me, width, pltpu.get_barrier_semaphore())

    tokens_x = LineGather(rowsbuf, natural, size, t, nt, x_sem)
    for s in range(pieces):
        tokens_x.start(s)
    gathers = []
    for w, (own, full, by_rows) in enumerate(
        ((own_qkv, wqkv_f, True), (wo, wo_f, False), (gate, gate_v, True), (up, up_v, True), (down, down_v, False))
    ):
        gathers.append(
            BlockGather(own, full, by_rows, me, width, hs.at[w], hr.at[w], ps.at[w], pr.at[w])
        )
    g_qkv, g_out, g_gate, g_up, g_down = gathers
    stages = g_qkv.stages

    def gain_copy(mask):
        return remote(
            gain, gall.at[me], gain_sem.at[0, mask], gain_sem.at[1, mask],
            {"dp": flip(me, mask, width)},
        )

    for mask in range(1, nd):
        gain_copy(mask).start()
    for g in (g_qkv, g_out, g_gate):
        g.send(0)
    for w, g in enumerate(gathers):
        g.place(place_sem.at[w]).start()
    gall[me] = gain[...]

    def forward(g, stage):
        g.wait(stage)
        if stage + 1 < stages:
            g.send(stage + 1)
        else:
            g.pair_send()

    for s in range(pieces):
        cf[pl.ds(pl.multiple_of(shuffled(t, s), size), size), :] = cot[s * size : (s + 1) * size, :]
    cots = LineGather(cf, shuffled, size, t, nt, cot_sem)
    scatter_o = LineScatter(part, shuffled, sent, arrived, t, nt, o_sem)

    def attention(na, wqkv_v, wo_v, bias, kpad, vpad):
        bias_into(bias, segr)
        rope_into(cos, sin, segr)
        lo[...] = jnp.zeros_like(lo)
        for mask in range(1, nd):
            slot = gall.at[flip(me, mask, width)]
            remote(
                slot, slot, gain_sem.at[0, mask], gain_sem.at[1, mask],
                {"dp": flip(me, mask, width)},
            ).wait_recv()

        def norm(j):
            @pl.loop(0, pieces)
            def _(s):
                these = pl.ds(pl.multiple_of(j * rows + s * size, size), size)
                value = rowsbuf[these, :].astype(F32)

                def store(cols, normed):
                    na[these, cols] = normed.astype(BF)

                times_gain(value * inverse_of(value), gall, 0, store)

        norm(t)
        for stage in range(stages - 1):
            forward(g_qkv, stage)
            forward(g_out, stage)
        fills = [
            lambda: (forward(g_gate, 0), g_up.send(0)),
            lambda: (forward(g_qkv, stages - 1), forward(g_out, stages - 1), g_down.send(0)),
        ]
        load = pltpu.make_async_copy(wqkv_f, wqkv_v, place_sem.at[5])
        load_out = pltpu.make_async_copy(wo_f, wo_v, place_sem.at[6])

        def fetch():
            g_qkv.place(place_sem.at[0]).wait()
            g_qkv.pair_wait()
            load.start()
            g_out.place(place_sem.at[1]).wait()
            g_out.pair_wait()
            load_out.start()

        for k in range(1, nt):
            if k == nt - 1:
                for fill in fills:
                    fill()
                fills = []
                with jax.named_scope("fetch"):
                    fetch()
            with jax.named_scope("x_step"):
                for s in range(pieces):
                    tokens_x.step(k, s)
            if k == nt - 1:
                for s in range(first_half):
                    cots.start(s)

            @pl.when(t >= k)
            def _():
                norm(t - k)

            @pl.when(t + k < nt)
            def _():
                norm(t + k)

            if fills:
                with jax.named_scope("x_fill"):
                    fills.pop(0)()
        keep = pltpu.make_async_copy(na, na_f, out_sem.at[0])
        keep.start()
        with jax.named_scope("wait_qkv"):
            load.wait()
        with jax.named_scope("qkv"):
            part[:, :wide] = dot(na[...], wqkv_v[...])
            c, s_ = cos[...], sin[...]
            for start in range(0, queries, LANES):
                lanes = slice(start, start + LANES)
                value = part[:, lanes]
                qo[:, lanes] = ((value * c + swapped(value) * s_) * HD ** (-0.5)).astype(BF)
            value = part[:, queries : queries + LANES]
            keyed = jnp.where(lane_index(value.shape) < HD, value * c + swapped(value) * s_, value)
            kvo[...] = keyed.astype(BF)
            pad_pair(keyed, kpad, vpad)
        pairs = queries // LANES
        with jax.named_scope("att"):
            attend_pairs(0, pairs, qo, kpad, vpad, bias, mo, lo)
        load_out.wait()
        with jax.named_scope("outproj"):
            mixed = jnp.concatenate(
                [
                    mo[natural(j, s) : natural(j, s) + size, :]
                    for s in range(pieces)
                    for j in range(nt)
                ],
                axis=0,
            )
            for start, width_ in tiles_of(model, 4):
                cols = slice(start, start + width_)
                part[:tokens, cols] = dot(mixed, wo_v[:, cols])
        keep.wait()
        tokens_x.finish()

    pl.run_scoped(
        attention,
        pltpu.VMEM((tokens, model), BF),
        pltpu.VMEM((model, wide), BF),
        pltpu.VMEM((queries, model), BF),
        pltpu.VMEM((tokens, tokens), F32),
        pltpu.VMEM((2, tokens, LANES), BF),
        pltpu.VMEM((2, tokens, LANES), BF),
    )

    gather_nf = LineGather(rowsbuf, shuffled, size, t, nt, nf_sem)

    def take_hidden(s):
        at = scatter_o.own(s)
        block = slice(s * size, (s + 1) * size)
        hidden_rows = x[block, :].astype(F32) + part[at, :model]
        hid[block, :] = hidden_rows
        there = pl.ds(pl.multiple_of(shuffled(t, s), size), size)

        def store(cols, normed):
            rowsbuf[there, cols] = normed.astype(BF)

        times_gain(hidden_rows * inverse_of(hidden_rows), gall, 1, store)
        gather_nf.start(s)

    def chunk_of(left, right):
        def chunk(d):
            return dot(left[:, pl.ds(pl.multiple_of(d * shard, shard), shard)], right[...], 0, 0)

        return chunk

    def cube(w, totals_, landed_, store):
        return BlockScatter(
            None, None, totals_, landed_, store, me, width, hs.at[w], hr.at[w], ps.at[w], pr.at[w]
        )

    def store_stage(at, value):
        stage_v[at, :] = value

    def store_down(at, value):
        d_down[:, at] = value.T

    def store_qkv(at, value):
        d_wq[at, :] = value[:, :queries]
        d_kv[:, at] = value[:, queries:].T

    def store_wo(at, value):
        d_wo[:, at] = value.T

    for_qkv, for_wo = pl.ds(0, wide), pl.ds(wide, queries)
    s_gate = cube(5, totals.at[0], landed.at[0], store_stage)
    s_up = cube(6, totals.at[1], landed.at[1], store_stage)
    s_down = cube(7, totals.at[0], landed.at[0], store_down)
    s_qkv = cube(8, totals.at[1, :, :, for_qkv], landed.at[1, :, :, :, for_qkv], store_qkv)
    s_out = cube(9, totals.at[1, :, :, for_wo], landed.at[1, :, :, :, for_wo], store_wo)

    def take(s):
        s.take()
        s.send(0)

    def on(s, stage):
        s.add(stage)
        if stage + 1 < stages:
            s.send(stage + 1)

    scatter_y = LineScatter(part, shuffled, sent, arrived, t, nt, y_sem)
    scope = jax.named_scope
    emitted = []

    def emit(src, dst):
        emitted.append(pltpu.make_async_copy(src, dst, emit_sem.at[len(emitted)]))
        emitted[-1].start()

    def y_part(h):
        mine = slice(h * (tokens // 2), (h + 1) * (tokens // 2))
        with scope("y_part"):
            for start, width_ in tiles_of(model, 4):
                cols = slice(start, start + width_)
                part[mine, cols] = dot(act[mine, :], down_v[:, cols])

    def y_near(s):
        with scope("y_near"):
            scatter_y.relay(scatter_y.near, s)

    def y_far(s):
        with scope("y_far"):
            scatter_y.relay(scatter_y.far, s)

    def y_own(s):
        with scope("y_own"):
            at = scatter_y.own(s)
            block_ = slice(s * size, (s + 1) * size)
            y[block_, :] = (hid[block_, :] + part[at, :model]).astype(BF)
            emit(y.at[pl.ds(s * size, size), :], y_o.at[pl.ds(s * size, size), :])

    def br(k, s):
        with scope("br_step"):
            gather_br.step(k, s)

    gsum[...] = jnp.zeros_like(gsum)
    gather_br = LineGather(branch, natural, size, t, nt, br_sem)

    def feed(dg, du, given):
        cuts = tiles_of(hidden, 6)
        span = max(width_ for _, width_ in cuts)
        half = tokens // 2
        block = 64

        def tile(h, i):
            start, width_ = cuts[i]
            at = slice(start, start + width_)
            mine = slice(h * half, (h + 1) * half)
            held = mine
            part[held, 0:width_] = dot(rowsbuf[mine, :], gate_v[:, at])
            part[held, span : span + width_] = dot(rowsbuf[mine, :], up_v[:, at])
            part[held, 2 * span : 2 * span + width_] = dot(cf[mine, :], down_v[at, :], 1, 1)

            @pl.loop(0, half // block)
            def _(k):
                from_ = pl.ds(pl.multiple_of(h * half + k * block, block), block)
                to = pl.ds(pl.multiple_of(h * half + k * block, block), block)
                g = part[from_, 0:width_]
                u = part[from_, span : span + width_]
                ga = part[from_, 2 * span : 2 * span + width_]
                sig = 1.0 / (1.0 + jnp.exp(-g))
                gs = g * sig
                act[to, at] = (gs * u).astype(BF)
                du[to, at] = (ga * gs).astype(BF)
                dg[to, at] = (ga * u * sig * (1.0 + g * (1.0 - sig))).astype(BF)

        def back_dots(h):
            mine = slice(h * half, (h + 1) * half)
            for start, width_ in tiles_of(model, 4):
                cols = slice(start, start + width_)
                part[mine, cols] = dot(dg[mine, :], gate_v[cols, :], 1, 1) + dot(
                    du[mine, :], up_v[cols, :], 1, 1
                )

        scatter_gn = LineScatter(part, shuffled, sent, arrived, t, nt, gn_sem)

        def take_grad(s):
            at = scatter_gn.own(s)
            block_ = slice(s * size, (s + 1) * size)
            there = pl.ds(pl.multiple_of(natural(t, s), size), size)

            def store(cols, value):
                total = cot[block_, cols].astype(F32) + value
                gi[block_, cols] = total
                branch[there, cols] = total.astype(BF)

            def store_gain(cols, value):
                gsum[1:2, cols] += value

            back_through_norm(
                lambda c: hid[block_, c], lambda c: part[at, c], gall, 1, store, store_gain
            )
            gather_br.start(s)

        s_gate.chunk, s_up.chunk = chunk_of(rowsbuf, dg), chunk_of(rowsbuf, du)
        s_gate.sent = s_up.sent = given

        half_a, half_b = range(first_half), range(first_half, pieces)
        def o_near(s):
            with scope("o_near"):
                scatter_o.relay(scatter_o.near, s)

        def o_far(s):
            with scope("o_far"):
                scatter_o.relay(scatter_o.far, s)

        def o_take(s):
            with scope("o_take"):
                take_hidden(s)

        def nf(k, s):
            with scope("nf_step"):
                gather_nf.step(k, s)

        def cot_steps(k, which):
            with scope("cot_step"):
                for s in which:
                    cots.step(k, s)

        def gn_near(s):
            with scope("gn_near"):
                scatter_gn.relay(scatter_gn.near, s)

        def gn_far(s):
            with scope("gn_far"):
                scatter_gn.relay(scatter_gn.far, s)

        def gn_take(s):
            with scope("gn_take"):
                take_grad(s)

        def weight(g, stage):
            with scope("weight"):
                if stage < stages:
                    forward(g, stage)

        scatter_o.edge(0)
        scatter_o.edge(1)
        cot_steps(1, half_a)
        weight(g_gate, 1)
        o_near(0)
        weight(g_up, 0)
        cot_steps(2, half_a)
        o_far(0)
        o_take(0)
        weight(g_down, 0)
        scatter_o.edge(2)
        o_near(1)
        nf(1, 0)
        cot_steps(3, half_a)
        o_far(1)
        o_take(1)
        scatter_o.edge(3)
        for s in half_b:
            cots.start(s)
        nf(2, 0)
        nf(1, 1)
        weight(g_up, 1)
        o_near(2)
        nf(3, 0)
        nf(2, 1)
        o_far(2)
        nf(3, 1)
        o_take(2)
        gather_nf.complete(half_a)
        cots.complete(half_a)
        weight(g_down, 1)
        for stage in range(2, stages):
            for g in (g_gate, g_up, g_down):
                weight(g, stage)
        o_near(3)
        with scope("wait_ffn"):
            for w in (2, 3, 4):
                gathers[w].place(place_sem.at[w]).wait()
                gathers[w].pair_wait()
        with scope("tile"):
            tile(0, 0)
        o_far(3)
        nf(1, 2)
        cot_steps(1, half_b)
        with scope("tile"):
            for i in range(1, len(cuts)):
                tile(0, i)
        o_take(3)
        nf(2, 2)
        with scope("back_dots"):
            scatter_o.finish(half_a)
            back_dots(0)
        scatter_gn.edge(0)
        scatter_gn.edge(1)
        nf(1, 3)
        cot_steps(2, half_b)
        gn_near(0)
        nf(3, 2)
        nf(2, 3)
        gn_far(0)
        cot_steps(3, half_b)
        gn_near(1)
        nf(3, 3)
        gather_nf.complete(half_b)
        cots.complete(half_b)
        with scope("tile"):
            tile(1, 0)
        gn_far(1)
        gn_take(0)
        with scope("tile"):
            for i in range(1, len(cuts)):
                tile(1, i)
        br(1, 0)
        with scope("back_dots"):
            scatter_o.finish(half_b)
            back_dots(1)
        scatter_gn.edge(2)
        gn_take(1)
        scatter_gn.edge(3)
        with scope("gn_fill"):
            s_gate.give()
            br(2, 0)
            take(s_gate)
        gn_near(2)
        br(1, 1)
        y_part(0)
        br(3, 0)
        gn_far(2)
        with scope("gn_fill"):
            s_gate.given()
            s_up.give()
        gn_near(3)
        gn_take(2)
        scatter_gn.finish(half_a)
        scatter_y.edge(0)
        br(2, 1)
        gn_far(3)
        with scope("gn_fill"):
            take(s_up)
        br(3, 1)
        gn_take(3)
        scatter_y.edge(1)
        br(1, 2)
        y_near(0)
        y_part(1)
        br(2, 2)
        br(1, 3)
        scatter_gn.finish(half_b)
        scatter_y.edge(2)
        scatter_y.edge(3)
        y_far(0)
        br(3, 2)
        br(2, 3)
        with scope("add0"):
            on(s_gate, 0)
        y_near(1)
        y_far(1)
        br(3, 3)
        gather_br.complete(range(pieces))
        s_up.given()

    pl.run_scoped(
        feed,
        pltpu.VMEM((tokens, hidden), BF),
        pltpu.VMEM((tokens, hidden), BF),
        pltpu.VMEM((nd // 2, shard, hidden), BF),
    )

    wo_v = down_v.at[pl.ds(0, queries), :]
    na_v = down_v.at[pl.ds(queries, tokens), :]
    wqkv_v = gate_v.at[:, pl.ds(0, wide)]
    gm = up_v.at[pl.ds(0, tokens), pl.ds(0, queries)]
    dqkv = up_v.at[pl.ds(tokens, tokens), pl.ds(0, wide)]

    def rear(bias, kpad, vpad, dkey, dval, given):
        inward = LineScatter(part, shuffled, sent, arrived, t, nt, gi_sem)
        for g in gathers:
            g.drain()
        loads = [
            pltpu.make_async_copy(wo_f, wo_v, place_sem.at[0]),
            pltpu.make_async_copy(wqkv_f, wqkv_v, place_sem.at[1]),
            pltpu.make_async_copy(na_f, na_v, place_sem.at[2]),
        ]
        for load in loads:
            load.start()
        bias_into(bias, segr)
        pad_pair(kvo[...].astype(F32), kpad, vpad)
        dkey[...] = jnp.zeros_like(dkey)
        dval[...] = jnp.zeros_like(dval)
        s_down.chunk, s_down.sent = chunk_of(cf, act), given
        s_qkv.chunk, s_qkv.sent = chunk_of(na_v, dqkv), given.at[:, :, for_qkv]
        s_out.chunk, s_out.sent = chunk_of(branch, mo), given.at[:, :, for_wo]

        def att(first, last):
            with scope("b_att"):
                attend_back_pairs(
                    first, last, qo, gm, mo, lo, kpad, vpad, bias, cos, sin, dqkv, dkey, dval
                )

        def free(s, out, slot):
            s.add(stages - 1)
            copy = pltpu.make_async_copy(stage_v, out, out_sem.at[1 + slot])
            copy.start()
            s.drain()
            for bit in range(width):
                pl.semaphore_signal(
                    ready.at[slot], inc=1, device_id={"dp": flip(me, 1 << bit, width)},
                    device_id_type=pl.DeviceIdType.MESH,
                )
            return copy

        def quiet(h):
            for step, there in ((-1, t > 0), (1, t < nt - 1)):
                @pl.when(there)
                def _():
                    pl.semaphore_signal(
                        calm.at[h], inc=1, device_id={"tensor": t + step},
                        device_id_type=pl.DeviceIdType.MESH,
                    )

        def gi_part(h):
            which = half_a if h == 0 else half_b
            mine = jnp.concatenate(
                [dqkv[natural(j, s) : natural(j, s) + size, :] for s in which for j in range(nt)],
                axis=0,
            )
            start_row = h * (tokens // 2)
            with scope("b_part"):
                for start, width_ in tiles_of(model, 4):
                    part[start_row : start_row + tokens // 2, start : start + width_] = dot(
                        mine, wqkv_v[start : start + width_, :], 1, 1
                    )
            with scope("calm"):
                pl.semaphore_wait(calm.at[h], lax.min(t, 1) + lax.min(nt - 1 - t, 1))
            for s in which:
                inward.edge(s)

        def gi_near(s):
            with scope("b_near"):
                inward.relay(inward.near, s)

        def gi_far(s):
            with scope("b_far"):
                inward.relay(inward.far, s)

        half_a, half_b = range(first_half), range(first_half, pieces)
        pairs = queries // LANES
        with scope("b_gm"):
            loads[0].wait()
            gm[...] = dot(branch[...], wo_v[...], 1, 1).astype(BF)
        for s in half_a:
            y_own(s)
        scatter_y.finish(half_a)
        quiet(0)
        with scope("add0"):
            on(s_up, 0)
        att(0, pairs // 2)
        y_near(2)
        with scope("free0"):
            copy_gate = free(s_gate, d_gate, 0)
        att(pairs // 2, pairs)
        y_near(3)
        key = dkey[0] + pltpu.roll(dkey[1], HD, 1)
        value = pltpu.roll(dval[0], HD, 1) + dval[1]
        key = key * cos[...] - swapped(key) * sin[...]
        dqkv[:, queries : queries + LANES] = jnp.where(
            lane_index(key.shape) < HD, key, value
        ).astype(BF)
        loads[1].wait()
        gi_part(0)
        with scope("b_give"):
            pl.semaphore_wait(ready.at[0], width)
            s_down.give()
        y_far(2)
        y_far(3)
        gi_near(0)
        with scope("b_take"):
            take(s_down)
        for s in half_b:
            y_own(s)
        scatter_y.finish(half_b)
        quiet(1)
        gi_part(1)
        gi_far(0)
        loads[2].wait()
        gi_near(1)

        with scope("b_done"):
            for mask in range(1, nd):
                gain_copy(mask).wait_send()
            cots.finish()
            gather_nf.finish()
            gather_br.finish()

        def take_grad(s):
            at = inward.own(s)
            block = slice(s * size, (s + 1) * size)

            def store(cols, value):
                gi[block, cols] += value

            def store_gain(cols, value):
                gsum[0:1, cols] += value

            back_through_norm(
                lambda c: x[block, c].astype(F32), lambda c: part[at, c], gall, 0, store, store_gain
            )

        copies = []

        def free_up():
            s_down.given()
            copy_gate.wait()
            copies.append(free(s_up, d_up, 1))

        def give_small():
            pl.semaphore_wait(ready.at[1], width)
            s_qkv.give()

        fills = [
            give_small,
            lambda: (take(s_qkv), s_out.give()),
            lambda: take(s_out),
        ]
        fills += [
            functools.partial(on, s, stage)
            for stage in range(stages)
            for s in (s_down, s_qkv, s_out)
        ]
        with scope("free1"):
            free_up()
        gi_far(1)
        with scope("b_fill"):
            fills.pop(0)()
        gi_near(2)
        with scope("b_fill"):
            fills.pop(0)()
        gi_far(2)
        with scope("b_fill"):
            fills.pop(0)()
        gi_near(3)
        gi_far(3)
        with jax.named_scope("b_own"):
            for s in range(pieces):
                take_grad(s)
                emit(gi.at[pl.ds(s * size, size), :], gi_o.at[pl.ds(s * size, size), :])
                if s < pieces - 1 and fills:
                    fills.pop(0)()
        with jax.named_scope("b_gains"):
            zslots[t] = gsum[...]

            def along(step):
                return remote(
                    zslots.at[t], zslots.at[t], zsem.at[0, step], zsem.at[1, step],
                    {"tensor": lax.rem(t + step, nt)},
                )

            for step in range(1, nt):
                along(step).start()
        with jax.named_scope("b_gains"):
            for step in range(1, nt):
                slot = zslots.at[lax.rem(t + nt - step, nt)]
                remote(
                    slot, slot, zsem.at[0, step], zsem.at[1, step], {"tensor": lax.rem(t + step, nt)}
                ).wait_recv()
            gsum[...] = sum(zslots[i] for i in range(nt))

            def across(mask):
                peer = flip(me, mask, width)
                return remote(
                    gsum.at[:, pl.ds(pl.multiple_of(peer * shard, shard), shard)], dslots.at[me],
                    dsem.at[0, mask], dsem.at[1, mask], {"dp": peer},
                )

            for mask in range(1, nd):
                across(mask).start()
            dslots[me] = gsum[:, pl.ds(pl.multiple_of(me * shard, shard), shard)]
        with jax.named_scope("b_rest"):
            for fill in fills:
                fill()
            for src, dst in ((d_wq, d_wq_o), (d_kv, d_kv_o), (d_wo, d_wo_o), (d_down, d_down_o)):
                emit(src, dst)
        with jax.named_scope("b_gains"):
            for mask in range(1, nd):
                peer = flip(me, mask, width)
                slot = dslots.at[peer]
                remote(slot, slot, dsem.at[0, mask], dsem.at[1, mask], {"dp": peer}).wait_recv()
            gain_out[...] = sum(dslots[i] for i in range(nd))
            emit(gain_out, gain_o)
            for step in range(1, nt):
                along(step).wait_send()
            for mask in range(1, nd):
                across(mask).wait_send()
        with jax.named_scope("end"):
            for s in (s_qkv, s_out):
                s.given()
            for s in (s_down, s_qkv, s_out):
                s.drain()
            inward.finish(range(pieces))
            for copy in copies + emitted:
                copy.wait()

    pl.run_scoped(
        rear,
        pltpu.VMEM((tokens, tokens), F32),
        pltpu.VMEM((2, tokens, LANES), BF),
        pltpu.VMEM((2, tokens, LANES), BF),
        pltpu.VMEM((2, tokens, LANES), F32),
        pltpu.VMEM((2, tokens, LANES), F32),
        pltpu.VMEM((nd // 2, shard, hidden), BF),
    )


def layer(nt, nd, x, cot, gain_a, gain_f, segr, wq, wkt, wvt, wo, gate, up, down):
    width = nd.bit_length() - 1
    rows, model = x.shape
    tokens = nt * rows
    queries = wq.shape[1]
    hidden = gate.shape[1]
    shard = model // nd
    half = nd // 2
    wide = queries + LANES
    span = max(width_ for _, width_ in tiles_of(hidden, 6))
    shape = jax.ShapeDtypeStruct
    outs = [
        (shape((rows, model), BF), hbm()),
        (shape((rows, model), F32), hbm()),
        (shape((8, shard), F32), hbm()),
        (shape((shard, queries), F32), hbm()),
        (shape((LANES, shard), F32), hbm()),
        (shape((queries, shard), F32), hbm()),
        (shape((hidden, shard), F32), hbm()),
        (shape((shard, hidden), F32), hbm()),
        (shape((shard, hidden), F32), hbm()),
        (shape((model, wide), BF), hbm()),
        (shape((queries, model), BF), hbm()),
        (shape((tokens, model), BF), hbm()),
    ]
    return pl.pallas_call(
        functools.partial(layer_kernel, nt, width),
        out_shape=[o for o, _ in outs],
        in_specs=[vmem()] * 8 + [hbm()] * 4,
        out_specs=[s for _, s in outs],
        scratch_shapes=[
            pltpu.VMEM((tokens, model), BF),
            pltpu.VMEM((tokens, model), BF),
            pltpu.VMEM((tokens, model), BF),
            pltpu.VMEM((tokens, hidden), BF),
            pltpu.VMEM((rows, model), F32),
            pltpu.VMEM((model, hidden), BF),
            pltpu.VMEM((model, hidden), BF),
            pltpu.VMEM((hidden, model), BF),
            pltpu.VMEM((max(tokens, 2 * shard), max(model, 3 * span)), F32),
        ]
        + line_scratch(nt, rows, model)
        + [
            pltpu.VMEM((2, half, shard, hidden), BF),
            pltpu.VMEM((2, 2, half - 1, shard // 2, hidden), BF),
            pltpu.VMEM((shard, hidden), F32),
            pltpu.VMEM((rows, model), BF),
            pltpu.VMEM((rows, model), F32),
            pltpu.VMEM((8, shard), F32),
            pltpu.VMEM((shard, queries), F32),
            pltpu.VMEM((LANES, shard), F32),
            pltpu.VMEM((queries, shard), F32),
            pltpu.VMEM((hidden, shard), F32),
            pltpu.VMEM((shard, wide), BF),
            pltpu.VMEM((8, shard), F32),
            pltpu.VMEM((nd, 8, shard), F32),
            pltpu.VMEM((tokens, queries), BF),
            pltpu.VMEM((tokens, LANES), BF),
            pltpu.VMEM((tokens, queries), BF),
            pltpu.VMEM((tokens, LANES), F32),
            pltpu.VMEM((tokens, LANES), F32),
            pltpu.VMEM((tokens, LANES), F32),
            pltpu.VMEM((8, model), F32),
            pltpu.VMEM((nt, 8, model), F32),
            pltpu.VMEM((nd, 8, shard), F32),
            dma(2, nd),
            dma(7),
            dma(3),
            dma(4, nt, PIECES),
            dma(4, nt, PIECES),
            dma(4, nt, PIECES),
            dma(4, nt, PIECES),
            dma(2, 2, nt, PIECES),
            dma(2, 2, nt, PIECES),
            dma(2, 2, nt, PIECES),
            dma(2, 2, nt, PIECES),
            dma(10, 2, half),
            dma(10, 2, half),
            dma(10, half),
            dma(10, half),
            dma(2, nt),
            dma(2, nd),
            dma(2 * PIECES + 5),
            pltpu.SemaphoreType.REGULAR((2,)),
            pltpu.SemaphoreType.REGULAR((2,)),
        ],
        compiler_params=pltpu.CompilerParams(
            collective_id=0, has_side_effects=True, vmem_limit_bytes=VMEM_BYTES
        ),
        name="layer",
    )(x, cot, gain_a, gain_f, segr, wq, wkt, wvt, wo, gate, up, down)


def hand_over_kernel(count, kv, *refs):
    sources, rest = refs[: count + 2], refs[count + 2 :]
    targets, rest = rest[: count + 4], rest[count + 4 :]
    held, (in_sem, out_sem) = rest[: count + 2], rest[count + 2 :]
    ins = [
        pltpu.make_async_copy(src, buf, in_sem.at[i])
        for i, (src, buf) in enumerate(zip(sources, held))
    ]
    for copy in ins:
        copy.start()
    outs = []
    for i in range(count):
        ins[i].wait()
        outs.append(pltpu.make_async_copy(held[i], targets[i], out_sem.at[i]))
        outs[-1].start()
    ins[count].wait()
    for i in range(2):
        outs.append(
            pltpu.make_async_copy(
                held[count].at[pl.ds(i * kv, kv), :], targets[count + i], out_sem.at[count + i]
            )
        )
        outs[-1].start()
    ins[count + 1].wait()
    gains = held[count + 1]
    for i in range(2):
        targets[count + 2 + i][...] = gains[i, :]
    for copy in outs:
        copy.wait()


def hand_over(arrays, d_kv, gains):
    count, kv = len(arrays), d_kv.shape[0] // 2
    shape = jax.ShapeDtypeStruct
    outs = [shape(a.shape, a.dtype) for a in arrays]
    outs += [shape((kv, d_kv.shape[1]), F32)] * 2 + [shape((gains.shape[1],), F32)] * 2
    inputs = (*arrays, d_kv, gains)
    return pl.pallas_call(
        functools.partial(hand_over_kernel, count, kv),
        out_shape=outs,
        in_specs=[hbm()] * len(inputs),
        out_specs=[hbm()] * (count + 2) + [vmem()] * 2,
        scratch_shapes=[pltpu.VMEM(a.shape, a.dtype) for a in inputs]
        + [dma(len(inputs)), dma(count + 2)],
        compiler_params=pltpu.CompilerParams(vmem_limit_bytes=VMEM_BYTES),
        name="hand_over",
    )(*inputs)


def narrow_scatter(value, axis, scatter_dimension, tiled):
    low = value.astype(BF) if value.ndim == 2 else value
    return lax.psum_scatter(low, axis, scatter_dimension=scatter_dimension, tiled=tiled).astype(F32)


def rope_tables(segments, head_dim):
    row_count = segments.shape[0]
    row_index = jnp.arange(row_count, dtype=jnp.int32)
    change = jnp.concatenate(
        [jnp.ones((1,), jnp.int32), (segments[1:] != segments[:-1]).astype(jnp.int32)]
    )
    starts = lax.cummax(jnp.where(change > 0, row_index, jnp.zeros_like(row_index)), axis=0)
    position = (row_index - starts).astype(F32)
    half_dim = head_dim // 2
    frequency = jnp.exp(jnp.arange(half_dim, dtype=F32) * (-math.log(10000.0) / half_dim))
    angles = position[:, None] * frequency[None, :]
    return (jnp.cos(angles)[:, None, :], jnp.sin(angles)[:, None, :])


def rotate(tensor, cosine, sine):
    half_dim = tensor.shape[-1] // 2
    first_half = tensor[..., :half_dim]
    second_half = tensor[..., half_dim:]
    return jnp.concatenate(
        [first_half * cosine - second_half * sine, second_half * cosine + first_half * sine],
        axis=-1,
    )


def unrotate(tensor, cosine, sine):
    half_dim = tensor.shape[-1] // 2
    first_half = tensor[..., :half_dim]
    second_half = tensor[..., half_dim:]
    return jnp.concatenate(
        [first_half * cosine + second_half * sine, second_half * cosine - first_half * sine],
        axis=-1,
    )


def visible(segments):
    row_index = jnp.arange(segments.shape[0], dtype=jnp.int32)
    same_seq = segments[:, None] == segments[None, :]
    return same_seq & (row_index[:, None] >= row_index[None, :])


def normalize(values, gain):
    inverse = lax.rsqrt(jnp.mean(values * values, axis=-1, keepdims=True) + EPSILON)
    unit_rows = values * inverse
    return (unit_rows, inverse, (unit_rows * gain.astype(F32)).astype(BF))


def normalize_back(grad_normed, unit_rows, inverse, gain):
    scaled = grad_normed * gain.astype(F32)
    grad_values = inverse * (
        scaled - unit_rows * jnp.mean(scaled * unit_rows, axis=-1, keepdims=True)
    )
    return (grad_values, jnp.sum(grad_normed * unit_rows, axis=0))


def contract(left, right, left_dim, right_dim):
    return lax.dot_general(
        left, right, (((left_dim,), (right_dim,)), ((), ())), preferred_element_type=F32
    )


def block_scores(query_block, key_heads, allowed_block, score_scale):
    scores = (
        jnp.einsum("rkgd,skd->kgrs", query_block, key_heads, preferred_element_type=F32)
        * score_scale
    )
    return jnp.where(allowed_block[None, None], scores, NEGATIVE)


def attend_forward(query_groups, key_heads, value_heads, allowed, score_scale):
    scores = block_scores(query_groups, key_heads, allowed, score_scale)
    row_max = jnp.max(scores, axis=-1, keepdims=True)
    log_total = row_max + jnp.log(jnp.sum(jnp.exp(scores - row_max), axis=-1, keepdims=True))
    probs_low = jnp.exp(scores - log_total).astype(BF)
    mixed_parts = jnp.einsum(
        "kgrs,skd->rkgd", probs_low, value_heads, preferred_element_type=F32
    ).astype(BF)
    return (mixed_parts, log_total)


def attend_backward(
    query_groups, key_heads, value_heads, mixed_heads, grad_mixed, log_totals, allowed, score_scale
):
    scores = block_scores(query_groups, key_heads, allowed, score_scale)
    attn_probs = jnp.exp(scores - log_totals)
    probs_low = attn_probs.astype(BF)
    grad_probs = jnp.einsum(
        "rkgd,skd->kgrs", grad_mixed, value_heads, preferred_element_type=F32
    )
    row_delta = jnp.sum(grad_mixed.astype(F32) * mixed_heads.astype(F32), axis=-1)
    row_delta = jnp.transpose(row_delta, (1, 2, 0))[..., None]
    grad_scores = (attn_probs * (grad_probs - row_delta)).astype(BF)
    query_parts = (
        jnp.einsum("kgrs,skd->rkgd", grad_scores, key_heads, preferred_element_type=F32)
        * score_scale
    )
    grad_key_rot = (
        jnp.einsum("kgrs,rkgd->skd", grad_scores, query_groups, preferred_element_type=F32)
        * score_scale
    )
    grad_value_heads = jnp.einsum(
        "kgrs,rkgd->skd", probs_low, grad_mixed, preferred_element_type=F32
    )
    return (query_parts, grad_key_rot, grad_value_heads)


def plain_device(
    layer_input,
    segment_ids,
    norm_attn,
    w_query,
    w_key,
    w_value,
    w_output,
    norm_ffn,
    w_gate,
    w_up,
    w_down,
    cotangent,
):
    score_scale = HD ** (-0.5)
    query_full, key_full, value_full, output_full, gain_attn = (
        lax.all_gather(w_query, "dp", axis=0, tiled=True),
        lax.all_gather(w_key, "dp", axis=0, tiled=True),
        lax.all_gather(w_value, "dp", axis=0, tiled=True),
        lax.all_gather(w_output, "dp", axis=1, tiled=True),
        lax.all_gather(norm_attn, "dp", axis=0, tiled=True),
    )
    gate_full, up_full, down_full, gain_ffn = (
        lax.all_gather(w_gate, "dp", axis=0, tiled=True),
        lax.all_gather(w_up, "dp", axis=0, tiled=True),
        lax.all_gather(w_down, "dp", axis=1, tiled=True),
        lax.all_gather(norm_ffn, "dp", axis=0, tiled=True),
    )
    heads_local = query_full.shape[1] // HD
    kv_local = key_full.shape[1] // HD
    group = heads_local // kv_local
    residual_in = layer_input.astype(F32)
    unit_attn, inverse_attn, normed_local = normalize(residual_in, gain_attn)
    normed_attn = lax.all_gather(normed_local, "tensor", axis=0, tiled=True)
    row_count = normed_attn.shape[0]
    cosine, sine = rope_tables(segment_ids, HD)
    allowed = visible(segment_ids)
    query_heads = rotate(
        jnp.dot(normed_attn, query_full, preferred_element_type=F32).reshape(
            row_count, heads_local, HD
        ),
        cosine,
        sine,
    ).astype(BF)
    query_groups = query_heads.reshape(row_count, kv_local, group, HD)
    key_heads = rotate(
        jnp.dot(normed_attn, key_full, preferred_element_type=F32).reshape(
            row_count, kv_local, HD
        ),
        cosine,
        sine,
    ).astype(BF)
    value_heads = (
        jnp.dot(normed_attn, value_full, preferred_element_type=F32)
        .astype(BF)
        .reshape(row_count, kv_local, HD)
    )
    mixed_heads, log_totals = attend_forward(
        query_groups, key_heads, value_heads, allowed, score_scale
    )
    mixed_flat = mixed_heads.reshape(row_count, heads_local * HD)
    hidden_res = residual_in + narrow_scatter(
        jnp.dot(mixed_flat, output_full, preferred_element_type=F32),
        "tensor",
        scatter_dimension=0,
        tiled=True,
    )
    unit_ffn, inverse_ffn, normed_ffn_local = normalize(hidden_res, gain_ffn)
    normed_ffn = lax.all_gather(normed_ffn_local, "tensor", axis=0, tiled=True)
    gate_rows = jnp.dot(normed_ffn, gate_full, preferred_element_type=F32)
    up_rows = jnp.dot(normed_ffn, up_full, preferred_element_type=F32)
    sigmoid_gate = jax.nn.sigmoid(gate_rows)
    active = (gate_rows * sigmoid_gate * up_rows).astype(BF)
    layer_output = (
        hidden_res
        + narrow_scatter(
            jnp.dot(active, down_full, preferred_element_type=F32).astype(BF),
            "tensor",
            scatter_dimension=0,
            tiled=True,
        ).astype(F32)
    ).astype(BF)
    query_full, key_full, value_full, output_full, gate_full, up_full, down_full = (
        lax.all_gather(w_query, "dp", axis=0, tiled=True),
        lax.all_gather(w_key, "dp", axis=0, tiled=True),
        lax.all_gather(w_value, "dp", axis=0, tiled=True),
        lax.all_gather(w_output, "dp", axis=1, tiled=True),
        lax.all_gather(w_gate, "dp", axis=0, tiled=True),
        lax.all_gather(w_up, "dp", axis=0, tiled=True),
        lax.all_gather(w_down, "dp", axis=1, tiled=True),
    )
    cotangent_full = lax.all_gather(cotangent, "tensor", axis=0, tiled=True)
    grad_active = contract(cotangent_full, down_full, 1, 1)
    grad_w_down = contract(active, cotangent_full, 0, 0)
    grad_up_rows = (grad_active * gate_rows * sigmoid_gate).astype(BF)
    grad_gate_rows = (
        grad_active * up_rows * sigmoid_gate * (1.0 + gate_rows * (1.0 - sigmoid_gate))
    ).astype(BF)
    grad_w_gate = contract(normed_ffn, grad_gate_rows, 0, 0)
    grad_w_up = contract(normed_ffn, grad_up_rows, 0, 0)
    grad_normed_ffn = narrow_scatter(
        contract(grad_gate_rows, gate_full, 1, 1) + contract(grad_up_rows, up_full, 1, 1),
        "tensor",
        scatter_dimension=0,
        tiled=True,
    )
    grad_hidden, gain_ffn_part = normalize_back(grad_normed_ffn, unit_ffn, inverse_ffn, gain_ffn)
    grad_hidden = cotangent.astype(F32) + grad_hidden
    branch_full = lax.all_gather(grad_hidden.astype(BF), "tensor", axis=0, tiled=True)
    grad_mixed = contract(branch_full, output_full, 1, 1).astype(BF)
    grad_w_output = contract(mixed_flat, branch_full, 0, 0)
    grad_query_rot, grad_key_rot, grad_value_heads = attend_backward(
        query_groups,
        key_heads,
        value_heads,
        mixed_heads,
        grad_mixed.reshape(row_count, kv_local, group, HD),
        log_totals,
        allowed,
        score_scale,
    )
    grad_queries = (
        unrotate(grad_query_rot.reshape(row_count, heads_local, HD), cosine, sine)
        .reshape(row_count, heads_local * HD)
        .astype(BF)
    )
    grad_keys = (
        unrotate(grad_key_rot, cosine, sine).reshape(row_count, kv_local * HD).astype(BF)
    )
    grad_values = grad_value_heads.reshape(row_count, kv_local * HD).astype(BF)
    grad_w_query = contract(normed_attn, grad_queries, 0, 0)
    grad_w_key = contract(normed_attn, grad_keys, 0, 0)
    grad_w_value = contract(normed_attn, grad_values, 0, 0)
    grad_normed_attn = narrow_scatter(
        contract(grad_queries, query_full, 1, 1)
        + contract(grad_keys, key_full, 1, 1)
        + contract(grad_values, value_full, 1, 1),
        "tensor",
        scatter_dimension=0,
        tiled=True,
    )
    grad_residual, gain_attn_part = normalize_back(
        grad_normed_attn, unit_attn, inverse_attn, gain_attn
    )
    grad_input = grad_hidden + grad_residual
    gain_attn_total, gain_ffn_total = lax.psum((gain_attn_part, gain_ffn_part), "tensor")
    owned = (
        narrow_scatter(grad_w_query, "dp", scatter_dimension=0, tiled=True),
        narrow_scatter(grad_w_key, "dp", scatter_dimension=0, tiled=True),
        narrow_scatter(grad_w_value, "dp", scatter_dimension=0, tiled=True),
        narrow_scatter(grad_w_output, "dp", scatter_dimension=1, tiled=True),
        narrow_scatter(gain_attn_total, "dp", scatter_dimension=0, tiled=True),
        narrow_scatter(gain_ffn_total, "dp", scatter_dimension=0, tiled=True),
        narrow_scatter(grad_w_gate, "dp", scatter_dimension=0, tiled=True),
        narrow_scatter(grad_w_up, "dp", scatter_dimension=0, tiled=True),
        narrow_scatter(grad_w_down, "dp", scatter_dimension=1, tiled=True),
    )
    return (
        layer_output,
        grad_input,
        owned[4],
        owned[0],
        owned[1],
        owned[2],
        owned[3],
        owned[5],
        owned[6],
        owned[7],
        owned[8],
    )


def with_kernels(nt, nd, layer_input, segment_ids, norm_attn, w_query, w_key, w_value, w_output, norm_ffn, w_gate, w_up, w_down, cotangent):
    y, gi, gains, d_wq, d_kv, d_wo, d_down, d_gate, d_up, *_ = layer(
        nt, nd, layer_input, cotangent, norm_attn, norm_ffn, segment_ids[None, :],
        w_query, w_key.T, w_value.T, w_output, w_gate, w_up, w_down,
    )
    y, gi, d_wq, d_wo, d_gate, d_up, d_down, d_k, d_v, d_attn, d_ffn = hand_over(
        (y, gi, d_wq, d_wo, d_gate, d_up, d_down), d_kv, gains
    )
    return (y, gi, d_attn, d_wq, d_k.T, d_v.T, d_wo, d_ffn, d_gate, d_up, d_down)


def fits(nt, nd, shards):
    layer_input, segment_ids, norm_attn, w_query, w_key, w_value, w_output, norm_ffn, w_gate, w_up, w_down, _ = shards
    return (
        nd >= 4
        and nd & (nd - 1) == 0
        and nt >= 2
        and norm_attn.shape[0] % LANES == 0
        and w_output.shape[1] % LANES == 0
        and w_gate.shape[1] % LANES == 0
        and w_query.shape[1] % LANES == 0
        and w_key.shape[1] == HD
        and segment_ids.shape[0] == nt * layer_input.shape[0]
        and segment_ids.shape[0] % LANES == 0
    )


def on_device(nt, nd, *shards):
    if fits(nt, nd, shards):
        return with_kernels(nt, nd, *shards)
    return plain_device(*shards)


def solution(mesh):
    placed = (
        P(("dp", "tensor"), None),
        P("dp"),
        P("dp"),
        P("dp", "tensor"),
        P("dp", "tensor"),
        P("dp", "tensor"),
        P("tensor", "dp"),
        P("dp"),
        P("dp", "tensor"),
        P("dp", "tensor"),
        P("tensor", "dp"),
        P(("dp", "tensor"), None),
    )
    return jax.shard_map(
        functools.partial(on_device, mesh.shape["tensor"], mesh.shape["dp"]),
        mesh=mesh,
        in_specs=placed,
        out_specs=(
            P(("dp", "tensor"), None),
            P(("dp", "tensor"), None),
            P("dp"),
            P("dp", "tensor"),
            P("dp", "tensor"),
            P("dp", "tensor"),
            P("tensor", "dp"),
            P("dp"),
            P("dp", "tensor"),
            P("dp", "tensor"),
            P("tensor", "dp"),
        ),
        check_vma=False,
    )
```

```python
import functools
import math

import jax
import jax.numpy as jnp
from jax import lax
from jax.experimental import pallas as pl
from jax.experimental.pallas import tpu as pltpu
from jax.sharding import PartitionSpec as P

HD = 64
EPSILON = 1e-05
NEGATIVE = -1e30
LANES = 128
BF = jnp.bfloat16
F32 = jnp.float32
VMEM_BYTES = 67_000_000


def spans(bits):
    masks = [0]
    for bit in bits:
        masks = masks + [mask | (1 << bit) for mask in masks]
    return masks


def flip(index, mask, width):
    total = 0
    for bit in range(width):
        own = lax.rem(lax.div(index, 1 << bit), 2)
        if isinstance(mask, int):
            other = (mask >> bit) & 1
        else:
            other = lax.rem(lax.div(mask, 1 << bit), 2)
        total = total + lax.rem(own + other, 2) * (1 << bit)
    return total


def aligned(value, step):
    return value if isinstance(value, int) else pl.multiple_of(value, step)


def remote(src, dst, send_sem, recv_sem, device):
    return pltpu.make_async_remote_copy(
        src_ref=src,
        dst_ref=dst,
        send_sem=send_sem,
        recv_sem=recv_sem,
        device_id=device,
        device_id_type=pl.DeviceIdType.MESH,
    )


def dot(left, right, left_dim=1, right_dim=0):
    return lax.dot_general(
        left, right, (((left_dim,), (right_dim,)), ((), ())), preferred_element_type=F32
    )


def tiles_of(size, most):
    units = size // LANES
    parts = -(-units // most)
    cuts, start = [], 0
    for part in range(parts):
        width = (units // parts + (1 if part < units % parts else 0)) * LANES
        cuts.append((start, width))
        start += width
    return cuts


def over_cols(size, width, body):
    @pl.loop(0, size // width)
    def _(i):
        body(pl.ds(pl.multiple_of(i * width, width), width))


def enter(t, nt, me, width, barrier, everyone_along_tensor=False):
    signal = functools.partial(
        pl.semaphore_signal, barrier, inc=1, device_id_type=pl.DeviceIdType.MESH
    )
    for mask in range(1, 1 << width):
        signal(device_id={"dp": flip(me, mask, width)})
    if everyone_along_tensor:
        for step in range(1, nt):
            signal(device_id={"tensor": lax.rem(t + step, nt)})
        pl.semaphore_wait(barrier, (1 << width) - 1 + nt - 1)
        return

    @pl.when(t > 0)
    def _():
        signal(device_id={"tensor": t - 1})

    @pl.when(t < nt - 1)
    def _():
        signal(device_id={"tensor": t + 1})

    neighbours = lax.min(t, 1) + lax.min(nt - 1 - t, 1)
    pl.semaphore_wait(barrier, (1 << width) - 1 + neighbours)


class LineGather:
    def __init__(self, full, row, size, t, nt, sems):
        self.full, self.row, self.size = full, row, size
        self.t, self.nt, self.sems = t, nt, sems
        self.pieces = sems.shape[2]
        self.done = set()

    def window(self, j, s):
        return self.full.at[pl.ds(aligned(self.row(j, s), self.size), self.size), :]

    def right(self, j, s):
        at = self.window(j, s)
        return remote(
            at, at, self.sems.at[0, j, s], self.sems.at[2, j, s],
            {"tensor": lax.rem(self.t + 1, self.nt)},
        )

    def left(self, j, s):
        at = self.window(j, s)
        return remote(
            at, at, self.sems.at[1, j, s], self.sems.at[3, j, s],
            {"tensor": lax.rem(self.t + self.nt - 1, self.nt)},
        )

    def start(self, s):
        @pl.when(self.t < self.nt - 1)
        def _():
            self.right(self.t, s).start()

        @pl.when(self.t > 0)
        def _():
            self.left(self.t, s).start()

    def step(self, k, s):
        t, nt = self.t, self.nt
        if k >= nt or (k, s) in self.done:
            return
        self.done.add((k, s))

        @pl.when(t >= k)
        def _():
            self.right(t - k, s).wait_recv()

            @pl.when(t < nt - 1)
            def _():
                self.right(t - k, s).start()

        @pl.when(t + k < nt)
        def _():
            self.left(t + k, s).wait_recv()

            @pl.when(t > 0)
            def _():
                self.left(t + k, s).start()

    def complete(self, pieces):
        for k in range(1, self.nt):
            for s in pieces:
                self.step(k, s)

    def finish(self, pieces):
        t, nt = self.t, self.nt

        @pl.loop(0, nt)
        def _(k):
            for s in pieces:
                @pl.when((t >= k) & (t < nt - 1))
                def _():
                    self.right(t - k, s).wait_send()

                @pl.when((t + k < nt) & (t > 0))
                def _():
                    self.left(t + k, s).wait_send()


class LineScatter:
    def __init__(self, part, row, sent, arrived, t, nt, sems):
        self.part, self.row, self.sent, self.arrived = part, row, sent, arrived
        self.t, self.nt, self.sems = t, nt, sems
        self.pieces = sems.shape[3]
        self.size = sent.shape[1] // self.pieces
        self.model = sent.shape[2]
        self.near = lax.div(2 * t, nt)
        self.far = 1 - self.near

    def sub(self, s):
        return pl.ds(s * self.size, self.size)

    def depth(self, way):
        return (1 - way) * self.t + way * (self.nt - 1 - self.t)

    def goal(self, way, i):
        return (1 - way) * (self.nt - 1 - i) + way * i

    def slot(self, way, j):
        return j + 1 - way

    def move(self, way, j, s):
        return remote(
            self.sent.at[j, self.sub(s), :], self.arrived.at[self.slot(way, j), self.sub(s), :],
            self.sems.at[0, way, j, s], self.sems.at[1, way, j, s],
            {"tensor": lax.rem(self.t + self.nt + 1 - 2 * way, self.nt)},
        )

    def rows(self, j, s):
        return pl.ds(aligned(self.row(j, s), self.size), self.size)

    def mine(self, j, s):
        return self.part[self.rows(j, s), : self.model]

    def edge(self, s):
        t, nt = self.t, self.nt

        @pl.when((t == 0) | (t == nt - 1))
        def _():
            way = lax.div(t, nt - 1)

            @pl.loop(0, nt - 1)
            def _(i):
                j = self.goal(way, i)
                self.sent[j, self.sub(s), :] = self.mine(j, s).astype(BF)
                self.move(way, j, s).start()

    def relay(self, way, s):
        depth = self.depth(way)

        @pl.when(depth > 0)
        def _():
            @pl.loop(0, self.nt - 1 - depth)
            def _(i):
                j = self.goal(way, i)
                self.move(way, j, s).wait_recv()
                total = self.mine(j, s) + self.arrived[self.slot(way, j), self.sub(s), :].astype(F32)
                self.sent[j, self.sub(s), :] = total.astype(BF)
                self.move(way, j, s).start()

    def own(self, s):
        t = self.t
        rows = self.rows(t, s)
        for way in (self.near, self.far):
            @pl.when(self.depth(way) > 0)
            def _():
                self.move(way, t, s).wait_recv()
                self.part[rows, : self.model] += self.arrived[self.slot(way, t), self.sub(s), :].astype(F32)

        return rows

    def finish(self, pieces):
        for way in range(2):
            @pl.loop(0, self.nt - 1 - self.depth(way))
            def _(i):
                for s in pieces:
                    self.move(way, self.goal(way, i), s).wait_send()


class Cube:
    def setup(self, me, width, half_send, half_recv, pair_send, pair_recv):
        self.me, self.width = me, width
        self.hs, self.hr, self.ps, self.pr = half_send, half_recv, pair_send, pair_recv
        self.bits = list(range(1, width))
        self.orders = (self.bits, self.bits[::-1])
        self.masks = spans(self.bits)
        self.stages = len(self.bits)

    def at(self, mask):
        return flip(self.me, mask, self.width)


class BlockGather(Cube):
    def __init__(self, own, full, by_rows, me, width, *sems):
        self.setup(me, width, *sems)
        self.own_ref, self.full, self.by_rows = own, full, by_rows

    def half(self, h):
        rows = self.own_ref.shape[0] // 2
        return self.own_ref.at[pl.ds(h * rows, rows), :]

    def window(self, who, h=None):
        rows, cols = self.own_ref.shape
        take, start = (rows, 0) if h is None else (rows // 2, h * (rows // 2))
        if self.by_rows:
            return self.full.at[pl.ds(aligned(who * rows + start, take), take), :]
        return self.full.at[pl.ds(start, take), pl.ds(aligned(who * cols, cols), cols)]

    def hop(self, stage, h, m):
        order = self.orders[h]
        bit = 1 << order[stage]
        slot = (m | bit) >> 1
        src = self.half(h) if m == 0 else self.window(self.at(m), h)
        return remote(
            src, self.window(self.at(m), h), self.hs.at[h, slot - 1], self.hr.at[h, slot - 1],
            {"dp": self.at(bit)},
        )

    def send(self, stage):
        for h in range(2):
            for m in spans(self.orders[h][:stage]):
                self.hop(stage, h, m).start()

    def wait(self, stage):
        for h in range(2):
            bit = 1 << self.orders[h][stage]
            for m in spans(self.orders[h][:stage]):
                slot = (m | bit) >> 1
                landed = self.window(self.at(m | bit), h)
                remote(
                    landed, landed, self.hs.at[h, slot - 1], self.hr.at[h, slot - 1],
                    {"dp": self.at(bit)},
                ).wait_recv()

    def pair(self, m):
        src = self.own_ref if m == 0 else self.window(self.at(m))
        return remote(
            src, self.window(self.at(m)), self.ps.at[m >> 1], self.pr.at[m >> 1],
            {"dp": self.at(1)},
        )

    def pair_own(self):
        self.pair(0).start()

    def pair_send(self):
        for m in self.masks:
            if m:
                self.pair(m).start()

    def pair_wait(self):
        for m in self.masks:
            landed = self.window(self.at(m | 1))
            remote(
                landed, landed, self.ps.at[m >> 1], self.pr.at[m >> 1], {"dp": self.at(1)}
            ).wait_recv()

    def place(self, sem):
        return pltpu.make_async_copy(self.own_ref, self.window(self.me), sem)

    def drain(self):
        for stage in range(self.stages):
            for h in range(2):
                for m in spans(self.orders[h][:stage]):
                    self.hop(stage, h, m).wait_send()
        for m in self.masks:
            self.pair(m).wait_send()


class BlockScatter(Cube):
    def __init__(self, chunk, out_sent, total, landed, store, me, width, *sems):
        self.setup(me, width, *sems)
        self.chunk, self.sent, self.total, self.landed = chunk, out_sent, total, landed
        self.store = store
        self.slots = 1 << (width - 1)

    def pair(self, slot):
        return remote(
            self.sent.at[slot], self.total.at[slot], self.ps.at[slot], self.pr.at[slot],
            {"dp": self.at(1)},
        )

    def give(self):
        @pl.loop(0, self.slots)
        def _(k):
            slot = self.slots - 1 - k
            self.sent[slot] = self.chunk(self.at(2 * slot + 1)).astype(BF)
            self.pair(slot).start()

    def given(self):
        @pl.loop(0, self.slots)
        def _(slot):
            self.pair(slot).wait_send()

    def take(self):
        @pl.loop(0, self.slots)
        def _(k):
            slot = self.slots - 1 - k
            term = self.chunk(self.at(2 * slot))
            self.pair(slot).wait_recv()
            self.total[slot] = (term + self.total[slot].astype(F32)).astype(BF)

    def moves(self, stage):
        for h in range(2):
            order = self.orders[h]
            last = self.stages - 1 - stage
            bit = 1 << order[last]
            for m in spans(order[:last]):
                yield h, bit, m | bit

    def hop(self, h, bit, m):
        rows = self.total.shape[1] // 2
        return remote(
            self.total.at[m >> 1, pl.ds(h * rows, rows), :], self.landed.at[h, (m >> 1) - 1],
            self.hs.at[h, (m >> 1) - 1], self.hr.at[h, (m >> 1) - 1], {"dp": self.at(bit)},
        )

    def send(self, stage):
        for h, bit, m in self.moves(stage):
            self.hop(h, bit, m).start()

    def add(self, stage):
        rows = self.total.shape[1] // 2
        for h, bit, m in self.moves(stage):
            self.hop(h, bit, m).wait_recv()
            keep = (m ^ bit) >> 1
            at = slice(h * rows, (h + 1) * rows)
            total = self.total[keep, at, :].astype(F32) + self.landed[h, (m >> 1) - 1].astype(F32)
            if stage == self.stages - 1:
                self.store(at, total)
            else:
                self.total[keep, at, :] = total.astype(BF)

    def drain(self):
        for stage in range(self.stages):
            for h, bit, m in self.moves(stage):
                self.hop(h, bit, m).wait_send()


def inverse_of(rows):
    return lax.rsqrt(jnp.mean(rows * rows, axis=-1, keepdims=True) + EPSILON)


def times_gain(unit, gains, which, store):
    parts, _, width = gains.shape
    for d in range(parts):
        cols = slice(d * width, (d + 1) * width)
        store(cols, unit[:, cols] * gains[d, which : which + 1, :])


def lane_index(shape):
    return lax.broadcasted_iota(jnp.int32, shape, len(shape) - 1)


def column_of(segr):
    rows = segr.shape[1]
    wide = jnp.broadcast_to(segr[...].astype(F32), (8, rows))
    return jnp.transpose(wide)[:, 0:1]


def rope_into(cos_ref, sin_ref, segr):
    rows = segr.shape[1]
    before = (segr[...].astype(F32) < column_of(segr)).astype(F32)
    start = jnp.sum(before, axis=1, keepdims=True)
    position = lax.broadcasted_iota(jnp.int32, (rows, 1), 0).astype(F32) - start
    lane = lane_index((rows, LANES))
    half = HD // 2
    frequency = jnp.exp(lax.rem(lane, half).astype(F32) * (-math.log(10000.0) / half))
    angle = position * frequency
    cos_ref[...] = jnp.cos(angle)
    sine = jnp.sin(angle)
    sin_ref[...] = jnp.where(lax.rem(lane, HD) < half, -sine, sine)


def swapped(x):
    lane = lane_index(x.shape)
    half = HD // 2
    return jnp.where(
        lax.rem(lane, HD) < half,
        pltpu.roll(x, LANES - half, 1),
        pltpu.roll(x, half, 1),
    )


def bias_into(bias, segr):
    rows = segr.shape[1]
    query = lax.broadcasted_iota(jnp.int32, (rows, rows), 0)
    key = lax.broadcasted_iota(jnp.int32, (rows, rows), 1)
    seen = (segr[...].astype(F32) == column_of(segr)) & (query >= key)
    bias[...] = jnp.where(seen, 0.0, NEGATIVE)


def pad_pair(keys_values, keys, values):
    low = lane_index(keys_values.shape) < HD
    key = jnp.where(low, keys_values, 0.0)
    value = jnp.where(low, 0.0, keys_values)
    keys[0] = key.astype(BF)
    keys[1] = pltpu.roll(key, HD, 1).astype(BF)
    values[0] = pltpu.roll(value, HD, 1).astype(BF)
    values[1] = value.astype(BF)


def query_cuts(rows):
    block = 256 if rows % 256 == 0 else rows
    return [(start, block, start + block) for start in range(0, rows, block)]


def attend_pairs(first, last, qo, kpad, vpad, bias, mo, lo):
    rows = qo.shape[0]
    lane = lane_index((1, LANES))

    @pl.loop(first, last)
    def _(pair):
        lanes = pl.ds(pl.multiple_of(pair * LANES, LANES), LANES)
        for start, block, seen in query_cuts(rows):
            at = slice(start, start + block)
            query = qo[at, lanes]
            mixed = jnp.zeros((block, LANES), F32)
            logs = lo[at, :]
            for side in range(2):
                scores = dot(query, kpad[side, :seen, :], 1, 1) + bias[at, :seen]
                top = jnp.max(scores, axis=-1, keepdims=True)
                probs = jnp.exp(scores - top)
                total = jnp.sum(probs, axis=-1, keepdims=True)
                mixed = mixed + dot(probs.astype(BF), vpad[side, :seen, :]) / total
                logs = jnp.where(lane == 2 * pair + side, top + jnp.log(total), logs)
            lo[at, :] = logs
            mo[at, lanes] = mixed.astype(BF)


def back_through_norm(raw, grads, gains, which, store, store_gain):
    parts, _, width = gains.shape
    cuts = [slice(d * width, (d + 1) * width) for d in range(parts)]
    model = parts * width
    square = sum(jnp.sum(raw(c) * raw(c), axis=-1, keepdims=True) for c in cuts)
    inverse = lax.rsqrt(square / model + EPSILON)
    mean = 0.0
    for d, c in enumerate(cuts):
        unit = raw(c) * inverse
        grad = grads(c)
        store_gain(c, jnp.sum(grad * unit, axis=0, keepdims=True))
        mean = mean + jnp.sum(grad * gains[d, which : which + 1, :] * unit, axis=-1, keepdims=True)
    mean = mean / model
    for d, c in enumerate(cuts):
        unit = raw(c) * inverse
        store(c, inverse * (grads(c) * gains[d, which : which + 1, :] - unit * mean))


def attend_back_pairs(first, last, qo, gm, mo, lo, kpad, vpad, bias, cos, sin, dqkv, dkey, dval):
    rows = qo.shape[0]

    @pl.loop(first, last)
    def _(pair):
        lanes = pl.ds(pl.multiple_of(pair * LANES, LANES), LANES)
        for start, block, seen in query_cuts(rows):
            at = slice(start, start + block)
            lane = lane_index((block, LANES))
            query, grad = qo[at, lanes], gm[at, lanes]
            both = grad.astype(F32) * mo[at, lanes].astype(F32)
            logs = lo[at, :]
            dq = jnp.zeros((block, LANES), F32)
            for side in range(2):
                inside = (lane >= HD) if side else (lane < HD)
                delta = jnp.sum(jnp.where(inside, both, 0.0), axis=-1, keepdims=True)
                log = jnp.sum(
                    jnp.where(lane == 2 * pair + side, logs, 0.0), axis=-1, keepdims=True
                )
                key, value = kpad[side, :seen, :], vpad[side, :seen, :]
                probs = jnp.exp(dot(query, key, 1, 1) + bias[at, :seen] - log)
                grad_scores = (probs * (dot(grad, value, 1, 1) - delta)).astype(BF)
                dq = dq + dot(grad_scores, key)
                dkey[side, :seen, :] += dot(grad_scores, query, 0, 0)
                dval[side, :seen, :] += dot(probs.astype(BF), grad, 0, 0)
            dq = dq * HD ** (-0.5)
            dqkv[at, lanes] = (dq * cos[at, :] - swapped(dq) * sin[at, :]).astype(BF)


PIECES = 4


def vmem():
    return pl.BlockSpec(memory_space=pltpu.VMEM)


def hbm():
    return pl.BlockSpec(memory_space=pl.ANY)


def dma(*shape):
    return pltpu.SemaphoreType.DMA(shape)


def line_scratch(nt, rows, model):
    return [pltpu.VMEM((nt, rows, model), BF), pltpu.VMEM((nt + 1, rows, model), BF)]


def ticks(pieces, nt):
    return [
        [(k, tick - k) for k in range(1, nt) if 0 <= tick - k < pieces]
        for tick in range(pieces + nt - 1)
    ]


def layer_kernel(
    nt, width,
    x, cot, gain_a, gain_f, segr, wq, wkt, wvt, wo, gate, up, down,
    y_o, gi_o, gain_o, d_wq_o, d_kv_o, d_wo_o, d_down_o, d_gate, d_up, wqkv_f, wo_f, na_f,
    rowsbuf, cf, branch, act, hid, gate_v, up_v, down_v, part, sent, arrived, totals, landed, stage_v,
    y, gi, gain_out, d_wq, d_kv, d_wo, d_down,
    own_qkv, gain, gall, qo, kvo, mo, lo, cos, sin, gsum, zslots, dslots,
    gain_sem, place_sem, out_sem, line_sem, cot_sem, sum_sem,
    hs, hr, ps, pr, zsem, dsem, emit_sem, ready, calm,
):
    me, t = lax.axis_index("dp"), lax.axis_index("tensor")
    nd = 1 << width
    rows, model = x.shape
    tokens = nt * rows
    queries = wq.shape[1]
    hidden = gate.shape[1]
    shard = model >> width
    wide = own_qkv.shape[1]
    pieces = PIECES
    first_half = pieces // 2
    size = rows // pieces
    cut = 512 if model % 512 == 0 else LANES

    def natural(j, s):
        return j * rows + s * size

    def shuffled(j, s):
        return (s * nt + j) * size

    local = pl.ds(pl.multiple_of(t * rows, rows), rows)
    rowsbuf[local, :] = x[...]
    gain[...] = jnp.zeros_like(gain)
    gain[0:1, :] = gain_a[...].astype(F32).reshape(1, shard)
    gain[1:2, :] = gain_f[...].astype(F32).reshape(1, shard)
    own_qkv[:, :queries] = wq[...]
    turned = jnp.concatenate([wkt[...].astype(F32), wvt[...].astype(F32)], axis=0)
    own_qkv[:, queries:] = jnp.transpose(turned).astype(BF)
    with jax.named_scope("enter"):
        enter(t, nt, me, width, pltpu.get_barrier_semaphore())

    tokens_x = LineGather(rowsbuf, natural, size, t, nt, line_sem)
    for s in range(pieces):
        tokens_x.start(s)
    gathers = []
    for w, (own, full, by_rows) in enumerate(
        ((own_qkv, wqkv_f, True), (wo, wo_f, False), (gate, gate_v, True), (up, up_v, True), (down, down_v, False))
    ):
        gathers.append(
            BlockGather(own, full, by_rows, me, width, hs.at[w], hr.at[w], ps.at[w], pr.at[w])
        )
    g_qkv, g_out, g_gate, g_up, g_down = gathers
    stages = g_qkv.stages

    def gain_copy(mask):
        return remote(
            gain, gall.at[me], gain_sem.at[0, mask], gain_sem.at[1, mask],
            {"dp": flip(me, mask, width)},
        )

    for mask in range(1, nd):
        gain_copy(mask).start()
    for g in (g_qkv, g_out, g_gate):
        g.send(0)
    for w, g in enumerate(gathers):
        g.place(place_sem.at[w]).start()
    gall[me] = gain[...]

    def forward(g, stage):
        g.wait(stage)
        if stage == 0:
            g.pair_own()
        if stage + 1 < stages:
            g.send(stage + 1)
        else:
            g.pair_send()

    for s in range(pieces):
        cf[pl.ds(pl.multiple_of(shuffled(t, s), size), size), :] = cot[s * size : (s + 1) * size, :]
    cots = LineGather(cf, shuffled, size, t, nt, cot_sem)
    scatter_o = LineScatter(part, shuffled, sent, arrived, t, nt, sum_sem)

    def attention(na, wqkv_v, wo_v, bias, kpad, vpad):
        bias_into(bias, segr)
        rope_into(cos, sin, segr)
        lo[...] = jnp.zeros_like(lo)
        for mask in range(1, nd):
            slot = gall.at[flip(me, mask, width)]
            remote(
                slot, slot, gain_sem.at[0, mask], gain_sem.at[1, mask],
                {"dp": flip(me, mask, width)},
            ).wait_recv()

        def norm(j):
            @pl.loop(0, pieces)
            def _(s):
                these = pl.ds(pl.multiple_of(j * rows + s * size, size), size)
                value = rowsbuf[these, :].astype(F32)

                def store(cols, normed):
                    na[these, cols] = normed.astype(BF)

                times_gain(value * inverse_of(value), gall, 0, store)

        norm(t)
        for stage in range(stages - 1):
            forward(g_qkv, stage)
            forward(g_out, stage)
        fills = [
            lambda: (forward(g_gate, 0), g_up.send(0)),
            lambda: (forward(g_qkv, stages - 1), forward(g_out, stages - 1), g_down.send(0)),
        ]
        load = pltpu.make_async_copy(wqkv_f, wqkv_v, place_sem.at[5])
        load_out = pltpu.make_async_copy(wo_f, wo_v, place_sem.at[6])

        def fetch():
            g_qkv.place(place_sem.at[0]).wait()
            g_qkv.pair_wait()
            load.start()
            g_out.place(place_sem.at[1]).wait()
            g_out.pair_wait()
            load_out.start()

        for k in range(1, nt):
            if k == nt - 1:
                for fill in fills:
                    fill()
                fills = []
                with jax.named_scope("fetch"):
                    fetch()
            with jax.named_scope("x_step"):
                for s in range(pieces):
                    tokens_x.step(k, s)
            if k == nt - 1:
                for s in range(first_half):
                    cots.start(s)

            @pl.when(t >= k)
            def _():
                norm(t - k)

            @pl.when(t + k < nt)
            def _():
                norm(t + k)

            if fills:
                with jax.named_scope("x_fill"):
                    fills.pop(0)()
        keep = pltpu.make_async_copy(na, na_f, out_sem.at[0])
        keep.start()
        with jax.named_scope("wait_qkv"):
            load.wait()
        with jax.named_scope("qkv"):
            part[:, :wide] = dot(na[...], wqkv_v[...])
            c, s_ = cos[...], sin[...]
            for start in range(0, queries, LANES):
                lanes = slice(start, start + LANES)
                value = part[:, lanes]
                qo[:, lanes] = ((value * c + swapped(value) * s_) * HD ** (-0.5)).astype(BF)
            value = part[:, queries : queries + LANES]
            keyed = jnp.where(lane_index(value.shape) < HD, value * c + swapped(value) * s_, value)
            kvo[...] = keyed.astype(BF)
            pad_pair(keyed, kpad, vpad)
        pairs = queries // LANES
        with jax.named_scope("att"):
            attend_pairs(0, pairs, qo, kpad, vpad, bias, mo, lo)
        load_out.wait()
        with jax.named_scope("outproj"):
            mixed = jnp.concatenate(
                [
                    mo[natural(j, s) : natural(j, s) + size, :]
                    for s in range(pieces)
                    for j in range(nt)
                ],
                axis=0,
            )

            def project(cols):
                part[:tokens, cols] = dot(mixed, wo_v[:, cols])

            over_cols(model, cut, project)
        keep.wait()
        tokens_x.finish(range(pieces))

    pl.run_scoped(
        attention,
        pltpu.VMEM((tokens, model), BF),
        pltpu.VMEM((model, wide), BF),
        pltpu.VMEM((queries, model), BF),
        pltpu.VMEM((tokens, tokens), F32),
        pltpu.VMEM((2, tokens, LANES), BF),
        pltpu.VMEM((2, tokens, LANES), BF),
    )

    gather_nf = LineGather(rowsbuf, shuffled, size, t, nt, line_sem)

    def take_hidden(s):
        at = scatter_o.own(s)
        block = slice(s * size, (s + 1) * size)
        hidden_rows = x[block, :].astype(F32) + part[at, :model]
        hid[block, :] = hidden_rows
        there = pl.ds(pl.multiple_of(shuffled(t, s), size), size)

        def store(cols, normed):
            rowsbuf[there, cols] = normed.astype(BF)

        times_gain(hidden_rows * inverse_of(hidden_rows), gall, 1, store)
        gather_nf.start(s)

    def chunk_of(left, right):
        def chunk(d):
            return dot(left[:, pl.ds(pl.multiple_of(d * shard, shard), shard)], right[...], 0, 0)

        return chunk

    def cube(w, totals_, landed_, store):
        return BlockScatter(
            None, None, totals_, landed_, store, me, width, hs.at[w], hr.at[w], ps.at[w], pr.at[w]
        )

    def store_stage(at, value):
        stage_v[at, :] = value

    def store_down(at, value):
        d_down[:, at] = value.T

    def store_qkv(at, value):
        d_wq[at, :] = value[:, :queries]
        d_kv[:, at] = value[:, queries:].T

    def store_wo(at, value):
        d_wo[:, at] = value.T

    for_qkv, for_wo = pl.ds(0, wide), pl.ds(wide, queries)
    s_gate = cube(5, totals.at[0], landed.at[0], store_stage)
    s_up = cube(6, totals.at[1], landed.at[1], store_stage)
    s_down = cube(5, totals.at[0], landed.at[0], store_down)
    s_qkv = cube(6, totals.at[1, :, :, for_qkv], landed.at[1, :, :, :, for_qkv], store_qkv)
    s_out = cube(7, totals.at[1, :, :, for_wo], landed.at[1, :, :, :, for_wo], store_wo)

    def take(s):
        s.take()
        s.send(0)

    def on(s, stage):
        s.add(stage)
        if stage + 1 < stages:
            s.send(stage + 1)

    scatter_y = LineScatter(part, shuffled, sent, arrived, t, nt, sum_sem)
    scope = jax.named_scope
    emitted = []

    def emit(src, dst):
        emitted.append(pltpu.make_async_copy(src, dst, emit_sem.at[len(emitted)]))
        emitted[-1].start()

    def y_part(h):
        mine = slice(h * (tokens // 2), (h + 1) * (tokens // 2))
        with scope("y_part"):

            def product(cols):
                part[mine, cols] = dot(act[mine, :], down_v[:, cols])

            over_cols(model, cut, product)

    def y_near(s):
        with scope("y_near"):
            scatter_y.relay(scatter_y.near, s)

    def y_far(s):
        with scope("y_far"):
            scatter_y.relay(scatter_y.far, s)

    def y_own(s):
        with scope("y_own"):
            at = scatter_y.own(s)
            block_ = slice(s * size, (s + 1) * size)
            y[block_, :] = (hid[block_, :] + part[at, :model]).astype(BF)
            emit(y.at[pl.ds(s * size, size), :], y_o.at[pl.ds(s * size, size), :])

    def br(k, s):
        with scope("br_step"):
            gather_br.step(k, s)

    gsum[...] = jnp.zeros_like(gsum)
    gather_br = LineGather(branch, natural, size, t, nt, line_sem)

    def feed(dg, du, given):
        cuts = tiles_of(hidden, 6)
        span = max(width_ for _, width_ in cuts)
        half = tokens // 2
        block = 64

        def tile_in(h, i):
            start, width_ = cuts[i]
            at = slice(start, start + width_)
            held = mine = slice(h * half, (h + 1) * half)
            part[held, 0:width_] = dot(rowsbuf[mine, :], gate_v[:, at])
            part[held, span : span + width_] = dot(rowsbuf[mine, :], up_v[:, at])

        def tile_out(h, i):
            start, width_ = cuts[i]
            at = slice(start, start + width_)
            held = mine = slice(h * half, (h + 1) * half)
            part[held, 2 * span : 2 * span + width_] = dot(cf[mine, :], down_v[at, :], 1, 1)

            @pl.loop(0, half // block)
            def _(k):
                from_ = pl.ds(pl.multiple_of(h * half + k * block, block), block)
                to = pl.ds(pl.multiple_of(h * half + k * block, block), block)
                g = part[from_, 0:width_]
                u = part[from_, span : span + width_]
                ga = part[from_, 2 * span : 2 * span + width_]
                sig = 1.0 / (1.0 + jnp.exp(-g))
                gs = g * sig
                act[to, at] = (gs * u).astype(BF)
                du[to, at] = (ga * gs).astype(BF)
                dg[to, at] = (ga * u * sig * (1.0 + g * (1.0 - sig))).astype(BF)

        def tile(h, i):
            with scope("tile"):
                tile_in(h, i)
                tile_out(h, i)

        def back_dots(h):
            mine = slice(h * half, (h + 1) * half)

            def product(cols):
                part[mine, cols] = dot(dg[mine, :], gate_v[cols, :], 1, 1) + dot(
                    du[mine, :], up_v[cols, :], 1, 1
                )

            over_cols(model, cut, product)

        scatter_gn = LineScatter(part, shuffled, sent, arrived, t, nt, sum_sem)

        def take_grad(s):
            at = scatter_gn.own(s)
            block_ = slice(s * size, (s + 1) * size)
            there = pl.ds(pl.multiple_of(natural(t, s), size), size)

            def store(cols, value):
                total = cot[block_, cols].astype(F32) + value
                gi[block_, cols] = total
                branch[there, cols] = total.astype(BF)

            def store_gain(cols, value):
                gsum[1:2, cols] += value

            back_through_norm(
                lambda c: hid[block_, c], lambda c: part[at, c], gall, 1, store, store_gain
            )
            gather_br.start(s)

        s_gate.chunk, s_up.chunk = chunk_of(rowsbuf, dg), chunk_of(rowsbuf, du)
        s_gate.sent = s_up.sent = given

        half_a, half_b = range(first_half), range(first_half, pieces)
        def o_near(s):
            with scope("o_near"):
                scatter_o.relay(scatter_o.near, s)

        def o_far(s):
            with scope("o_far"):
                scatter_o.relay(scatter_o.far, s)

        def o_take(s):
            with scope("o_take"):
                take_hidden(s)

        def nf(k, s):
            with scope("nf_step"):
                gather_nf.step(k, s)

        def cot_steps(k, which):
            with scope("cot_step"):
                for s in which:
                    cots.step(k, s)

        def gn_near(s):
            with scope("gn_near"):
                scatter_gn.relay(scatter_gn.near, s)

        def gn_far(s):
            with scope("gn_far"):
                scatter_gn.relay(scatter_gn.far, s)

        def gn_take(s):
            with scope("gn_take"):
                take_grad(s)

        def weight(g, stage):
            with scope("weight"):
                if stage < stages:
                    forward(g, stage)

        scatter_o.edge(0)
        scatter_o.edge(1)
        cot_steps(1, half_a)
        weight(g_gate, 1)
        cot_steps(2, half_a)
        o_near(0)
        weight(g_up, 0)
        o_far(0)
        o_take(0)
        weight(g_down, 0)
        scatter_o.edge(2)
        o_near(1)
        o_far(1)
        nf(1, 0)
        cot_steps(3, half_a)
        o_take(1)
        scatter_o.edge(3)
        nf(1, 1)
        nf(2, 0)
        o_near(2)
        nf(2, 1)
        weight(g_up, 1)
        nf(3, 0)
        o_far(2)
        for s in half_b:
            cots.start(s)
        nf(3, 1)
        o_take(2)
        gather_nf.complete(half_a)
        cots.complete(half_a)
        weight(g_down, 1)
        for stage in range(2, stages):
            for g in (g_gate, g_up, g_down):
                weight(g, stage)
        o_near(3)
        with scope("wait_ffn"):
            for w in (2, 3):
                gathers[w].place(place_sem.at[w]).wait()
                gathers[w].pair_wait()
        with scope("tile"):
            tile_in(0, 0)
        with scope("wait_ffn"):
            g_down.place(place_sem.at[4]).wait()
            g_down.pair_wait()
        with scope("tile"):
            tile_out(0, 0)
        o_far(3)
        nf(1, 2)
        cot_steps(1, half_b)
        for i in range(1, len(cuts)):
            tile(0, i)
        o_take(3)
        nf(2, 2)
        with scope("back_dots"):
            scatter_o.finish(half_a)
            back_dots(0)
        scatter_gn.edge(0)
        scatter_gn.edge(1)
        nf(1, 3)
        cot_steps(2, half_b)
        gn_near(0)
        nf(3, 2)
        nf(2, 3)
        gn_far(0)
        cot_steps(3, half_b)
        gn_near(1)
        nf(3, 3)
        gather_nf.complete(half_b)
        cots.complete(half_b)
        gather_nf.finish(half_a)
        tile(1, 0)
        gn_far(1)
        gn_take(0)
        for i in range(1, len(cuts)):
            tile(1, i)
        with scope("back_dots"):
            scatter_o.finish(half_b)
            back_dots(1)
        scatter_gn.edge(2)
        gn_take(1)
        scatter_gn.edge(3)
        br(1, 0)
        with scope("gn_fill"):
            s_gate.give()
            br(2, 0)
            take(s_gate)
        gn_near(2)
        with scope("gn_fill"):
            s_gate.given()
            s_up.give()
        gn_far(2)
        br(1, 1)
        br(3, 0)
        with scope("gn_fill"):
            take(s_up)
        gn_near(3)
        gather_nf.finish(half_b)
        gn_take(2)
        y_part(0)
        scatter_gn.finish(half_a)
        scatter_y.edge(0)
        br(2, 1)
        gn_far(3)
        gn_take(3)
        scatter_y.edge(1)
        br(3, 1)
        br(1, 2)
        y_near(0)
        y_part(1)
        br(2, 2)
        br(1, 3)
        scatter_gn.finish(half_b)
        scatter_y.edge(2)
        scatter_y.edge(3)
        y_far(0)
        br(3, 2)
        br(2, 3)
        with scope("add0"):
            on(s_gate, 0)
        y_near(1)
        y_far(1)
        br(3, 3)
        gather_br.complete(range(pieces))
        s_up.given()

    pl.run_scoped(
        feed,
        pltpu.VMEM((tokens, hidden), BF),
        pltpu.VMEM((tokens, hidden), BF),
        pltpu.VMEM((nd // 2, shard, hidden), BF),
    )

    wo_v = down_v.at[pl.ds(0, queries), :]
    na_v = down_v.at[pl.ds(queries, tokens), :]
    wqkv_v = gate_v.at[:, pl.ds(0, wide)]
    gm = up_v.at[pl.ds(0, tokens), pl.ds(0, queries)]
    dqkv = up_v.at[pl.ds(tokens, tokens), pl.ds(0, wide)]

    def rear(bias, kpad, vpad, dkey, dval, given):
        inward = LineScatter(part, shuffled, sent, arrived, t, nt, sum_sem)
        for g in gathers:
            g.drain()
        loads = [
            pltpu.make_async_copy(wo_f, wo_v, place_sem.at[0]),
            pltpu.make_async_copy(wqkv_f, wqkv_v, place_sem.at[1]),
            pltpu.make_async_copy(na_f, na_v, place_sem.at[2]),
        ]
        for load in loads:
            load.start()
        bias_into(bias, segr)
        pad_pair(kvo[...].astype(F32), kpad, vpad)
        dkey[...] = jnp.zeros_like(dkey)
        dval[...] = jnp.zeros_like(dval)
        s_down.chunk, s_down.sent = chunk_of(cf, act), given
        s_qkv.chunk, s_qkv.sent = chunk_of(na_v, dqkv), given.at[:, :, for_qkv]
        s_out.chunk, s_out.sent = chunk_of(branch, mo), given.at[:, :, for_wo]

        def att(first, last):
            with scope("b_att"):
                attend_back_pairs(
                    first, last, qo, gm, mo, lo, kpad, vpad, bias, cos, sin, dqkv, dkey, dval
                )

        def free(s, out, slot):
            s.add(stages - 1)
            copy = pltpu.make_async_copy(stage_v, out, out_sem.at[1 + slot])
            copy.start()
            s.drain()
            for bit in range(width):
                pl.semaphore_signal(
                    ready.at[slot], inc=1, device_id={"dp": flip(me, 1 << bit, width)},
                    device_id_type=pl.DeviceIdType.MESH,
                )
            return copy

        def quiet(h):
            for step, there in ((-1, t > 0), (1, t < nt - 1)):
                @pl.when(there)
                def _():
                    pl.semaphore_signal(
                        calm.at[h], inc=1, device_id={"tensor": t + step},
                        device_id_type=pl.DeviceIdType.MESH,
                    )

        def gi_part(h):
            which = half_a if h == 0 else half_b
            mine = jnp.concatenate(
                [dqkv[natural(j, s) : natural(j, s) + size, :] for s in which for j in range(nt)],
                axis=0,
            )
            start_row = h * (tokens // 2)
            with scope("b_part"):

                def product(cols):
                    part[start_row : start_row + tokens // 2, cols] = dot(
                        mine, wqkv_v[cols, :], 1, 1
                    )

                over_cols(model, cut, product)
            with scope("calm"):
                pl.semaphore_wait(calm.at[h], lax.min(t, 1) + lax.min(nt - 1 - t, 1))
            for s in which:
                inward.edge(s)

        def gi_near(s):
            with scope("b_near"):
                inward.relay(inward.near, s)

        def gi_far(s):
            with scope("b_far"):
                inward.relay(inward.far, s)

        half_a, half_b = range(first_half), range(first_half, pieces)
        pairs = queries // LANES
        with scope("b_gm"):
            loads[0].wait()
            gm[...] = dot(branch[...], wo_v[...], 1, 1).astype(BF)
        for s in half_a:
            y_own(s)
        scatter_y.finish(half_a)
        quiet(0)
        with scope("add0"):
            on(s_up, 0)
        with scope("free0"):
            copy_gate = free(s_gate, d_gate, 0)

        @pl.loop(0, 2)
        def _(h):
            att(h * (pairs // 2), (h + 1) * (pairs // 2))

            @pl.when(h == 0)
            def _():
                y_near(2)

        with scope("b_give"):
            pl.semaphore_wait(ready.at[0], width)
            s_down.give()
        y_near(3)
        key = dkey[0] + pltpu.roll(dkey[1], HD, 1)
        value = pltpu.roll(dval[0], HD, 1) + dval[1]
        key = key * cos[...] - swapped(key) * sin[...]
        dqkv[:, queries : queries + LANES] = jnp.where(
            lane_index(key.shape) < HD, key, value
        ).astype(BF)
        loads[1].wait()
        gi_part(0)
        with scope("b_take"):
            take(s_down)
        y_far(2)
        with scope("free1"):
            copy_gate.wait()
            copies = [free(s_up, d_up, 1)]
        y_far(3)
        gi_near(0)
        with scope("b_fill"):
            loads[2].wait()
            s_down.given()
            pl.semaphore_wait(ready.at[1], width)
            s_qkv.give()
        for s in half_b:
            y_own(s)
        scatter_y.finish(half_b)
        quiet(1)
        gi_part(1)
        gi_far(0)
        with scope("b_fill"):
            take(s_qkv)
        gi_near(1)
        with scope("b_fill"):
            s_out.give()

        with scope("b_done"):
            for mask in range(1, nd):
                gain_copy(mask).wait_send()
            cots.finish(range(pieces))
            gather_br.finish(range(pieces))

        def take_grad(s):
            at = inward.own(s)
            block = slice(s * size, (s + 1) * size)

            def store(cols, value):
                gi[block, cols] += value

            def store_gain(cols, value):
                gsum[0:1, cols] += value

            back_through_norm(
                lambda c: x[block, c].astype(F32), lambda c: part[at, c], gall, 0, store, store_gain
            )

        fills = [
            functools.partial(on, s, stage)
            for stage in range(stages)
            for s in (s_down, s_qkv, s_out)
        ]
        gi_far(1)
        with scope("b_fill"):
            take(s_out)
        gi_near(2)
        gi_far(2)
        with scope("b_fill"):
            fills.pop(0)()
        gi_near(3)
        gi_far(3)
        with jax.named_scope("b_own"):
            for s in range(pieces):
                take_grad(s)
                emit(gi.at[pl.ds(s * size, size), :], gi_o.at[pl.ds(s * size, size), :])
                if s < pieces - 1 and fills:
                    fills.pop(0)()
        with jax.named_scope("b_gains"):
            zslots[t] = gsum[...]

            def along(step):
                return remote(
                    zslots.at[t], zslots.at[t], zsem.at[0, step], zsem.at[1, step],
                    {"tensor": lax.rem(t + step, nt)},
                )

            for step in range(1, nt):
                along(step).start()
        with jax.named_scope("b_gains"):
            for step in range(1, nt):
                slot = zslots.at[lax.rem(t + nt - step, nt)]
                remote(
                    slot, slot, zsem.at[0, step], zsem.at[1, step], {"tensor": lax.rem(t + step, nt)}
                ).wait_recv()
            gsum[...] = sum(zslots[i] for i in range(nt))

            def across(mask):
                peer = flip(me, mask, width)
                return remote(
                    gsum.at[:, pl.ds(pl.multiple_of(peer * shard, shard), shard)], dslots.at[me],
                    dsem.at[0, mask], dsem.at[1, mask], {"dp": peer},
                )

            for mask in range(1, nd):
                across(mask).start()
            dslots[me] = gsum[:, pl.ds(pl.multiple_of(me * shard, shard), shard)]
        with jax.named_scope("b_rest"):
            for fill in fills:
                fill()
            for src, dst in ((d_wq, d_wq_o), (d_kv, d_kv_o), (d_wo, d_wo_o), (d_down, d_down_o)):
                emit(src, dst)
        with jax.named_scope("b_gains"):
            for mask in range(1, nd):
                peer = flip(me, mask, width)
                slot = dslots.at[peer]
                remote(slot, slot, dsem.at[0, mask], dsem.at[1, mask], {"dp": peer}).wait_recv()
            gain_out[...] = sum(dslots[i] for i in range(nd))
            emit(gain_out, gain_o)
            for step in range(1, nt):
                along(step).wait_send()
            for mask in range(1, nd):
                across(mask).wait_send()
        with jax.named_scope("end"):
            for s in (s_qkv, s_out):
                s.given()
            for s in (s_down, s_qkv, s_out):
                s.drain()
            inward.finish(range(pieces))
            for copy in copies + emitted:
                copy.wait()

    pl.run_scoped(
        rear,
        pltpu.VMEM((tokens, tokens), F32),
        pltpu.VMEM((2, tokens, LANES), BF),
        pltpu.VMEM((2, tokens, LANES), BF),
        pltpu.VMEM((2, tokens, LANES), F32),
        pltpu.VMEM((2, tokens, LANES), F32),
        pltpu.VMEM((nd // 2, shard, hidden), BF),
    )


def layer(nt, nd, x, cot, gain_a, gain_f, segr, wq, wkt, wvt, wo, gate, up, down):
    width = nd.bit_length() - 1
    rows, model = x.shape
    tokens = nt * rows
    queries = wq.shape[1]
    hidden = gate.shape[1]
    shard = model // nd
    half = nd // 2
    wide = queries + LANES
    span = max(width_ for _, width_ in tiles_of(hidden, 6))
    shape = jax.ShapeDtypeStruct
    outs = [
        (shape((rows, model), BF), hbm()),
        (shape((rows, model), F32), hbm()),
        (shape((8, shard), F32), hbm()),
        (shape((shard, queries), F32), hbm()),
        (shape((LANES, shard), F32), hbm()),
        (shape((queries, shard), F32), hbm()),
        (shape((hidden, shard), F32), hbm()),
        (shape((shard, hidden), F32), hbm()),
        (shape((shard, hidden), F32), hbm()),
        (shape((model, wide), BF), hbm()),
        (shape((queries, model), BF), hbm()),
        (shape((tokens, model), BF), hbm()),
    ]
    return pl.pallas_call(
        functools.partial(layer_kernel, nt, width),
        out_shape=[o for o, _ in outs],
        in_specs=[vmem()] * 8 + [hbm()] * 4,
        out_specs=[s for _, s in outs],
        scratch_shapes=[
            pltpu.VMEM((tokens, model), BF),
            pltpu.VMEM((tokens, model), BF),
            pltpu.VMEM((tokens, model), BF),
            pltpu.VMEM((tokens, hidden), BF),
            pltpu.VMEM((rows, model), F32),
            pltpu.VMEM((model, hidden), BF),
            pltpu.VMEM((model, hidden), BF),
            pltpu.VMEM((hidden, model), BF),
            pltpu.VMEM((max(tokens, 2 * shard), max(model, 3 * span)), F32),
        ]
        + line_scratch(nt, rows, model)
        + [
            pltpu.VMEM((2, half, shard, hidden), BF),
            pltpu.VMEM((2, 2, half - 1, shard // 2, hidden), BF),
            pltpu.VMEM((shard, hidden), F32),
            pltpu.VMEM((rows, model), BF),
            pltpu.VMEM((rows, model), F32),
            pltpu.VMEM((8, shard), F32),
            pltpu.VMEM((shard, queries), F32),
            pltpu.VMEM((LANES, shard), F32),
            pltpu.VMEM((queries, shard), F32),
            pltpu.VMEM((hidden, shard), F32),
            pltpu.VMEM((shard, wide), BF),
            pltpu.VMEM((8, shard), F32),
            pltpu.VMEM((nd, 8, shard), F32),
            pltpu.VMEM((tokens, queries), BF),
            pltpu.VMEM((tokens, LANES), BF),
            pltpu.VMEM((tokens, queries), BF),
            pltpu.VMEM((tokens, LANES), F32),
            pltpu.VMEM((tokens, LANES), F32),
            pltpu.VMEM((tokens, LANES), F32),
            pltpu.VMEM((8, model), F32),
            pltpu.VMEM((nt, 8, model), F32),
            pltpu.VMEM((nd, 8, shard), F32),
            dma(2, nd),
            dma(7),
            dma(3),
            dma(4, nt, PIECES),
            dma(4, nt, PIECES),
            dma(2, 2, nt, PIECES),
            dma(8, 2, half - 1),
            dma(8, 2, half - 1),
            dma(8, half),
            dma(8, half),
            dma(2, nt),
            dma(2, nd),
            dma(2 * PIECES + 5),
            pltpu.SemaphoreType.REGULAR((2,)),
            pltpu.SemaphoreType.REGULAR((2,)),
        ],
        compiler_params=pltpu.CompilerParams(
            collective_id=0, has_side_effects=True, vmem_limit_bytes=VMEM_BYTES
        ),
        name="layer",
    )(x, cot, gain_a, gain_f, segr, wq, wkt, wvt, wo, gate, up, down)


def hand_over_kernel(count, kv, *refs):
    sources, rest = refs[: count + 2], refs[count + 2 :]
    targets, rest = rest[: count + 4], rest[count + 4 :]
    held, (in_sem, out_sem) = rest[: count + 2], rest[count + 2 :]
    ins = [
        pltpu.make_async_copy(src, buf, in_sem.at[i])
        for i, (src, buf) in enumerate(zip(sources, held))
    ]
    for copy in ins:
        copy.start()
    outs = []
    for i in range(count):
        ins[i].wait()
        outs.append(pltpu.make_async_copy(held[i], targets[i], out_sem.at[i]))
        outs[-1].start()
    ins[count].wait()
    for i in range(2):
        outs.append(
            pltpu.make_async_copy(
                held[count].at[pl.ds(i * kv, kv), :], targets[count + i], out_sem.at[count + i]
            )
        )
        outs[-1].start()
    ins[count + 1].wait()
    gains = held[count + 1]
    for i in range(2):
        targets[count + 2 + i][...] = gains[i, :]
    for copy in outs:
        copy.wait()


def hand_over(arrays, d_kv, gains):
    count, kv = len(arrays), d_kv.shape[0] // 2
    shape = jax.ShapeDtypeStruct
    outs = [shape(a.shape, a.dtype) for a in arrays]
    outs += [shape((kv, d_kv.shape[1]), F32)] * 2 + [shape((gains.shape[1],), F32)] * 2
    inputs = (*arrays, d_kv, gains)
    return pl.pallas_call(
        functools.partial(hand_over_kernel, count, kv),
        out_shape=outs,
        in_specs=[hbm()] * len(inputs),
        out_specs=[hbm()] * (count + 2) + [vmem()] * 2,
        scratch_shapes=[pltpu.VMEM(a.shape, a.dtype) for a in inputs]
        + [dma(len(inputs)), dma(count + 2)],
        compiler_params=pltpu.CompilerParams(vmem_limit_bytes=VMEM_BYTES),
        name="hand_over",
    )(*inputs)


def narrow_scatter(value, axis, scatter_dimension, tiled):
    low = value.astype(BF) if value.ndim == 2 else value
    return lax.psum_scatter(low, axis, scatter_dimension=scatter_dimension, tiled=tiled).astype(F32)


def rope_tables(segments, head_dim):
    row_count = segments.shape[0]
    row_index = jnp.arange(row_count, dtype=jnp.int32)
    change = jnp.concatenate(
        [jnp.ones((1,), jnp.int32), (segments[1:] != segments[:-1]).astype(jnp.int32)]
    )
    starts = lax.cummax(jnp.where(change > 0, row_index, jnp.zeros_like(row_index)), axis=0)
    position = (row_index - starts).astype(F32)
    half_dim = head_dim // 2
    frequency = jnp.exp(jnp.arange(half_dim, dtype=F32) * (-math.log(10000.0) / half_dim))
    angles = position[:, None] * frequency[None, :]
    return (jnp.cos(angles)[:, None, :], jnp.sin(angles)[:, None, :])


def rotate(tensor, cosine, sine):
    half_dim = tensor.shape[-1] // 2
    first_half = tensor[..., :half_dim]
    second_half = tensor[..., half_dim:]
    return jnp.concatenate(
        [first_half * cosine - second_half * sine, second_half * cosine + first_half * sine],
        axis=-1,
    )


def unrotate(tensor, cosine, sine):
    half_dim = tensor.shape[-1] // 2
    first_half = tensor[..., :half_dim]
    second_half = tensor[..., half_dim:]
    return jnp.concatenate(
        [first_half * cosine + second_half * sine, second_half * cosine - first_half * sine],
        axis=-1,
    )


def visible(segments):
    row_index = jnp.arange(segments.shape[0], dtype=jnp.int32)
    same_seq = segments[:, None] == segments[None, :]
    return same_seq & (row_index[:, None] >= row_index[None, :])


def normalize(values, gain):
    inverse = lax.rsqrt(jnp.mean(values * values, axis=-1, keepdims=True) + EPSILON)
    unit_rows = values * inverse
    return (unit_rows, inverse, (unit_rows * gain.astype(F32)).astype(BF))


def normalize_back(grad_normed, unit_rows, inverse, gain):
    scaled = grad_normed * gain.astype(F32)
    grad_values = inverse * (
        scaled - unit_rows * jnp.mean(scaled * unit_rows, axis=-1, keepdims=True)
    )
    return (grad_values, jnp.sum(grad_normed * unit_rows, axis=0))


def contract(left, right, left_dim, right_dim):
    return lax.dot_general(
        left, right, (((left_dim,), (right_dim,)), ((), ())), preferred_element_type=F32
    )


def block_scores(query_block, key_heads, allowed_block, score_scale):
    scores = (
        jnp.einsum("rkgd,skd->kgrs", query_block, key_heads, preferred_element_type=F32)
        * score_scale
    )
    return jnp.where(allowed_block[None, None], scores, NEGATIVE)


def attend_forward(query_groups, key_heads, value_heads, allowed, score_scale):
    scores = block_scores(query_groups, key_heads, allowed, score_scale)
    row_max = jnp.max(scores, axis=-1, keepdims=True)
    log_total = row_max + jnp.log(jnp.sum(jnp.exp(scores - row_max), axis=-1, keepdims=True))
    probs_low = jnp.exp(scores - log_total).astype(BF)
    mixed_parts = jnp.einsum(
        "kgrs,skd->rkgd", probs_low, value_heads, preferred_element_type=F32
    ).astype(BF)
    return (mixed_parts, log_total)


def attend_backward(
    query_groups, key_heads, value_heads, mixed_heads, grad_mixed, log_totals, allowed, score_scale
):
    scores = block_scores(query_groups, key_heads, allowed, score_scale)
    attn_probs = jnp.exp(scores - log_totals)
    probs_low = attn_probs.astype(BF)
    grad_probs = jnp.einsum(
        "rkgd,skd->kgrs", grad_mixed, value_heads, preferred_element_type=F32
    )
    row_delta = jnp.sum(grad_mixed.astype(F32) * mixed_heads.astype(F32), axis=-1)
    row_delta = jnp.transpose(row_delta, (1, 2, 0))[..., None]
    grad_scores = (attn_probs * (grad_probs - row_delta)).astype(BF)
    query_parts = (
        jnp.einsum("kgrs,skd->rkgd", grad_scores, key_heads, preferred_element_type=F32)
        * score_scale
    )
    grad_key_rot = (
        jnp.einsum("kgrs,rkgd->skd", grad_scores, query_groups, preferred_element_type=F32)
        * score_scale
    )
    grad_value_heads = jnp.einsum(
        "kgrs,rkgd->skd", probs_low, grad_mixed, preferred_element_type=F32
    )
    return (query_parts, grad_key_rot, grad_value_heads)


def plain_device(
    layer_input,
    segment_ids,
    norm_attn,
    w_query,
    w_key,
    w_value,
    w_output,
    norm_ffn,
    w_gate,
    w_up,
    w_down,
    cotangent,
):
    score_scale = HD ** (-0.5)
    query_full, key_full, value_full, output_full, gain_attn = (
        lax.all_gather(w_query, "dp", axis=0, tiled=True),
        lax.all_gather(w_key, "dp", axis=0, tiled=True),
        lax.all_gather(w_value, "dp", axis=0, tiled=True),
        lax.all_gather(w_output, "dp", axis=1, tiled=True),
        lax.all_gather(norm_attn, "dp", axis=0, tiled=True),
    )
    gate_full, up_full, down_full, gain_ffn = (
        lax.all_gather(w_gate, "dp", axis=0, tiled=True),
        lax.all_gather(w_up, "dp", axis=0, tiled=True),
        lax.all_gather(w_down, "dp", axis=1, tiled=True),
        lax.all_gather(norm_ffn, "dp", axis=0, tiled=True),
    )
    heads_local = query_full.shape[1] // HD
    kv_local = key_full.shape[1] // HD
    group = heads_local // kv_local
    residual_in = layer_input.astype(F32)
    unit_attn, inverse_attn, normed_local = normalize(residual_in, gain_attn)
    normed_attn = lax.all_gather(normed_local, "tensor", axis=0, tiled=True)
    row_count = normed_attn.shape[0]
    cosine, sine = rope_tables(segment_ids, HD)
    allowed = visible(segment_ids)
    query_heads = rotate(
        jnp.dot(normed_attn, query_full, preferred_element_type=F32).reshape(
            row_count, heads_local, HD
        ),
        cosine,
        sine,
    ).astype(BF)
    query_groups = query_heads.reshape(row_count, kv_local, group, HD)
    key_heads = rotate(
        jnp.dot(normed_attn, key_full, preferred_element_type=F32).reshape(
            row_count, kv_local, HD
        ),
        cosine,
        sine,
    ).astype(BF)
    value_heads = (
        jnp.dot(normed_attn, value_full, preferred_element_type=F32)
        .astype(BF)
        .reshape(row_count, kv_local, HD)
    )
    mixed_heads, log_totals = attend_forward(
        query_groups, key_heads, value_heads, allowed, score_scale
    )
    mixed_flat = mixed_heads.reshape(row_count, heads_local * HD)
    hidden_res = residual_in + narrow_scatter(
        jnp.dot(mixed_flat, output_full, preferred_element_type=F32),
        "tensor",
        scatter_dimension=0,
        tiled=True,
    )
    unit_ffn, inverse_ffn, normed_ffn_local = normalize(hidden_res, gain_ffn)
    normed_ffn = lax.all_gather(normed_ffn_local, "tensor", axis=0, tiled=True)
    gate_rows = jnp.dot(normed_ffn, gate_full, preferred_element_type=F32)
    up_rows = jnp.dot(normed_ffn, up_full, preferred_element_type=F32)
    sigmoid_gate = jax.nn.sigmoid(gate_rows)
    active = (gate_rows * sigmoid_gate * up_rows).astype(BF)
    layer_output = (
        hidden_res
        + narrow_scatter(
            jnp.dot(active, down_full, preferred_element_type=F32).astype(BF),
            "tensor",
            scatter_dimension=0,
            tiled=True,
        ).astype(F32)
    ).astype(BF)
    query_full, key_full, value_full, output_full, gate_full, up_full, down_full = (
        lax.all_gather(w_query, "dp", axis=0, tiled=True),
        lax.all_gather(w_key, "dp", axis=0, tiled=True),
        lax.all_gather(w_value, "dp", axis=0, tiled=True),
        lax.all_gather(w_output, "dp", axis=1, tiled=True),
        lax.all_gather(w_gate, "dp", axis=0, tiled=True),
        lax.all_gather(w_up, "dp", axis=0, tiled=True),
        lax.all_gather(w_down, "dp", axis=1, tiled=True),
    )
    cotangent_full = lax.all_gather(cotangent, "tensor", axis=0, tiled=True)
    grad_active = contract(cotangent_full, down_full, 1, 1)
    grad_w_down = contract(active, cotangent_full, 0, 0)
    grad_up_rows = (grad_active * gate_rows * sigmoid_gate).astype(BF)
    grad_gate_rows = (
        grad_active * up_rows * sigmoid_gate * (1.0 + gate_rows * (1.0 - sigmoid_gate))
    ).astype(BF)
    grad_w_gate = contract(normed_ffn, grad_gate_rows, 0, 0)
    grad_w_up = contract(normed_ffn, grad_up_rows, 0, 0)
    grad_normed_ffn = narrow_scatter(
        contract(grad_gate_rows, gate_full, 1, 1) + contract(grad_up_rows, up_full, 1, 1),
        "tensor",
        scatter_dimension=0,
        tiled=True,
    )
    grad_hidden, gain_ffn_part = normalize_back(grad_normed_ffn, unit_ffn, inverse_ffn, gain_ffn)
    grad_hidden = cotangent.astype(F32) + grad_hidden
    branch_full = lax.all_gather(grad_hidden.astype(BF), "tensor", axis=0, tiled=True)
    grad_mixed = contract(branch_full, output_full, 1, 1).astype(BF)
    grad_w_output = contract(mixed_flat, branch_full, 0, 0)
    grad_query_rot, grad_key_rot, grad_value_heads = attend_backward(
        query_groups,
        key_heads,
        value_heads,
        mixed_heads,
        grad_mixed.reshape(row_count, kv_local, group, HD),
        log_totals,
        allowed,
        score_scale,
    )
    grad_queries = (
        unrotate(grad_query_rot.reshape(row_count, heads_local, HD), cosine, sine)
        .reshape(row_count, heads_local * HD)
        .astype(BF)
    )
    grad_keys = (
        unrotate(grad_key_rot, cosine, sine).reshape(row_count, kv_local * HD).astype(BF)
    )
    grad_values = grad_value_heads.reshape(row_count, kv_local * HD).astype(BF)
    grad_w_query = contract(normed_attn, grad_queries, 0, 0)
    grad_w_key = contract(normed_attn, grad_keys, 0, 0)
    grad_w_value = contract(normed_attn, grad_values, 0, 0)
    grad_normed_attn = narrow_scatter(
        contract(grad_queries, query_full, 1, 1)
        + contract(grad_keys, key_full, 1, 1)
        + contract(grad_values, value_full, 1, 1),
        "tensor",
        scatter_dimension=0,
        tiled=True,
    )
    grad_residual, gain_attn_part = normalize_back(
        grad_normed_attn, unit_attn, inverse_attn, gain_attn
    )
    grad_input = grad_hidden + grad_residual
    gain_attn_total, gain_ffn_total = lax.psum((gain_attn_part, gain_ffn_part), "tensor")
    owned = (
        narrow_scatter(grad_w_query, "dp", scatter_dimension=0, tiled=True),
        narrow_scatter(grad_w_key, "dp", scatter_dimension=0, tiled=True),
        narrow_scatter(grad_w_value, "dp", scatter_dimension=0, tiled=True),
        narrow_scatter(grad_w_output, "dp", scatter_dimension=1, tiled=True),
        narrow_scatter(gain_attn_total, "dp", scatter_dimension=0, tiled=True),
        narrow_scatter(gain_ffn_total, "dp", scatter_dimension=0, tiled=True),
        narrow_scatter(grad_w_gate, "dp", scatter_dimension=0, tiled=True),
        narrow_scatter(grad_w_up, "dp", scatter_dimension=0, tiled=True),
        narrow_scatter(grad_w_down, "dp", scatter_dimension=1, tiled=True),
    )
    return (
        layer_output,
        grad_input,
        owned[4],
        owned[0],
        owned[1],
        owned[2],
        owned[3],
        owned[5],
        owned[6],
        owned[7],
        owned[8],
    )


def with_kernels(nt, nd, layer_input, segment_ids, norm_attn, w_query, w_key, w_value, w_output, norm_ffn, w_gate, w_up, w_down, cotangent):
    y, gi, gains, d_wq, d_kv, d_wo, d_down, d_gate, d_up, *_ = layer(
        nt, nd, layer_input, cotangent, norm_attn, norm_ffn, segment_ids[None, :],
        w_query, w_key.T, w_value.T, w_output, w_gate, w_up, w_down,
    )
    y, gi, d_wq, d_wo, d_gate, d_up, d_down, d_k, d_v, d_attn, d_ffn = hand_over(
        (y, gi, d_wq, d_wo, d_gate, d_up, d_down), d_kv, gains
    )
    return (y, gi, d_attn, d_wq, d_k.T, d_v.T, d_wo, d_ffn, d_gate, d_up, d_down)


def fits(nt, nd, shards):
    layer_input, segment_ids, norm_attn, w_query, w_key, w_value, w_output, norm_ffn, w_gate, w_up, w_down, _ = shards
    return (
        nd >= 4
        and nd & (nd - 1) == 0
        and nt >= 2
        and norm_attn.shape[0] % LANES == 0
        and w_output.shape[1] % LANES == 0
        and w_gate.shape[1] % LANES == 0
        and w_query.shape[1] % LANES == 0
        and w_key.shape[1] == HD
        and segment_ids.shape[0] == nt * layer_input.shape[0]
        and segment_ids.shape[0] % LANES == 0
    )


def on_device(nt, nd, *shards):
    if fits(nt, nd, shards):
        return with_kernels(nt, nd, *shards)
    return plain_device(*shards)


def solution(mesh):
    placed = (
        P(("dp", "tensor"), None),
        P("dp"),
        P("dp"),
        P("dp", "tensor"),
        P("dp", "tensor"),
        P("dp", "tensor"),
        P("tensor", "dp"),
        P("dp"),
        P("dp", "tensor"),
        P("dp", "tensor"),
        P("tensor", "dp"),
        P(("dp", "tensor"), None),
    )
    return jax.shard_map(
        functools.partial(on_device, mesh.shape["tensor"], mesh.shape["dp"]),
        mesh=mesh,
        in_specs=placed,
        out_specs=(
            P(("dp", "tensor"), None),
            P(("dp", "tensor"), None),
            P("dp"),
            P("dp", "tensor"),
            P("dp", "tensor"),
            P("dp", "tensor"),
            P("tensor", "dp"),
            P("dp"),
            P("dp", "tensor"),
            P("dp", "tensor"),
            P("tensor", "dp"),
        ),
        check_vma=False,
    )
```

```python
import functools
import math

import jax
import jax.numpy as jnp
from jax import lax
from jax.experimental import pallas as pl
from jax.experimental.pallas import tpu as pltpu
from jax.sharding import PartitionSpec as P

HD = 64
EPSILON = 1e-05
NEGATIVE = -1e30
LANES = 128
BF = jnp.bfloat16
F32 = jnp.float32
VMEM_BYTES = 67_000_000


def spans(bits):
    masks = [0]
    for bit in bits:
        masks = masks + [mask | (1 << bit) for mask in masks]
    return masks


def flip(index, mask, width):
    total = 0
    for bit in range(width):
        own = lax.rem(lax.div(index, 1 << bit), 2)
        if isinstance(mask, int):
            other = (mask >> bit) & 1
        else:
            other = lax.rem(lax.div(mask, 1 << bit), 2)
        total = total + lax.rem(own + other, 2) * (1 << bit)
    return total


def aligned(value, step):
    return value if isinstance(value, int) else pl.multiple_of(value, step)


def remote(src, dst, send_sem, recv_sem, device):
    return pltpu.make_async_remote_copy(
        src_ref=src,
        dst_ref=dst,
        send_sem=send_sem,
        recv_sem=recv_sem,
        device_id=device,
        device_id_type=pl.DeviceIdType.MESH,
    )


def dot(left, right, left_dim=1, right_dim=0):
    return lax.dot_general(
        left, right, (((left_dim,), (right_dim,)), ((), ())), preferred_element_type=F32
    )


def tiles_of(size, most):
    units = size // LANES
    parts = -(-units // most)
    cuts, start = [], 0
    for part in range(parts):
        width = (units // parts + (1 if part < units % parts else 0)) * LANES
        cuts.append((start, width))
        start += width
    return cuts


def over_cols(size, width, body):
    @pl.loop(0, size // width)
    def _(i):
        body(pl.ds(pl.multiple_of(i * width, width), width))


def enter(t, nt, me, width, barrier, everyone_along_tensor=False):
    signal = functools.partial(
        pl.semaphore_signal, barrier, inc=1, device_id_type=pl.DeviceIdType.MESH
    )
    for mask in range(1, 1 << width):
        signal(device_id={"dp": flip(me, mask, width)})
    if everyone_along_tensor:
        for step in range(1, nt):
            signal(device_id={"tensor": lax.rem(t + step, nt)})
        pl.semaphore_wait(barrier, (1 << width) - 1 + nt - 1)
        return

    @pl.when(t > 0)
    def _():
        signal(device_id={"tensor": t - 1})

    @pl.when(t < nt - 1)
    def _():
        signal(device_id={"tensor": t + 1})

    neighbours = lax.min(t, 1) + lax.min(nt - 1 - t, 1)
    pl.semaphore_wait(barrier, (1 << width) - 1 + neighbours)


class LineGather:
    def __init__(self, full, row, size, t, nt, sems):
        self.full, self.row, self.size = full, row, size
        self.t, self.nt, self.sems = t, nt, sems
        self.pieces = sems.shape[2]
        self.done = set()

    def window(self, j, s):
        return self.full.at[pl.ds(aligned(self.row(j, s), self.size), self.size), :]

    def right(self, j, s):
        at = self.window(j, s)
        return remote(
            at, at, self.sems.at[0, j, s], self.sems.at[2, j, s],
            {"tensor": lax.rem(self.t + 1, self.nt)},
        )

    def left(self, j, s):
        at = self.window(j, s)
        return remote(
            at, at, self.sems.at[1, j, s], self.sems.at[3, j, s],
            {"tensor": lax.rem(self.t + self.nt - 1, self.nt)},
        )

    def start(self, s):
        @pl.when(self.t < self.nt - 1)
        def _():
            self.right(self.t, s).start()

        @pl.when(self.t > 0)
        def _():
            self.left(self.t, s).start()

    def step(self, k, s):
        t, nt = self.t, self.nt
        if k >= nt or (k, s) in self.done:
            return
        self.done.add((k, s))

        @pl.when(t >= k)
        def _():
            self.right(t - k, s).wait_recv()

            @pl.when(t < nt - 1)
            def _():
                self.right(t - k, s).start()

        @pl.when(t + k < nt)
        def _():
            self.left(t + k, s).wait_recv()

            @pl.when(t > 0)
            def _():
                self.left(t + k, s).start()

    def complete(self, pieces):
        for k in range(1, self.nt):
            for s in pieces:
                self.step(k, s)

    def finish(self, pieces):
        t, nt = self.t, self.nt

        @pl.loop(0, nt)
        def _(k):
            for s in pieces:
                @pl.when((t >= k) & (t < nt - 1))
                def _():
                    self.right(t - k, s).wait_send()

                @pl.when((t + k < nt) & (t > 0))
                def _():
                    self.left(t + k, s).wait_send()


class LineScatter:
    def __init__(self, part, row, sent, arrived, t, nt, sems):
        self.part, self.row, self.sent, self.arrived = part, row, sent, arrived
        self.t, self.nt, self.sems = t, nt, sems
        self.pieces = sems.shape[3]
        self.size = sent.shape[1] // self.pieces
        self.model = sent.shape[2]
        self.near = lax.div(2 * t, nt)
        self.far = 1 - self.near

    def sub(self, s):
        return pl.ds(s * self.size, self.size)

    def depth(self, way):
        return (1 - way) * self.t + way * (self.nt - 1 - self.t)

    def goal(self, way, i):
        return (1 - way) * (self.nt - 1 - i) + way * i

    def slot(self, way, j):
        return j + 1 - way

    def move(self, way, j, s):
        return remote(
            self.sent.at[j, self.sub(s), :], self.arrived.at[self.slot(way, j), self.sub(s), :],
            self.sems.at[0, way, j, s], self.sems.at[1, way, j, s],
            {"tensor": lax.rem(self.t + self.nt + 1 - 2 * way, self.nt)},
        )

    def rows(self, j, s):
        return pl.ds(aligned(self.row(j, s), self.size), self.size)

    def mine(self, j, s):
        return self.part[self.rows(j, s), : self.model].astype(F32)

    def edge(self, s):
        t, nt = self.t, self.nt

        @pl.when((t == 0) | (t == nt - 1))
        def _():
            way = lax.div(t, nt - 1)

            @pl.loop(0, nt - 1)
            def _(i):
                j = self.goal(way, i)
                self.sent[j, self.sub(s), :] = self.mine(j, s).astype(BF)
                self.move(way, j, s).start()

    def relay(self, way, s):
        depth = self.depth(way)

        @pl.when(depth > 0)
        def _():
            @pl.loop(0, self.nt - 1 - depth)
            def _(i):
                j = self.goal(way, i)
                self.move(way, j, s).wait_recv()
                total = self.mine(j, s) + self.arrived[self.slot(way, j), self.sub(s), :].astype(F32)
                self.sent[j, self.sub(s), :] = total.astype(BF)
                self.move(way, j, s).start()

    def own(self, s):
        t = self.t
        rows = self.rows(t, s)
        for way in (self.near, self.far):
            @pl.when(self.depth(way) > 0)
            def _():
                self.move(way, t, s).wait_recv()
                self.part[rows, : self.model] += self.arrived[self.slot(way, t), self.sub(s), :].astype(F32)

        return rows

    def own_into(self, s, total, at):
        total[at, :] += self.mine(self.t, s)
        for way in (self.near, self.far):
            @pl.when(self.depth(way) > 0)
            def _():
                self.move(way, self.t, s).wait_recv()
                total[at, :] += self.arrived[self.slot(way, self.t), self.sub(s), :].astype(F32)

    def finish(self, pieces):
        for way in range(2):
            @pl.loop(0, self.nt - 1 - self.depth(way))
            def _(i):
                for s in pieces:
                    self.move(way, self.goal(way, i), s).wait_send()


class Cube:
    def setup(self, me, width, half_send, half_recv, pair_send, pair_recv):
        self.me, self.width = me, width
        self.hs, self.hr, self.ps, self.pr = half_send, half_recv, pair_send, pair_recv
        self.bits = list(range(1, width))
        self.orders = (self.bits, self.bits[::-1])
        self.masks = spans(self.bits)
        self.stages = len(self.bits)

    def at(self, mask):
        return flip(self.me, mask, self.width)


class BlockGather(Cube):
    def __init__(self, own, full, by_rows, me, width, *sems):
        self.setup(me, width, *sems)
        self.own_ref, self.full, self.by_rows = own, full, by_rows

    def half(self, h):
        rows = self.own_ref.shape[0] // 2
        return self.own_ref.at[pl.ds(h * rows, rows), :]

    def window(self, who, h=None):
        rows, cols = self.own_ref.shape
        take, start = (rows, 0) if h is None else (rows // 2, h * (rows // 2))
        if self.by_rows:
            return self.full.at[pl.ds(aligned(who * rows + start, take), take), :]
        return self.full.at[pl.ds(start, take), pl.ds(aligned(who * cols, cols), cols)]

    def hop(self, stage, h, m):
        order = self.orders[h]
        bit = 1 << order[stage]
        slot = (m | bit) >> 1
        src = self.half(h) if m == 0 else self.window(self.at(m), h)
        return remote(
            src, self.window(self.at(m), h), self.hs.at[h, slot - 1], self.hr.at[h, slot - 1],
            {"dp": self.at(bit)},
        )

    def send(self, stage):
        for h in range(2):
            for m in spans(self.orders[h][:stage]):
                self.hop(stage, h, m).start()

    def wait(self, stage):
        for h in range(2):
            bit = 1 << self.orders[h][stage]
            for m in spans(self.orders[h][:stage]):
                slot = (m | bit) >> 1
                landed = self.window(self.at(m | bit), h)
                remote(
                    landed, landed, self.hs.at[h, slot - 1], self.hr.at[h, slot - 1],
                    {"dp": self.at(bit)},
                ).wait_recv()

    def pair(self, m):
        src = self.own_ref if m == 0 else self.window(self.at(m))
        return remote(
            src, self.window(self.at(m)), self.ps.at[m >> 1], self.pr.at[m >> 1],
            {"dp": self.at(1)},
        )

    def pair_own(self):
        self.pair(0).start()

    def pair_send(self):
        for m in self.masks:
            if m:
                self.pair(m).start()

    def pair_wait(self):
        for m in self.masks:
            landed = self.window(self.at(m | 1))
            remote(
                landed, landed, self.ps.at[m >> 1], self.pr.at[m >> 1], {"dp": self.at(1)}
            ).wait_recv()

    def place(self, sem):
        return pltpu.make_async_copy(self.own_ref, self.window(self.me), sem)

    def drain(self):
        for stage in range(self.stages):
            for h in range(2):
                for m in spans(self.orders[h][:stage]):
                    self.hop(stage, h, m).wait_send()
        for m in self.masks:
            self.pair(m).wait_send()


class BlockScatter(Cube):
    def __init__(self, chunk, out_sent, total, landed, store, me, width, *sems):
        self.setup(me, width, *sems)
        self.chunk, self.sent, self.total, self.landed = chunk, out_sent, total, landed
        self.store = store
        self.slots = 1 << (width - 1)

    def pair(self, slot):
        return remote(
            self.sent.at[slot], self.total.at[slot], self.ps.at[slot], self.pr.at[slot],
            {"dp": self.at(1)},
        )

    def give(self):
        @pl.loop(0, self.slots)
        def _(k):
            slot = self.slots - 1 - k
            self.sent[slot] = self.chunk(self.at(2 * slot + 1)).astype(BF)
            self.pair(slot).start()

    def given(self):
        @pl.loop(0, self.slots)
        def _(slot):
            self.pair(slot).wait_send()

    def take(self):
        @pl.loop(0, self.slots)
        def _(k):
            slot = self.slots - 1 - k
            term = self.chunk(self.at(2 * slot))
            self.pair(slot).wait_recv()
            self.total[slot] = (term + self.total[slot].astype(F32)).astype(BF)

    def moves(self, stage):
        for h in range(2):
            order = self.orders[h]
            last = self.stages - 1 - stage
            bit = 1 << order[last]
            for m in spans(order[:last]):
                yield h, bit, m | bit

    def hop(self, h, bit, m):
        rows = self.total.shape[1] // 2
        return remote(
            self.total.at[m >> 1, pl.ds(h * rows, rows), :], self.landed.at[h, (m >> 1) - 1],
            self.hs.at[h, (m >> 1) - 1], self.hr.at[h, (m >> 1) - 1], {"dp": self.at(bit)},
        )

    def send(self, stage):
        for h, bit, m in self.moves(stage):
            self.hop(h, bit, m).start()

    def add(self, stage):
        rows = self.total.shape[1] // 2
        for h, bit, m in self.moves(stage):
            self.hop(h, bit, m).wait_recv()
            keep = (m ^ bit) >> 1
            at = slice(h * rows, (h + 1) * rows)
            total = self.total[keep, at, :].astype(F32) + self.landed[h, (m >> 1) - 1].astype(F32)
            if stage == self.stages - 1:
                self.store(at, total)
            else:
                self.total[keep, at, :] = total.astype(BF)

    def drain(self):
        for stage in range(self.stages):
            for h, bit, m in self.moves(stage):
                self.hop(h, bit, m).wait_send()


def inverse_of(rows):
    return lax.rsqrt(jnp.mean(rows * rows, axis=-1, keepdims=True) + EPSILON)


def times_gain(unit, gains, which, store):
    parts, _, width = gains.shape
    for d in range(parts):
        cols = slice(d * width, (d + 1) * width)
        store(cols, unit[:, cols] * gains[d, which : which + 1, :])


def lane_index(shape):
    return lax.broadcasted_iota(jnp.int32, shape, len(shape) - 1)


def column_of(segr):
    rows = segr.shape[1]
    wide = jnp.broadcast_to(segr[...].astype(F32), (8, rows))
    return jnp.transpose(wide)[:, 0:1]


def rope_into(cos_ref, sin_ref, segr):
    rows = segr.shape[1]
    before = (segr[...].astype(F32) < column_of(segr)).astype(F32)
    start = jnp.sum(before, axis=1, keepdims=True)
    position = lax.broadcasted_iota(jnp.int32, (rows, 1), 0).astype(F32) - start
    lane = lane_index((rows, LANES))
    half = HD // 2
    frequency = jnp.exp(lax.rem(lane, half).astype(F32) * (-math.log(10000.0) / half))
    angle = position * frequency
    cos_ref[...] = jnp.cos(angle)
    sine = jnp.sin(angle)
    sin_ref[...] = jnp.where(lax.rem(lane, HD) < half, -sine, sine)


def swapped(x):
    lane = lane_index(x.shape)
    half = HD // 2
    return jnp.where(
        lax.rem(lane, HD) < half,
        pltpu.roll(x, LANES - half, 1),
        pltpu.roll(x, half, 1),
    )


def bias_into(bias, segr):
    rows = segr.shape[1]
    query = lax.broadcasted_iota(jnp.int32, (rows, rows), 0)
    key = lax.broadcasted_iota(jnp.int32, (rows, rows), 1)
    seen = (segr[...].astype(F32) == column_of(segr)) & (query >= key)
    bias[...] = jnp.where(seen, 0.0, NEGATIVE)


def pad_pair(keys_values, keys, values):
    low = lane_index(keys_values.shape) < HD
    key = jnp.where(low, keys_values, 0.0)
    value = jnp.where(low, 0.0, keys_values)
    keys[0] = key.astype(BF)
    keys[1] = pltpu.roll(key, HD, 1).astype(BF)
    values[0] = pltpu.roll(value, HD, 1).astype(BF)
    values[1] = value.astype(BF)


def query_cuts(rows):
    block = 256 if rows % 256 == 0 else rows
    return [(start, block, start + block) for start in range(0, rows, block)]


def attend_pairs(first, last, qo, kpad, vpad, bias, mo, lo):
    rows = qo.shape[0]
    lane = lane_index((1, LANES))

    @pl.loop(first, last)
    def _(pair):
        lanes = pl.ds(pl.multiple_of(pair * LANES, LANES), LANES)
        for start, block, seen in query_cuts(rows):
            at = slice(start, start + block)
            query = qo[at, lanes]
            mixed = jnp.zeros((block, LANES), F32)
            logs = lo[at, :]
            for side in range(2):
                scores = dot(query, kpad[side, :seen, :], 1, 1) + bias[at, :seen]
                top = jnp.max(scores, axis=-1, keepdims=True)
                probs = jnp.exp(scores - top)
                total = jnp.sum(probs, axis=-1, keepdims=True)
                mixed = mixed + dot(probs.astype(BF), vpad[side, :seen, :]) / total
                logs = jnp.where(lane == 2 * pair + side, top + jnp.log(total), logs)
            lo[at, :] = logs
            mo[at, lanes] = mixed.astype(BF)


def back_through_norm(raw, grads, gains, which, store, store_gain):
    parts, _, width = gains.shape
    cuts = [slice(d * width, (d + 1) * width) for d in range(parts)]
    model = parts * width
    square = sum(jnp.sum(raw(c) * raw(c), axis=-1, keepdims=True) for c in cuts)
    inverse = lax.rsqrt(square / model + EPSILON)
    mean = 0.0
    for d, c in enumerate(cuts):
        unit = raw(c) * inverse
        grad = grads(c)
        store_gain(c, jnp.sum(grad * unit, axis=0, keepdims=True))
        mean = mean + jnp.sum(grad * gains[d, which : which + 1, :] * unit, axis=-1, keepdims=True)
    mean = mean / model
    for d, c in enumerate(cuts):
        unit = raw(c) * inverse
        store(c, inverse * (grads(c) * gains[d, which : which + 1, :] - unit * mean))


def attend_back_pairs(first, last, qo, gm, mo, lo, kpad, vpad, bias, cos, sin, dqkv, dkey, dval):
    rows = qo.shape[0]

    @pl.loop(first, last)
    def _(pair):
        lanes = pl.ds(pl.multiple_of(pair * LANES, LANES), LANES)
        for start, block, seen in query_cuts(rows):
            at = slice(start, start + block)
            lane = lane_index((block, LANES))
            query, grad = qo[at, lanes], gm[at, lanes]
            both = grad.astype(F32) * mo[at, lanes].astype(F32)
            logs = lo[at, :]
            dq = jnp.zeros((block, LANES), F32)
            for side in range(2):
                inside = (lane >= HD) if side else (lane < HD)
                delta = jnp.sum(jnp.where(inside, both, 0.0), axis=-1, keepdims=True)
                log = jnp.sum(
                    jnp.where(lane == 2 * pair + side, logs, 0.0), axis=-1, keepdims=True
                )
                key, value = kpad[side, :seen, :], vpad[side, :seen, :]
                probs = jnp.exp(dot(query, key, 1, 1) + bias[at, :seen] - log)
                grad_scores = (probs * (dot(grad, value, 1, 1) - delta)).astype(BF)
                dq = dq + dot(grad_scores, key)
                dkey[side, :seen, :] += dot(grad_scores, query, 0, 0)
                dval[side, :seen, :] += dot(probs.astype(BF), grad, 0, 0)
            dq = dq * HD ** (-0.5)
            dqkv[at, lanes] = (dq * cos[at, :] - swapped(dq) * sin[at, :]).astype(BF)


PIECES = 4


def vmem():
    return pl.BlockSpec(memory_space=pltpu.VMEM)


def hbm():
    return pl.BlockSpec(memory_space=pl.ANY)


def dma(*shape):
    return pltpu.SemaphoreType.DMA(shape)


def line_scratch(nt, rows, model):
    return [pltpu.VMEM((nt, rows, model), BF), pltpu.VMEM((nt + 1, rows, model), BF)]


def ticks(pieces, nt):
    return [
        [(k, tick - k) for k in range(1, nt) if 0 <= tick - k < pieces]
        for tick in range(pieces + nt - 1)
    ]


def layer_kernel(
    nt, width,
    x, cot, gain_a, gain_f, segr, wq, wkt, wvt, wo, gate, up, down,
    y_o, gi_o, gain_o, d_wq_o, d_kv_o, d_wo_o, d_down_o, d_gate, d_up, wqkv_f, wo_f, na_f,
    rowsbuf, cf, branch, act, hid, gate_v, up_v, down_v, part, sent, arrived, y_arrived, totals, landed, stage_v,
    y, gi, gain_out, d_kv, d_down,
    own_qkv, gain, gall, qo, kvo, mo, lo, cos, sin, gsum, zslots, dslots,
    gain_sem, place_sem, out_sem, line_sem, cot_sem, sum_sem, first_sem,
    hs, hr, ps, pr, zsem, dsem, emit_sem, ready, calm,
):
    me, t = lax.axis_index("dp"), lax.axis_index("tensor")
    nd = 1 << width
    rows, model = x.shape
    tokens = nt * rows
    queries = wq.shape[1]
    hidden = gate.shape[1]
    shard = model >> width
    wide = own_qkv.shape[1]
    pieces = PIECES
    first_half = pieces // 2
    size = rows // pieces
    cut = 512 if model % 512 == 0 else LANES

    def natural(j, s):
        return j * rows + s * size

    def shuffled(j, s):
        return (s * nt + j) * size

    local = pl.ds(pl.multiple_of(t * rows, rows), rows)
    rowsbuf[local, :] = x[...]
    gain[...] = jnp.zeros_like(gain)
    gain[0:1, :] = gain_a[...].astype(F32).reshape(1, shard)
    gain[1:2, :] = gain_f[...].astype(F32).reshape(1, shard)
    own_qkv[:, :queries] = wq[...]
    turned = jnp.concatenate([wkt[...].astype(F32), wvt[...].astype(F32)], axis=0)
    own_qkv[:, queries:] = jnp.transpose(turned).astype(BF)
    with jax.named_scope("enter"):
        enter(t, nt, me, width, pltpu.get_barrier_semaphore())

    tokens_x = LineGather(rowsbuf, natural, size, t, nt, line_sem)
    for s in range(pieces):
        tokens_x.start(s)
    gathers = []
    for w, (own, full, by_rows) in enumerate(
        ((own_qkv, wqkv_f, True), (wo, wo_f, False), (gate, gate_v, True), (up, up_v, True), (down, down_v, False))
    ):
        gathers.append(
            BlockGather(own, full, by_rows, me, width, hs.at[w], hr.at[w], ps.at[w], pr.at[w])
        )
    g_qkv, g_out, g_gate, g_up, g_down = gathers
    stages = g_qkv.stages

    def gain_copy(mask):
        return remote(
            gain, gall.at[me], gain_sem.at[0, mask], gain_sem.at[1, mask],
            {"dp": flip(me, mask, width)},
        )

    for mask in range(1, nd):
        gain_copy(mask).start()
    for g in (g_qkv, g_out, g_gate):
        g.send(0)
    for w, g in enumerate(gathers):
        g.place(place_sem.at[w]).start()
    gall[me] = gain[...]

    def forward(g, stage):
        g.wait(stage)
        if stage == 0:
            g.pair_own()
        if stage + 1 < stages:
            g.send(stage + 1)
        else:
            g.pair_send()

    for s in range(pieces):
        cf[pl.ds(pl.multiple_of(shuffled(t, s), size), size), :] = cot[s * size : (s + 1) * size, :]
    cots = LineGather(cf, shuffled, size, t, nt, cot_sem)
    scatter_o = LineScatter(part, shuffled, sent, arrived, t, nt, sum_sem)

    def attention(na, wqkv_v, wo_v, bias, kpad, vpad):
        bias_into(bias, segr)
        rope_into(cos, sin, segr)
        lo[...] = jnp.zeros_like(lo)
        for mask in range(1, nd):
            slot = gall.at[flip(me, mask, width)]
            remote(
                slot, slot, gain_sem.at[0, mask], gain_sem.at[1, mask],
                {"dp": flip(me, mask, width)},
            ).wait_recv()

        def norm(j):
            @pl.loop(0, pieces)
            def _(s):
                these = pl.ds(pl.multiple_of(j * rows + s * size, size), size)
                value = rowsbuf[these, :].astype(F32)

                def store(cols, normed):
                    na[these, cols] = normed.astype(BF)

                times_gain(value * inverse_of(value), gall, 0, store)

        norm(t)
        for stage in range(stages - 1):
            forward(g_qkv, stage)
            forward(g_out, stage)
        fills = [
            lambda: (forward(g_gate, 0), g_up.send(0)),
            lambda: (forward(g_qkv, stages - 1), forward(g_out, stages - 1), g_down.send(0)),
        ]
        load = pltpu.make_async_copy(wqkv_f, wqkv_v, place_sem.at[5])
        load_out = pltpu.make_async_copy(wo_f, wo_v, place_sem.at[6])

        def fetch():
            g_qkv.place(place_sem.at[0]).wait()
            g_qkv.pair_wait()
            load.start()
            g_out.place(place_sem.at[1]).wait()
            g_out.pair_wait()
            load_out.start()

        for k in range(1, nt):
            if k == nt - 1:
                for fill in fills:
                    fill()
                fills = []
                with jax.named_scope("fetch"):
                    fetch()
            with jax.named_scope("x_step"):
                for s in range(pieces):
                    tokens_x.step(k, s)
            if k == nt - 1:
                for s in range(first_half):
                    cots.start(s)

            @pl.when(t >= k)
            def _():
                norm(t - k)

            @pl.when(t + k < nt)
            def _():
                norm(t + k)

            if fills:
                with jax.named_scope("x_fill"):
                    fills.pop(0)()
        keep = pltpu.make_async_copy(na, na_f, out_sem.at[0])
        keep.start()
        with jax.named_scope("wait_qkv"):
            load.wait()
        with jax.named_scope("qkv"):
            part[:, :wide] = dot(na[...], wqkv_v[...])
            c, s_ = cos[...], sin[...]
            for start in range(0, queries, LANES):
                lanes = slice(start, start + LANES)
                value = part[:, lanes]
                qo[:, lanes] = ((value * c + swapped(value) * s_) * HD ** (-0.5)).astype(BF)
            value = part[:, queries : queries + LANES]
            keyed = jnp.where(lane_index(value.shape) < HD, value * c + swapped(value) * s_, value)
            kvo[...] = keyed.astype(BF)
            pad_pair(keyed, kpad, vpad)
        pairs = queries // LANES
        with jax.named_scope("att"):
            attend_pairs(0, pairs, qo, kpad, vpad, bias, mo, lo)
        load_out.wait()
        with jax.named_scope("outproj"):
            mixed = jnp.concatenate(
                [
                    mo[natural(j, s) : natural(j, s) + size, :]
                    for s in range(pieces)
                    for j in range(nt)
                ],
                axis=0,
            )

            def project(cols):
                part[:tokens, cols] = dot(mixed, wo_v[:, cols])

            over_cols(model, cut, project)
        keep.wait()
        tokens_x.finish(range(pieces))

    pl.run_scoped(
        attention,
        pltpu.VMEM((tokens, model), BF),
        pltpu.VMEM((model, wide), BF),
        pltpu.VMEM((queries, model), BF),
        pltpu.VMEM((tokens, tokens), F32),
        pltpu.VMEM((2, tokens, LANES), BF),
        pltpu.VMEM((2, tokens, LANES), BF),
    )

    gather_nf = LineGather(rowsbuf, shuffled, size, t, nt, line_sem)

    def take_hidden(s):
        at = scatter_o.own(s)
        block = slice(s * size, (s + 1) * size)
        hidden_rows = x[block, :].astype(F32) + part[at, :model]
        hid[block, :] = hidden_rows
        there = pl.ds(pl.multiple_of(shuffled(t, s), size), size)

        def store(cols, normed):
            rowsbuf[there, cols] = normed.astype(BF)

        times_gain(hidden_rows * inverse_of(hidden_rows), gall, 1, store)
        gather_nf.start(s)

    def chunk_of(left, right):
        def chunk(d):
            return dot(left[:, pl.ds(pl.multiple_of(d * shard, shard), shard)], right[...], 0, 0)

        return chunk

    def cube(w, totals_, landed_, store):
        return BlockScatter(
            None, None, totals_, landed_, store, me, width, hs.at[w], hr.at[w], ps.at[w], pr.at[w]
        )

    def store_stage(at, value):
        stage_v[at, :] = value

    def store_down(at, value):
        d_down[:, at] = value.T

    def store_qkv(at, value):
        stage_v[at, :queries] = value[:, :queries]
        d_kv[:, at] = value[:, queries:].T

    def store_wo(at, value):
        part[:queries, model + at.start : model + at.stop] = value.T

    for_qkv, for_wo = pl.ds(0, wide), pl.ds(wide, queries)
    s_gate = cube(5, totals.at[0], landed.at[0], store_stage)
    s_up = cube(6, totals.at[1], landed.at[1], store_stage)
    s_down = cube(5, totals.at[0], landed.at[0], store_down)
    s_qkv = cube(6, totals.at[1, :, :, for_qkv], landed.at[1, :, :, :, for_qkv], store_qkv)
    s_out = cube(7, totals.at[1, :, :, for_wo], landed.at[1, :, :, :, for_wo], store_wo)

    def take(s):
        s.take()
        s.send(0)

    def on(s, stage):
        s.add(stage)
        if stage + 1 < stages:
            s.send(stage + 1)

    scatter_y = LineScatter(part, shuffled, sent, arrived, t, nt, sum_sem)
    scope = jax.named_scope
    emitted = []

    def emit(src, dst):
        emitted.append(pltpu.make_async_copy(src, dst, emit_sem.at[len(emitted)]))
        emitted[-1].start()

    def y_part(h):
        mine = slice(h * (tokens // 2), (h + 1) * (tokens // 2))
        with scope("y_part"):

            def product(cols):
                part[mine, cols] = dot(act[mine, :], down_v[:, cols])

            over_cols(model, cut, product)

    def y_near(s):
        with scope("y_near"):
            scatter_y.relay(scatter_y.near, s)

    def y_far(s):
        with scope("y_far"):
            scatter_y.relay(scatter_y.far, s)

    def y_own(s):
        with scope("y_own"):
            at = scatter_y.own(s)
            block_ = slice(s * size, (s + 1) * size)
            y[block_, :] = (hid[block_, :] + part[at, :model]).astype(BF)
            emit(y.at[pl.ds(s * size, size), :], y_o.at[pl.ds(s * size, size), :])

    def br(k, s):
        with scope("br_step"):
            gather_br.step(k, s)

    gsum[...] = jnp.zeros_like(gsum)
    gather_br = LineGather(branch, natural, size, t, nt, line_sem)

    def second_part(y_first, y_sent):
        scatter_ya = LineScatter(y_first, shuffled, y_sent, y_arrived, t, nt, first_sem)

        def feed(dg, du, given):
            cuts = tiles_of(hidden, 6)
            span = max(width_ for _, width_ in cuts)
            half = tokens // 2
            block = 64

            def tile_in(h, i):
                start, width_ = cuts[i]
                at = slice(start, start + width_)
                held = mine = slice(h * half, (h + 1) * half)
                part[held, 0:width_] = dot(rowsbuf[mine, :], gate_v[:, at])
                part[held, span : span + width_] = dot(rowsbuf[mine, :], up_v[:, at])

            def tile_out(h, i):
                start, width_ = cuts[i]
                at = slice(start, start + width_)
                held = mine = slice(h * half, (h + 1) * half)
                part[held, 2 * span : 2 * span + width_] = dot(cf[mine, :], down_v[at, :], 1, 1)

                @pl.loop(0, half // block)
                def _(k):
                    from_ = pl.ds(pl.multiple_of(h * half + k * block, block), block)
                    to = pl.ds(pl.multiple_of(h * half + k * block, block), block)
                    g = part[from_, 0:width_]
                    u = part[from_, span : span + width_]
                    ga = part[from_, 2 * span : 2 * span + width_]
                    sig = 1.0 / (1.0 + jnp.exp(-g))
                    gs = g * sig
                    act[to, at] = (gs * u).astype(BF)
                    du[to, at] = (ga * gs).astype(BF)
                    dg[to, at] = (ga * u * sig * (1.0 + g * (1.0 - sig))).astype(BF)

            def tile(h, i):
                with scope("tile"):
                    tile_in(h, i)
                    tile_out(h, i)

            def back_dots(h):
                mine = slice(h * half, (h + 1) * half)

                def product(cols):
                    part[mine, cols] = dot(dg[mine, :], gate_v[cols, :], 1, 1) + dot(
                        du[mine, :], up_v[cols, :], 1, 1
                    )

                over_cols(model, cut, product)

            scatter_gn = LineScatter(part, shuffled, sent, arrived, t, nt, sum_sem)

            def take_grad(s):
                at = scatter_gn.own(s)
                block_ = slice(s * size, (s + 1) * size)
                there = pl.ds(pl.multiple_of(natural(t, s), size), size)

                def store(cols, value):
                    total = cot[block_, cols].astype(F32) + value
                    gi[block_, cols] = total
                    branch[there, cols] = total.astype(BF)

                def store_gain(cols, value):
                    gsum[1:2, cols] += value

                back_through_norm(
                    lambda c: hid[block_, c], lambda c: part[at, c], gall, 1, store, store_gain
                )
                gather_br.start(s)

            s_gate.chunk, s_up.chunk = chunk_of(rowsbuf, dg), chunk_of(rowsbuf, du)
            s_gate.sent = s_up.sent = given

            half_a, half_b = range(first_half), range(first_half, pieces)
            def o_near(s):
                with scope("o_near"):
                    scatter_o.relay(scatter_o.near, s)

            def o_far(s):
                with scope("o_far"):
                    scatter_o.relay(scatter_o.far, s)

            def o_take(s):
                with scope("o_take"):
                    take_hidden(s)

            def nf(k, s):
                with scope("nf_step"):
                    gather_nf.step(k, s)

            def cot_steps(k, which):
                with scope("cot_step"):
                    for s in which:
                        cots.step(k, s)

            def gn_near(s):
                with scope("gn_near"):
                    scatter_gn.relay(scatter_gn.near, s)

            def gn_far(s):
                with scope("gn_far"):
                    scatter_gn.relay(scatter_gn.far, s)

            def ya_near(s):
                with scope("ya_near"):
                    scatter_ya.relay(scatter_ya.near, s)

            def ya_far(s):
                with scope("ya_far"):
                    scatter_ya.relay(scatter_ya.far, s)

            def gn_take(s):
                with scope("gn_take"):
                    take_grad(s)

            def weight(g, stage):
                with scope("weight"):
                    if stage < stages:
                        forward(g, stage)

            scatter_o.edge(0)
            scatter_o.edge(1)
            cot_steps(1, half_a)
            weight(g_gate, 1)
            cot_steps(2, half_a)
            o_near(0)
            weight(g_up, 0)
            o_far(0)
            o_take(0)
            weight(g_down, 0)
            scatter_o.edge(2)
            o_near(1)
            o_far(1)
            nf(1, 0)
            cot_steps(3, half_a)
            o_take(1)
            scatter_o.edge(3)
            nf(1, 1)
            nf(2, 0)
            o_near(2)
            nf(2, 1)
            weight(g_up, 1)
            o_far(2)
            o_near(3)
            nf(3, 0)
            for s in half_b:
                cots.start(s)
            nf(3, 1)
            o_take(2)
            o_far(3)
            gather_nf.complete(half_a)
            cots.complete(half_a)
            weight(g_down, 1)
            for stage in range(2, stages):
                for g in (g_gate, g_up, g_down):
                    weight(g, stage)
            with scope("wait_ffn"):
                for w in (2, 3):
                    gathers[w].place(place_sem.at[w]).wait()
                    gathers[w].pair_wait()
            with scope("tile"):
                tile_in(0, 0)
            with scope("wait_ffn"):
                g_down.place(place_sem.at[4]).wait()
                g_down.pair_wait()
            with scope("tile"):
                tile_out(0, 0)
            o_take(3)
            nf(1, 2)
            cot_steps(1, half_b)
            for i in range(1, len(cuts)):
                tile(0, i)
            nf(2, 2)
            nf(1, 3)
            with scope("back_dots"):
                scatter_o.finish(half_a)
                back_dots(0)
            scatter_gn.edge(0)
            scatter_gn.edge(1)
            cot_steps(2, half_b)
            with scope("y_part"):
                def product(cols):
                    y_first[:, cols] = dot(act[: tokens // 2, :], down_v[:, cols]).astype(BF)

                over_cols(model, cut, product)
            gn_near(0)
            scatter_ya.edge(0)
            nf(3, 2)
            nf(2, 3)
            gn_far(0)
            cot_steps(3, half_b)
            gn_near(1)
            nf(3, 3)
            gather_nf.complete(half_b)
            cots.complete(half_b)
            gather_nf.finish(half_a)
            tile(1, 0)
            gn_far(1)
            gn_take(0)
            for i in range(1, len(cuts)):
                tile(1, i)
            with scope("back_dots"):
                scatter_o.finish(half_b)
                back_dots(1)
            scatter_gn.edge(2)
            gn_take(1)
            scatter_gn.edge(3)
            with scope("gn_fill"):
                s_gate.give()
            br(1, 0)
            with scope("gn_fill"):
                take(s_gate)
            gn_near(2)
            br(2, 0)
            with scope("gn_fill"):
                s_gate.given()
                s_up.give()
            gn_far(2)
            br(1, 1)
            br(3, 0)
            with scope("gn_fill"):
                take(s_up)
            gn_near(3)
            gather_nf.finish(half_b)
            gn_take(2)
            scatter_ya.edge(1)
            gn_far(3)
            ya_near(0)
            gn_take(3)
            with scope("add0"):
                on(s_gate, 0)
            br(2, 1)
            br(1, 2)
            br(3, 1)
            ya_far(0)
            y_part(1)
            br(2, 2)
            br(1, 3)
            scatter_gn.finish(half_b)
            scatter_y.edge(2)
            scatter_y.edge(3)
            br(3, 2)
            br(2, 3)
            ya_near(1)
            with scope("add0"):
                on(s_up, 0)
            scatter_gn.finish(half_a)
            s_up.given()

        pl.run_scoped(
            feed,
            pltpu.VMEM((tokens, hidden), BF),
            pltpu.VMEM((tokens, hidden), BF),
            pltpu.VMEM((nd // 2, shard, hidden), BF),
        )

        wo_v = down_v.at[pl.ds(0, queries), :]
        na_v = down_v.at[pl.ds(queries, tokens), :]
        wqkv_v = gate_v.at[:, pl.ds(0, wide)]
        gm = up_v.at[pl.ds(0, tokens), pl.ds(0, queries)]
        dqkv = up_v.at[pl.ds(tokens, tokens), pl.ds(0, wide)]

        def rear(bias, kpad, vpad, dkey, dval, given):
            inward = LineScatter(part, shuffled, sent, arrived, t, nt, sum_sem)
            for g in gathers:
                g.drain()
            loads = [
                pltpu.make_async_copy(wo_f, wo_v, place_sem.at[0]),
                pltpu.make_async_copy(wqkv_f, wqkv_v, place_sem.at[1]),
                pltpu.make_async_copy(na_f, na_v, place_sem.at[2]),
            ]
            for load in loads:
                load.start()
            bias_into(bias, segr)
            pad_pair(kvo[...].astype(F32), kpad, vpad)
            dkey[...] = jnp.zeros_like(dkey)
            dval[...] = jnp.zeros_like(dval)
            s_down.chunk, s_down.sent = chunk_of(cf, act), given
            s_qkv.chunk, s_qkv.sent = chunk_of(na_v, dqkv), given.at[:, :, for_qkv]
            s_out.chunk, s_out.sent = chunk_of(branch, mo), given.at[:, :, for_wo]

            def att(first, last):
                with scope("b_att"):
                    attend_back_pairs(
                        first, last, qo, gm, mo, lo, kpad, vpad, bias, cos, sin, dqkv, dkey, dval
                    )

            def freed(out, slot):
                return pltpu.make_async_copy(stage_v, out, out_sem.at[1 + slot])

            def free(s, out, slot):
                s.add(stages - 1)
                freed(out, slot).start()
                s.drain()
                for bit in range(width):
                    pl.semaphore_signal(
                        ready.at[slot], inc=1, device_id={"dp": flip(me, 1 << bit, width)},
                        device_id_type=pl.DeviceIdType.MESH,
                    )

            def quiet(h):
                for step, there in ((-1, t > 0), (1, t < nt - 1)):
                    @pl.when(there)
                    def _():
                        pl.semaphore_signal(
                            calm.at[h], inc=1, device_id={"tensor": t + step},
                            device_id_type=pl.DeviceIdType.MESH,
                        )

            def gi_part(h):
                which = half_a if h == 0 else half_b
                mine = jnp.concatenate(
                    [dqkv[natural(j, s) : natural(j, s) + size, :] for s in which for j in range(nt)],
                    axis=0,
                )
                start_row = h * (tokens // 2)
                with scope("b_part"):

                    def product(cols):
                        part[start_row : start_row + tokens // 2, cols] = dot(
                            mine, wqkv_v[cols, :], 1, 1
                        )

                    over_cols(model, cut, product)
                with scope("calm"):
                    pl.semaphore_wait(calm.at[h], lax.min(t, 1) + lax.min(nt - 1 - t, 1))
                for s in which:
                    inward.edge(s)

            def gi_near(s):
                with scope("b_near"):
                    inward.relay(inward.near, s)

            def gi_far(s):
                with scope("b_far"):
                    inward.relay(inward.far, s)

            half_a, half_b = range(first_half), range(first_half, pieces)
            pairs = queries // LANES
            with scope("free0"):
                free(s_gate, d_gate, 0)
            with scope("b_give"):
                pl.semaphore_wait(ready.at[0], width)
                s_down.give()
            br(3, 3)
            gather_br.complete(range(pieces))
            with scope("b_gm"):
                loads[0].wait()
                gm[...] = dot(branch[...], wo_v[...], 1, 1).astype(BF)
            quiet(0)

            @pl.loop(0, 2)
            def _(h):
                att(h * (pairs // 2), (h + 1) * (pairs // 2))

                @pl.when(h == 0)
                def _():
                    y_near(2)
                    with scope("b_take"):
                        take(s_down)

            y_near(3)
            key = dkey[0] + pltpu.roll(dkey[1], HD, 1)
            value = pltpu.roll(dval[0], HD, 1) + dval[1]
            key = key * cos[...] - swapped(key) * sin[...]
            dqkv[:, queries : queries + LANES] = jnp.where(
                lane_index(key.shape) < HD, key, value
            ).astype(BF)
            loads[1].wait()
            gi_part(0)
            y_far(2)
            with scope("ya_far"):
                scatter_ya.relay(scatter_ya.far, 1)
            y_far(3)
            with scope("free1"):
                freed(d_gate, 0).wait()
                free(s_up, d_up, 1)
            gi_near(0)
            for s in half_b:
                y_own(s)
            scatter_y.finish(half_b)
            quiet(1)
            gi_part(1)
            gi_far(0)
            with scope("b_fill"):
                loads[2].wait()
                s_down.given()
                pl.semaphore_wait(ready.at[1], width)
                s_qkv.give()
            gi_near(1)
            with scope("b_fill"):
                take(s_qkv)
                s_out.give()
            for s in half_a:
                with scope("y_own"):
                    block_ = slice(s * size, (s + 1) * size)
                    scatter_ya.own_into(s, hid, block_)
                    y[block_, :] = hid[block_, :].astype(BF)
                    emit(y.at[pl.ds(s * size, size), :], y_o.at[pl.ds(s * size, size), :])
            scatter_ya.finish(half_a)
            with scope("b_done"):
                for mask in range(1, nd):
                    gain_copy(mask).wait_send()
                cots.finish(range(pieces))
                gather_br.finish(range(pieces))

            def take_grad(s):
                at = inward.own(s)
                block = slice(s * size, (s + 1) * size)

                def store(cols, value):
                    gi[block, cols] += value

                def store_gain(cols, value):
                    gsum[0:1, cols] += value

                back_through_norm(
                    lambda c: x[block, c].astype(F32), lambda c: part[at, c], gall, 0, store, store_gain
                )

            fills = [
                functools.partial(on, s, stage)
                for stage in range(stages)
                for s in (s_down, s_qkv, s_out)
            ]
            gi_far(1)
            with scope("b_fill"):
                take(s_out)
            gi_near(2)
            gi_far(2)
            with scope("b_fill"):
                fills.pop(0)()
            gi_near(3)
            gi_far(3)
            freed(d_up, 1).wait()
            with jax.named_scope("b_own"):
                for s in range(pieces):
                    take_grad(s)
                    emit(gi.at[pl.ds(s * size, size), :], gi_o.at[pl.ds(s * size, size), :])
                    if s == pieces - 2:
                        for _ in range(2):
                            fills.pop(0)()
            with jax.named_scope("b_gains"):
                fold = model // 4
                for i in range(4):
                    cols = slice(i * fold, (i + 1) * fold)
                    zslots[t, 2 * i : 2 * i + 2, :] = gsum[0:2, cols]

                def along(step):
                    return remote(
                        zslots.at[t], zslots.at[t], zsem.at[0, step], zsem.at[1, step],
                        {"tensor": lax.rem(t + step, nt)},
                    )

                for step in range(1, nt):
                    along(step).start()
            with jax.named_scope("b_gains"):
                for step in range(1, nt):
                    slot = zslots.at[lax.rem(t + nt - step, nt)]
                    remote(
                        slot, slot, zsem.at[0, step], zsem.at[1, step], {"tensor": lax.rem(t + step, nt)}
                    ).wait_recv()
                total = sum(zslots[i] for i in range(nt))
                for i in range(4):
                    gsum[0:2, i * fold : (i + 1) * fold] = total[2 * i : 2 * i + 2, :]

                def across(mask):
                    peer = flip(me, mask, width)
                    return remote(
                        gsum.at[:, pl.ds(pl.multiple_of(peer * shard, shard), shard)], dslots.at[me],
                        dsem.at[0, mask], dsem.at[1, mask], {"dp": peer},
                    )

                for mask in range(1, nd):
                    across(mask).start()
                dslots[me] = gsum[:, pl.ds(pl.multiple_of(me * shard, shard), shard)]
            with jax.named_scope("b_rest"):
                for fill in fills:
                    fill()
                emit(stage_v.at[:, pl.ds(0, queries)], d_wq_o)
                emit(part.at[pl.ds(0, queries), pl.ds(model, shard)], d_wo_o)
                emit(d_kv, d_kv_o)
                emit(d_down, d_down_o)
            with jax.named_scope("b_gains"):
                for mask in range(1, nd):
                    peer = flip(me, mask, width)
                    slot = dslots.at[peer]
                    remote(slot, slot, dsem.at[0, mask], dsem.at[1, mask], {"dp": peer}).wait_recv()
                gain_out[...] = sum(dslots[i] for i in range(nd))
                emit(gain_out, gain_o)
                for step in range(1, nt):
                    along(step).wait_send()
                for mask in range(1, nd):
                    across(mask).wait_send()
            with jax.named_scope("end"):
                for s in (s_qkv, s_out):
                    s.given()
                for s in (s_down, s_qkv, s_out):
                    s.drain()
                inward.finish(range(pieces))
                for copy in emitted:
                    copy.wait()

        pl.run_scoped(
            rear,
            pltpu.VMEM((tokens, tokens), F32),
            pltpu.VMEM((2, tokens, LANES), BF),
            pltpu.VMEM((2, tokens, LANES), BF),
            pltpu.VMEM((2, tokens, LANES), F32),
            pltpu.VMEM((2, tokens, LANES), F32),
            pltpu.VMEM((nd // 2, shard, hidden), BF),
        )

    pl.run_scoped(
        second_part, pltpu.VMEM((tokens // 2, model), BF), pltpu.VMEM((nt, rows // 2, model), BF)
    )


def layer(nt, nd, x, cot, gain_a, gain_f, segr, wq, wkt, wvt, wo, gate, up, down):
    width = nd.bit_length() - 1
    rows, model = x.shape
    tokens = nt * rows
    queries = wq.shape[1]
    hidden = gate.shape[1]
    shard = model // nd
    half = nd // 2
    wide = queries + LANES
    span = max(width_ for _, width_ in tiles_of(hidden, 6))
    shape = jax.ShapeDtypeStruct
    outs = [
        (shape((rows, model), BF), hbm()),
        (shape((rows, model), F32), hbm()),
        (shape((8, shard), F32), hbm()),
        (shape((shard, queries), F32), hbm()),
        (shape((LANES, shard), F32), hbm()),
        (shape((queries, shard), F32), hbm()),
        (shape((hidden, shard), F32), hbm()),
        (shape((shard, hidden), F32), hbm()),
        (shape((shard, hidden), F32), hbm()),
        (shape((model, wide), BF), hbm()),
        (shape((queries, model), BF), hbm()),
        (shape((tokens, model), BF), hbm()),
    ]
    return pl.pallas_call(
        functools.partial(layer_kernel, nt, width),
        out_shape=[o for o, _ in outs],
        in_specs=[vmem()] * 8 + [hbm()] * 4,
        out_specs=[s for _, s in outs],
        scratch_shapes=[
            pltpu.VMEM((tokens, model), BF),
            pltpu.VMEM((tokens, model), BF),
            pltpu.VMEM((tokens, model), BF),
            pltpu.VMEM((tokens, hidden), BF),
            pltpu.VMEM((rows, model), F32),
            pltpu.VMEM((model, hidden), BF),
            pltpu.VMEM((model, hidden), BF),
            pltpu.VMEM((hidden, model), BF),
            pltpu.VMEM((max(tokens, queries), max(model + shard, 3 * span)), F32),
        ]
        + line_scratch(nt, rows, model)
        + [
            pltpu.VMEM((nt + 1, rows // 2, model), BF),
            pltpu.VMEM((2, half, shard, hidden), BF),
            pltpu.VMEM((2, 2, half - 1, shard // 2, hidden), BF),
            pltpu.VMEM((shard, hidden), F32),
            pltpu.VMEM((rows, model), BF),
            pltpu.VMEM((rows, model), F32),
            pltpu.VMEM((8, shard), F32),
            pltpu.VMEM((LANES, shard), F32),
            pltpu.VMEM((hidden, shard), F32),
            pltpu.VMEM((shard, wide), BF),
            pltpu.VMEM((8, shard), F32),
            pltpu.VMEM((nd, 8, shard), F32),
            pltpu.VMEM((tokens, queries), BF),
            pltpu.VMEM((tokens, LANES), BF),
            pltpu.VMEM((tokens, queries), BF),
            pltpu.VMEM((tokens, LANES), F32),
            pltpu.VMEM((tokens, LANES), F32),
            pltpu.VMEM((tokens, LANES), F32),
            pltpu.VMEM((8, model), F32),
            pltpu.VMEM((nt, 8, model // 4), F32),
            pltpu.VMEM((nd, 8, shard), F32),
            dma(2, nd),
            dma(7),
            dma(3),
            dma(4, nt, PIECES),
            dma(4, nt, PIECES),
            dma(2, 2, nt, PIECES),
            dma(2, 2, nt, PIECES // 2),
            dma(8, 2, half - 1),
            dma(8, 2, half - 1),
            dma(8, half),
            dma(8, half),
            dma(2, nt),
            dma(2, nd),
            dma(2 * PIECES + 5),
            pltpu.SemaphoreType.REGULAR((2,)),
            pltpu.SemaphoreType.REGULAR((2,)),
        ],
        compiler_params=pltpu.CompilerParams(
            collective_id=0, has_side_effects=True, vmem_limit_bytes=VMEM_BYTES
        ),
        name="layer",
    )(x, cot, gain_a, gain_f, segr, wq, wkt, wvt, wo, gate, up, down)


def hand_over_kernel(count, kv, *refs):
    sources, rest = refs[: count + 2], refs[count + 2 :]
    targets, rest = rest[: count + 4], rest[count + 4 :]
    held, (in_sem, out_sem) = rest[: count + 2], rest[count + 2 :]
    ins = [
        pltpu.make_async_copy(src, buf, in_sem.at[i])
        for i, (src, buf) in enumerate(zip(sources, held))
    ]
    for copy in ins:
        copy.start()
    outs = []
    for i in range(count):
        ins[i].wait()
        outs.append(pltpu.make_async_copy(held[i], targets[i], out_sem.at[i]))
        outs[-1].start()
    ins[count].wait()
    for i in range(2):
        outs.append(
            pltpu.make_async_copy(
                held[count].at[pl.ds(i * kv, kv), :], targets[count + i], out_sem.at[count + i]
            )
        )
        outs[-1].start()
    ins[count + 1].wait()
    gains = held[count + 1]
    for i in range(2):
        targets[count + 2 + i][...] = gains[i, :]
    for copy in outs:
        copy.wait()


def hand_over(arrays, d_kv, gains):
    count, kv = len(arrays), d_kv.shape[0] // 2
    shape = jax.ShapeDtypeStruct
    outs = [shape(a.shape, a.dtype) for a in arrays]
    outs += [shape((kv, d_kv.shape[1]), F32)] * 2 + [shape((gains.shape[1],), F32)] * 2
    inputs = (*arrays, d_kv, gains)
    return pl.pallas_call(
        functools.partial(hand_over_kernel, count, kv),
        out_shape=outs,
        in_specs=[hbm()] * len(inputs),
        out_specs=[hbm()] * (count + 2) + [vmem()] * 2,
        scratch_shapes=[pltpu.VMEM(a.shape, a.dtype) for a in inputs]
        + [dma(len(inputs)), dma(count + 2)],
        compiler_params=pltpu.CompilerParams(vmem_limit_bytes=VMEM_BYTES),
        name="hand_over",
    )(*inputs)


def narrow_scatter(value, axis, scatter_dimension, tiled):
    low = value.astype(BF) if value.ndim == 2 else value
    return lax.psum_scatter(low, axis, scatter_dimension=scatter_dimension, tiled=tiled).astype(F32)


def rope_tables(segments, head_dim):
    row_count = segments.shape[0]
    row_index = jnp.arange(row_count, dtype=jnp.int32)
    change = jnp.concatenate(
        [jnp.ones((1,), jnp.int32), (segments[1:] != segments[:-1]).astype(jnp.int32)]
    )
    starts = lax.cummax(jnp.where(change > 0, row_index, jnp.zeros_like(row_index)), axis=0)
    position = (row_index - starts).astype(F32)
    half_dim = head_dim // 2
    frequency = jnp.exp(jnp.arange(half_dim, dtype=F32) * (-math.log(10000.0) / half_dim))
    angles = position[:, None] * frequency[None, :]
    return (jnp.cos(angles)[:, None, :], jnp.sin(angles)[:, None, :])


def rotate(tensor, cosine, sine):
    half_dim = tensor.shape[-1] // 2
    first_half = tensor[..., :half_dim]
    second_half = tensor[..., half_dim:]
    return jnp.concatenate(
        [first_half * cosine - second_half * sine, second_half * cosine + first_half * sine],
        axis=-1,
    )


def unrotate(tensor, cosine, sine):
    half_dim = tensor.shape[-1] // 2
    first_half = tensor[..., :half_dim]
    second_half = tensor[..., half_dim:]
    return jnp.concatenate(
        [first_half * cosine + second_half * sine, second_half * cosine - first_half * sine],
        axis=-1,
    )


def visible(segments):
    row_index = jnp.arange(segments.shape[0], dtype=jnp.int32)
    same_seq = segments[:, None] == segments[None, :]
    return same_seq & (row_index[:, None] >= row_index[None, :])


def normalize(values, gain):
    inverse = lax.rsqrt(jnp.mean(values * values, axis=-1, keepdims=True) + EPSILON)
    unit_rows = values * inverse
    return (unit_rows, inverse, (unit_rows * gain.astype(F32)).astype(BF))


def normalize_back(grad_normed, unit_rows, inverse, gain):
    scaled = grad_normed * gain.astype(F32)
    grad_values = inverse * (
        scaled - unit_rows * jnp.mean(scaled * unit_rows, axis=-1, keepdims=True)
    )
    return (grad_values, jnp.sum(grad_normed * unit_rows, axis=0))


def contract(left, right, left_dim, right_dim):
    return lax.dot_general(
        left, right, (((left_dim,), (right_dim,)), ((), ())), preferred_element_type=F32
    )


def block_scores(query_block, key_heads, allowed_block, score_scale):
    scores = (
        jnp.einsum("rkgd,skd->kgrs", query_block, key_heads, preferred_element_type=F32)
        * score_scale
    )
    return jnp.where(allowed_block[None, None], scores, NEGATIVE)


def attend_forward(query_groups, key_heads, value_heads, allowed, score_scale):
    scores = block_scores(query_groups, key_heads, allowed, score_scale)
    row_max = jnp.max(scores, axis=-1, keepdims=True)
    log_total = row_max + jnp.log(jnp.sum(jnp.exp(scores - row_max), axis=-1, keepdims=True))
    probs_low = jnp.exp(scores - log_total).astype(BF)
    mixed_parts = jnp.einsum(
        "kgrs,skd->rkgd", probs_low, value_heads, preferred_element_type=F32
    ).astype(BF)
    return (mixed_parts, log_total)


def attend_backward(
    query_groups, key_heads, value_heads, mixed_heads, grad_mixed, log_totals, allowed, score_scale
):
    scores = block_scores(query_groups, key_heads, allowed, score_scale)
    attn_probs = jnp.exp(scores - log_totals)
    probs_low = attn_probs.astype(BF)
    grad_probs = jnp.einsum(
        "rkgd,skd->kgrs", grad_mixed, value_heads, preferred_element_type=F32
    )
    row_delta = jnp.sum(grad_mixed.astype(F32) * mixed_heads.astype(F32), axis=-1)
    row_delta = jnp.transpose(row_delta, (1, 2, 0))[..., None]
    grad_scores = (attn_probs * (grad_probs - row_delta)).astype(BF)
    query_parts = (
        jnp.einsum("kgrs,skd->rkgd", grad_scores, key_heads, preferred_element_type=F32)
        * score_scale
    )
    grad_key_rot = (
        jnp.einsum("kgrs,rkgd->skd", grad_scores, query_groups, preferred_element_type=F32)
        * score_scale
    )
    grad_value_heads = jnp.einsum(
        "kgrs,rkgd->skd", probs_low, grad_mixed, preferred_element_type=F32
    )
    return (query_parts, grad_key_rot, grad_value_heads)


def plain_device(
    layer_input,
    segment_ids,
    norm_attn,
    w_query,
    w_key,
    w_value,
    w_output,
    norm_ffn,
    w_gate,
    w_up,
    w_down,
    cotangent,
):
    score_scale = HD ** (-0.5)
    query_full, key_full, value_full, output_full, gain_attn = (
        lax.all_gather(w_query, "dp", axis=0, tiled=True),
        lax.all_gather(w_key, "dp", axis=0, tiled=True),
        lax.all_gather(w_value, "dp", axis=0, tiled=True),
        lax.all_gather(w_output, "dp", axis=1, tiled=True),
        lax.all_gather(norm_attn, "dp", axis=0, tiled=True),
    )
    gate_full, up_full, down_full, gain_ffn = (
        lax.all_gather(w_gate, "dp", axis=0, tiled=True),
        lax.all_gather(w_up, "dp", axis=0, tiled=True),
        lax.all_gather(w_down, "dp", axis=1, tiled=True),
        lax.all_gather(norm_ffn, "dp", axis=0, tiled=True),
    )
    heads_local = query_full.shape[1] // HD
    kv_local = key_full.shape[1] // HD
    group = heads_local // kv_local
    residual_in = layer_input.astype(F32)
    unit_attn, inverse_attn, normed_local = normalize(residual_in, gain_attn)
    normed_attn = lax.all_gather(normed_local, "tensor", axis=0, tiled=True)
    row_count = normed_attn.shape[0]
    cosine, sine = rope_tables(segment_ids, HD)
    allowed = visible(segment_ids)
    query_heads = rotate(
        jnp.dot(normed_attn, query_full, preferred_element_type=F32).reshape(
            row_count, heads_local, HD
        ),
        cosine,
        sine,
    ).astype(BF)
    query_groups = query_heads.reshape(row_count, kv_local, group, HD)
    key_heads = rotate(
        jnp.dot(normed_attn, key_full, preferred_element_type=F32).reshape(
            row_count, kv_local, HD
        ),
        cosine,
        sine,
    ).astype(BF)
    value_heads = (
        jnp.dot(normed_attn, value_full, preferred_element_type=F32)
        .astype(BF)
        .reshape(row_count, kv_local, HD)
    )
    mixed_heads, log_totals = attend_forward(
        query_groups, key_heads, value_heads, allowed, score_scale
    )
    mixed_flat = mixed_heads.reshape(row_count, heads_local * HD)
    hidden_res = residual_in + narrow_scatter(
        jnp.dot(mixed_flat, output_full, preferred_element_type=F32),
        "tensor",
        scatter_dimension=0,
        tiled=True,
    )
    unit_ffn, inverse_ffn, normed_ffn_local = normalize(hidden_res, gain_ffn)
    normed_ffn = lax.all_gather(normed_ffn_local, "tensor", axis=0, tiled=True)
    gate_rows = jnp.dot(normed_ffn, gate_full, preferred_element_type=F32)
    up_rows = jnp.dot(normed_ffn, up_full, preferred_element_type=F32)
    sigmoid_gate = jax.nn.sigmoid(gate_rows)
    active = (gate_rows * sigmoid_gate * up_rows).astype(BF)
    layer_output = (
        hidden_res
        + narrow_scatter(
            jnp.dot(active, down_full, preferred_element_type=F32).astype(BF),
            "tensor",
            scatter_dimension=0,
            tiled=True,
        ).astype(F32)
    ).astype(BF)
    query_full, key_full, value_full, output_full, gate_full, up_full, down_full = (
        lax.all_gather(w_query, "dp", axis=0, tiled=True),
        lax.all_gather(w_key, "dp", axis=0, tiled=True),
        lax.all_gather(w_value, "dp", axis=0, tiled=True),
        lax.all_gather(w_output, "dp", axis=1, tiled=True),
        lax.all_gather(w_gate, "dp", axis=0, tiled=True),
        lax.all_gather(w_up, "dp", axis=0, tiled=True),
        lax.all_gather(w_down, "dp", axis=1, tiled=True),
    )
    cotangent_full = lax.all_gather(cotangent, "tensor", axis=0, tiled=True)
    grad_active = contract(cotangent_full, down_full, 1, 1)
    grad_w_down = contract(active, cotangent_full, 0, 0)
    grad_up_rows = (grad_active * gate_rows * sigmoid_gate).astype(BF)
    grad_gate_rows = (
        grad_active * up_rows * sigmoid_gate * (1.0 + gate_rows * (1.0 - sigmoid_gate))
    ).astype(BF)
    grad_w_gate = contract(normed_ffn, grad_gate_rows, 0, 0)
    grad_w_up = contract(normed_ffn, grad_up_rows, 0, 0)
    grad_normed_ffn = narrow_scatter(
        contract(grad_gate_rows, gate_full, 1, 1) + contract(grad_up_rows, up_full, 1, 1),
        "tensor",
        scatter_dimension=0,
        tiled=True,
    )
    grad_hidden, gain_ffn_part = normalize_back(grad_normed_ffn, unit_ffn, inverse_ffn, gain_ffn)
    grad_hidden = cotangent.astype(F32) + grad_hidden
    branch_full = lax.all_gather(grad_hidden.astype(BF), "tensor", axis=0, tiled=True)
    grad_mixed = contract(branch_full, output_full, 1, 1).astype(BF)
    grad_w_output = contract(mixed_flat, branch_full, 0, 0)
    grad_query_rot, grad_key_rot, grad_value_heads = attend_backward(
        query_groups,
        key_heads,
        value_heads,
        mixed_heads,
        grad_mixed.reshape(row_count, kv_local, group, HD),
        log_totals,
        allowed,
        score_scale,
    )
    grad_queries = (
        unrotate(grad_query_rot.reshape(row_count, heads_local, HD), cosine, sine)
        .reshape(row_count, heads_local * HD)
        .astype(BF)
    )
    grad_keys = (
        unrotate(grad_key_rot, cosine, sine).reshape(row_count, kv_local * HD).astype(BF)
    )
    grad_values = grad_value_heads.reshape(row_count, kv_local * HD).astype(BF)
    grad_w_query = contract(normed_attn, grad_queries, 0, 0)
    grad_w_key = contract(normed_attn, grad_keys, 0, 0)
    grad_w_value = contract(normed_attn, grad_values, 0, 0)
    grad_normed_attn = narrow_scatter(
        contract(grad_queries, query_full, 1, 1)
        + contract(grad_keys, key_full, 1, 1)
        + contract(grad_values, value_full, 1, 1),
        "tensor",
        scatter_dimension=0,
        tiled=True,
    )
    grad_residual, gain_attn_part = normalize_back(
        grad_normed_attn, unit_attn, inverse_attn, gain_attn
    )
    grad_input = grad_hidden + grad_residual
    gain_attn_total, gain_ffn_total = lax.psum((gain_attn_part, gain_ffn_part), "tensor")
    owned = (
        narrow_scatter(grad_w_query, "dp", scatter_dimension=0, tiled=True),
        narrow_scatter(grad_w_key, "dp", scatter_dimension=0, tiled=True),
        narrow_scatter(grad_w_value, "dp", scatter_dimension=0, tiled=True),
        narrow_scatter(grad_w_output, "dp", scatter_dimension=1, tiled=True),
        narrow_scatter(gain_attn_total, "dp", scatter_dimension=0, tiled=True),
        narrow_scatter(gain_ffn_total, "dp", scatter_dimension=0, tiled=True),
        narrow_scatter(grad_w_gate, "dp", scatter_dimension=0, tiled=True),
        narrow_scatter(grad_w_up, "dp", scatter_dimension=0, tiled=True),
        narrow_scatter(grad_w_down, "dp", scatter_dimension=1, tiled=True),
    )
    return (
        layer_output,
        grad_input,
        owned[4],
        owned[0],
        owned[1],
        owned[2],
        owned[3],
        owned[5],
        owned[6],
        owned[7],
        owned[8],
    )


def with_kernels(nt, nd, layer_input, segment_ids, norm_attn, w_query, w_key, w_value, w_output, norm_ffn, w_gate, w_up, w_down, cotangent):
    y, gi, gains, d_wq, d_kv, d_wo, d_down, d_gate, d_up, *_ = layer(
        nt, nd, layer_input, cotangent, norm_attn, norm_ffn, segment_ids[None, :],
        w_query, w_key.T, w_value.T, w_output, w_gate, w_up, w_down,
    )
    y, gi, d_wq, d_wo, d_gate, d_up, d_down, d_k, d_v, d_attn, d_ffn = hand_over(
        (y, gi, d_wq, d_wo, d_gate, d_up, d_down), d_kv, gains
    )
    return (y, gi, d_attn, d_wq, d_k.T, d_v.T, d_wo, d_ffn, d_gate, d_up, d_down)


def fits(nt, nd, shards):
    layer_input, segment_ids, norm_attn, w_query, w_key, w_value, w_output, norm_ffn, w_gate, w_up, w_down, _ = shards
    return (
        nd >= 4
        and nd & (nd - 1) == 0
        and nt >= 2
        and norm_attn.shape[0] % LANES == 0
        and w_output.shape[1] % LANES == 0
        and w_gate.shape[1] % LANES == 0
        and w_query.shape[1] % LANES == 0
        and w_key.shape[1] == HD
        and segment_ids.shape[0] == nt * layer_input.shape[0]
        and segment_ids.shape[0] % (8 * LANES // 2) == 0
        and w_gate.shape[1] >= w_query.shape[1] + segment_ids.shape[0]
        and layer_input.shape[1] >= 2 * segment_ids.shape[0]
    )


def on_device(nt, nd, *shards):
    if fits(nt, nd, shards):
        return with_kernels(nt, nd, *shards)
    return plain_device(*shards)


def solution(mesh):
    placed = (
        P(("dp", "tensor"), None),
        P("dp"),
        P("dp"),
        P("dp", "tensor"),
        P("dp", "tensor"),
        P("dp", "tensor"),
        P("tensor", "dp"),
        P("dp"),
        P("dp", "tensor"),
        P("dp", "tensor"),
        P("tensor", "dp"),
        P(("dp", "tensor"), None),
    )
    return jax.shard_map(
        functools.partial(on_device, mesh.shape["tensor"], mesh.shape["dp"]),
        mesh=mesh,
        in_specs=placed,
        out_specs=(
            P(("dp", "tensor"), None),
            P(("dp", "tensor"), None),
            P("dp"),
            P("dp", "tensor"),
            P("dp", "tensor"),
            P("dp", "tensor"),
            P("tensor", "dp"),
            P("dp"),
            P("dp", "tensor"),
            P("dp", "tensor"),
            P("tensor", "dp"),
        ),
        check_vma=False,
    )
```

```python
import functools
import math

import jax
import jax.numpy as jnp
from jax import lax
from jax.experimental import pallas as pl
from jax.experimental.pallas import tpu as pltpu
from jax.sharding import PartitionSpec as P

HD = 64
EPSILON = 1e-05
NEGATIVE = -1e30
LANES = 128
BF = jnp.bfloat16
F32 = jnp.float32
VMEM_BYTES = 67_000_000


def spans(bits):
    masks = [0]
    for bit in bits:
        masks = masks + [mask | (1 << bit) for mask in masks]
    return masks


def flip(index, mask, width):
    total = 0
    for bit in range(width):
        own = lax.rem(lax.div(index, 1 << bit), 2)
        if isinstance(mask, int):
            other = (mask >> bit) & 1
        else:
            other = lax.rem(lax.div(mask, 1 << bit), 2)
        total = total + lax.rem(own + other, 2) * (1 << bit)
    return total


def aligned(value, step):
    return value if isinstance(value, int) else pl.multiple_of(value, step)


def remote(src, dst, send_sem, recv_sem, device):
    return pltpu.make_async_remote_copy(
        src_ref=src,
        dst_ref=dst,
        send_sem=send_sem,
        recv_sem=recv_sem,
        device_id=device,
        device_id_type=pl.DeviceIdType.MESH,
    )


def dot(left, right, left_dim=1, right_dim=0):
    return lax.dot_general(
        left, right, (((left_dim,), (right_dim,)), ((), ())), preferred_element_type=F32
    )


def tiles_of(size, most):
    units = size // LANES
    parts = -(-units // most)
    cuts, start = [], 0
    for part in range(parts):
        width = (units // parts + (1 if part < units % parts else 0)) * LANES
        cuts.append((start, width))
        start += width
    return cuts


def over_cols(size, width, body):
    @pl.loop(0, size // width)
    def _(i):
        body(pl.ds(pl.multiple_of(i * width, width), width))


def enter(t, nt, me, width, barrier, everyone_along_tensor=False):
    signal = functools.partial(
        pl.semaphore_signal, barrier, inc=1, device_id_type=pl.DeviceIdType.MESH
    )
    for mask in range(1, 1 << width):
        signal(device_id={"dp": flip(me, mask, width)})
    if everyone_along_tensor:
        for step in range(1, nt):
            signal(device_id={"tensor": lax.rem(t + step, nt)})
        pl.semaphore_wait(barrier, (1 << width) - 1 + nt - 1)
        return

    @pl.when(t > 0)
    def _():
        signal(device_id={"tensor": t - 1})

    @pl.when(t < nt - 1)
    def _():
        signal(device_id={"tensor": t + 1})

    neighbours = lax.min(t, 1) + lax.min(nt - 1 - t, 1)
    pl.semaphore_wait(barrier, (1 << width) - 1 + neighbours)


class LineGather:
    def __init__(self, full, row, size, t, nt, sems):
        self.full, self.row, self.size = full, row, size
        self.t, self.nt, self.sems = t, nt, sems
        self.pieces = sems.shape[2]
        self.done = set()

    def window(self, j, s):
        return self.full.at[pl.ds(aligned(self.row(j, s), self.size), self.size), :]

    def right(self, j, s):
        at = self.window(j, s)
        return remote(
            at, at, self.sems.at[0, j, s], self.sems.at[2, j, s],
            {"tensor": lax.rem(self.t + 1, self.nt)},
        )

    def left(self, j, s):
        at = self.window(j, s)
        return remote(
            at, at, self.sems.at[1, j, s], self.sems.at[3, j, s],
            {"tensor": lax.rem(self.t + self.nt - 1, self.nt)},
        )

    def start(self, s):
        @pl.when(self.t < self.nt - 1)
        def _():
            self.right(self.t, s).start()

        @pl.when(self.t > 0)
        def _():
            self.left(self.t, s).start()

    def step(self, k, s):
        t, nt = self.t, self.nt
        if k >= nt or (k, s) in self.done:
            return
        self.done.add((k, s))

        @pl.when(t >= k)
        def _():
            self.right(t - k, s).wait_recv()

            @pl.when(t < nt - 1)
            def _():
                self.right(t - k, s).start()

        @pl.when(t + k < nt)
        def _():
            self.left(t + k, s).wait_recv()

            @pl.when(t > 0)
            def _():
                self.left(t + k, s).start()

    def complete(self, pieces):
        for k in range(1, self.nt):
            for s in pieces:
                self.step(k, s)

    def finish(self, pieces):
        t, nt = self.t, self.nt

        @pl.loop(0, nt)
        def _(k):
            for s in pieces:
                @pl.when((t >= k) & (t < nt - 1))
                def _():
                    self.right(t - k, s).wait_send()

                @pl.when((t + k < nt) & (t > 0))
                def _():
                    self.left(t + k, s).wait_send()


class LineScatter:
    def __init__(self, part, row, sent, arrived, t, nt, sems):
        self.part, self.row, self.sent, self.arrived = part, row, sent, arrived
        self.t, self.nt, self.sems = t, nt, sems
        self.pieces = sems.shape[3]
        self.size = sent.shape[1] // self.pieces
        self.model = sent.shape[2]
        self.near = lax.div(2 * t, nt)
        self.far = 1 - self.near

    def sub(self, s):
        return pl.ds(s * self.size, self.size)

    def depth(self, way):
        return (1 - way) * self.t + way * (self.nt - 1 - self.t)

    def goal(self, way, i):
        return (1 - way) * (self.nt - 1 - i) + way * i

    def slot(self, way, j):
        return j + 1 - way

    def move(self, way, j, s):
        return remote(
            self.sent.at[j, self.sub(s), :], self.arrived.at[self.slot(way, j), self.sub(s), :],
            self.sems.at[0, way, j, s], self.sems.at[1, way, j, s],
            {"tensor": lax.rem(self.t + self.nt + 1 - 2 * way, self.nt)},
        )

    def rows(self, j, s):
        return pl.ds(aligned(self.row(j, s), self.size), self.size)

    def mine(self, j, s):
        return self.part[self.rows(j, s), : self.model].astype(F32)

    def edge(self, s):
        t, nt = self.t, self.nt

        @pl.when((t == 0) | (t == nt - 1))
        def _():
            way = lax.div(t, nt - 1)

            @pl.loop(0, nt - 1)
            def _(i):
                j = self.goal(way, i)
                self.sent[j, self.sub(s), :] = self.mine(j, s).astype(BF)
                self.move(way, j, s).start()

    def relay(self, way, s):
        depth = self.depth(way)

        @pl.when(depth > 0)
        def _():
            @pl.loop(0, self.nt - 1 - depth)
            def _(i):
                j = self.goal(way, i)
                self.move(way, j, s).wait_recv()
                total = self.mine(j, s) + self.arrived[self.slot(way, j), self.sub(s), :].astype(F32)
                self.sent[j, self.sub(s), :] = total.astype(BF)
                self.move(way, j, s).start()

    def own(self, s):
        t = self.t
        rows = self.rows(t, s)
        for way in (self.near, self.far):
            @pl.when(self.depth(way) > 0)
            def _():
                self.move(way, t, s).wait_recv()
                self.part[rows, : self.model] += self.arrived[self.slot(way, t), self.sub(s), :].astype(F32)

        return rows

    def own_into(self, s, total, at):
        total[at, :] += self.mine(self.t, s)
        for way in (self.near, self.far):
            @pl.when(self.depth(way) > 0)
            def _():
                self.move(way, self.t, s).wait_recv()
                total[at, :] += self.arrived[self.slot(way, self.t), self.sub(s), :].astype(F32)

    def finish(self, pieces):
        for way in range(2):
            @pl.loop(0, self.nt - 1 - self.depth(way))
            def _(i):
                for s in pieces:
                    self.move(way, self.goal(way, i), s).wait_send()


class Cube:
    def setup(self, me, width, half_send, half_recv, pair_send, pair_recv):
        self.me, self.width = me, width
        self.hs, self.hr, self.ps, self.pr = half_send, half_recv, pair_send, pair_recv
        self.bits = list(range(1, width))
        self.orders = (self.bits, self.bits[::-1])
        self.masks = spans(self.bits)
        self.stages = len(self.bits)

    def at(self, mask):
        return flip(self.me, mask, self.width)


class BlockGather(Cube):
    def __init__(self, own, full, by_rows, me, width, *sems):
        self.setup(me, width, *sems)
        self.own_ref, self.full, self.by_rows = own, full, by_rows

    def half(self, h):
        rows = self.own_ref.shape[0] // 2
        return self.own_ref.at[pl.ds(h * rows, rows), :]

    def window(self, who, h=None):
        rows, cols = self.own_ref.shape
        take, start = (rows, 0) if h is None else (rows // 2, h * (rows // 2))
        if self.by_rows:
            return self.full.at[pl.ds(aligned(who * rows + start, take), take), :]
        return self.full.at[pl.ds(start, take), pl.ds(aligned(who * cols, cols), cols)]

    def hop(self, stage, h, m):
        order = self.orders[h]
        bit = 1 << order[stage]
        slot = (m | bit) >> 1
        src = self.half(h) if m == 0 else self.window(self.at(m), h)
        return remote(
            src, self.window(self.at(m), h), self.hs.at[h, slot - 1], self.hr.at[h, slot - 1],
            {"dp": self.at(bit)},
        )

    def send(self, stage):
        for h in range(2):
            for m in spans(self.orders[h][:stage]):
                self.hop(stage, h, m).start()

    def wait(self, stage):
        for h in range(2):
            bit = 1 << self.orders[h][stage]
            for m in spans(self.orders[h][:stage]):
                slot = (m | bit) >> 1
                landed = self.window(self.at(m | bit), h)
                remote(
                    landed, landed, self.hs.at[h, slot - 1], self.hr.at[h, slot - 1],
                    {"dp": self.at(bit)},
                ).wait_recv()

    def pair(self, m):
        src = self.own_ref if m == 0 else self.window(self.at(m))
        return remote(
            src, self.window(self.at(m)), self.ps.at[m >> 1], self.pr.at[m >> 1],
            {"dp": self.at(1)},
        )

    def pair_own(self):
        self.pair(0).start()

    def pair_send(self):
        for m in self.masks:
            if m:
                self.pair(m).start()

    def pair_wait(self):
        for m in self.masks:
            landed = self.window(self.at(m | 1))
            remote(
                landed, landed, self.ps.at[m >> 1], self.pr.at[m >> 1], {"dp": self.at(1)}
            ).wait_recv()

    def place(self, sem):
        return pltpu.make_async_copy(self.own_ref, self.window(self.me), sem)

    def drain(self):
        for stage in range(self.stages):
            for h in range(2):
                for m in spans(self.orders[h][:stage]):
                    self.hop(stage, h, m).wait_send()
        for m in self.masks:
            self.pair(m).wait_send()


class BlockScatter(Cube):
    def __init__(self, chunk, out_sent, total, landed, store, me, width, *sems):
        self.setup(me, width, *sems)
        self.chunk, self.sent, self.total, self.landed = chunk, out_sent, total, landed
        self.store = store
        self.slots = 1 << (width - 1)

    def pair(self, slot):
        return remote(
            self.sent.at[slot], self.total.at[slot], self.ps.at[slot], self.pr.at[slot],
            {"dp": self.at(1)},
        )

    def give(self):
        @pl.loop(0, self.slots)
        def _(k):
            slot = self.slots - 1 - k
            self.sent[slot] = self.chunk(self.at(2 * slot + 1)).astype(BF)
            self.pair(slot).start()

    def prepare(self):
        @pl.loop(0, self.slots)
        def _(k):
            slot = self.slots - 1 - k
            self.sent[slot] = self.chunk(self.at(2 * slot + 1)).astype(BF)

    def dispatch(self):
        @pl.loop(0, self.slots)
        def _(k):
            self.pair(self.slots - 1 - k).start()

    def given(self):
        @pl.loop(0, self.slots)
        def _(slot):
            self.pair(slot).wait_send()

    def take(self):
        @pl.loop(0, self.slots)
        def _(k):
            slot = self.slots - 1 - k
            term = self.chunk(self.at(2 * slot))
            self.pair(slot).wait_recv()
            self.total[slot] = (term + self.total[slot].astype(F32)).astype(BF)

    def moves(self, stage):
        for h in range(2):
            order = self.orders[h]
            last = self.stages - 1 - stage
            bit = 1 << order[last]
            for m in spans(order[:last]):
                yield h, bit, m | bit

    def hop(self, h, bit, m):
        rows = self.total.shape[1] // 2
        return remote(
            self.total.at[m >> 1, pl.ds(h * rows, rows), :], self.landed.at[h, (m >> 1) - 1],
            self.hs.at[h, (m >> 1) - 1], self.hr.at[h, (m >> 1) - 1], {"dp": self.at(bit)},
        )

    def send(self, stage):
        for h, bit, m in self.moves(stage):
            self.hop(h, bit, m).start()

    def add(self, stage):
        rows = self.total.shape[1] // 2
        for h, bit, m in self.moves(stage):
            self.hop(h, bit, m).wait_recv()
            keep = (m ^ bit) >> 1
            at = slice(h * rows, (h + 1) * rows)
            total = self.total[keep, at, :].astype(F32) + self.landed[h, (m >> 1) - 1].astype(F32)
            if stage == self.stages - 1:
                self.store(at, total)
            else:
                self.total[keep, at, :] = total.astype(BF)

    def drain(self):
        for stage in range(self.stages):
            for h, bit, m in self.moves(stage):
                self.hop(h, bit, m).wait_send()


def inverse_of(rows):
    return lax.rsqrt(jnp.mean(rows * rows, axis=-1, keepdims=True) + EPSILON)


def times_gain(unit, gains, which, store):
    parts, _, width = gains.shape
    for d in range(parts):
        cols = slice(d * width, (d + 1) * width)
        store(cols, unit[:, cols] * gains[d, which : which + 1, :])


def lane_index(shape):
    return lax.broadcasted_iota(jnp.int32, shape, len(shape) - 1)


def column_of(segr):
    rows = segr.shape[1]
    wide = jnp.broadcast_to(segr[...].astype(F32), (8, rows))
    return jnp.transpose(wide)[:, 0:1]


def rope_into(cos_ref, sin_ref, segr):
    rows = segr.shape[1]
    before = (segr[...].astype(F32) < column_of(segr)).astype(F32)
    start = jnp.sum(before, axis=1, keepdims=True)
    position = lax.broadcasted_iota(jnp.int32, (rows, 1), 0).astype(F32) - start
    lane = lane_index((rows, LANES))
    half = HD // 2
    frequency = jnp.exp(lax.rem(lane, half).astype(F32) * (-math.log(10000.0) / half))
    angle = position * frequency
    cos_ref[...] = jnp.cos(angle)
    sine = jnp.sin(angle)
    sin_ref[...] = jnp.where(lax.rem(lane, HD) < half, -sine, sine)


def swapped(x):
    lane = lane_index(x.shape)
    half = HD // 2
    return jnp.where(
        lax.rem(lane, HD) < half,
        pltpu.roll(x, LANES - half, 1),
        pltpu.roll(x, half, 1),
    )


def bias_into(bias, segr):
    rows = segr.shape[1]
    query = lax.broadcasted_iota(jnp.int32, (rows, rows), 0)
    key = lax.broadcasted_iota(jnp.int32, (rows, rows), 1)
    seen = (segr[...].astype(F32) == column_of(segr)) & (query >= key)
    bias[...] = jnp.where(seen, 0.0, NEGATIVE)


def pad_pair(keys_values, keys, values):
    low = lane_index(keys_values.shape) < HD
    key = jnp.where(low, keys_values, 0.0)
    value = jnp.where(low, 0.0, keys_values)
    keys[0] = key.astype(BF)
    keys[1] = pltpu.roll(key, HD, 1).astype(BF)
    values[0] = pltpu.roll(value, HD, 1).astype(BF)
    values[1] = value.astype(BF)


def query_cuts(rows):
    block = 256 if rows % 256 == 0 else rows
    return [(start, block, start + block) for start in range(0, rows, block)]


def attend_pairs(first, last, qo, kpad, vpad, bias, mo, lo):
    rows = qo.shape[0]
    lane = lane_index((1, LANES))

    @pl.loop(first, last)
    def _(pair):
        lanes = pl.ds(pl.multiple_of(pair * LANES, LANES), LANES)
        for start, block, seen in query_cuts(rows):
            at = slice(start, start + block)
            query = qo[at, lanes]
            mixed = jnp.zeros((block, LANES), F32)
            logs = lo[at, :]
            for side in range(2):
                scores = dot(query, kpad[side, :seen, :], 1, 1) + bias[at, :seen]
                top = jnp.max(scores, axis=-1, keepdims=True)
                probs = jnp.exp(scores - top)
                total = jnp.sum(probs, axis=-1, keepdims=True)
                mixed = mixed + dot(probs.astype(BF), vpad[side, :seen, :]) / total
                logs = jnp.where(lane == 2 * pair + side, top + jnp.log(total), logs)
            lo[at, :] = logs
            mo[at, lanes] = mixed.astype(BF)


def back_through_norm(raw, grads, gains, which, store, store_gain):
    parts, _, width = gains.shape
    cuts = [slice(d * width, (d + 1) * width) for d in range(parts)]
    model = parts * width
    square = sum(jnp.sum(raw(c) * raw(c), axis=-1, keepdims=True) for c in cuts)
    inverse = lax.rsqrt(square / model + EPSILON)
    mean = 0.0
    for d, c in enumerate(cuts):
        unit = raw(c) * inverse
        grad = grads(c)
        store_gain(c, jnp.sum(grad * unit, axis=0, keepdims=True))
        mean = mean + jnp.sum(grad * gains[d, which : which + 1, :] * unit, axis=-1, keepdims=True)
    mean = mean / model
    for d, c in enumerate(cuts):
        unit = raw(c) * inverse
        store(c, inverse * (grads(c) * gains[d, which : which + 1, :] - unit * mean))


def attend_back_pairs(first, last, qo, gm, mo, lo, kpad, vpad, bias, cos, sin, dqkv, dkey, dval):
    rows = qo.shape[0]

    @pl.loop(first, last)
    def _(pair):
        lanes = pl.ds(pl.multiple_of(pair * LANES, LANES), LANES)
        for start, block, seen in query_cuts(rows):
            at = slice(start, start + block)
            lane = lane_index((block, LANES))
            query, grad = qo[at, lanes], gm[at, lanes]
            both = grad.astype(F32) * mo[at, lanes].astype(F32)
            logs = lo[at, :]
            dq = jnp.zeros((block, LANES), F32)
            for side in range(2):
                inside = (lane >= HD) if side else (lane < HD)
                delta = jnp.sum(jnp.where(inside, both, 0.0), axis=-1, keepdims=True)
                log = jnp.sum(
                    jnp.where(lane == 2 * pair + side, logs, 0.0), axis=-1, keepdims=True
                )
                key, value = kpad[side, :seen, :], vpad[side, :seen, :]
                probs = jnp.exp(dot(query, key, 1, 1) + bias[at, :seen] - log)
                grad_scores = (probs * (dot(grad, value, 1, 1) - delta)).astype(BF)
                dq = dq + dot(grad_scores, key)
                dkey[side, :seen, :] += dot(grad_scores, query, 0, 0)
                dval[side, :seen, :] += dot(probs.astype(BF), grad, 0, 0)
            dq = dq * HD ** (-0.5)
            dqkv[at, lanes] = (dq * cos[at, :] - swapped(dq) * sin[at, :]).astype(BF)


PIECES = 4


def vmem():
    return pl.BlockSpec(memory_space=pltpu.VMEM)


def hbm():
    return pl.BlockSpec(memory_space=pl.ANY)


def dma(*shape):
    return pltpu.SemaphoreType.DMA(shape)


def line_scratch(nt, rows, model):
    return [pltpu.VMEM((nt, rows, model), BF), pltpu.VMEM((nt + 1, rows, model), BF)]


def ticks(pieces, nt):
    return [
        [(k, tick - k) for k in range(1, nt) if 0 <= tick - k < pieces]
        for tick in range(pieces + nt - 1)
    ]


def layer_kernel(
    nt, width,
    x, cot, gain_a, gain_f, segr, wq, wkt, wvt, wo, gate, up, down,
    y_o, gi_o, gain_o, d_wq_o, d_kv_o, d_wo_o, d_down_o, d_gate, d_up, wqkv_f, wo_f, na_f,
    rowsbuf, cf, branch, act, hid, gate_v, up_v, down_v, part, sent, arrived, y_arrived, totals, landed, stage_v,
    y, gi, gain_out, d_kv, d_down,
    own_qkv, gain, gall, qo, kvo, mo, lo, cos, sin, gsum, zslots, dslots,
    gain_sem, place_sem, out_sem, line_sem, cot_sem, sum_sem, first_sem,
    hs, hr, ps, pr, zsem, dsem, emit_sem, ready, calm,
):
    me, t = lax.axis_index("dp"), lax.axis_index("tensor")
    nd = 1 << width
    rows, model = x.shape
    tokens = nt * rows
    queries = wq.shape[1]
    hidden = gate.shape[1]
    shard = model >> width
    wide = own_qkv.shape[1]
    pieces = PIECES
    first_half = pieces // 2
    size = rows // pieces
    cut = 512 if model % 512 == 0 else LANES

    def natural(j, s):
        return j * rows + s * size

    def shuffled(j, s):
        return (s * nt + j) * size

    local = pl.ds(pl.multiple_of(t * rows, rows), rows)
    rowsbuf[local, :] = x[...]
    gain[...] = jnp.zeros_like(gain)
    gain[0:1, :] = gain_a[...].astype(F32).reshape(1, shard)
    gain[1:2, :] = gain_f[...].astype(F32).reshape(1, shard)
    own_qkv[:, :queries] = wq[...]
    turned = jnp.concatenate([wkt[...].astype(F32), wvt[...].astype(F32)], axis=0)
    own_qkv[:, queries:] = jnp.transpose(turned).astype(BF)
    with jax.named_scope("enter"):
        enter(t, nt, me, width, pltpu.get_barrier_semaphore())

    tokens_x = LineGather(rowsbuf, natural, size, t, nt, line_sem)
    for s in range(pieces):
        tokens_x.start(s)
    gathers = []
    for w, (own, full, by_rows) in enumerate(
        ((own_qkv, wqkv_f, True), (wo, wo_f, False), (gate, gate_v, True), (up, up_v, True), (down, down_v, False))
    ):
        gathers.append(
            BlockGather(own, full, by_rows, me, width, hs.at[w], hr.at[w], ps.at[w], pr.at[w])
        )
    g_qkv, g_out, g_gate, g_up, g_down = gathers
    stages = g_qkv.stages

    def gain_copy(mask):
        return remote(
            gain, gall.at[me], gain_sem.at[0, mask], gain_sem.at[1, mask],
            {"dp": flip(me, mask, width)},
        )

    for mask in range(1, nd):
        gain_copy(mask).start()
    for g in (g_qkv, g_out, g_gate):
        g.send(0)
    for w, g in enumerate(gathers):
        g.place(place_sem.at[w]).start()
    gall[me] = gain[...]

    def forward(g, stage):
        g.wait(stage)
        if stage == 0:
            g.pair_own()
        if stage + 1 < stages:
            g.send(stage + 1)
        else:
            g.pair_send()

    for s in range(pieces):
        cf[pl.ds(pl.multiple_of(shuffled(t, s), size), size), :] = cot[s * size : (s + 1) * size, :]
    cots = LineGather(cf, shuffled, size, t, nt, cot_sem)
    scatter_o = LineScatter(part, shuffled, sent, arrived, t, nt, sum_sem)

    def attention(na, wqkv_v, wo_v, bias, kpad, vpad):
        bias_into(bias, segr)
        rope_into(cos, sin, segr)
        lo[...] = jnp.zeros_like(lo)
        for mask in range(1, nd):
            slot = gall.at[flip(me, mask, width)]
            remote(
                slot, slot, gain_sem.at[0, mask], gain_sem.at[1, mask],
                {"dp": flip(me, mask, width)},
            ).wait_recv()

        def norm(j):
            @pl.loop(0, pieces)
            def _(s):
                these = pl.ds(pl.multiple_of(j * rows + s * size, size), size)
                value = rowsbuf[these, :].astype(F32)

                def store(cols, normed):
                    na[these, cols] = normed.astype(BF)

                times_gain(value * inverse_of(value), gall, 0, store)

        norm(t)
        for stage in range(stages - 1):
            forward(g_qkv, stage)
            forward(g_out, stage)
        fills = [
            lambda: (forward(g_gate, 0), g_up.send(0)),
            lambda: (forward(g_qkv, stages - 1), forward(g_out, stages - 1), g_down.send(0)),
        ]
        load = pltpu.make_async_copy(wqkv_f, wqkv_v, place_sem.at[5])
        load_out = pltpu.make_async_copy(wo_f, wo_v, place_sem.at[6])

        def fetch():
            g_qkv.place(place_sem.at[0]).wait()
            g_qkv.pair_wait()
            load.start()
            g_out.place(place_sem.at[1]).wait()
            g_out.pair_wait()
            load_out.start()

        for k in range(1, nt):
            if k == nt - 1:
                for fill in fills:
                    fill()
                fills = []
                with jax.named_scope("fetch"):
                    fetch()
            with jax.named_scope("x_step"):
                for s in range(pieces):
                    tokens_x.step(k, s)
            if k == nt - 1:
                for s in range(first_half):
                    cots.start(s)

            @pl.when(t >= k)
            def _():
                norm(t - k)

            @pl.when(t + k < nt)
            def _():
                norm(t + k)

            if fills:
                with jax.named_scope("x_fill"):
                    fills.pop(0)()
        keep = pltpu.make_async_copy(na, na_f, out_sem.at[0])
        keep.start()
        with jax.named_scope("wait_qkv"):
            load.wait()
        with jax.named_scope("qkv"):
            part[:, :wide] = dot(na[...], wqkv_v[...])
            c, s_ = cos[...], sin[...]
            for start in range(0, queries, LANES):
                lanes = slice(start, start + LANES)
                value = part[:, lanes]
                qo[:, lanes] = ((value * c + swapped(value) * s_) * HD ** (-0.5)).astype(BF)
            value = part[:, queries : queries + LANES]
            keyed = jnp.where(lane_index(value.shape) < HD, value * c + swapped(value) * s_, value)
            kvo[...] = keyed.astype(BF)
            pad_pair(keyed, kpad, vpad)
        pairs = queries // LANES
        with jax.named_scope("att"):
            attend_pairs(0, pairs, qo, kpad, vpad, bias, mo, lo)
        load_out.wait()
        with jax.named_scope("outproj"):
            mixed = jnp.concatenate(
                [
                    mo[natural(j, s) : natural(j, s) + size, :]
                    for s in range(pieces)
                    for j in range(nt)
                ],
                axis=0,
            )

            def project(cols):
                part[:tokens, cols] = dot(mixed, wo_v[:, cols])

            over_cols(model, cut, project)
        keep.wait()
        tokens_x.finish(range(pieces))

    pl.run_scoped(
        attention,
        pltpu.VMEM((tokens, model), BF),
        pltpu.VMEM((model, wide), BF),
        pltpu.VMEM((queries, model), BF),
        pltpu.VMEM((tokens, tokens), F32),
        pltpu.VMEM((2, tokens, LANES), BF),
        pltpu.VMEM((2, tokens, LANES), BF),
    )

    gather_nf = LineGather(rowsbuf, shuffled, size, t, nt, line_sem)

    def take_hidden(s):
        at = scatter_o.own(s)
        block = slice(s * size, (s + 1) * size)
        hidden_rows = x[block, :].astype(F32) + part[at, :model]
        hid[block, :] = hidden_rows
        there = pl.ds(pl.multiple_of(shuffled(t, s), size), size)

        def store(cols, normed):
            rowsbuf[there, cols] = normed.astype(BF)

        times_gain(hidden_rows * inverse_of(hidden_rows), gall, 1, store)
        gather_nf.start(s)

    def chunk_of(left, right):
        def chunk(d):
            return dot(left[:, pl.ds(pl.multiple_of(d * shard, shard), shard)], right[...], 0, 0)

        return chunk

    def cube(w, totals_, landed_, store):
        return BlockScatter(
            None, None, totals_, landed_, store, me, width, hs.at[w], hr.at[w], ps.at[w], pr.at[w]
        )

    def store_stage(at, value):
        stage_v[at, :] = value

    def store_down(at, value):
        d_down[:, at] = value.T

    def store_qkv(at, value):
        stage_v[at, :queries] = value[:, :queries]
        d_kv[:, at] = value[:, queries:].T

    def store_wo(at, value):
        part[:queries, model + at.start : model + at.stop] = value.T

    for_qkv, for_wo = pl.ds(0, wide), pl.ds(wide, queries)
    s_gate = cube(5, totals.at[0], landed.at[0], store_stage)
    s_up = cube(6, totals.at[1], landed.at[1], store_stage)
    s_down = cube(5, totals.at[0], landed.at[0], store_down)
    s_qkv = cube(6, totals.at[1, :, :, for_qkv], landed.at[1, :, :, :, for_qkv], store_qkv)
    s_out = cube(7, totals.at[1, :, :, for_wo], landed.at[1, :, :, :, for_wo], store_wo)

    def take(s):
        s.take()
        s.send(0)

    def on(s, stage):
        s.add(stage)
        if stage + 1 < stages:
            s.send(stage + 1)

    scatter_y = LineScatter(part, shuffled, sent, arrived, t, nt, sum_sem)
    scope = jax.named_scope
    emitted = []

    def emit(src, dst):
        emitted.append(pltpu.make_async_copy(src, dst, emit_sem.at[len(emitted)]))
        emitted[-1].start()

    def y_part(h):
        mine = slice(h * (tokens // 2), (h + 1) * (tokens // 2))
        with scope("y_part"):

            def product(cols):
                part[mine, cols] = dot(act[mine, :], down_v[:, cols])

            over_cols(model, cut, product)

    def y_near(s):
        with scope("y_near"):
            scatter_y.relay(scatter_y.near, s)

    def y_far(s):
        with scope("y_far"):
            scatter_y.relay(scatter_y.far, s)

    def y_own(s):
        with scope("y_own"):
            at = scatter_y.own(s)
            block_ = slice(s * size, (s + 1) * size)
            y[block_, :] = (hid[block_, :] + part[at, :model]).astype(BF)
            emit(y.at[pl.ds(s * size, size), :], y_o.at[pl.ds(s * size, size), :])

    def br(k, s):
        with scope("br_step"):
            gather_br.step(k, s)

    gsum[...] = jnp.zeros_like(gsum)
    gather_br = LineGather(branch, natural, size, t, nt, line_sem)

    def second_part(y_first, y_sent, given):
        scatter_ya = LineScatter(y_first, shuffled, y_sent, y_arrived, t, nt, first_sem)

        def freed(out, slot):
            return pltpu.make_async_copy(stage_v, out, out_sem.at[1 + slot])

        def free(s, out, slot):
            s.add(stages - 1)
            freed(out, slot).start()
            s.drain()
            for bit in range(width):
                pl.semaphore_signal(
                    ready.at[slot], inc=1, device_id={"dp": flip(me, 1 << bit, width)},
                    device_id_type=pl.DeviceIdType.MESH,
                )

        def feed(dg, du):
            cuts = tiles_of(hidden, 6)
            span = max(width_ for _, width_ in cuts)
            half = tokens // 2
            block = 64

            def tile_in(h, i):
                start, width_ = cuts[i]
                at = slice(start, start + width_)
                held = mine = slice(h * half, (h + 1) * half)
                part[held, 0:width_] = dot(rowsbuf[mine, :], gate_v[:, at])
                part[held, span : span + width_] = dot(rowsbuf[mine, :], up_v[:, at])

            def tile_down(h, i):
                start, width_ = cuts[i]
                at = slice(start, start + width_)
                held = mine = slice(h * half, (h + 1) * half)
                part[held, 2 * span : 2 * span + width_] = dot(cf[mine, :], down_v[at, :], 1, 1)

            def tile_out(h, i):
                start, width_ = cuts[i]
                at = slice(start, start + width_)

                @pl.loop(0, half // block)
                def _(k):
                    from_ = pl.ds(pl.multiple_of(h * half + k * block, block), block)
                    to = pl.ds(pl.multiple_of(h * half + k * block, block), block)
                    g = part[from_, 0:width_]
                    u = part[from_, span : span + width_]
                    ga = part[from_, 2 * span : 2 * span + width_]
                    sig = 1.0 / (1.0 + jnp.exp(-g))
                    gs = g * sig
                    act[to, at] = (gs * u).astype(BF)
                    du[to, at] = (ga * gs).astype(BF)
                    dg[to, at] = (ga * u * sig * (1.0 + g * (1.0 - sig))).astype(BF)

            def tile(h, i):
                with scope("tile"):
                    tile_in(h, i)
                    tile_down(h, i)
                    tile_out(h, i)

            def back_dots(h):
                mine = slice(h * half, (h + 1) * half)

                def product(cols):
                    part[mine, cols] = dot(dg[mine, :], gate_v[cols, :], 1, 1) + dot(
                        du[mine, :], up_v[cols, :], 1, 1
                    )

                over_cols(model, cut, product)

            scatter_gn = LineScatter(part, shuffled, sent, arrived, t, nt, sum_sem)

            def take_grad(s):
                at = scatter_gn.own(s)
                block_ = slice(s * size, (s + 1) * size)
                there = pl.ds(pl.multiple_of(natural(t, s), size), size)

                def store(cols, value):
                    total = cot[block_, cols].astype(F32) + value
                    gi[block_, cols] = total
                    branch[there, cols] = total.astype(BF)

                def store_gain(cols, value):
                    gsum[1:2, cols] += value

                back_through_norm(
                    lambda c: hid[block_, c], lambda c: part[at, c], gall, 1, store, store_gain
                )
                gather_br.start(s)

            s_gate.chunk, s_up.chunk = chunk_of(rowsbuf, dg), chunk_of(rowsbuf, du)
            s_gate.sent = s_up.sent = given

            half_a, half_b = range(first_half), range(first_half, pieces)
            def o_near(s):
                with scope("o_near"):
                    scatter_o.relay(scatter_o.near, s)

            def o_far(s):
                with scope("o_far"):
                    scatter_o.relay(scatter_o.far, s)

            def o_take(s):
                with scope("o_take"):
                    take_hidden(s)

            def nf(k, s):
                with scope("nf_step"):
                    gather_nf.step(k, s)

            def cot_steps(k, which):
                with scope("cot_step"):
                    for s in which:
                        cots.step(k, s)

            def gn_near(s):
                with scope("gn_near"):
                    scatter_gn.relay(scatter_gn.near, s)

            def gn_far(s):
                with scope("gn_far"):
                    scatter_gn.relay(scatter_gn.far, s)

            def ya_near(s):
                with scope("ya_near"):
                    scatter_ya.relay(scatter_ya.near, s)

            def ya_far(s):
                with scope("ya_far"):
                    scatter_ya.relay(scatter_ya.far, s)

            def gn_take(s):
                with scope("gn_take"):
                    take_grad(s)

            def weight(g, stage):
                with scope("weight"):
                    if stage < stages:
                        forward(g, stage)

            scatter_o.edge(0)
            scatter_o.edge(1)
            cot_steps(1, half_a)
            weight(g_gate, 1)
            cot_steps(2, half_a)
            o_near(0)
            weight(g_up, 0)
            o_far(0)
            o_take(0)
            weight(g_down, 0)
            scatter_o.edge(2)
            o_near(1)
            o_far(1)
            nf(1, 0)
            cot_steps(3, half_a)
            o_take(1)
            scatter_o.edge(3)
            nf(1, 1)
            nf(2, 0)
            o_near(2)
            nf(2, 1)
            weight(g_up, 1)
            o_far(2)
            o_near(3)
            nf(3, 0)
            for s in half_b:
                cots.start(s)
            nf(3, 1)
            o_take(2)
            o_far(3)
            gather_nf.complete(half_a)
            cots.complete(half_a)
            weight(g_down, 1)
            for stage in range(2, stages):
                for g in (g_gate, g_up, g_down):
                    weight(g, stage)
            with scope("wait_ffn"):
                for w in (2, 3):
                    gathers[w].place(place_sem.at[w]).wait()
                    gathers[w].pair_wait()
            with scope("tile"):
                tile_in(0, 0)
            with scope("wait_ffn"):
                g_down.place(place_sem.at[4]).wait()
                g_down.pair_wait()
            with scope("tile"):
                tile_down(0, 0)
                tile_out(0, 0)
            o_take(3)
            nf(1, 2)
            cot_steps(1, half_b)
            for i in range(1, len(cuts)):
                tile(0, i)
            nf(2, 2)
            nf(1, 3)
            with scope("back_dots"):
                scatter_o.finish(half_a)
                back_dots(0)
            scatter_gn.edge(0)
            scatter_gn.edge(1)
            cot_steps(2, half_b)
            with scope("y_part"):
                def product(cols):
                    y_first[:, cols] = dot(act[: tokens // 2, :], down_v[:, cols]).astype(BF)

                over_cols(model, cut, product)
            gn_near(0)
            scatter_ya.edge(0)
            nf(3, 2)
            nf(2, 3)
            gn_far(0)
            cot_steps(3, half_b)
            cots.complete(half_b)
            gn_near(1)
            with scope("tile"):
                tile_down(1, 0)
            nf(3, 3)
            gather_nf.complete(half_b)
            gather_nf.finish(half_a)
            with scope("tile"):
                tile_in(1, 0)
                tile_out(1, 0)
            gn_far(1)
            gn_take(0)
            for i in range(1, len(cuts)):
                tile(1, i)
            with scope("back_dots"):
                scatter_o.finish(half_b)
                back_dots(1)
            scatter_gn.edge(2)
            gn_take(1)
            scatter_gn.edge(3)
            with scope("gn_fill"):
                s_gate.give()
            br(1, 0)
            with scope("gn_fill"):
                take(s_gate)
            gn_near(2)
            br(2, 0)
            with scope("gn_fill"):
                s_gate.given()
                s_up.give()
            gn_far(2)
            br(1, 1)
            br(3, 0)
            with scope("gn_fill"):
                s_up.take()
            gn_near(3)
            gather_nf.finish(half_b)
            gn_take(2)
            scatter_ya.edge(1)
            gn_far(3)
            ya_near(0)
            at_end = (t == 0) | (t == nt - 1)

            def gate_on():
                with scope("add0"):
                    on(s_gate, 0)
                    s_up.send(0)

            pl.when(at_end)(gate_on)
            gn_take(3)
            pl.when(jnp.logical_not(at_end))(gate_on)
            br(2, 1)
            br(1, 2)
            br(3, 1)
            ya_far(0)
            y_part(1)
            br(2, 2)
            br(1, 3)
            scatter_gn.finish(half_b)
            scatter_y.edge(2)
            scatter_y.edge(3)
            with scope("b_give"):
                s_up.given()
                s_down.chunk, s_down.sent = chunk_of(cf, act), given
                s_down.prepare()
            with scope("free0"):
                free(s_gate, d_gate, 0)
            with scope("b_give"):
                pl.semaphore_wait(ready.at[0], width)
                s_down.dispatch()
            scatter_gn.finish(half_a)

        pl.run_scoped(
            feed,
            pltpu.VMEM((tokens, hidden), BF),
            pltpu.VMEM((tokens, hidden), BF),
        )

        wo_v = down_v.at[pl.ds(0, queries), :]
        na_v = down_v.at[pl.ds(queries, tokens), :]
        wqkv_v = gate_v.at[:, pl.ds(0, wide)]
        gm = up_v.at[pl.ds(0, tokens), pl.ds(0, queries)]
        dqkv = up_v.at[pl.ds(tokens, tokens), pl.ds(0, wide)]

        def rear(bias, kpad, vpad, dkey, dval):
            inward = LineScatter(part, shuffled, sent, arrived, t, nt, sum_sem)
            for g in gathers:
                g.drain()
            loads = [
                pltpu.make_async_copy(wo_f, wo_v, place_sem.at[0]),
                pltpu.make_async_copy(wqkv_f, wqkv_v, place_sem.at[1]),
                pltpu.make_async_copy(na_f, na_v, place_sem.at[2]),
            ]
            for load in loads:
                load.start()
            bias_into(bias, segr)
            pad_pair(kvo[...].astype(F32), kpad, vpad)
            dkey[...] = jnp.zeros_like(dkey)
            dval[...] = jnp.zeros_like(dval)
            s_qkv.chunk, s_qkv.sent = chunk_of(na_v, dqkv), given.at[:, :, for_qkv]
            s_out.chunk, s_out.sent = chunk_of(branch, mo), given.at[:, :, for_wo]

            def att(first, last):
                with scope("b_att"):
                    attend_back_pairs(
                        first, last, qo, gm, mo, lo, kpad, vpad, bias, cos, sin, dqkv, dkey, dval
                    )

            def quiet(h):
                for step, there in ((-1, t > 0), (1, t < nt - 1)):
                    @pl.when(there)
                    def _():
                        pl.semaphore_signal(
                            calm.at[h], inc=1, device_id={"tensor": t + step},
                            device_id_type=pl.DeviceIdType.MESH,
                        )

            def gi_part(h):
                which = half_a if h == 0 else half_b
                mine = jnp.concatenate(
                    [dqkv[natural(j, s) : natural(j, s) + size, :] for s in which for j in range(nt)],
                    axis=0,
                )
                start_row = h * (tokens // 2)
                with scope("b_part"):

                    def product(cols):
                        part[start_row : start_row + tokens // 2, cols] = dot(
                            mine, wqkv_v[cols, :], 1, 1
                        )

                    over_cols(model, cut, product)
                with scope("calm"):
                    pl.semaphore_wait(calm.at[h], lax.min(t, 1) + lax.min(nt - 1 - t, 1))
                for s in which:
                    inward.edge(s)

            def gi_near(s):
                with scope("b_near"):
                    inward.relay(inward.near, s)

            def gi_far(s):
                with scope("b_far"):
                    inward.relay(inward.far, s)

            half_a, half_b = range(first_half), range(first_half, pieces)
            pairs = queries // LANES
            br(3, 2)
            br(2, 3)
            scatter_ya.relay(scatter_ya.near, 1)
            with scope("b_take"):
                s_down.take()
            with scope("add0"):
                on(s_up, 0)
                s_down.send(0)
            br(3, 3)
            gather_br.complete(range(pieces))
            with scope("b_gm"):
                loads[0].wait()
                gm[...] = dot(branch[...], wo_v[...], 1, 1).astype(BF)
            quiet(0)

            @pl.loop(0, 2)
            def _(h):
                att(h * (pairs // 2), (h + 1) * (pairs // 2))

                @pl.when(h == 0)
                def _():
                    y_near(2)

            y_near(3)
            key = dkey[0] + pltpu.roll(dkey[1], HD, 1)
            value = pltpu.roll(dval[0], HD, 1) + dval[1]
            key = key * cos[...] - swapped(key) * sin[...]
            dqkv[:, queries : queries + LANES] = jnp.where(
                lane_index(key.shape) < HD, key, value
            ).astype(BF)
            loads[1].wait()
            gi_part(0)
            y_far(2)
            with scope("ya_far"):
                scatter_ya.relay(scatter_ya.far, 1)
            y_far(3)
            with scope("free1"):
                freed(d_gate, 0).wait()
                free(s_up, d_up, 1)
            gi_near(0)
            for s in half_b:
                y_own(s)
            scatter_y.finish(half_b)
            quiet(1)
            gi_part(1)
            gi_far(0)
            with scope("b_fill"):
                loads[2].wait()
                s_down.given()
                pl.semaphore_wait(ready.at[1], width)
                s_qkv.give()
            gi_near(1)
            with scope("b_fill"):
                take(s_qkv)
                s_out.give()
            for s in half_a:
                with scope("y_own"):
                    block_ = slice(s * size, (s + 1) * size)
                    scatter_ya.own_into(s, hid, block_)
                    y[block_, :] = hid[block_, :].astype(BF)
                    emit(y.at[pl.ds(s * size, size), :], y_o.at[pl.ds(s * size, size), :])
            scatter_ya.finish(half_a)
            with scope("b_done"):
                for mask in range(1, nd):
                    gain_copy(mask).wait_send()
                cots.finish(range(pieces))
                gather_br.finish(range(pieces))

            def take_grad(s):
                at = inward.own(s)
                block = slice(s * size, (s + 1) * size)

                def store(cols, value):
                    gi[block, cols] += value

                def store_gain(cols, value):
                    gsum[0:1, cols] += value

                back_through_norm(
                    lambda c: x[block, c].astype(F32), lambda c: part[at, c], gall, 0, store, store_gain
                )

            fills = [
                functools.partial(on, s, stage)
                for stage in range(stages)
                for s in (s_down, s_qkv, s_out)
            ]
            gi_far(1)
            with scope("b_fill"):
                take(s_out)
            gi_near(2)
            gi_far(2)
            with scope("b_fill"):
                fills.pop(0)()
            gi_near(3)
            gi_far(3)
            freed(d_up, 1).wait()
            with jax.named_scope("b_own"):
                for s in range(pieces):
                    take_grad(s)
                    emit(gi.at[pl.ds(s * size, size), :], gi_o.at[pl.ds(s * size, size), :])
                    if s == pieces - 2:
                        for _ in range(2):
                            fills.pop(0)()
            with jax.named_scope("b_gains"):
                fold = model // 4
                for i in range(4):
                    cols = slice(i * fold, (i + 1) * fold)
                    zslots[t, 2 * i : 2 * i + 2, :] = gsum[0:2, cols]

                def along(step):
                    return remote(
                        zslots.at[t], zslots.at[t], zsem.at[0, step], zsem.at[1, step],
                        {"tensor": lax.rem(t + step, nt)},
                    )

                for step in range(1, nt):
                    along(step).start()
            with jax.named_scope("b_gains"):
                for step in range(1, nt):
                    slot = zslots.at[lax.rem(t + nt - step, nt)]
                    remote(
                        slot, slot, zsem.at[0, step], zsem.at[1, step], {"tensor": lax.rem(t + step, nt)}
                    ).wait_recv()
                total = sum(zslots[i] for i in range(nt))
                for i in range(4):
                    gsum[0:2, i * fold : (i + 1) * fold] = total[2 * i : 2 * i + 2, :]

                def across(mask):
                    peer = flip(me, mask, width)
                    return remote(
                        gsum.at[:, pl.ds(pl.multiple_of(peer * shard, shard), shard)], dslots.at[me],
                        dsem.at[0, mask], dsem.at[1, mask], {"dp": peer},
                    )

                for mask in range(1, nd):
                    across(mask).start()
                dslots[me] = gsum[:, pl.ds(pl.multiple_of(me * shard, shard), shard)]
            with jax.named_scope("b_rest"):
                for fill in fills:
                    fill()
                emit(stage_v.at[:, pl.ds(0, queries)], d_wq_o)
                emit(part.at[pl.ds(0, queries), pl.ds(model, shard)], d_wo_o)
                emit(d_kv, d_kv_o)
                emit(d_down, d_down_o)
            with jax.named_scope("b_gains"):
                for mask in range(1, nd):
                    peer = flip(me, mask, width)
                    slot = dslots.at[peer]
                    remote(slot, slot, dsem.at[0, mask], dsem.at[1, mask], {"dp": peer}).wait_recv()
                gain_out[...] = sum(dslots[i] for i in range(nd))
                emit(gain_out, gain_o)
                for step in range(1, nt):
                    along(step).wait_send()
                for mask in range(1, nd):
                    across(mask).wait_send()
            with jax.named_scope("end"):
                for s in (s_qkv, s_out):
                    s.given()
                for s in (s_down, s_qkv, s_out):
                    s.drain()
                inward.finish(range(pieces))
                for copy in emitted:
                    copy.wait()

        pl.run_scoped(
            rear,
            pltpu.VMEM((tokens, tokens), F32),
            pltpu.VMEM((2, tokens, LANES), BF),
            pltpu.VMEM((2, tokens, LANES), BF),
            pltpu.VMEM((2, tokens, LANES), F32),
            pltpu.VMEM((2, tokens, LANES), F32),
        )

    pl.run_scoped(
        second_part,
        pltpu.VMEM((tokens // 2, model), BF),
        pltpu.VMEM((nt, rows // 2, model), BF),
        pltpu.VMEM((nd // 2, shard, hidden), BF),
    )


def layer(nt, nd, x, cot, gain_a, gain_f, segr, wq, wkt, wvt, wo, gate, up, down):
    width = nd.bit_length() - 1
    rows, model = x.shape
    tokens = nt * rows
    queries = wq.shape[1]
    hidden = gate.shape[1]
    shard = model // nd
    half = nd // 2
    wide = queries + LANES
    span = max(width_ for _, width_ in tiles_of(hidden, 6))
    shape = jax.ShapeDtypeStruct
    outs = [
        (shape((rows, model), BF), hbm()),
        (shape((rows, model), F32), hbm()),
        (shape((8, shard), F32), hbm()),
        (shape((shard, queries), F32), hbm()),
        (shape((LANES, shard), F32), hbm()),
        (shape((queries, shard), F32), hbm()),
        (shape((hidden, shard), F32), hbm()),
        (shape((shard, hidden), F32), hbm()),
        (shape((shard, hidden), F32), hbm()),
        (shape((model, wide), BF), hbm()),
        (shape((queries, model), BF), hbm()),
        (shape((tokens, model), BF), hbm()),
    ]
    return pl.pallas_call(
        functools.partial(layer_kernel, nt, width),
        out_shape=[o for o, _ in outs],
        in_specs=[vmem()] * 8 + [hbm()] * 4,
        out_specs=[s for _, s in outs],
        scratch_shapes=[
            pltpu.VMEM((tokens, model), BF),
            pltpu.VMEM((tokens, model), BF),
            pltpu.VMEM((tokens, model), BF),
            pltpu.VMEM((tokens, hidden), BF),
            pltpu.VMEM((rows, model), F32),
            pltpu.VMEM((model, hidden), BF),
            pltpu.VMEM((model, hidden), BF),
            pltpu.VMEM((hidden, model), BF),
            pltpu.VMEM((max(tokens, queries), max(model + shard, 3 * span)), F32),
        ]
        + line_scratch(nt, rows, model)
        + [
            pltpu.VMEM((nt + 1, rows // 2, model), BF),
            pltpu.VMEM((2, half, shard, hidden), BF),
            pltpu.VMEM((2, 2, half - 1, shard // 2, hidden), BF),
            pltpu.VMEM((shard, hidden), F32),
            pltpu.VMEM((rows, model), BF),
            pltpu.VMEM((rows, model), F32),
            pltpu.VMEM((8, shard), F32),
            pltpu.VMEM((LANES, shard), F32),
            pltpu.VMEM((hidden, shard), F32),
            pltpu.VMEM((shard, wide), BF),
            pltpu.VMEM((8, shard), F32),
            pltpu.VMEM((nd, 8, shard), F32),
            pltpu.VMEM((tokens, queries), BF),
            pltpu.VMEM((tokens, LANES), BF),
            pltpu.VMEM((tokens, queries), BF),
            pltpu.VMEM((tokens, LANES), F32),
            pltpu.VMEM((tokens, LANES), F32),
            pltpu.VMEM((tokens, LANES), F32),
            pltpu.VMEM((8, model), F32),
            pltpu.VMEM((nt, 8, model // 4), F32),
            pltpu.VMEM((nd, 8, shard), F32),
            dma(2, nd),
            dma(7),
            dma(3),
            dma(4, nt, PIECES),
            dma(4, nt, PIECES),
            dma(2, 2, nt, PIECES),
            dma(2, 2, nt, PIECES // 2),
            dma(8, 2, half - 1),
            dma(8, 2, half - 1),
            dma(8, half),
            dma(8, half),
            dma(2, nt),
            dma(2, nd),
            dma(2 * PIECES + 5),
            pltpu.SemaphoreType.REGULAR((2,)),
            pltpu.SemaphoreType.REGULAR((2,)),
        ],
        compiler_params=pltpu.CompilerParams(
            collective_id=0, has_side_effects=True, vmem_limit_bytes=VMEM_BYTES
        ),
        name="layer",
    )(x, cot, gain_a, gain_f, segr, wq, wkt, wvt, wo, gate, up, down)


def hand_over_kernel(count, kv, *refs):
    sources, rest = refs[: count + 2], refs[count + 2 :]
    targets, rest = rest[: count + 4], rest[count + 4 :]
    held, (in_sem, out_sem) = rest[: count + 2], rest[count + 2 :]
    ins = [
        pltpu.make_async_copy(src, buf, in_sem.at[i])
        for i, (src, buf) in enumerate(zip(sources, held))
    ]
    for copy in ins:
        copy.start()
    outs = []
    for i in range(count):
        ins[i].wait()
        outs.append(pltpu.make_async_copy(held[i], targets[i], out_sem.at[i]))
        outs[-1].start()
    ins[count].wait()
    for i in range(2):
        outs.append(
            pltpu.make_async_copy(
                held[count].at[pl.ds(i * kv, kv), :], targets[count + i], out_sem.at[count + i]
            )
        )
        outs[-1].start()
    ins[count + 1].wait()
    gains = held[count + 1]
    for i in range(2):
        targets[count + 2 + i][...] = gains[i, :]
    for copy in outs:
        copy.wait()


def hand_over(arrays, d_kv, gains):
    count, kv = len(arrays), d_kv.shape[0] // 2
    shape = jax.ShapeDtypeStruct
    outs = [shape(a.shape, a.dtype) for a in arrays]
    outs += [shape((kv, d_kv.shape[1]), F32)] * 2 + [shape((gains.shape[1],), F32)] * 2
    inputs = (*arrays, d_kv, gains)
    return pl.pallas_call(
        functools.partial(hand_over_kernel, count, kv),
        out_shape=outs,
        in_specs=[hbm()] * len(inputs),
        out_specs=[hbm()] * (count + 2) + [vmem()] * 2,
        scratch_shapes=[pltpu.VMEM(a.shape, a.dtype) for a in inputs]
        + [dma(len(inputs)), dma(count + 2)],
        compiler_params=pltpu.CompilerParams(vmem_limit_bytes=VMEM_BYTES),
        name="hand_over",
    )(*inputs)


def narrow_scatter(value, axis, scatter_dimension, tiled):
    low = value.astype(BF) if value.ndim == 2 else value
    return lax.psum_scatter(low, axis, scatter_dimension=scatter_dimension, tiled=tiled).astype(F32)


def rope_tables(segments, head_dim):
    row_count = segments.shape[0]
    row_index = jnp.arange(row_count, dtype=jnp.int32)
    change = jnp.concatenate(
        [jnp.ones((1,), jnp.int32), (segments[1:] != segments[:-1]).astype(jnp.int32)]
    )
    starts = lax.cummax(jnp.where(change > 0, row_index, jnp.zeros_like(row_index)), axis=0)
    position = (row_index - starts).astype(F32)
    half_dim = head_dim // 2
    frequency = jnp.exp(jnp.arange(half_dim, dtype=F32) * (-math.log(10000.0) / half_dim))
    angles = position[:, None] * frequency[None, :]
    return (jnp.cos(angles)[:, None, :], jnp.sin(angles)[:, None, :])


def rotate(tensor, cosine, sine):
    half_dim = tensor.shape[-1] // 2
    first_half = tensor[..., :half_dim]
    second_half = tensor[..., half_dim:]
    return jnp.concatenate(
        [first_half * cosine - second_half * sine, second_half * cosine + first_half * sine],
        axis=-1,
    )


def unrotate(tensor, cosine, sine):
    half_dim = tensor.shape[-1] // 2
    first_half = tensor[..., :half_dim]
    second_half = tensor[..., half_dim:]
    return jnp.concatenate(
        [first_half * cosine + second_half * sine, second_half * cosine - first_half * sine],
        axis=-1,
    )


def visible(segments):
    row_index = jnp.arange(segments.shape[0], dtype=jnp.int32)
    same_seq = segments[:, None] == segments[None, :]
    return same_seq & (row_index[:, None] >= row_index[None, :])


def normalize(values, gain):
    inverse = lax.rsqrt(jnp.mean(values * values, axis=-1, keepdims=True) + EPSILON)
    unit_rows = values * inverse
    return (unit_rows, inverse, (unit_rows * gain.astype(F32)).astype(BF))


def normalize_back(grad_normed, unit_rows, inverse, gain):
    scaled = grad_normed * gain.astype(F32)
    grad_values = inverse * (
        scaled - unit_rows * jnp.mean(scaled * unit_rows, axis=-1, keepdims=True)
    )
    return (grad_values, jnp.sum(grad_normed * unit_rows, axis=0))


def contract(left, right, left_dim, right_dim):
    return lax.dot_general(
        left, right, (((left_dim,), (right_dim,)), ((), ())), preferred_element_type=F32
    )


def block_scores(query_block, key_heads, allowed_block, score_scale):
    scores = (
        jnp.einsum("rkgd,skd->kgrs", query_block, key_heads, preferred_element_type=F32)
        * score_scale
    )
    return jnp.where(allowed_block[None, None], scores, NEGATIVE)


def attend_forward(query_groups, key_heads, value_heads, allowed, score_scale):
    scores = block_scores(query_groups, key_heads, allowed, score_scale)
    row_max = jnp.max(scores, axis=-1, keepdims=True)
    log_total = row_max + jnp.log(jnp.sum(jnp.exp(scores - row_max), axis=-1, keepdims=True))
    probs_low = jnp.exp(scores - log_total).astype(BF)
    mixed_parts = jnp.einsum(
        "kgrs,skd->rkgd", probs_low, value_heads, preferred_element_type=F32
    ).astype(BF)
    return (mixed_parts, log_total)


def attend_backward(
    query_groups, key_heads, value_heads, mixed_heads, grad_mixed, log_totals, allowed, score_scale
):
    scores = block_scores(query_groups, key_heads, allowed, score_scale)
    attn_probs = jnp.exp(scores - log_totals)
    probs_low = attn_probs.astype(BF)
    grad_probs = jnp.einsum(
        "rkgd,skd->kgrs", grad_mixed, value_heads, preferred_element_type=F32
    )
    row_delta = jnp.sum(grad_mixed.astype(F32) * mixed_heads.astype(F32), axis=-1)
    row_delta = jnp.transpose(row_delta, (1, 2, 0))[..., None]
    grad_scores = (attn_probs * (grad_probs - row_delta)).astype(BF)
    query_parts = (
        jnp.einsum("kgrs,skd->rkgd", grad_scores, key_heads, preferred_element_type=F32)
        * score_scale
    )
    grad_key_rot = (
        jnp.einsum("kgrs,rkgd->skd", grad_scores, query_groups, preferred_element_type=F32)
        * score_scale
    )
    grad_value_heads = jnp.einsum(
        "kgrs,rkgd->skd", probs_low, grad_mixed, preferred_element_type=F32
    )
    return (query_parts, grad_key_rot, grad_value_heads)


def plain_device(
    layer_input,
    segment_ids,
    norm_attn,
    w_query,
    w_key,
    w_value,
    w_output,
    norm_ffn,
    w_gate,
    w_up,
    w_down,
    cotangent,
):
    score_scale = HD ** (-0.5)
    query_full, key_full, value_full, output_full, gain_attn = (
        lax.all_gather(w_query, "dp", axis=0, tiled=True),
        lax.all_gather(w_key, "dp", axis=0, tiled=True),
        lax.all_gather(w_value, "dp", axis=0, tiled=True),
        lax.all_gather(w_output, "dp", axis=1, tiled=True),
        lax.all_gather(norm_attn, "dp", axis=0, tiled=True),
    )
    gate_full, up_full, down_full, gain_ffn = (
        lax.all_gather(w_gate, "dp", axis=0, tiled=True),
        lax.all_gather(w_up, "dp", axis=0, tiled=True),
        lax.all_gather(w_down, "dp", axis=1, tiled=True),
        lax.all_gather(norm_ffn, "dp", axis=0, tiled=True),
    )
    heads_local = query_full.shape[1] // HD
    kv_local = key_full.shape[1] // HD
    group = heads_local // kv_local
    residual_in = layer_input.astype(F32)
    unit_attn, inverse_attn, normed_local = normalize(residual_in, gain_attn)
    normed_attn = lax.all_gather(normed_local, "tensor", axis=0, tiled=True)
    row_count = normed_attn.shape[0]
    cosine, sine = rope_tables(segment_ids, HD)
    allowed = visible(segment_ids)
    query_heads = rotate(
        jnp.dot(normed_attn, query_full, preferred_element_type=F32).reshape(
            row_count, heads_local, HD
        ),
        cosine,
        sine,
    ).astype(BF)
    query_groups = query_heads.reshape(row_count, kv_local, group, HD)
    key_heads = rotate(
        jnp.dot(normed_attn, key_full, preferred_element_type=F32).reshape(
            row_count, kv_local, HD
        ),
        cosine,
        sine,
    ).astype(BF)
    value_heads = (
        jnp.dot(normed_attn, value_full, preferred_element_type=F32)
        .astype(BF)
        .reshape(row_count, kv_local, HD)
    )
    mixed_heads, log_totals = attend_forward(
        query_groups, key_heads, value_heads, allowed, score_scale
    )
    mixed_flat = mixed_heads.reshape(row_count, heads_local * HD)
    hidden_res = residual_in + narrow_scatter(
        jnp.dot(mixed_flat, output_full, preferred_element_type=F32),
        "tensor",
        scatter_dimension=0,
        tiled=True,
    )
    unit_ffn, inverse_ffn, normed_ffn_local = normalize(hidden_res, gain_ffn)
    normed_ffn = lax.all_gather(normed_ffn_local, "tensor", axis=0, tiled=True)
    gate_rows = jnp.dot(normed_ffn, gate_full, preferred_element_type=F32)
    up_rows = jnp.dot(normed_ffn, up_full, preferred_element_type=F32)
    sigmoid_gate = jax.nn.sigmoid(gate_rows)
    active = (gate_rows * sigmoid_gate * up_rows).astype(BF)
    layer_output = (
        hidden_res
        + narrow_scatter(
            jnp.dot(active, down_full, preferred_element_type=F32).astype(BF),
            "tensor",
            scatter_dimension=0,
            tiled=True,
        ).astype(F32)
    ).astype(BF)
    query_full, key_full, value_full, output_full, gate_full, up_full, down_full = (
        lax.all_gather(w_query, "dp", axis=0, tiled=True),
        lax.all_gather(w_key, "dp", axis=0, tiled=True),
        lax.all_gather(w_value, "dp", axis=0, tiled=True),
        lax.all_gather(w_output, "dp", axis=1, tiled=True),
        lax.all_gather(w_gate, "dp", axis=0, tiled=True),
        lax.all_gather(w_up, "dp", axis=0, tiled=True),
        lax.all_gather(w_down, "dp", axis=1, tiled=True),
    )
    cotangent_full = lax.all_gather(cotangent, "tensor", axis=0, tiled=True)
    grad_active = contract(cotangent_full, down_full, 1, 1)
    grad_w_down = contract(active, cotangent_full, 0, 0)
    grad_up_rows = (grad_active * gate_rows * sigmoid_gate).astype(BF)
    grad_gate_rows = (
        grad_active * up_rows * sigmoid_gate * (1.0 + gate_rows * (1.0 - sigmoid_gate))
    ).astype(BF)
    grad_w_gate = contract(normed_ffn, grad_gate_rows, 0, 0)
    grad_w_up = contract(normed_ffn, grad_up_rows, 0, 0)
    grad_normed_ffn = narrow_scatter(
        contract(grad_gate_rows, gate_full, 1, 1) + contract(grad_up_rows, up_full, 1, 1),
        "tensor",
        scatter_dimension=0,
        tiled=True,
    )
    grad_hidden, gain_ffn_part = normalize_back(grad_normed_ffn, unit_ffn, inverse_ffn, gain_ffn)
    grad_hidden = cotangent.astype(F32) + grad_hidden
    branch_full = lax.all_gather(grad_hidden.astype(BF), "tensor", axis=0, tiled=True)
    grad_mixed = contract(branch_full, output_full, 1, 1).astype(BF)
    grad_w_output = contract(mixed_flat, branch_full, 0, 0)
    grad_query_rot, grad_key_rot, grad_value_heads = attend_backward(
        query_groups,
        key_heads,
        value_heads,
        mixed_heads,
        grad_mixed.reshape(row_count, kv_local, group, HD),
        log_totals,
        allowed,
        score_scale,
    )
    grad_queries = (
        unrotate(grad_query_rot.reshape(row_count, heads_local, HD), cosine, sine)
        .reshape(row_count, heads_local * HD)
        .astype(BF)
    )
    grad_keys = (
        unrotate(grad_key_rot, cosine, sine).reshape(row_count, kv_local * HD).astype(BF)
    )
    grad_values = grad_value_heads.reshape(row_count, kv_local * HD).astype(BF)
    grad_w_query = contract(normed_attn, grad_queries, 0, 0)
    grad_w_key = contract(normed_attn, grad_keys, 0, 0)
    grad_w_value = contract(normed_attn, grad_values, 0, 0)
    grad_normed_attn = narrow_scatter(
        contract(grad_queries, query_full, 1, 1)
        + contract(grad_keys, key_full, 1, 1)
        + contract(grad_values, value_full, 1, 1),
        "tensor",
        scatter_dimension=0,
        tiled=True,
    )
    grad_residual, gain_attn_part = normalize_back(
        grad_normed_attn, unit_attn, inverse_attn, gain_attn
    )
    grad_input = grad_hidden + grad_residual
    gain_attn_total, gain_ffn_total = lax.psum((gain_attn_part, gain_ffn_part), "tensor")
    owned = (
        narrow_scatter(grad_w_query, "dp", scatter_dimension=0, tiled=True),
        narrow_scatter(grad_w_key, "dp", scatter_dimension=0, tiled=True),
        narrow_scatter(grad_w_value, "dp", scatter_dimension=0, tiled=True),
        narrow_scatter(grad_w_output, "dp", scatter_dimension=1, tiled=True),
        narrow_scatter(gain_attn_total, "dp", scatter_dimension=0, tiled=True),
        narrow_scatter(gain_ffn_total, "dp", scatter_dimension=0, tiled=True),
        narrow_scatter(grad_w_gate, "dp", scatter_dimension=0, tiled=True),
        narrow_scatter(grad_w_up, "dp", scatter_dimension=0, tiled=True),
        narrow_scatter(grad_w_down, "dp", scatter_dimension=1, tiled=True),
    )
    return (
        layer_output,
        grad_input,
        owned[4],
        owned[0],
        owned[1],
        owned[2],
        owned[3],
        owned[5],
        owned[6],
        owned[7],
        owned[8],
    )


def with_kernels(nt, nd, layer_input, segment_ids, norm_attn, w_query, w_key, w_value, w_output, norm_ffn, w_gate, w_up, w_down, cotangent):
    y, gi, gains, d_wq, d_kv, d_wo, d_down, d_gate, d_up, *_ = layer(
        nt, nd, layer_input, cotangent, norm_attn, norm_ffn, segment_ids[None, :],
        w_query, w_key.T, w_value.T, w_output, w_gate, w_up, w_down,
    )
    y, gi, d_wq, d_wo, d_gate, d_up, d_down, d_k, d_v, d_attn, d_ffn = hand_over(
        (y, gi, d_wq, d_wo, d_gate, d_up, d_down), d_kv, gains
    )
    return (y, gi, d_attn, d_wq, d_k.T, d_v.T, d_wo, d_ffn, d_gate, d_up, d_down)


def fits(nt, nd, shards):
    layer_input, segment_ids, norm_attn, w_query, w_key, w_value, w_output, norm_ffn, w_gate, w_up, w_down, _ = shards
    return (
        nd >= 4
        and nd & (nd - 1) == 0
        and nt >= 2
        and norm_attn.shape[0] % LANES == 0
        and w_output.shape[1] % LANES == 0
        and w_gate.shape[1] % LANES == 0
        and w_query.shape[1] % LANES == 0
        and w_key.shape[1] == HD
        and segment_ids.shape[0] == nt * layer_input.shape[0]
        and segment_ids.shape[0] % (8 * LANES // 2) == 0
        and w_gate.shape[1] >= w_query.shape[1] + segment_ids.shape[0]
        and layer_input.shape[1] >= 2 * segment_ids.shape[0]
    )


def on_device(nt, nd, *shards):
    if fits(nt, nd, shards):
        return with_kernels(nt, nd, *shards)
    return plain_device(*shards)


def solution(mesh):
    placed = (
        P(("dp", "tensor"), None),
        P("dp"),
        P("dp"),
        P("dp", "tensor"),
        P("dp", "tensor"),
        P("dp", "tensor"),
        P("tensor", "dp"),
        P("dp"),
        P("dp", "tensor"),
        P("dp", "tensor"),
        P("tensor", "dp"),
        P(("dp", "tensor"), None),
    )
    return jax.shard_map(
        functools.partial(on_device, mesh.shape["tensor"], mesh.shape["dp"]),
        mesh=mesh,
        in_specs=placed,
        out_specs=(
            P(("dp", "tensor"), None),
            P(("dp", "tensor"), None),
            P("dp"),
            P("dp", "tensor"),
            P("dp", "tensor"),
            P("dp", "tensor"),
            P("tensor", "dp"),
            P("dp"),
            P("dp", "tensor"),
            P("dp", "tensor"),
            P("tensor", "dp"),
        ),
        check_vma=False,
    )
```
